32 devices in a mesh: group: 2 (over x), expert: 4 (over z), shard: 4 (over y, core).
Axes of the slice: x: 2, y: 2, z: 4, core: 2. Of those that a mesh axis runs over, the one named last changes fastest.
Arguments:
- hidden_in: bfloat16 [6144, 768], P(('group', 'expert', 'shard')), may hold values from -6 to 6
- segment_ids: int32 [2, 3072], P('group'), may hold values from 0 to 8, never falling along the last dimension, each value on 1 to 1536 neighbouring positions
- routes: int32 [6144, 2], P(('group', 'expert', 'shard')), may hold values from 0 to 7, all different within a row; in each aligned block of 192 rows (0 to 191, 192 to 383, ...) at most 48 rows name the same one
- attn_gain: float32 [768], replicated, may hold values from 0.5 to 1.5
- w_query: bfloat16 [768, 768], P('shard'), may hold values from -0.21875 to 0.21875
- w_key: bfloat16 [768, 768], P('shard'), may hold values from -0.21875 to 0.21875
- w_value: bfloat16 [768, 768], P('shard'), may hold values from -0.21875 to 0.21875
- w_out: bfloat16 [768, 768], P('shard'), may hold values from -2.5 to 2.5
- moe_gain: float32 [768], replicated, may hold values from 0.5 to 1.5
- w_router: float32 [768, 8], replicated, may hold values from -0.15625 to 0.15625
- const_mix: float32 [768, 4], replicated, may hold values from -0.21875 to 0.21875
- const_vec: float32 [2, 768], replicated, may hold values from -6 to 6
- w_gate: bfloat16 [4, 768, 2048], P('expert'), may hold values from -0.21875 to 0.21875
- w_up: bfloat16 [4, 768, 2048], P('expert'), may hold values from -0.21875 to 0.21875
- w_down: bfloat16 [4, 2048, 768], P('expert'), may hold values from -0.1875 to 0.1875
- out_grad: bfloat16 [6144, 768], P(('group', 'expert', 'shard')), may hold values from -6 to 6
Outputs:
- layer_out: bfloat16 [6144, 768], P(('group', 'expert', 'shard'))
- input_grad: float32 [6144, 768], P(('group', 'expert', 'shard'))
- attn_gain_grad: float32 [768], replicated
- query_grad: float32 [768, 768], P(('expert', 'shard'))
- key_grad: float32 [768, 768], P(('expert', 'shard'))
- value_grad: float32 [768, 768], P(('expert', 'shard'))
- out_proj_grad: float32 [768, 768], P(('expert', 'shard'))
- moe_gain_grad: float32 [768], replicated
- router_grad: float32 [768, 8], replicated
- mix_grad: float32 [768, 4], replicated
- vec_grad: float32 [2, 768], replicated
- gate_grad: float32 [4, 768, 2048], P('expert', 'shard')
- up_grad: float32 [4, 768, 2048], P('expert', 'shard')
- down_grad: float32 [4, 2048, 768], P('expert', 'shard')
The draws below stay inside these ranges and needn't reach their ends.
Inputs may be any that keep to these rules, and one draw needn't show every extreme that they name: Each row names two different ids; ids below 4 are feed-forward experts, 4 is the zero expert, 5 the copy expert, 6 and 7 the constant experts. Among the routes of the 192 tokens of one device no id is named more than 48 times, a bound that some block reaches. `segment_ids`: each row numbers the documents of one group in order, never falling, starting at 0; document 0 is the prompt that every later document of the row attends; each of the 9 documents has at least one position and one has exactly 1536.
All inputs are finite; a program needn't handle non-finite values.
Results may differ from the reference program's by a relative error of at most 0.02.
Values may be sent and summed in bfloat16 or wider, within the bound.
A program may use at most 192 MiB of HBM per device.

```python
import math
import jax
import jax.numpy as jnp
import numpy as np
from jax import lax

D = 768
HEADS = 12
HEAD_DIM = 64
FF = 2048
TOK_DEV = 192
SEGS = 9
EXPERTS = 4
NIDS = 8
CAP = 48
GROUP_TOK = 3072
GROUPS = 2
TOKENS = 6144
PROMPT_MOST = 1536


def steps_of(stream_key, shape, split, least, high):
    level = 1.0
    for dim, parts in split:
        draws = jax.random.uniform(jax.random.fold_in(jax.random.fold_in(stream_key, 6), dim), (parts,), jnp.float32, least / len(split), high / len(split))
        level = level * jnp.repeat(jnp.exp(draws), shape[dim] // parts).reshape((-1,) + (1,) * (len(shape) - 1 - dim))
    return level


def length_profile(count, total, limit, skew):
    loads = [(1 << 20) // math.isqrt(standing ** skew) + 1 for standing in range(2, count + 1)]
    rest, given = total - limit - (count - 1), [1] * (count - 1)
    while rest > 0:
        free = [i for i in range(count - 1) if given[i] < limit]
        mass, left = sum([loads[i] for i in free]), rest
        for i in free:
            extra = min(limit - given[i], max(1, left * loads[i] // mass), rest)
            given[i] = given[i] + extra
            rest = rest - extra
    return np.array([limit] + given)


def ragged(rng, count, total, bound, slope):
    if count == 2:
        one = jax.random.randint(rng, (), max(1, total - bound), min(bound, total - 1) + 1)
        return jnp.stack([one, total - one])
    lengths = jnp.asarray(length_profile(count, total, bound, slope), jnp.int32)
    twos = (count - 1) // 2
    source_of, receiver = lengths[1:1 + 2 * twos:2], lengths[2:2 + 2 * twos:2]
    room = jnp.minimum(source_of - 1, bound - receiver)
    passed = jax.random.randint(jax.random.fold_in(rng, 1), (twos,), 0, 1 << 20) % (room + 1)
    lengths = lengths.at[1:1 + 2 * twos:2].set(source_of - passed).at[2:2 + 2 * twos:2].set(receiver + passed)
    return lengths[jax.random.permutation(jax.random.fold_in(rng, 2), count)]


def routed_block(rng, own, number, rows, count, top, bound, slope):
    sequence = jax.random.permutation(rng, count)
    crowded, usual = shares(count, rows * top, bound, slope, True), shares(count, rows * top, bound, slope, False)
    places = jnp.arange(count)

    def named(tallies, rotation):
        used = int((tallies > 0).sum())
        fixed = max(1, used // 4)
        passed = fixed + (places - fixed + rotation * (used - fixed)) % max(1, count - fixed)
        return jnp.zeros((count,), jnp.int32).at[sequence[jnp.where(places < fixed, places, passed)]].set(jnp.asarray(tallies, jnp.int32))

    tallies = jnp.where(number % 4 == 0, named(crowded, number // 4), named(usual, number - number // 4 - 1))
    mixed = jax.random.permutation(jax.random.fold_in(own, 3), count)
    source_of, taker = mixed[0:count // 2 * 2:2], mixed[1:count // 2 * 2:2]
    margin = jnp.minimum(tallies[source_of] - 1, bound - tallies[taker]) // 2
    margin = jnp.where((source_of == sequence[0]) | (taker == sequence[0]) | (tallies[taker] == 0), 0, jnp.maximum(margin, 0))
    passed = jax.random.randint(jax.random.fold_in(own, 4), (count // 2,), 0, 1 << 20) % (margin + 1)
    tallies = tallies.at[source_of].add(-passed).at[taker].add(passed)
    items = jnp.searchsorted(jnp.cumsum(tallies), jnp.arange(rows * top), side="right").astype(jnp.int32)
    grid = items.reshape(top, rows).T
    grid = grid[jax.random.permutation(jax.random.fold_in(own, 1), rows)]
    rotation = jax.random.randint(jax.random.fold_in(own, 2), (rows, 1), 0, top)
    return jnp.take_along_axis(grid, (jnp.arange(top)[None, :] + rotation) % top, axis=1)


def shares(amount, total, bound, skew, full):
    portions = [(1 << 20) // math.isqrt(grade ** skew) + 1 for grade in range(1, amount + 1)]
    largest = bound if full else min(bound, max(-(-total // amount), total * portions[0] // sum(portions)))
    least = 1 if total - largest >= amount - 1 else 0
    given, surplus = [largest] + [least] * (amount - 1), total - largest - least * (amount - 1)
    while surplus > 0:
        movable = [i for i in range(1, amount) if given[i] < largest] or [i for i in range(1, amount) if given[i] < bound]
        mass, budget = sum([portions[i] for i in movable]), surplus
        for i in movable:
            extra = min(bound - given[i], max(1, budget * portions[i] // mass), surplus)
            given[i] = given[i] + extra
            surplus = surplus - extra
    return np.array(given)


def bell_draw(rng, shape, width, limit, cuts=(), kind=jnp.bfloat16):
    drawn = width * jax.random.normal(rng, shape, jnp.float32)
    if cuts:
        drawn = drawn * steps_of(rng, shape, cuts, -0.22, 0.18)
    return jnp.clip(drawn, -limit, limit).astype(kind)


def setup_inputs(seed: int = 0) -> dict:
    key_of = jax.random.split(jax.random.key(seed), 17)
    hidden_in = bell_draw(key_of[0], (TOKENS, D), 1.0, 6.0, ((0, 32),))
    segment_ids = jax.vmap(lambda own: jnp.searchsorted(jnp.cumsum(ragged(own, SEGS, GROUP_TOK, PROMPT_MOST, 2)), jnp.arange(GROUP_TOK), side="right"))(jax.random.split(key_of[1], GROUPS)).reshape((GROUPS, GROUP_TOK)).astype(jnp.int32)
    routes_keys = jax.random.split(jax.random.fold_in(key_of[2], 1), TOKENS // TOK_DEV)
    routes_turns = jax.random.permutation(jax.random.fold_in(key_of[2], 3), TOKENS // TOK_DEV)
    routes = jax.vmap(lambda own, number: routed_block(jax.random.fold_in(key_of[2], 2), own, number, TOK_DEV, NIDS, 2, CAP, 1))(routes_keys, routes_turns).reshape((TOKENS, 2))
    attn_gain = jnp.clip(1.0 + 0.1 * jax.random.normal(key_of[3], (D,), jnp.float32), 0.5, 1.5)
    w_query = bell_draw(key_of[4], (D, D), D ** -0.5, 0.21875, ((0, 4),))
    w_key = bell_draw(key_of[5], (D, D), D ** -0.5, 0.21875, ((0, 4),))
    w_value = bell_draw(key_of[6], (D, D), D ** -0.5, 0.21875, ((0, 4),))
    w_out = bell_draw(key_of[7], (D, D), (max(D // 128, 1)) ** -0.5, 2.5, ((0, 4),))
    moe_gain = jnp.clip(1.0 + 0.1 * jax.random.normal(key_of[8], (D,), jnp.float32), 0.5, 1.5)
    w_router = bell_draw(key_of[9], (D, NIDS), (2 * D) ** -0.5, 0.15625, (), jnp.float32)
    const_mix = bell_draw(key_of[10], (D, 4), D ** -0.5, 0.21875, (), jnp.float32)
    const_vec = bell_draw(key_of[11], (2, D), 1.0, 6.0, (), jnp.float32)
    w_gate = bell_draw(key_of[12], (EXPERTS, D, FF), D ** -0.5, 0.21875, ((0, 4),))
    w_up = bell_draw(key_of[13], (EXPERTS, D, FF), D ** -0.5, 0.21875, ((0, 4),))
    w_down = bell_draw(key_of[14], (EXPERTS, FF, D), (FF // 2) ** -0.5, 0.1875, ((0, 4),))
    out_grad = bell_draw(key_of[15], (TOKENS, D), 1.0, 6.0, ((0, 32),))
    return dict(hidden_in=hidden_in, segment_ids=segment_ids, routes=routes, attn_gain=attn_gain, w_query=w_query, w_key=w_key, w_value=w_value, w_out=w_out, moe_gain=moe_gain, w_router=w_router, const_mix=const_mix, const_vec=const_vec, w_gate=w_gate, w_up=w_up, w_down=w_down, out_grad=out_grad)


neg_fill = -1e+30
norm_eps = 1e-05

@jax.custom_vjp
def low(v):
    return lax.optimization_barrier(v.astype(jnp.bfloat16)).astype(jnp.float32)

@jax.custom_vjp
def low_back(v):
    return v

def low_keep(v):
    return (low(v), None)

def low_pass(kept, grad):
    return (grad,)

def back_keep(v):
    return (v, None)

def back_low(kept, grad):
    return (low(grad),)
low.defvjp(low_keep, low_pass)
low_back.defvjp(back_keep, back_low)

def dense32(left_side, right_side):
    return jnp.dot(left_side, right_side, precision=lax.Precision.HIGHEST)

def rms_norm(values, gain_vec):
    return values * lax.rsqrt(lax.optimization_barrier(jnp.mean(values * values, axis=1, keepdims=True)) + norm_eps) * gain_vec

def attend_block(query_blk, query_pos, query_seg, keys_grp, values_grp, seg_grp):
    key_pos = jnp.arange(GROUP_TOK, dtype=jnp.int32)
    scores = jnp.einsum('qhd,khd->hqk', query_blk, keys_grp, precision=lax.Precision.HIGHEST) * HEAD_DIM ** (-0.5)
    scores = low_back(scores)
    same_doc = (seg_grp[None, :] == query_seg[:, None]) | (seg_grp[None, :] == 0)
    allowed = same_doc & (key_pos[None, :] <= query_pos[:, None])
    scores = jnp.where(allowed[None], scores, neg_fill)
    prob_rows = low(jax.nn.softmax(scores, axis=-1))
    return jnp.einsum('hqk,khd->qhd', prob_rows, values_grp, precision=lax.Precision.HIGHEST)

def attend_group(operands):
    query_grp, keys_grp, values_grp, seg_grp = operands
    block_len = min(512, GROUP_TOK)
    blocks = GROUP_TOK // block_len
    positions = jnp.arange(GROUP_TOK, dtype=jnp.int32)

    def one_block(pieces):
        return attend_block(pieces[0], pieces[1], pieces[2], keys_grp, values_grp, seg_grp)
    result = lax.map(jax.checkpoint(one_block), (query_grp.reshape(blocks, block_len, HEADS, HEAD_DIM), positions.reshape(blocks, block_len), seg_grp.reshape(blocks, block_len)))
    return result.reshape(GROUP_TOK, HEADS, HEAD_DIM)

def expert_rows(operands):
    rows_in, gate_w, up_w, down_w = operands
    gate_pre = low_back(dense32(rows_in, gate_w))
    up_pre = low_back(dense32(rows_in, up_w))
    hidden_act = low(jax.nn.silu(gate_pre) * up_pre)
    return low_back(low(dense32(hidden_act, down_w)))

def forward(inputs, attn_gain, w_query, w_key, w_value, w_out, moe_gain, w_router, const_mix, const_vec, w_gate, w_up, w_down, segment_ids, routes):
    attn_in = low(rms_norm(inputs, attn_gain))
    queries = low_back(low(dense32(attn_in, w_query)))
    keys_all = low_back(low(dense32(attn_in, w_key)))
    values_all = low_back(low(dense32(attn_in, w_value)))
    grouped = (GROUPS, GROUP_TOK, HEADS, HEAD_DIM)
    attended = lax.map(attend_group, (queries.reshape(grouped), keys_all.reshape(grouped), values_all.reshape(grouped), segment_ids))
    attn_vec = low_back(low(attended.reshape(TOKENS, D)))
    resid_one = inputs + low_back(dense32(attn_vec, w_out))
    moe_in = rms_norm(resid_one, moe_gain)
    moe_low = low(moe_in)
    logits = dense32(moe_in, w_router)
    gate_probs = jax.nn.softmax(jnp.take_along_axis(logits, routes, axis=1), axis=1)
    mix_alpha = jax.nn.softmax(dense32(moe_in, const_mix).reshape(TOKENS, 2, 2), axis=2)
    const_rows = mix_alpha[:, :, 0:1] * moe_in[:, None, :] + mix_alpha[:, :, 1:2] * const_vec[None]
    devices = TOKENS // TOK_DEV
    by_device = routes.reshape(devices, 2 * TOK_DEV)
    id_hot = (by_device[:, :, None] == jnp.arange(NIDS, dtype=jnp.int32)).astype(jnp.int32)
    earlier = jnp.cumsum(id_hot, axis=1, dtype=jnp.int32) - id_hot
    slot_num = lax.optimization_barrier(jnp.sum(earlier * id_hot, axis=2, dtype=jnp.int32))
    device_num = jnp.arange(devices, dtype=jnp.int32)[:, None]
    slot_total = EXPERTS * devices * CAP
    slot_of_route = jnp.where(by_device < EXPERTS, (by_device * devices + device_num) * CAP + slot_num, slot_total).reshape(-1).astype(jnp.int32)
    route_of_slot = jnp.zeros(slot_total + 1, jnp.int32).at[slot_of_route].set(jnp.arange(2 * TOKENS, dtype=jnp.int32))[:slot_total]
    slot_used = jnp.zeros(slot_total + 1, jnp.float32).at[slot_of_route].set(1.0)[:slot_total]
    rows_in = low_back(moe_low[route_of_slot // 2] * slot_used[:, None])
    expert_out = lax.map(jax.checkpoint(expert_rows), (rows_in.reshape(EXPERTS, devices * CAP, D), w_gate, w_up, w_down))
    padded = jnp.concatenate([expert_out.reshape(slot_total, D), jnp.zeros((1, D), jnp.float32)], axis=0)
    route_out = padded[slot_of_route].reshape(TOKENS, 2, D)
    ffn_mask = (routes < EXPERTS).astype(jnp.float32)
    copy_mask = (routes == EXPERTS + 1).astype(jnp.float32)
    const_mask = (routes[:, :, None] == EXPERTS + 2 + jnp.arange(2, dtype=jnp.int32)).astype(jnp.float32)
    copy_gate = lax.optimization_barrier(jnp.sum(gate_probs * copy_mask, axis=1))
    const_gate = lax.optimization_barrier(jnp.sum(gate_probs[:, :, None] * const_mask, axis=1))
    moe_sum = lax.optimization_barrier(jnp.sum((gate_probs * ffn_mask)[:, :, None] * route_out, axis=1)) + copy_gate[:, None] * moe_in + lax.optimization_barrier(jnp.sum(const_gate[:, :, None] * const_rows, axis=1))
    return resid_one + moe_sum

def reference(hidden_in, segment_ids, routes, attn_gain, w_query, w_key, w_value, w_out, moe_gain, w_router, const_mix, const_vec, w_gate, w_up, w_down, out_grad):
    params = (hidden_in.astype(jnp.float32), attn_gain, w_query.astype(jnp.float32), w_key.astype(jnp.float32), w_value.astype(jnp.float32), w_out.astype(jnp.float32), moe_gain, w_router, const_mix, const_vec, w_gate.astype(jnp.float32), w_up.astype(jnp.float32), w_down.astype(jnp.float32))

    def layer_fn(*weights):
        return forward(*weights, segment_ids, routes)
    result, pullback = jax.vjp(layer_fn, *params)
    gradients = pullback(out_grad.astype(jnp.float32))
    return (result.astype(jnp.bfloat16), gradients[0], gradients[1], gradients[2], gradients[3], gradients[4], gradients[5], gradients[6], gradients[7], gradients[8], gradients[9], gradients[10], gradients[11], gradients[12])
```

```python
import functools

import jax
import jax.numpy as jnp
from jax import lax
from jax.experimental import pallas as pl
from jax.experimental.pallas import tpu as pltpu
from jax.sharding import PartitionSpec as P

HEADS = 12
HEAD_DIM = 64
CAP = 48
KEY_BLK = 256
EX, SH, GR = ("expert", "shard", "group")
GATHER, GATHER_SUM, SWAP, SWAP_SUM = range(4)


neg_fill = -1e30
norm_eps = 1e-05
bf16 = jnp.bfloat16
f32 = jnp.float32
VM = pl.BlockSpec(memory_space=pltpu.VMEM)
SM = pl.BlockSpec(memory_space=pltpu.SMEM)
HIGH = lax.Precision.HIGHEST


def contract(a, b, da, db, precision=None):
    return lax.dot_general(
        a, b, (((da,), (db,)), ((), ())), preferred_element_type=f32, precision=precision
    )


def dense32(left_side, right_side):
    return jnp.dot(left_side, right_side, precision=lax.Precision.HIGHEST)


def allowed_mask(query_pos, query_seg, key_pos, key_seg):
    same_doc = (key_seg[None, :] == query_seg[:, None]) | (key_seg[None, :] == 0)
    return same_doc & (key_pos[None, :] <= query_pos[:, None])


def rms_back(inputs, inverse, gain_vec, upstream):
    scaled = upstream * gain_vec
    return inverse * scaled - inputs * inverse**3 * jnp.mean(scaled * inputs, axis=1, keepdims=True)


def block_scores(query_blk, keys_blk, score_scale):
    return (
        jnp.einsum("qhd,khd->hqk", query_blk, keys_blk, preferred_element_type=jnp.float32)
        * score_scale
    )


def grad_pieces(
    query_blk, back_blk, keys_blk, values_blk, norm_blk, delta_blk, key_mask, score_scale
):
    scores = block_scores(query_blk, keys_blk, score_scale)
    prob_rows = jnp.where(key_mask[None], jnp.exp(scores - norm_blk[:, :, None]), 0.0)
    prob_grad = jnp.einsum("qhd,khd->hqk", back_blk, values_blk, preferred_element_type=jnp.float32)
    score_low = (prob_rows * (prob_grad - delta_blk[:, :, None])).astype(jnp.bfloat16)
    return (prob_rows.astype(jnp.bfloat16), score_low)


def shards(
    hidden_in,
    segment_ids,
    routes,
    attn_gain,
    w_query,
    w_key,
    w_value,
    w_out,
    moe_gain,
    w_router,
    const_mix,
    const_vec,
    w_gate,
    w_up,
    w_down,
    out_grad,
):
    tok_rows, model_width = hidden_in.shape
    score_scale = HEAD_DIM ** (-0.5)
    inner_rank = lax.axis_index((EX, SH))
    seg_group = segment_ids[0]
    group_len = seg_group.shape[0]
    key_block = min(512, group_len)
    num_blocks = group_len // key_block
    row_start = inner_rank * tok_rows
    own_pos = row_start + jnp.arange(tok_rows, dtype=jnp.int32)
    own_seg = lax.dynamic_slice_in_dim(seg_group, row_start, tok_rows)
    wq_full, wk_full, wv_full, wo_full = (
        lax.all_gather(w_query, SH, axis=0, tiled=True),
        lax.all_gather(w_key, SH, axis=0, tiled=True),
        lax.all_gather(w_value, SH, axis=0, tiled=True),
        lax.all_gather(w_out, SH, axis=0, tiled=True),
    )
    inputs = hidden_in.astype(jnp.float32)
    inv_one = lax.rsqrt(jnp.mean(inputs * inputs, axis=1, keepdims=True) + norm_eps)
    normed_one = inputs * inv_one
    attn_in = (normed_one * attn_gain).astype(jnp.bfloat16)
    queries = jnp.dot(attn_in, wq_full, preferred_element_type=jnp.float32).astype(jnp.bfloat16)
    keys_own = jnp.dot(attn_in, wk_full, preferred_element_type=jnp.float32).astype(jnp.bfloat16)
    values_own = jnp.dot(attn_in, wv_full, preferred_element_type=jnp.float32).astype(jnp.bfloat16)
    keys_all, values_all = (
        lax.all_gather(keys_own, (EX, SH), axis=0, tiled=True),
        lax.all_gather(values_own, (EX, SH), axis=0, tiled=True),
    )
    query_heads = queries.reshape(tok_rows, HEADS, HEAD_DIM)

    def fetch_block(source, block_index):
        return lax.dynamic_slice_in_dim(source, block_index * key_block, key_block).reshape(
            key_block, HEADS, HEAD_DIM
        )

    def block_mask(block_index):
        key_pos = block_index * key_block + jnp.arange(key_block, dtype=jnp.int32)
        key_seg = lax.dynamic_slice_in_dim(seg_group, block_index * key_block, key_block)
        return allowed_mask(own_pos, own_seg, key_pos, key_seg)

    def stats_step(carry_now, block_index):
        key_mask = block_mask(block_index)

        def stats_live_block(carry_in):
            row_max, row_sum = carry_in
            scores = jnp.where(
                key_mask[None],
                block_scores(query_heads, fetch_block(keys_all, block_index), score_scale),
                neg_fill,
            )
            new_max = jnp.maximum(row_max, jnp.max(scores, axis=2))
            weights = jnp.where(key_mask[None], jnp.exp(scores - new_max[:, :, None]), 0.0)
            return (new_max, row_sum * jnp.exp(row_max - new_max) + jnp.sum(weights, axis=2))

        return (
            lax.cond(jnp.any(key_mask), stats_live_block, lambda carry_in: carry_in, carry_now),
            None,
        )

    start_max = jnp.full((HEADS, tok_rows), neg_fill, jnp.float32)
    row_max, row_sum = lax.scan(
        stats_step, (start_max, jnp.zeros_like(start_max)), jnp.arange(num_blocks)
    )[0]
    log_norm = row_max + jnp.log(row_sum)

    def output_step(running, block_index):
        key_mask = block_mask(block_index)

        def output_live_block(carry_in):
            scores = block_scores(query_heads, fetch_block(keys_all, block_index), score_scale)
            prob_rows = jnp.where(
                key_mask[None], jnp.exp(scores - log_norm[:, :, None]), 0.0
            ).astype(jnp.bfloat16)
            return carry_in + jnp.einsum(
                "hqk,khd->qhd",
                prob_rows,
                fetch_block(values_all, block_index),
                preferred_element_type=jnp.float32,
            )

        return (
            lax.cond(jnp.any(key_mask), output_live_block, lambda carry_in: carry_in, running),
            None,
        )

    zero_heads = jnp.zeros((tok_rows, HEADS, HEAD_DIM), jnp.float32)
    attn_sum = lax.scan(output_step, zero_heads, jnp.arange(num_blocks))[0]
    attn_low = attn_sum.reshape(tok_rows, model_width).astype(jnp.bfloat16)
    resid_one = inputs + jnp.dot(attn_low, wo_full, preferred_element_type=jnp.float32)
    inv_two = lax.rsqrt(jnp.mean(resid_one * resid_one, axis=1, keepdims=True) + norm_eps)
    normed_two = resid_one * inv_two
    moe_in = normed_two * moe_gain
    moe_low = moe_in.astype(jnp.bfloat16)
    n_ids = w_router.shape[1]
    local_experts = w_gate.shape[0]
    owners = lax.axis_size(EX)
    ffn_count = local_experts * owners
    id_table = jnp.arange(n_ids, dtype=jnp.int32)
    route_hot = (routes[:, :, None] == id_table).astype(jnp.float32)
    logits = dense32(moe_in, w_router)
    chosen = jnp.einsum("rkn,rn->rk", route_hot, logits, precision=lax.Precision.HIGHEST)
    gate_probs = jax.nn.softmax(chosen, axis=1)
    mix_alpha = jax.nn.softmax(dense32(moe_in, const_mix).reshape(tok_rows, 2, 2), axis=2)
    const_rows = mix_alpha[:, :, 0:1] * moe_in[:, None, :] + mix_alpha[:, :, 1:2] * const_vec[None]
    ffn_mask = (routes < ffn_count).astype(jnp.float32)
    copy_mask = (routes == ffn_count + 1).astype(jnp.float32)
    const_mask = (routes[:, :, None] == ffn_count + 2 + jnp.arange(2, dtype=jnp.int32)).astype(
        jnp.float32
    )
    copy_gate = jnp.sum(gate_probs * copy_mask, axis=1)
    const_gate = jnp.sum(gate_probs[:, :, None] * const_mask, axis=1)
    ffn_gate = gate_probs * ffn_mask
    flat_ids = routes.reshape(-1)
    id_hot = (flat_ids[:, None] == id_table).astype(jnp.int32)
    earlier = jnp.cumsum(id_hot, axis=0, dtype=jnp.int32) - id_hot
    slot_num = jnp.sum(earlier * id_hot, axis=1, dtype=jnp.int32)
    slot_total = ffn_count * CAP
    slot_of_route = jnp.where(flat_ids < ffn_count, flat_ids * CAP + slot_num, slot_total)
    route_count = flat_ids.shape[0]
    route_of_slot = (
        jnp.zeros(slot_total + 1, jnp.int32)
        .at[slot_of_route]
        .set(jnp.arange(route_count, dtype=jnp.int32))[:slot_total]
    )
    slot_used = jnp.zeros(slot_total + 1, jnp.bool_).at[slot_of_route].set(True)[:slot_total]
    send_rows = jnp.where(
        slot_used[:, None], moe_low[route_of_slot // 2], jnp.zeros((), jnp.bfloat16)
    )
    recv_rows = lax.all_to_all(
        send_rows.reshape(owners, local_experts * CAP, model_width),
        EX,
        split_axis=0,
        concat_axis=0,
        tiled=True,
    )
    expert_in = recv_rows.reshape(owners, local_experts, CAP, model_width)
    gate_pre = jnp.einsum("sjcd,jdf->sjcf", expert_in, w_gate, preferred_element_type=jnp.float32)
    up_pre = jnp.einsum("sjcd,jdf->sjcf", expert_in, w_up, preferred_element_type=jnp.float32)
    gate_sigmoid = jax.nn.sigmoid(gate_pre)
    hidden_act = (gate_pre * gate_sigmoid * up_pre).astype(jnp.bfloat16)
    expert_out = jnp.einsum(
        "sjcf,jfd->sjcd", hidden_act, w_down, preferred_element_type=jnp.float32
    ).astype(jnp.bfloat16)
    returned = lax.all_to_all(
        expert_out.reshape(owners, local_experts * CAP, model_width),
        EX,
        split_axis=0,
        concat_axis=0,
        tiled=True,
    )
    padded_out = jnp.concatenate(
        [returned.reshape(slot_total, model_width), jnp.zeros((1, model_width), jnp.bfloat16)],
        axis=0,
    )
    route_out = padded_out[slot_of_route].astype(jnp.float32).reshape(tok_rows, 2, model_width)
    moe_sum = (
        jnp.sum(ffn_gate[:, :, None] * route_out, axis=1)
        + copy_gate[:, None] * moe_in
        + jnp.sum(const_gate[:, :, None] * const_rows, axis=1)
    )
    layer_out = (resid_one + moe_sum).astype(jnp.bfloat16)
    upstream = out_grad.astype(jnp.float32)
    route_dot = jnp.sum(upstream[:, None, :] * route_out, axis=2)
    copy_dot = jnp.sum(upstream * moe_in, axis=1)
    const_dot = jnp.sum(upstream[:, None, :] * const_rows, axis=2)
    gate_back_r = (
        ffn_mask * route_dot
        + copy_mask * copy_dot[:, None]
        + jnp.sum(const_mask * const_dot[:, None, :], axis=2)
    )
    chosen_grad = gate_probs * (
        gate_back_r - jnp.sum(gate_probs * gate_back_r, axis=1, keepdims=True)
    )
    logit_grad = jnp.einsum("rk,rkn->rn", chosen_grad, route_hot, precision=lax.Precision.HIGHEST)
    const_up = const_gate[:, :, None] * upstream[:, None, :]
    alpha_grad = jnp.stack(
        [
            jnp.sum(const_up * moe_in[:, None, :], axis=2),
            jnp.sum(const_up * const_vec[None], axis=2),
        ],
        axis=2,
    )
    mix_back = (
        mix_alpha * (alpha_grad - jnp.sum(mix_alpha * alpha_grad, axis=2, keepdims=True))
    ).reshape(tok_rows, 4)
    vec_grad = jnp.sum(mix_alpha[:, :, 1:2] * const_up, axis=0)
    route_weight = ffn_gate.reshape(-1)
    grad_send = (route_weight[route_of_slot][:, None] * upstream[route_of_slot // 2]).astype(
        jnp.bfloat16
    )
    grad_send = jnp.where(slot_used[:, None], grad_send, jnp.zeros((), jnp.bfloat16))
    grad_recv = lax.all_to_all(
        grad_send.reshape(owners, local_experts * CAP, model_width),
        EX,
        split_axis=0,
        concat_axis=0,
        tiled=True,
    )
    grad_recv = grad_recv.reshape(owners, local_experts, CAP, model_width)
    hidden_grad = jnp.einsum(
        "sjcd,jfd->sjcf", grad_recv, w_down, preferred_element_type=jnp.float32
    )
    down_term = jnp.einsum(
        "sjcf,sjcd->jfd", hidden_act, grad_recv, preferred_element_type=jnp.float32
    )
    gate_back = (
        hidden_grad * up_pre * gate_sigmoid * (1.0 + gate_pre * (1.0 - gate_sigmoid))
    ).astype(jnp.bfloat16)
    up_back = (hidden_grad * gate_pre * gate_sigmoid).astype(jnp.bfloat16)
    gate_term = jnp.einsum(
        "sjcd,sjcf->jdf", expert_in, gate_back, preferred_element_type=jnp.float32
    )
    up_term = jnp.einsum("sjcd,sjcf->jdf", expert_in, up_back, preferred_element_type=jnp.float32)
    input_back = (
        jnp.einsum("sjcf,jdf->sjcd", gate_back, w_gate, preferred_element_type=jnp.float32)
        + jnp.einsum("sjcf,jdf->sjcd", up_back, w_up, preferred_element_type=jnp.float32)
    ).astype(jnp.bfloat16)
    input_ret = lax.all_to_all(
        input_back.reshape(owners, local_experts * CAP, model_width),
        EX,
        split_axis=0,
        concat_axis=0,
        tiled=True,
    )
    padded_in = jnp.concatenate(
        [input_ret.reshape(slot_total, model_width), jnp.zeros((1, model_width), jnp.bfloat16)],
        axis=0,
    )
    ffn_in_grad = jnp.sum(
        padded_in[slot_of_route].astype(jnp.float32).reshape(tok_rows, 2, model_width), axis=1
    )
    moe_in_grad = (
        ffn_in_grad
        + copy_gate[:, None] * upstream
        + jnp.sum(mix_alpha[:, :, 0:1] * const_up, axis=1)
        + dense32(mix_back, const_mix.T)
        + dense32(logit_grad, w_router.T)
    )
    moe_gain_grad = jnp.sum(moe_in_grad * normed_two, axis=0)
    router_grad = dense32(moe_in.T, logit_grad)
    mix_grad = dense32(moe_in.T, mix_back)
    resid_grad = upstream + rms_back(resid_one, inv_two, moe_gain, moe_in_grad)
    branch_low = resid_grad.astype(jnp.bfloat16)
    out_proj_term = jnp.dot(attn_low.T, branch_low, preferred_element_type=jnp.float32)
    attn_back = jnp.dot(branch_low, wo_full.T, preferred_element_type=jnp.float32).astype(
        jnp.bfloat16
    )
    back_heads = attn_back.reshape(tok_rows, HEADS, HEAD_DIM)
    row_delta = jnp.sum(back_heads.astype(jnp.float32) * attn_sum, axis=2).T

    def back_step(query_acc, block_index):
        key_mask = block_mask(block_index)
        keys_blk = fetch_block(keys_all, block_index)
        values_blk = fetch_block(values_all, block_index)

        def back_live_block(running):
            prob_low, score_low = grad_pieces(
                query_heads,
                back_heads,
                keys_blk,
                values_blk,
                log_norm,
                row_delta,
                key_mask,
                score_scale,
            )
            value_part = jnp.einsum(
                "hqk,qhd->khd", prob_low, back_heads, preferred_element_type=jnp.float32
            )
            key_part = (
                jnp.einsum(
                    "hqk,qhd->khd", score_low, query_heads, preferred_element_type=jnp.float32
                )
                * score_scale
            )
            running = (
                running
                + jnp.einsum(
                    "hqk,khd->qhd", score_low, keys_blk, preferred_element_type=jnp.float32
                )
                * score_scale
            )
            return (
                running,
                (
                    key_part.reshape(key_block, model_width),
                    value_part.reshape(key_block, model_width),
                ),
            )

        def dead_block(running):
            empty_rows = jnp.zeros((key_block, model_width), jnp.float32)
            return (running, (empty_rows, empty_rows))

        return lax.cond(jnp.any(key_mask), back_live_block, dead_block, query_acc)

    query_grad32, key_terms = lax.scan(back_step, zero_heads, jnp.arange(num_blocks))
    key_grad32, value_grad32 = (
        lax.psum_scatter(
            key_terms[0].reshape(group_len, model_width).astype(jnp.bfloat16),
            (EX, SH),
            scatter_dimension=0,
            tiled=True,
        ).astype(jnp.float32),
        lax.psum_scatter(
            key_terms[1].reshape(group_len, model_width).astype(jnp.bfloat16),
            (EX, SH),
            scatter_dimension=0,
            tiled=True,
        ).astype(jnp.float32),
    )
    query_low = query_grad32.reshape(tok_rows, model_width).astype(jnp.bfloat16)
    key_low = key_grad32.astype(jnp.bfloat16)
    value_low = value_grad32.astype(jnp.bfloat16)
    query_term = jnp.dot(attn_in.T, query_low, preferred_element_type=jnp.float32)
    key_term = jnp.dot(attn_in.T, key_low, preferred_element_type=jnp.float32)
    value_term = jnp.dot(attn_in.T, value_low, preferred_element_type=jnp.float32)
    attn_in_grad = (
        jnp.dot(query_low, wq_full.T, preferred_element_type=jnp.float32)
        + jnp.dot(key_low, wk_full.T, preferred_element_type=jnp.float32)
        + jnp.dot(value_low, wv_full.T, preferred_element_type=jnp.float32)
    )
    attn_gain_grad = jnp.sum(attn_in_grad * normed_one, axis=0)
    input_grad = resid_grad + rms_back(inputs, inv_one, attn_gain, attn_in_grad)
    query_part, key_part_w, value_part_w, out_part = (
        lax.psum_scatter(
            query_term.astype(jnp.bfloat16), (EX, SH), scatter_dimension=0, tiled=True
        ).astype(jnp.float32),
        lax.psum_scatter(
            key_term.astype(jnp.bfloat16), (EX, SH), scatter_dimension=0, tiled=True
        ).astype(jnp.float32),
        lax.psum_scatter(
            value_term.astype(jnp.bfloat16), (EX, SH), scatter_dimension=0, tiled=True
        ).astype(jnp.float32),
        lax.psum_scatter(
            out_proj_term.astype(jnp.bfloat16), (EX, SH), scatter_dimension=0, tiled=True
        ).astype(jnp.float32),
    )
    gate_part, up_part, down_part = (
        lax.psum_scatter(
            gate_term.astype(jnp.bfloat16), SH, scatter_dimension=1, tiled=True
        ).astype(jnp.float32),
        lax.psum_scatter(
            up_term.astype(jnp.bfloat16), SH, scatter_dimension=1, tiled=True
        ).astype(jnp.float32),
        lax.psum_scatter(
            down_term.astype(jnp.bfloat16), SH, scatter_dimension=1, tiled=True
        ).astype(jnp.float32),
    )
    summed = (
        lax.psum(query_part.astype(jnp.bfloat16), GR).astype(jnp.float32),
        lax.psum(key_part_w.astype(jnp.bfloat16), GR).astype(jnp.float32),
        lax.psum(value_part_w.astype(jnp.bfloat16), GR).astype(jnp.float32),
        lax.psum(out_part.astype(jnp.bfloat16), GR).astype(jnp.float32),
        lax.psum(gate_part.astype(jnp.bfloat16), GR).astype(jnp.float32),
        lax.psum(up_part.astype(jnp.bfloat16), GR).astype(jnp.float32),
        lax.psum(down_part.astype(jnp.bfloat16), GR).astype(jnp.float32),
    )
    small_sums = lax.psum(
        (attn_gain_grad, moe_gain_grad, router_grad, mix_grad, vec_grad),
        (GR, EX, SH),
    )
    return (
        layer_out,
        input_grad,
        small_sums[0],
        summed[0],
        summed[1],
        summed[2],
        summed[3],
        small_sums[1],
        small_sums[2],
        small_sums[3],
        small_sums[4],
        summed[4],
        summed[5],
        summed[6],
    )


def greet(peers):
    barrier = pltpu.get_barrier_semaphore()
    for axis, peer in peers:
        pl.semaphore_signal(
            barrier, inc=1, device_id={axis: peer}, device_id_type=pl.DeviceIdType.MESH
        )
    pl.semaphore_wait(barrier, len(peers))


def send(src, dst, sems, index, axis, peer):
    copy = pltpu.make_async_remote_copy(
        src_ref=src,
        dst_ref=dst,
        send_sem=sems.at[0, index],
        recv_sem=sems.at[1, index],
        device_id={axis: peer},
        device_id_type=pl.DeviceIdType.MESH,
    )
    copy.start()
    return copy


def comm_call(body, name, collective_id, out_shapes, scratch, copies, operands):
    return pl.pallas_call(
        body,
        out_shape=out_shapes,
        in_specs=[VM] * len(operands),
        out_specs=[VM] * len(out_shapes),
        scratch_shapes=list(scratch) + [pltpu.SemaphoreType.DMA((2, copies))],
        compiler_params=pltpu.CompilerParams(collective_id=collective_id, has_side_effects=True),
        name=name,
    )(*operands)


def exchange(parts, collective_id, name):
    sizes = [lax.axis_size(axis) for axis, _, _ in parts]
    count = len(parts)
    out_shapes, scratch = [], []
    for (axis, kind, x), n in zip(parts, sizes):
        piece = x.shape if kind in (GATHER, GATHER_SUM) else x.shape[1:]
        if kind in (GATHER_SUM, SWAP_SUM):
            out_shapes.append(jax.ShapeDtypeStruct(piece, f32))
            scratch.append(pltpu.VMEM((n,) + piece, x.dtype))
        else:
            out_shapes.append(jax.ShapeDtypeStruct((n,) + piece, x.dtype))
    copies = sum(n - 1 for n in sizes)

    def body(*refs):
        ins, outs = refs[:count], refs[count : 2 * count]
        lands, sems = list(refs[2 * count : -1]), refs[-1]
        peers, seen = [], set()
        for (axis, _, _), n in zip(parts, sizes):
            if axis not in seen:
                seen.add(axis)
                me = lax.axis_index(axis)
                peers += [(axis, lax.rem(me + d, n)) for d in range(1, n)]
        greet(peers)
        started, index, slots = [], 0, []
        for k, ((axis, kind, _), n) in enumerate(zip(parts, sizes)):
            land = lands.pop(0) if kind in (GATHER_SUM, SWAP_SUM) else outs[k]
            slots.append(land)
            me = lax.axis_index(axis)
            for d in range(1, n):
                peer = lax.rem(me + d, n)
                src = ins[k] if kind in (GATHER, GATHER_SUM) else ins[k].at[peer]
                started.append(send(src, land.at[me], sems, index, axis, peer))
                index += 1
        for k, ((axis, kind, _), n) in enumerate(zip(parts, sizes)):
            me = lax.axis_index(axis)
            own = ins[k][...] if kind in (GATHER, GATHER_SUM) else ins[k][me]
            slots[k][me] = own
        index = 0
        for k, ((axis, kind, _), n) in enumerate(zip(parts, sizes)):
            for d in range(1, n):
                started[index].wait()
                index += 1
            if kind in (GATHER_SUM, SWAP_SUM):
                total = slots[k][0].astype(f32)
                for j in range(1, n):
                    total = total + slots[k][j].astype(f32)
                outs[k][...] = total

    return comm_call(
        body, name, collective_id, out_shapes, scratch, copies, [x for _, _, x in parts]
    )


def tree_gather(x, collective_id, name):
    lines = x.shape[0]
    half = lines // 2

    def body(x_ref, out_ref, sems):
        me = lax.axis_index(SH)
        near, far = lax.rem(me + 1, 2) + 2 * (me // 2), lax.rem(me + 2, 4)
        greet([(SH, near), (SH, far)])
        lo, hi = pl.ds(0, half), pl.ds(half, half)
        far_lo = send(x_ref.at[lo], out_ref.at[lo, me], sems, 0, SH, far)
        far_hi = send(x_ref.at[hi], out_ref.at[hi, me], sems, 1, SH, far)
        own = send(x_ref, out_ref.at[:, me], sems, 2, SH, near)
        out_ref[:, me] = x_ref[...]
        far_lo.wait_recv()
        pass_lo = send(out_ref.at[lo, far], out_ref.at[lo, far], sems, 3, SH, near)
        far_hi.wait_recv()
        pass_hi = send(out_ref.at[hi, far], out_ref.at[hi, far], sems, 4, SH, near)
        far_lo.wait_send()
        far_hi.wait_send()
        own.wait()
        pass_lo.wait()
        pass_hi.wait()

    shape = (lines, 4) + x.shape[1:]
    return comm_call(
        body, name, collective_id, [jax.ShapeDtypeStruct(shape, x.dtype)], [], 5, [x]
    )[0]


def tree_reduce(arrays, collective_id, name):
    count = len(arrays)
    scratch = []
    for x in arrays:
        scratch += [pltpu.VMEM((2,) + x.shape[1:], bf16)] + [pltpu.VMEM(x.shape[1:], bf16)] * 2

    def body(*refs):
        ins, outs = refs[:count], refs[count : 2 * count]
        sems = refs[-1]
        me = lax.axis_index(SH)
        side, core = me // 2, lax.rem(me, 2)
        near, far = 2 * side + 1 - core, 2 * (1 - side) + core
        other = 1 - side
        greet([(SH, near), (SH, far)])
        first = []
        for k in range(count):
            land = refs[2 * count + 3 * k]
            first.append(
                (
                    send(
                        ins[k].at[2 * other + 1 - core], land.at[0], sems, 3 * k, SH, near
                    ),
                    send(
                        ins[k].at[2 * side + 1 - core], land.at[1], sems, 3 * k + 1, SH, near
                    ),
                )
            )
        second = []
        for k in range(count):
            land, mine, got = refs[2 * count + 3 * k : 2 * count + 3 * k + 3]
            first[k][0].wait_recv()
            mine[...] = (ins[k][far].astype(f32) + land[0].astype(f32)).astype(bf16)
            second.append(send(mine, got, sems, 3 * k + 2, SH, far))
        for k in range(count):
            land, mine, got = refs[2 * count + 3 * k : 2 * count + 3 * k + 3]
            first[k][1].wait_recv()
            outs[k][...] = ins[k][me].astype(f32) + land[1].astype(f32)
        for k in range(count):
            got = refs[2 * count + 3 * k + 2]
            second[k].wait_recv()
            outs[k][...] += got[...].astype(f32)
            first[k][0].wait_send()
            first[k][1].wait_send()
            second[k].wait_send()

    return comm_call(
        body,
        name,
        collective_id,
        [jax.ShapeDtypeStruct(x.shape[1:], f32) for x in arrays],
        scratch,
        3 * count,
        arrays,
    )


def head_columns(h, shape, axis):
    return lax.broadcasted_iota(jnp.int32, shape, axis) // HEAD_DIM == h


def allowed(block, key_blk, qpos, qstart, prompt):
    kpos = block * key_blk + lax.broadcasted_iota(jnp.int32, (key_blk, qpos.shape[1]), 0)
    return (kpos <= qpos) & ((kpos >= qstart) | (kpos < prompt))


def attend_body(lines, heads, info_ref, q_ref, kv_ref, qinfo_ref, o_ref, low_ref, lse_ref, k_s, vt_s, acc_s, ml_s, qm_s):
    shard = lax.axis_index(SH)
    rows, width = q_ref.shape[1:]
    blocks = vt_s.shape[0]
    key_blk = vt_s.shape[2]
    prompt = info_ref[0]

    @pl.loop(0, blocks)
    def _(j):
        at = pl.ds(pl.multiple_of(j * key_blk, key_blk), key_blk)
        k_s[at, :] = kv_ref[at, :width]
        vt_s[j] = jnp.transpose(kv_ref[at, width:].astype(f32)).astype(bf16)

    @pl.loop(0, lines)
    def _(line):
        start = (line * 4 + shard) * rows
        queries = q_ref[line].astype(f32) * HEAD_DIM**-0.5
        qpos = start + lax.broadcasted_iota(jnp.int32, (1, rows), 1)
        qstart = qinfo_ref[line, 0:1, :]
        first = info_ref[1 + line]
        for h in range(heads):
            qm_s[h] = jnp.where(head_columns(h, queries.shape, 1), queries, 0.0).astype(bf16)
        acc_s[...] = jnp.zeros_like(acc_s)
        for h in range(heads):
            ml_s[h, 0:1, :] = jnp.full((1, rows), neg_fill, f32)
            ml_s[h, 1:2, :] = jnp.zeros((1, rows), f32)

        @pl.loop(0, (start + rows + key_blk - 1) // key_blk)
        def _(j):
            @pl.when((j * key_blk < prompt) | ((j + 1) * key_blk > first))
            def _():
                keys = k_s[pl.ds(pl.multiple_of(j * key_blk, key_blk), key_blk), :]
                ok = allowed(j, key_blk, qpos, qstart, prompt)
                for h in range(heads):
                    scores = jnp.where(ok, contract(keys, qm_s[h], 1, 1), neg_fill)
                    old = ml_s[h, 0:1, :]
                    new = jnp.maximum(old, jnp.max(scores, axis=0, keepdims=True))
                    probs = jnp.exp(scores - new)
                    scale = jnp.exp(old - new)
                    ml_s[h, 0:1, :] = new
                    ml_s[h, 1:2, :] = ml_s[h, 1:2, :] * scale + jnp.sum(
                        probs, axis=0, keepdims=True
                    )
                    part = slice(h * HEAD_DIM, (h + 1) * HEAD_DIM)
                    acc_s[part, :] = acc_s[part, :] * scale + jnp.dot(
                        vt_s[j, part, :], probs.astype(bf16), preferred_element_type=f32
                    )

        for h in range(heads):
            part = slice(h * HEAD_DIM, (h + 1) * HEAD_DIM)
            total = ml_s[h, 1:2, :]
            acc_s[part, :] = acc_s[part, :] / total
            lse_ref[line, h : h + 1, :] = ml_s[h, 0:1, :] + jnp.log(total)
        result = jnp.transpose(acc_s[...])
        o_ref[line] = result
        low_ref[line] = result.astype(bf16)


def attend(info, q, kv, qinfo):
    lines, rows, width = q.shape
    heads = width // HEAD_DIM
    length = kv.shape[0]
    key_blk = KEY_BLK
    shape = jax.ShapeDtypeStruct
    return pl.pallas_call(
        functools.partial(attend_body, lines, heads),
        out_shape=[
            shape((lines, rows, width), f32),
            shape((lines, rows, width), bf16),
            shape((lines, 8, rows), f32),
        ],
        in_specs=[SM, VM, VM, VM],
        out_specs=[VM] * 3,
        scratch_shapes=[
            pltpu.VMEM((length, width), bf16),
            pltpu.VMEM((length // key_blk, width, key_blk), bf16),
            pltpu.VMEM((width, rows), f32),
            pltpu.VMEM((heads, 8, rows), f32),
            pltpu.VMEM((heads, rows, width), bf16),
        ],
        cost_estimate=pl.CostEstimate(flops=2 * 10**9, bytes_accessed=8 * 10**6, transcendentals=4 * 10**6),
        name="attend",
    )(info, q, kv, qinfo)


def attend_back_body(lines, heads, info_ref, q_ref, kv_ref, qinfo_ref, o_ref, lse_ref, back_ref, dq_ref, dkv_ref, k_s, v_s, dk_s, dv_s, dq_s, qm_s, bm_s, delta_s):
    shard = lax.axis_index(SH)
    rows, width = q_ref.shape[1:]
    key_blk = KEY_BLK
    blocks = k_s.shape[0] // key_blk
    prompt = info_ref[0]

    @pl.loop(0, blocks)
    def _(j):
        at = pl.ds(pl.multiple_of(j * key_blk, key_blk), key_blk)
        k_s[at, :] = kv_ref[at, :width]
        v_s[at, :] = kv_ref[at, width:]
        dk_s[at, :] = jnp.zeros((key_blk, width), f32)
        dv_s[at, :] = jnp.zeros((key_blk, width), f32)

    @pl.loop(0, lines)
    def _(line):
        start = (line * 4 + shard) * rows
        queries = q_ref[line].astype(f32) * HEAD_DIM**-0.5
        back = back_ref[line].astype(f32)
        qpos = start + lax.broadcasted_iota(jnp.int32, (1, rows), 1)
        qstart = qinfo_ref[line, 0:1, :]
        first = info_ref[1 + line]
        picks = (
            lax.broadcasted_iota(jnp.int32, (8, width), 1) // HEAD_DIM
            == lax.broadcasted_iota(jnp.int32, (8, width), 0)
        ).astype(f32)
        delta_s[...] = contract(picks, back * o_ref[line], 1, 1, HIGH)
        for h in range(heads):
            mine = head_columns(h, queries.shape, 1)
            qm_s[h] = jnp.where(mine, queries, 0.0).astype(bf16)
            bm_s[h] = jnp.where(mine, back, 0.0).astype(bf16)
        dq_s[...] = jnp.zeros_like(dq_s)

        @pl.loop(0, (start + rows + key_blk - 1) // key_blk)
        def _(j):
            @pl.when((j * key_blk < prompt) | ((j + 1) * key_blk > first))
            def _():
                at = pl.ds(pl.multiple_of(j * key_blk, key_blk), key_blk)
                keys, values = k_s[at, :], v_s[at, :]
                ok = allowed(j, key_blk, qpos, qstart, prompt)
                dk = jnp.zeros((key_blk, width), f32)
                dv = jnp.zeros((key_blk, width), f32)
                for h in range(heads):
                    scores = contract(keys, qm_s[h], 1, 1)
                    probs = jnp.where(ok, jnp.exp(scores - lse_ref[line, h : h + 1, :]), 0.0)
                    grads = contract(values, bm_s[h], 1, 1)
                    slow = (probs * (grads - delta_s[h : h + 1, :])).astype(bf16)
                    dv = dv + jnp.dot(probs.astype(bf16), bm_s[h], preferred_element_type=f32)
                    dk = dk + jnp.dot(slow, qm_s[h], preferred_element_type=f32)
                    dq_s[h] += contract(slow, keys, 0, 0)
                dk_s[at, :] += dk
                dv_s[at, :] += dv

        total = jnp.zeros(queries.shape, f32)
        for h in range(heads):
            total = jnp.where(head_columns(h, queries.shape, 1), dq_s[h], total)
        dq_ref[line] = (total * HEAD_DIM**-0.5).astype(bf16)

    @pl.loop(0, lines)
    def _(line):
        for piece in range(4):
            at = pl.ds(pl.multiple_of((line * 4 + piece) * rows, rows), rows)
            dkv_ref[piece, line, :, :width] = dk_s[at, :].astype(bf16)
            dkv_ref[piece, line, :, width:] = dv_s[at, :].astype(bf16)


def attend_back(info, q, kv, qinfo, o, lse, back):
    lines, rows, width = q.shape
    heads = width // HEAD_DIM
    length = kv.shape[0]
    shape = jax.ShapeDtypeStruct
    return pl.pallas_call(
        functools.partial(attend_back_body, lines, heads),
        out_shape=[
            shape((lines, rows, width), bf16),
            shape((4, lines, rows, 2 * width), bf16),
        ],
        in_specs=[SM] + [VM] * 6,
        out_specs=[VM] * 2,
        scratch_shapes=[
            pltpu.VMEM((length, width), bf16),
            pltpu.VMEM((length, width), bf16),
            pltpu.VMEM((length, width), f32),
            pltpu.VMEM((length, width), f32),
            pltpu.VMEM((heads, rows, width), f32),
            pltpu.VMEM((heads, rows, width), bf16),
            pltpu.VMEM((heads, rows, width), bf16),
            pltpu.VMEM((8, rows), f32),
        ],
        cost_estimate=pl.CostEstimate(flops=5 * 10**9, bytes_accessed=12 * 10**6, transcendentals=4 * 10**6),
        name="attend_back",
    )(info, q, kv, qinfo, o, lse, back)


def swap(x, axis, partner):
    n = lax.axis_size(axis)
    return lax.ppermute(x, axis, [(i, partner(i)) for i in range(n)])


def pick(x, index):
    return lax.dynamic_index_in_dim(x, index, axis=0, keepdims=False)


def reduce_expert(term):
    me = lax.axis_index(SH)
    side, core = me // 2, lax.rem(me, 2)
    rows, cols = term.shape
    parts = term.reshape(2, 2, rows // 4, cols).swapaxes(0, 1)
    kept, sent = pick(parts, core), pick(parts, 1 - core).astype(bf16)
    both = kept + swap(sent, SH, lambda i: i ^ 1).astype(f32)
    kept, sent = pick(both, side), pick(both, 1 - side).astype(bf16)
    mine = (kept + swap(sent, SH, lambda i: i ^ 2).astype(f32)).astype(bf16)
    n = lax.axis_size(GR)
    if n == 2:
        return mine.astype(f32) + swap(mine, GR, lambda i: 1 - i).astype(f32)
    return jnp.sum(lax.all_gather(mine, GR).astype(f32), axis=0)


def fast_shards(
    hidden_in,
    segment_ids,
    routes,
    attn_gain,
    w_query,
    w_key,
    w_value,
    w_out,
    moe_gain,
    w_router,
    const_mix,
    const_vec,
    w_gate,
    w_up,
    w_down,
    out_grad,
):
    rows, model = hidden_in.shape
    lines = lax.axis_size(EX)
    line, shard = lax.axis_index(EX), lax.axis_index(SH)
    width = model // lines
    seg = segment_ids[0]
    length = seg.shape[0]

    w_mine = lax.dynamic_slice_in_dim(
        jnp.stack([w_query, w_key, w_value]), line * width, width, axis=2
    )
    hidden_all, w_cols, w_out_all = exchange(
        [(EX, GATHER, hidden_in), (SH, GATHER, w_mine), (SH, GATHER, w_out)],
        0,
        "gather_in",
    )
    w_heads = w_cols.swapaxes(0, 1).reshape(3, model, width)
    wo_full = w_out_all.reshape(model, model)
    inputs_all = hidden_all.reshape(lines * rows, model).astype(f32)
    inv_all = lax.rsqrt(jnp.mean(inputs_all * inputs_all, axis=1, keepdims=True) + norm_eps)
    attn_in = (inputs_all * inv_all * attn_gain).astype(bf16)
    q = jnp.dot(attn_in, w_heads[0], preferred_element_type=f32).astype(bf16)
    w_kv = jnp.concatenate([w_heads[1], w_heads[2]], axis=1)
    kv = jnp.dot(attn_in, w_kv, preferred_element_type=f32).astype(bf16)
    q = q.reshape(lines, rows, width)
    kv_all = tree_gather(kv.reshape(lines, rows, 2 * width), 1, "gather_kv")
    kv_all = kv_all.reshape(length, 2 * width)

    own_seg = jnp.take(seg.reshape(lines, 4, rows), shard, axis=1)
    qstart = jnp.sum(
        (seg[None, None, :] < own_seg[:, :, None]).astype(jnp.int32), axis=2, dtype=jnp.int32
    )
    prompt = jnp.sum((seg == 0).astype(jnp.int32), dtype=jnp.int32)
    info = jnp.concatenate([prompt[None], qstart[:, 0]])
    qinfo = jnp.broadcast_to(qstart[:, None, :], (lines, 8, rows))
    attn_vec, attn_low_heads, lse = attend(info, q, kv_all, qinfo)
    (attn_parts,) = exchange([(EX, SWAP, attn_low_heads)], 2, "heads_out")
    attn_low = attn_parts.swapaxes(0, 1).reshape(rows, model)

    inputs = hidden_in.astype(f32)
    inv_one = lax.rsqrt(jnp.mean(inputs * inputs, axis=1, keepdims=True) + norm_eps)
    resid_one = inputs + jnp.dot(attn_low, wo_full, preferred_element_type=f32)
    inv_two = lax.rsqrt(jnp.mean(resid_one * resid_one, axis=1, keepdims=True) + norm_eps)
    normed_two = resid_one * inv_two
    moe_in = normed_two * moe_gain
    moe_low = moe_in.astype(bf16)
    n_ids = w_router.shape[1]
    ids = jnp.arange(n_ids, dtype=jnp.int32)
    hot = (routes[:, :, None] == ids).astype(f32)
    small_w = jnp.concatenate([w_router, const_mix], axis=1)
    small = dense32(moe_in, small_w)
    chosen = jnp.sum(hot * small[:, None, :n_ids], axis=2)
    gate_probs = jax.nn.softmax(chosen, axis=1)
    mix_alpha = jax.nn.softmax(small[:, n_ids:].reshape(rows, 2, 2), axis=2)
    ffn_mask = (routes < lines).astype(f32)
    copy_mask = (routes == lines + 1).astype(f32)
    const_mask = hot[:, :, lines + 2 : lines + 4]
    copy_gate = jnp.sum(gate_probs * copy_mask, axis=1)
    const_gate = jnp.sum(gate_probs[:, :, None] * const_mask, axis=1)
    ffn_gate = gate_probs * ffn_mask
    before = (jnp.arange(rows)[:, None] > jnp.arange(rows)[None, :]).astype(bf16)
    earlier = jnp.dot(before, jnp.sum(hot, axis=1).astype(bf16), preferred_element_type=f32)
    slot_num = jnp.sum(hot * earlier[:, None, :], axis=2).astype(jnp.int32)
    slot = jnp.where(routes < lines, routes * CAP + slot_num, -1)
    slots = lines * CAP
    sits = slot[:, :, None] == jnp.arange(slots, dtype=jnp.int32)
    sit_gate = jnp.sum(jnp.where(sits, ffn_gate[:, :, None], 0.0), axis=(0, 1))
    place = [sits[:, k].astype(bf16) for k in range(2)]
    either = place[0] + place[1]
    send_rows = contract(either, moe_low, 0, 0).astype(bf16)
    grad_send = (contract(either, out_grad, 0, 0) * sit_gate[:, None]).astype(bf16)
    recv_rows, recv_grads = exchange(
        [
            (EX, SWAP, send_rows.reshape(lines, CAP, model)),
            (EX, SWAP, grad_send.reshape(lines, CAP, model)),
        ],
        3,
        "dispatch",
    )

    expert_in = recv_rows.reshape(slots, model)
    out_back = recv_grads.reshape(slots, model)
    wg, wu, wd = w_gate[0], w_up[0], w_down[0]
    gate_pre = jnp.dot(expert_in, wg, preferred_element_type=f32)
    up_pre = jnp.dot(expert_in, wu, preferred_element_type=f32)
    gate_sigmoid = jax.nn.sigmoid(gate_pre)
    hidden_act = (gate_pre * gate_sigmoid * up_pre).astype(bf16)
    expert_out = jnp.dot(hidden_act, wd, preferred_element_type=f32).astype(bf16)
    hidden_grad = contract(out_back, wd, 1, 1)
    gate_back = (
        hidden_grad * up_pre * gate_sigmoid * (1.0 + gate_pre * (1.0 - gate_sigmoid))
    ).astype(bf16)
    up_back = (hidden_grad * gate_pre * gate_sigmoid).astype(bf16)
    input_back = (contract(gate_back, wg, 1, 1) + contract(up_back, wu, 1, 1)).astype(bf16)
    returned, input_ret = exchange(
        [
            (EX, SWAP, expert_out.reshape(lines, CAP, model)),
            (EX, SWAP, input_back.reshape(lines, CAP, model)),
        ],
        4,
        "combine",
    )
    down_part = reduce_expert(contract(hidden_act, out_back, 0, 0))
    gate_part = reduce_expert(contract(expert_in, gate_back, 0, 0))
    up_part = reduce_expert(contract(expert_in, up_back, 0, 0))

    returned = returned.reshape(slots, model)
    route_out = jnp.stack(
        [jnp.dot(place[k], returned, preferred_element_type=f32) for k in range(2)], axis=1
    )
    ffn_in_grad = jnp.dot(either, input_ret.reshape(slots, model), preferred_element_type=f32)
    const_rows = mix_alpha[:, :, 0:1] * moe_in[:, None, :] + mix_alpha[:, :, 1:2] * const_vec[None]
    moe_sum = (
        jnp.sum(ffn_gate[:, :, None] * route_out, axis=1)
        + copy_gate[:, None] * moe_in
        + jnp.sum(const_gate[:, :, None] * const_rows, axis=1)
    )
    layer_out = (resid_one + moe_sum).astype(bf16)
    upstream = out_grad.astype(f32)
    route_dot = jnp.sum(upstream[:, None, :] * route_out, axis=2)
    copy_dot = jnp.sum(upstream * moe_in, axis=1)
    const_dot = jnp.sum(upstream[:, None, :] * const_rows, axis=2)
    gate_back_r = (
        ffn_mask * route_dot
        + copy_mask * copy_dot[:, None]
        + jnp.sum(const_mask * const_dot[:, None, :], axis=2)
    )
    chosen_grad = gate_probs * (
        gate_back_r - jnp.sum(gate_probs * gate_back_r, axis=1, keepdims=True)
    )
    logit_grad = jnp.sum(chosen_grad[:, :, None] * hot, axis=1)
    up_dot_vec = jnp.sum(upstream[:, None, :] * const_vec[None], axis=2)
    alpha_grad = jnp.stack(
        [const_gate * copy_dot[:, None], const_gate * up_dot_vec], axis=2
    )
    mix_back = (
        mix_alpha * (alpha_grad - jnp.sum(mix_alpha * alpha_grad, axis=2, keepdims=True))
    ).reshape(rows, 4)
    vec_scale = mix_alpha[:, :, 1] * const_gate
    small_back = jnp.concatenate([logit_grad, mix_back], axis=1)
    moe_in_grad = (
        ffn_in_grad
        + (copy_gate + jnp.sum(mix_alpha[:, :, 0] * const_gate, axis=1))[:, None] * upstream
        + dense32(small_back, small_w.T)
    )
    moe_gain_grad = jnp.sum(moe_in_grad * normed_two, axis=0)
    small_grad = contract(small_back, moe_in, 0, 0, HIGH)
    vec_grad = contract(vec_scale, upstream, 0, 0, HIGH)
    resid_grad = upstream + rms_back(resid_one, inv_two, moe_gain, moe_in_grad)
    branch_low = resid_grad.astype(bf16)
    attn_back = contract(branch_low, wo_full, 1, 1).astype(bf16)
    attn_back = attn_back.reshape(rows, lines, width).swapaxes(0, 1)
    (back_heads,) = exchange([(EX, SWAP, attn_back)], 5, "heads_back")
    out_proj_term = contract(attn_low, branch_low, 0, 0).astype(bf16)

    dq, dkv = attend_back(info, q, kv_all, qinfo, attn_vec, lse, back_heads)
    (dkv_own,) = tree_reduce([dkv], 6, "reduce_kv")
    dkv_own = dkv_own.reshape(lines * rows, 2 * width).astype(bf16)
    dq = dq.reshape(lines * rows, width)
    back_in = (
        contract(dq, w_heads[0], 1, 1) + contract(dkv_own, w_kv, 1, 1)
    ).astype(bf16)
    own = rows // lines
    q_term = contract(attn_in, dq, 0, 0)
    kv_term = contract(attn_in, dkv_own, 0, 0)
    qkv_term = jnp.concatenate([q_term, kv_term], axis=1).astype(bf16)
    qkv_term = qkv_term.reshape(lines, 4, own, 3 * width).swapaxes(0, 1)
    out_term = out_proj_term.reshape(lines, 4, own, model).swapaxes(0, 1)
    (attn_in_grad,) = exchange(
        [(EX, SWAP_SUM, back_in.reshape(lines, rows, model))], 7, "input_back"
    )
    qkv_sum, out_sum = tree_reduce([qkv_term, out_term], 8, "reduce_w")
    qkv_part, out_part = exchange(
        [
            (EX, SWAP, qkv_sum.astype(bf16)),
            (EX, SWAP_SUM, out_sum.astype(bf16)),
        ],
        9,
        "lines_w",
    )
    normed_one = inputs * inv_one
    attn_gain_grad = jnp.sum(attn_in_grad * normed_one, axis=0)
    input_grad = resid_grad + rms_back(inputs, inv_one, attn_gain, attn_in_grad)

    packed = jnp.concatenate(
        [attn_gain_grad[None], moe_gain_grad[None], vec_grad, small_grad], axis=0
    )
    packed, qkv_part, out_part = exchange(
        [
            (GR, GATHER_SUM, packed),
            (GR, GATHER_SUM, qkv_part),
            (GR, GATHER_SUM, out_part.astype(bf16)),
        ],
        10,
        "group_sum",
    )
    (packed,) = exchange([(EX, GATHER_SUM, packed)], 11, "small_lines")
    (packed,) = exchange([(SH, GATHER_SUM, packed)], 12, "small_shards")
    grads = [
        qkv_part[:, :, k * width : (k + 1) * width].swapaxes(0, 1).reshape(own, model)
        for k in range(3)
    ]
    return (
        layer_out,
        input_grad,
        packed[0],
        grads[0],
        grads[1],
        grads[2],
        out_part,
        packed[1],
        packed[4 : 4 + n_ids].T,
        packed[4 + n_ids :].T,
        packed[2:4],
        gate_part[None],
        up_part[None],
        down_part[None],
    )


def solution(mesh):
    placed = (
        P((GR, EX, SH), None),
        P(GR, None),
        P((GR, EX, SH), None),
        P(),
        P(SH, None),
        P(SH, None),
        P(SH, None),
        P(SH, None),
        P(),
        P(),
        P(),
        P(),
        P(EX, None, None),
        P(EX, None, None),
        P(EX, None, None),
        P((GR, EX, SH), None),
    )
    sizes = dict(mesh.shape)
    lines = sizes[EX]
    fast = sizes[SH] == 4 and lines == 4 and HEADS % lines == 0
    return jax.shard_map(
        fast_shards if fast else shards,
        mesh=mesh,
        in_specs=placed,
        out_specs=(
            P((GR, EX, SH), None),
            P((GR, EX, SH), None),
            P(),
            P((EX, SH), None),
            P((EX, SH), None),
            P((EX, SH), None),
            P((EX, SH), None),
            P(),
            P(),
            P(),
            P(),
            P(EX, SH, None),
            P(EX, SH, None),
            P(EX, SH, None),
        ),
        check_vma=False,
    )
```

```python
import functools

import jax
import jax.numpy as jnp
from jax import lax
from jax.experimental import pallas as pl
from jax.experimental.pallas import tpu as pltpu
from jax.sharding import PartitionSpec as P

HEADS = 12
HEAD_DIM = 64
CAP = 48
KEY_BLK = 256
EX, SH, GR = ("expert", "shard", "group")
GATHER, GATHER_SUM, SWAP, SWAP_SUM = range(4)


neg_fill = -1e30
norm_eps = 1e-05
bf16 = jnp.bfloat16
f32 = jnp.float32
VM = pl.BlockSpec(memory_space=pltpu.VMEM)
SM = pl.BlockSpec(memory_space=pltpu.SMEM)
HIGH = lax.Precision.HIGHEST


def contract(a, b, da, db, precision=None):
    return lax.dot_general(
        a, b, (((da,), (db,)), ((), ())), preferred_element_type=f32, precision=precision
    )


def dense32(left_side, right_side):
    return jnp.dot(left_side, right_side, precision=lax.Precision.HIGHEST)


def allowed_mask(query_pos, query_seg, key_pos, key_seg):
    same_doc = (key_seg[None, :] == query_seg[:, None]) | (key_seg[None, :] == 0)
    return same_doc & (key_pos[None, :] <= query_pos[:, None])


def rms_back(inputs, inverse, gain_vec, upstream):
    scaled = upstream * gain_vec
    return inverse * scaled - inputs * inverse**3 * jnp.mean(scaled * inputs, axis=1, keepdims=True)


def block_scores(query_blk, keys_blk, score_scale):
    return (
        jnp.einsum("qhd,khd->hqk", query_blk, keys_blk, preferred_element_type=jnp.float32)
        * score_scale
    )


def grad_pieces(
    query_blk, back_blk, keys_blk, values_blk, norm_blk, delta_blk, key_mask, score_scale
):
    scores = block_scores(query_blk, keys_blk, score_scale)
    prob_rows = jnp.where(key_mask[None], jnp.exp(scores - norm_blk[:, :, None]), 0.0)
    prob_grad = jnp.einsum("qhd,khd->hqk", back_blk, values_blk, preferred_element_type=jnp.float32)
    score_low = (prob_rows * (prob_grad - delta_blk[:, :, None])).astype(jnp.bfloat16)
    return (prob_rows.astype(jnp.bfloat16), score_low)


def shards(
    hidden_in,
    segment_ids,
    routes,
    attn_gain,
    w_query,
    w_key,
    w_value,
    w_out,
    moe_gain,
    w_router,
    const_mix,
    const_vec,
    w_gate,
    w_up,
    w_down,
    out_grad,
):
    tok_rows, model_width = hidden_in.shape
    score_scale = HEAD_DIM ** (-0.5)
    inner_rank = lax.axis_index((EX, SH))
    seg_group = segment_ids[0]
    group_len = seg_group.shape[0]
    key_block = min(512, group_len)
    num_blocks = group_len // key_block
    row_start = inner_rank * tok_rows
    own_pos = row_start + jnp.arange(tok_rows, dtype=jnp.int32)
    own_seg = lax.dynamic_slice_in_dim(seg_group, row_start, tok_rows)
    wq_full, wk_full, wv_full, wo_full = (
        lax.all_gather(w_query, SH, axis=0, tiled=True),
        lax.all_gather(w_key, SH, axis=0, tiled=True),
        lax.all_gather(w_value, SH, axis=0, tiled=True),
        lax.all_gather(w_out, SH, axis=0, tiled=True),
    )
    inputs = hidden_in.astype(jnp.float32)
    inv_one = lax.rsqrt(jnp.mean(inputs * inputs, axis=1, keepdims=True) + norm_eps)
    normed_one = inputs * inv_one
    attn_in = (normed_one * attn_gain).astype(jnp.bfloat16)
    queries = jnp.dot(attn_in, wq_full, preferred_element_type=jnp.float32).astype(jnp.bfloat16)
    keys_own = jnp.dot(attn_in, wk_full, preferred_element_type=jnp.float32).astype(jnp.bfloat16)
    values_own = jnp.dot(attn_in, wv_full, preferred_element_type=jnp.float32).astype(jnp.bfloat16)
    keys_all, values_all = (
        lax.all_gather(keys_own, (EX, SH), axis=0, tiled=True),
        lax.all_gather(values_own, (EX, SH), axis=0, tiled=True),
    )
    query_heads = queries.reshape(tok_rows, HEADS, HEAD_DIM)

    def fetch_block(source, block_index):
        return lax.dynamic_slice_in_dim(source, block_index * key_block, key_block).reshape(
            key_block, HEADS, HEAD_DIM
        )

    def block_mask(block_index):
        key_pos = block_index * key_block + jnp.arange(key_block, dtype=jnp.int32)
        key_seg = lax.dynamic_slice_in_dim(seg_group, block_index * key_block, key_block)
        return allowed_mask(own_pos, own_seg, key_pos, key_seg)

    def stats_step(carry_now, block_index):
        key_mask = block_mask(block_index)

        def stats_live_block(carry_in):
            row_max, row_sum = carry_in
            scores = jnp.where(
                key_mask[None],
                block_scores(query_heads, fetch_block(keys_all, block_index), score_scale),
                neg_fill,
            )
            new_max = jnp.maximum(row_max, jnp.max(scores, axis=2))
            weights = jnp.where(key_mask[None], jnp.exp(scores - new_max[:, :, None]), 0.0)
            return (new_max, row_sum * jnp.exp(row_max - new_max) + jnp.sum(weights, axis=2))

        return (
            lax.cond(jnp.any(key_mask), stats_live_block, lambda carry_in: carry_in, carry_now),
            None,
        )

    start_max = jnp.full((HEADS, tok_rows), neg_fill, jnp.float32)
    row_max, row_sum = lax.scan(
        stats_step, (start_max, jnp.zeros_like(start_max)), jnp.arange(num_blocks)
    )[0]
    log_norm = row_max + jnp.log(row_sum)

    def output_step(running, block_index):
        key_mask = block_mask(block_index)

        def output_live_block(carry_in):
            scores = block_scores(query_heads, fetch_block(keys_all, block_index), score_scale)
            prob_rows = jnp.where(
                key_mask[None], jnp.exp(scores - log_norm[:, :, None]), 0.0
            ).astype(jnp.bfloat16)
            return carry_in + jnp.einsum(
                "hqk,khd->qhd",
                prob_rows,
                fetch_block(values_all, block_index),
                preferred_element_type=jnp.float32,
            )

        return (
            lax.cond(jnp.any(key_mask), output_live_block, lambda carry_in: carry_in, running),
            None,
        )

    zero_heads = jnp.zeros((tok_rows, HEADS, HEAD_DIM), jnp.float32)
    attn_sum = lax.scan(output_step, zero_heads, jnp.arange(num_blocks))[0]
    attn_low = attn_sum.reshape(tok_rows, model_width).astype(jnp.bfloat16)
    resid_one = inputs + jnp.dot(attn_low, wo_full, preferred_element_type=jnp.float32)
    inv_two = lax.rsqrt(jnp.mean(resid_one * resid_one, axis=1, keepdims=True) + norm_eps)
    normed_two = resid_one * inv_two
    moe_in = normed_two * moe_gain
    moe_low = moe_in.astype(jnp.bfloat16)
    n_ids = w_router.shape[1]
    local_experts = w_gate.shape[0]
    owners = lax.axis_size(EX)
    ffn_count = local_experts * owners
    id_table = jnp.arange(n_ids, dtype=jnp.int32)
    route_hot = (routes[:, :, None] == id_table).astype(jnp.float32)
    logits = dense32(moe_in, w_router)
    chosen = jnp.einsum("rkn,rn->rk", route_hot, logits, precision=lax.Precision.HIGHEST)
    gate_probs = jax.nn.softmax(chosen, axis=1)
    mix_alpha = jax.nn.softmax(dense32(moe_in, const_mix).reshape(tok_rows, 2, 2), axis=2)
    const_rows = mix_alpha[:, :, 0:1] * moe_in[:, None, :] + mix_alpha[:, :, 1:2] * const_vec[None]
    ffn_mask = (routes < ffn_count).astype(jnp.float32)
    copy_mask = (routes == ffn_count + 1).astype(jnp.float32)
    const_mask = (routes[:, :, None] == ffn_count + 2 + jnp.arange(2, dtype=jnp.int32)).astype(
        jnp.float32
    )
    copy_gate = jnp.sum(gate_probs * copy_mask, axis=1)
    const_gate = jnp.sum(gate_probs[:, :, None] * const_mask, axis=1)
    ffn_gate = gate_probs * ffn_mask
    flat_ids = routes.reshape(-1)
    id_hot = (flat_ids[:, None] == id_table).astype(jnp.int32)
    earlier = jnp.cumsum(id_hot, axis=0, dtype=jnp.int32) - id_hot
    slot_num = jnp.sum(earlier * id_hot, axis=1, dtype=jnp.int32)
    slot_total = ffn_count * CAP
    slot_of_route = jnp.where(flat_ids < ffn_count, flat_ids * CAP + slot_num, slot_total)
    route_count = flat_ids.shape[0]
    route_of_slot = (
        jnp.zeros(slot_total + 1, jnp.int32)
        .at[slot_of_route]
        .set(jnp.arange(route_count, dtype=jnp.int32))[:slot_total]
    )
    slot_used = jnp.zeros(slot_total + 1, jnp.bool_).at[slot_of_route].set(True)[:slot_total]
    send_rows = jnp.where(
        slot_used[:, None], moe_low[route_of_slot // 2], jnp.zeros((), jnp.bfloat16)
    )
    recv_rows = lax.all_to_all(
        send_rows.reshape(owners, local_experts * CAP, model_width),
        EX,
        split_axis=0,
        concat_axis=0,
        tiled=True,
    )
    expert_in = recv_rows.reshape(owners, local_experts, CAP, model_width)
    gate_pre = jnp.einsum("sjcd,jdf->sjcf", expert_in, w_gate, preferred_element_type=jnp.float32)
    up_pre = jnp.einsum("sjcd,jdf->sjcf", expert_in, w_up, preferred_element_type=jnp.float32)
    gate_sigmoid = jax.nn.sigmoid(gate_pre)
    hidden_act = (gate_pre * gate_sigmoid * up_pre).astype(jnp.bfloat16)
    expert_out = jnp.einsum(
        "sjcf,jfd->sjcd", hidden_act, w_down, preferred_element_type=jnp.float32
    ).astype(jnp.bfloat16)
    returned = lax.all_to_all(
        expert_out.reshape(owners, local_experts * CAP, model_width),
        EX,
        split_axis=0,
        concat_axis=0,
        tiled=True,
    )
    padded_out = jnp.concatenate(
        [returned.reshape(slot_total, model_width), jnp.zeros((1, model_width), jnp.bfloat16)],
        axis=0,
    )
    route_out = padded_out[slot_of_route].astype(jnp.float32).reshape(tok_rows, 2, model_width)
    moe_sum = (
        jnp.sum(ffn_gate[:, :, None] * route_out, axis=1)
        + copy_gate[:, None] * moe_in
        + jnp.sum(const_gate[:, :, None] * const_rows, axis=1)
    )
    layer_out = (resid_one + moe_sum).astype(jnp.bfloat16)
    upstream = out_grad.astype(jnp.float32)
    route_dot = jnp.sum(upstream[:, None, :] * route_out, axis=2)
    copy_dot = jnp.sum(upstream * moe_in, axis=1)
    const_dot = jnp.sum(upstream[:, None, :] * const_rows, axis=2)
    gate_back_r = (
        ffn_mask * route_dot
        + copy_mask * copy_dot[:, None]
        + jnp.sum(const_mask * const_dot[:, None, :], axis=2)
    )
    chosen_grad = gate_probs * (
        gate_back_r - jnp.sum(gate_probs * gate_back_r, axis=1, keepdims=True)
    )
    logit_grad = jnp.einsum("rk,rkn->rn", chosen_grad, route_hot, precision=lax.Precision.HIGHEST)
    const_up = const_gate[:, :, None] * upstream[:, None, :]
    alpha_grad = jnp.stack(
        [
            jnp.sum(const_up * moe_in[:, None, :], axis=2),
            jnp.sum(const_up * const_vec[None], axis=2),
        ],
        axis=2,
    )
    mix_back = (
        mix_alpha * (alpha_grad - jnp.sum(mix_alpha * alpha_grad, axis=2, keepdims=True))
    ).reshape(tok_rows, 4)
    vec_grad = jnp.sum(mix_alpha[:, :, 1:2] * const_up, axis=0)
    route_weight = ffn_gate.reshape(-1)
    grad_send = (route_weight[route_of_slot][:, None] * upstream[route_of_slot // 2]).astype(
        jnp.bfloat16
    )
    grad_send = jnp.where(slot_used[:, None], grad_send, jnp.zeros((), jnp.bfloat16))
    grad_recv = lax.all_to_all(
        grad_send.reshape(owners, local_experts * CAP, model_width),
        EX,
        split_axis=0,
        concat_axis=0,
        tiled=True,
    )
    grad_recv = grad_recv.reshape(owners, local_experts, CAP, model_width)
    hidden_grad = jnp.einsum(
        "sjcd,jfd->sjcf", grad_recv, w_down, preferred_element_type=jnp.float32
    )
    down_term = jnp.einsum(
        "sjcf,sjcd->jfd", hidden_act, grad_recv, preferred_element_type=jnp.float32
    )
    gate_back = (
        hidden_grad * up_pre * gate_sigmoid * (1.0 + gate_pre * (1.0 - gate_sigmoid))
    ).astype(jnp.bfloat16)
    up_back = (hidden_grad * gate_pre * gate_sigmoid).astype(jnp.bfloat16)
    gate_term = jnp.einsum(
        "sjcd,sjcf->jdf", expert_in, gate_back, preferred_element_type=jnp.float32
    )
    up_term = jnp.einsum("sjcd,sjcf->jdf", expert_in, up_back, preferred_element_type=jnp.float32)
    input_back = (
        jnp.einsum("sjcf,jdf->sjcd", gate_back, w_gate, preferred_element_type=jnp.float32)
        + jnp.einsum("sjcf,jdf->sjcd", up_back, w_up, preferred_element_type=jnp.float32)
    ).astype(jnp.bfloat16)
    input_ret = lax.all_to_all(
        input_back.reshape(owners, local_experts * CAP, model_width),
        EX,
        split_axis=0,
        concat_axis=0,
        tiled=True,
    )
    padded_in = jnp.concatenate(
        [input_ret.reshape(slot_total, model_width), jnp.zeros((1, model_width), jnp.bfloat16)],
        axis=0,
    )
    ffn_in_grad = jnp.sum(
        padded_in[slot_of_route].astype(jnp.float32).reshape(tok_rows, 2, model_width), axis=1
    )
    moe_in_grad = (
        ffn_in_grad
        + copy_gate[:, None] * upstream
        + jnp.sum(mix_alpha[:, :, 0:1] * const_up, axis=1)
        + dense32(mix_back, const_mix.T)
        + dense32(logit_grad, w_router.T)
    )
    moe_gain_grad = jnp.sum(moe_in_grad * normed_two, axis=0)
    router_grad = dense32(moe_in.T, logit_grad)
    mix_grad = dense32(moe_in.T, mix_back)
    resid_grad = upstream + rms_back(resid_one, inv_two, moe_gain, moe_in_grad)
    branch_low = resid_grad.astype(jnp.bfloat16)
    out_proj_term = jnp.dot(attn_low.T, branch_low, preferred_element_type=jnp.float32)
    attn_back = jnp.dot(branch_low, wo_full.T, preferred_element_type=jnp.float32).astype(
        jnp.bfloat16
    )
    back_heads = attn_back.reshape(tok_rows, HEADS, HEAD_DIM)
    row_delta = jnp.sum(back_heads.astype(jnp.float32) * attn_sum, axis=2).T

    def back_step(query_acc, block_index):
        key_mask = block_mask(block_index)
        keys_blk = fetch_block(keys_all, block_index)
        values_blk = fetch_block(values_all, block_index)

        def back_live_block(running):
            prob_low, score_low = grad_pieces(
                query_heads,
                back_heads,
                keys_blk,
                values_blk,
                log_norm,
                row_delta,
                key_mask,
                score_scale,
            )
            value_part = jnp.einsum(
                "hqk,qhd->khd", prob_low, back_heads, preferred_element_type=jnp.float32
            )
            key_part = (
                jnp.einsum(
                    "hqk,qhd->khd", score_low, query_heads, preferred_element_type=jnp.float32
                )
                * score_scale
            )
            running = (
                running
                + jnp.einsum(
                    "hqk,khd->qhd", score_low, keys_blk, preferred_element_type=jnp.float32
                )
                * score_scale
            )
            return (
                running,
                (
                    key_part.reshape(key_block, model_width),
                    value_part.reshape(key_block, model_width),
                ),
            )

        def dead_block(running):
            empty_rows = jnp.zeros((key_block, model_width), jnp.float32)
            return (running, (empty_rows, empty_rows))

        return lax.cond(jnp.any(key_mask), back_live_block, dead_block, query_acc)

    query_grad32, key_terms = lax.scan(back_step, zero_heads, jnp.arange(num_blocks))
    key_grad32, value_grad32 = (
        lax.psum_scatter(
            key_terms[0].reshape(group_len, model_width).astype(jnp.bfloat16),
            (EX, SH),
            scatter_dimension=0,
            tiled=True,
        ).astype(jnp.float32),
        lax.psum_scatter(
            key_terms[1].reshape(group_len, model_width).astype(jnp.bfloat16),
            (EX, SH),
            scatter_dimension=0,
            tiled=True,
        ).astype(jnp.float32),
    )
    query_low = query_grad32.reshape(tok_rows, model_width).astype(jnp.bfloat16)
    key_low = key_grad32.astype(jnp.bfloat16)
    value_low = value_grad32.astype(jnp.bfloat16)
    query_term = jnp.dot(attn_in.T, query_low, preferred_element_type=jnp.float32)
    key_term = jnp.dot(attn_in.T, key_low, preferred_element_type=jnp.float32)
    value_term = jnp.dot(attn_in.T, value_low, preferred_element_type=jnp.float32)
    attn_in_grad = (
        jnp.dot(query_low, wq_full.T, preferred_element_type=jnp.float32)
        + jnp.dot(key_low, wk_full.T, preferred_element_type=jnp.float32)
        + jnp.dot(value_low, wv_full.T, preferred_element_type=jnp.float32)
    )
    attn_gain_grad = jnp.sum(attn_in_grad * normed_one, axis=0)
    input_grad = resid_grad + rms_back(inputs, inv_one, attn_gain, attn_in_grad)
    query_part, key_part_w, value_part_w, out_part = (
        lax.psum_scatter(
            query_term.astype(jnp.bfloat16), (EX, SH), scatter_dimension=0, tiled=True
        ).astype(jnp.float32),
        lax.psum_scatter(
            key_term.astype(jnp.bfloat16), (EX, SH), scatter_dimension=0, tiled=True
        ).astype(jnp.float32),
        lax.psum_scatter(
            value_term.astype(jnp.bfloat16), (EX, SH), scatter_dimension=0, tiled=True
        ).astype(jnp.float32),
        lax.psum_scatter(
            out_proj_term.astype(jnp.bfloat16), (EX, SH), scatter_dimension=0, tiled=True
        ).astype(jnp.float32),
    )
    gate_part, up_part, down_part = (
        lax.psum_scatter(
            gate_term.astype(jnp.bfloat16), SH, scatter_dimension=1, tiled=True
        ).astype(jnp.float32),
        lax.psum_scatter(
            up_term.astype(jnp.bfloat16), SH, scatter_dimension=1, tiled=True
        ).astype(jnp.float32),
        lax.psum_scatter(
            down_term.astype(jnp.bfloat16), SH, scatter_dimension=1, tiled=True
        ).astype(jnp.float32),
    )
    summed = (
        lax.psum(query_part.astype(jnp.bfloat16), GR).astype(jnp.float32),
        lax.psum(key_part_w.astype(jnp.bfloat16), GR).astype(jnp.float32),
        lax.psum(value_part_w.astype(jnp.bfloat16), GR).astype(jnp.float32),
        lax.psum(out_part.astype(jnp.bfloat16), GR).astype(jnp.float32),
        lax.psum(gate_part.astype(jnp.bfloat16), GR).astype(jnp.float32),
        lax.psum(up_part.astype(jnp.bfloat16), GR).astype(jnp.float32),
        lax.psum(down_part.astype(jnp.bfloat16), GR).astype(jnp.float32),
    )
    small_sums = lax.psum(
        (attn_gain_grad, moe_gain_grad, router_grad, mix_grad, vec_grad),
        (GR, EX, SH),
    )
    return (
        layer_out,
        input_grad,
        small_sums[0],
        summed[0],
        summed[1],
        summed[2],
        summed[3],
        small_sums[1],
        small_sums[2],
        small_sums[3],
        small_sums[4],
        summed[4],
        summed[5],
        summed[6],
    )


def greet(peers):
    barrier = pltpu.get_barrier_semaphore()
    for axis, peer in peers:
        pl.semaphore_signal(
            barrier, inc=1, device_id={axis: peer}, device_id_type=pl.DeviceIdType.MESH
        )
    pl.semaphore_wait(barrier, len(peers))


def send(src, dst, sems, index, axis, peer):
    copy = pltpu.make_async_remote_copy(
        src_ref=src,
        dst_ref=dst,
        send_sem=sems.at[0, index],
        recv_sem=sems.at[1, index],
        device_id={axis: peer},
        device_id_type=pl.DeviceIdType.MESH,
    )
    copy.start()
    return copy


def shard_peers():
    me = lax.axis_index(SH)
    side, core = me // 2, lax.rem(me, 2)
    return me, side, core, 2 * side + 1 - core, 2 * (1 - side) + core


class Part:
    def __init__(self, axes, ins, outs, scratch, copies, phases, specs=None):
        self.axes, self.ins, self.outs, self.scratch = axes, ins, outs, scratch
        self.copies, self.phases = copies, phases
        self.specs = specs or [VM] * len(ins)


def run_parts(parts, collective_id, name=None, cost=None):
    ins = sum([p.ins for p in parts], [])
    outs = sum([p.outs for p in parts], [])
    scratch = sum([p.scratch for p in parts], [])
    copies = sum(p.copies for p in parts)
    axes = sorted(set(sum([list(p.axes) for p in parts], [])))

    def body(*refs):
        sems = refs[-1]
        in_refs, out_refs = list(refs[: len(ins)]), list(refs[len(ins) : len(ins) + len(outs)])
        scr = list(refs[len(ins) + len(outs) : -1])
        peers = []
        for axis in axes:
            me, n = lax.axis_index(axis), lax.axis_size(axis)
            peers += [(axis, lax.rem(me + d, n)) for d in range(1, n)]
        greet(peers)
        base, running = 0, []
        for p in parts:
            take = lambda pool, k: [pool.pop(0) for _ in range(k)]
            refs_p = (take(in_refs, len(p.ins)), take(out_refs, len(p.outs)), take(scr, len(p.scratch)))
            counter = [base]

            def go(src, dst, axis, peer, counter=counter):
                counter[0] += 1
                return send(src, dst, sems, counter[0] - 1, axis, peer)

            running.append(p.phases(*refs_p, go))
            base += p.copies
        while running:
            running = [r for r in running if next(r, True) is None]

    return pl.pallas_call(
        body,
        out_shape=outs,
        in_specs=sum([p.specs for p in parts], []),
        out_specs=[VM] * len(outs),
        scratch_shapes=scratch + [pltpu.SemaphoreType.DMA((2, copies))],
        compiler_params=pltpu.CompilerParams(collective_id=collective_id, has_side_effects=True),
        cost_estimate=cost,
        name=name,
    )(*ins)


def start_swap(go, src, land, axis, gather):
    me, n = lax.axis_index(axis), lax.axis_size(axis)
    started = []
    for d in range(1, n):
        peer = lax.rem(me + d, n)
        started.append(go(src if gather else src.at[peer], land.at[me], axis, peer))
    land[me] = src[...] if gather else src[me]
    return started


def total_of(land, n):
    total = land[0].astype(f32)
    for j in range(1, n):
        total = total + land[j].astype(f32)
    return total


def exchange(axis, kind, x):
    n = lax.axis_size(axis)
    gather, summed = kind in (GATHER, GATHER_SUM), kind in (GATHER_SUM, SWAP_SUM)
    piece = x.shape if gather else x.shape[1:]
    shape = jax.ShapeDtypeStruct
    outs = [shape(piece, f32) if summed else shape((n,) + piece, x.dtype)]
    scratch = [pltpu.VMEM((n,) + piece, x.dtype)] if summed else []

    def phases(ins, outs, scr, go):
        land = scr[0] if summed else outs[0]
        started = start_swap(go, ins[0], land, axis, gather)
        yield
        for copy in started:
            copy.wait()
        if summed:
            outs[0][...] = total_of(land, n)

    return Part([axis], [x], outs, scratch, n - 1, phases)


def tree_gather(x):
    lines = x.shape[0]
    cuts = [(0, lines // 2), (lines // 2, lines)] if lines > 1 else [(0, 1)]
    cuts = [pl.ds(lo, hi - lo) for lo, hi in cuts]

    def phases(ins, outs, scr, go):
        x_ref, out_ref = ins[0], outs[0]
        me, _, _, near, far = shard_peers()
        across = [go(x_ref.at[c], out_ref.at[c, me], SH, far) for c in cuts]
        own = go(x_ref, out_ref.at[:, me], SH, near)
        out_ref[:, me] = x_ref[...]
        yield
        handed = []
        for c, copy in zip(cuts, across):
            copy.wait_recv()
            handed.append(go(out_ref.at[c, far], out_ref.at[c, far], SH, near))
        yield
        for copy in across:
            copy.wait_send()
        own.wait()
        for copy in handed:
            copy.wait()

    shape = (lines, 4) + x.shape[1:]
    return Part([SH], [x], [jax.ShapeDtypeStruct(shape, x.dtype)], [], 2 * len(cuts) + 1, phases)


def core_sum(x):
    piece = x.shape[1:]
    shape = jax.ShapeDtypeStruct

    def phases(ins, outs, scr, go):
        x_ref, (here, there), (land, kept, sems) = ins[0], outs, scr
        near = shard_peers()[3]
        sent = [go(x_ref.at[3], land.at[1], SH, near), go(x_ref.at[2], land.at[0], SH, near)]
        local = [pltpu.make_async_copy(x_ref.at[k], kept.at[k], sems.at[k]) for k in range(2)]
        for copy in local:
            copy.start()
        yield
        for k, out in ((1, there), (0, here)):
            sent[1 - k].wait()
            local[k].wait()
            out[...] = (kept[k].astype(f32) + land[k].astype(f32)).astype(bf16)

    return Part(
        [SH],
        [x],
        [shape(piece, bf16)] * 2,
        [pltpu.VMEM((2,) + piece, bf16)] * 2 + [pltpu.SemaphoreType.DMA((2,))],
        2,
        phases,
        [pl.BlockSpec(memory_space=pl.ANY)],
    )


class Tree:
    copies = 3

    @staticmethod
    def scratch(piece):
        return [pltpu.VMEM((2,) + piece, bf16)] + [pltpu.VMEM(piece, bf16)] * 2

    def __init__(self, x, scr, go):
        self.x, (self.land, self.mine, self.got), self.go = x, scr, go
        self.me, self.side, self.core, self.near, self.far = shard_peers()
        other = 2 * (1 - self.side) + 1 - self.core
        self.first = [
            go(x.at[other], self.land.at[0], SH, self.near),
            go(x.at[self.near], self.land.at[1], SH, self.near),
        ]

    def across(self):
        self.first[0].wait_recv()
        self.mine[...] = (self.x[self.far].astype(f32) + self.land[0].astype(f32)).astype(bf16)
        self.second = self.go(self.mine, self.got, SH, self.far)

    def result(self):
        self.first[1].wait_recv()
        total = self.x[self.me].astype(f32) + self.land[1].astype(f32)
        self.second.wait_recv()
        return total + self.got[...].astype(f32)

    def close(self):
        for copy in (*self.first, self.second):
            copy.wait_send()


def tail(dkv, dq, attn_in, weights, out_term, packed, hidden, resid_grad, gain):
    lines, rows, width = dq.shape
    model = lines * width
    own = rows // lines
    groups = lax.axis_size(GR)
    shape = jax.ShapeDtypeStruct
    vmem = pltpu.VMEM
    tok = lines * rows
    dkv_piece, q_piece = (lines, rows, 2 * width), (lines, own, width)
    kv_piece, o_piece = (lines, own, 2 * width), (lines, own, model)
    part_dims = (width, 2 * width, model)

    def phases(ins, outs, scr, go):
        dkv_ref, dq_ref, attn_ref, w_ref, o_ref, packed_ref, hid_ref, resid_ref, gain_ref = ins
        input_ref, qkv_out, out_out, packed_out, gain_out = outs
        scr = list(scr)
        take = lambda k: [scr.pop(0) for _ in range(k)]
        kv_scr, q_scr, kvw_scr, o_scr = take(3), take(3), take(3), take(3)
        own_kv, q_t, kv_t, dq_all, dkv_all, dq_full = take(6)
        sums, lands, halves, gots = take(3), take(3), take(3), take(3)
        pk_l, pk_s, pk_g = take(3)
        mid_l, mid_s = take(2)
        gn_l, gn_s, gn_g, gn_0, gn_1, gn_2 = take(6)
        me = lax.axis_index(SH)

        kv_tree = Tree(dkv_ref, kv_scr, go)
        dq_swap = start_swap(go, dq_ref, dq_all, EX, False)
        o_tree = Tree(o_ref, o_scr, go)
        pk1 = start_swap(go, packed_ref, pk_l, EX, True)

        def term(rows_ref, out):
            value = contract(attn_ref[...], rows_ref[...].reshape(tok, rows_ref.shape[-1]), 0, 0)
            value = value.astype(bf16)
            for line in range(lines):
                for piece in range(4):
                    at = (line * 4 + piece) * own
                    out[piece, line] = value[at : at + own]

        kv_tree.across()
        term(dq_ref, q_t)
        o_tree.across()
        q_tree = Tree(q_t, q_scr, go)
        trees = [q_tree, None, o_tree]

        def lines_out(k):
            sums[k][...] = trees[k].result().astype(bf16)
            return start_swap(go, sums[k], lands[k], EX, False)

        own_kv[...] = kv_tree.result().astype(bf16)
        dkv_swap = start_swap(go, own_kv, dkv_all, EX, False)
        o_lines = lines_out(2)
        q_tree.across()
        term(own_kv, kv_t)
        kvw_tree = Tree(kv_t, kvw_scr, go)
        trees[1] = kvw_tree
        for copy in pk1:
            copy.wait()
        mid_l[...] = total_of(pk_l, lines)
        pk2 = start_swap(go, mid_l, pk_s, SH, True)
        kvw_tree.across()
        q_lines = lines_out(0)
        for copy in dq_swap:
            copy.wait()
        for line in range(lines):
            dq_full[:, line * width : (line + 1) * width] = dq_all[line]
        grad = contract(dq_full[...], w_ref[0], 1, 1)
        for copy in pk2:
            copy.wait()
        mid_s[...] = total_of(pk_s, 4)
        pk3 = start_swap(go, mid_s, pk_g, GR, True)
        kv_lines = lines_out(1)
        for copy in dkv_swap:
            copy.wait()
        for half in range(2):
            for line in range(lines):
                dq_full[:, line * width : (line + 1) * width] = dkv_all[
                    line, :, half * width : (half + 1) * width
                ]
            grad = grad + contract(dq_full[...], w_ref[1 + half], 1, 1)
        inputs = hid_ref[...].astype(f32)
        inv = lax.rsqrt(jnp.mean(inputs * inputs, axis=1, keepdims=True) + norm_eps)
        normed = inputs * inv
        gn_0[...] = jnp.sum((grad * normed).reshape(rows // 8, 8, model), axis=0)
        gn1 = start_swap(go, gn_0, gn_l, EX, True)
        input_ref[...] = resid_ref[...] + rms_back(inputs, inv, gain_ref[...], grad)
        swaps = [None] * 3
        for k, copies in ((2, o_lines), (0, q_lines)):
            for copy in copies:
                copy.wait()
            if k == 2:
                halves[k][...] = total_of(lands[k], lines).astype(bf16)
            else:
                halves[k][...] = lands[k][...]
            swaps[k] = start_swap(go, halves[k], gots[k], GR, True)
        for copy in gn1:
            copy.wait()
        gn_1[...] = total_of(gn_l, lines)
        gn2 = start_swap(go, gn_1, gn_s, SH, True)
        for copy in kv_lines:
            copy.wait()
        halves[1][...] = lands[1][...]
        swaps[1] = start_swap(go, halves[1], gots[1], GR, True)
        for copy in gn2:
            copy.wait()
        gn_2[...] = total_of(gn_s, 4)
        gn3 = start_swap(go, gn_2, gn_g, GR, True)
        for copy in pk3:
            copy.wait()
        packed_out[...] = total_of(pk_g, groups)
        for k in (2, 0, 1):
            for copy in swaps[k]:
                copy.wait()
            value = total_of(gots[k], groups)
            if k == 2:
                out_out[...] = value
            elif k == 0:
                for line in range(lines):
                    qkv_out[0, :, line * width : (line + 1) * width] = value[line]
            else:
                for half in range(2):
                    for line in range(lines):
                        qkv_out[1 + half, :, line * width : (line + 1) * width] = value[
                            line, :, half * width : (half + 1) * width
                        ]
        for copy in gn3:
            copy.wait()
        gain_out[...] = jnp.sum(total_of(gn_g, groups), axis=0, keepdims=True)
        for tree in (kv_tree, o_tree, q_tree, kvw_tree):
            tree.close()
        yield

    pieces = [(lines, own, d) for d in part_dims]
    got_pieces = pieces[:2] + [(own, model)]
    scratch = Tree.scratch(dkv_piece) + Tree.scratch(q_piece) + Tree.scratch(kv_piece)
    scratch += Tree.scratch(o_piece)
    scratch += [
        vmem(dkv_piece, bf16),
        vmem((4,) + q_piece, bf16),
        vmem((4,) + kv_piece, bf16),
        vmem((lines, rows, width), bf16),
        vmem((lines, rows, 2 * width), bf16),
        vmem((rows, model), bf16),
    ]
    scratch += [vmem(p, bf16) for p in pieces] + [vmem(p, bf16) for p in pieces]
    scratch += [vmem(p, bf16) for p in got_pieces] + [vmem((groups,) + p, bf16) for p in got_pieces]
    scratch += [vmem((n,) + packed.shape, f32) for n in (lines, 4, groups)]
    scratch += [vmem(packed.shape, f32)] * 2
    scratch += [vmem((n, 8, model), f32) for n in (lines, 4, groups)] + [vmem((8, model), f32)] * 3
    copies = 4 * Tree.copies + 7 * (lines - 1) + 2 * 3 + 5 * (groups - 1)
    outs = [
        shape((rows, model), f32),
        shape((3, own, model), f32),
        shape((own, model), f32),
        shape(packed.shape, f32),
        shape((1, model), f32),
    ]
    ins = [dkv, dq, attn_in, weights, out_term, packed, hidden, resid_grad, gain]
    return Part([EX, SH, GR], ins, outs, scratch, copies, phases)


def expert_body(steps, x_ref, g_ref, wg_ref, wu_ref, wd_ref, eo_ref, ib_ref, gu_ref, d_ref, eo_s, ib_s):
    i = pl.program_id(0)
    me, side, core, _, _ = shard_peers()

    @pl.when(i == 0)
    def _():
        eo_s[...] = jnp.zeros_like(eo_s)
        ib_s[...] = jnp.zeros_like(ib_s)

    x, g = x_ref[...], g_ref[...]
    wg, wu, wd = wg_ref[...], wu_ref[...], wd_ref[...]
    gate_pre = jnp.dot(x, wg, preferred_element_type=f32)
    up_pre = jnp.dot(x, wu, preferred_element_type=f32)
    hidden_grad = contract(g, wd, 1, 1)
    gate_sigmoid = jax.nn.sigmoid(gate_pre)
    act = (gate_pre * gate_sigmoid * up_pre).astype(bf16)
    gate_back = (
        hidden_grad * up_pre * gate_sigmoid * (1.0 + gate_pre * (1.0 - gate_sigmoid))
    ).astype(bf16)
    up_back = (hidden_grad * gate_pre * gate_sigmoid).astype(bf16)
    eo_s[...] += jnp.dot(act, wd, preferred_element_type=f32)
    ib_s[...] += contract(gate_back, wg, 1, 1) + contract(up_back, wu, 1, 1)

    def place(quarter):
        return 2 * lax.rem(lax.rem(quarter, 2) + core, 2) + lax.rem(quarter // 2 + side, 2)

    rows = gu_ref.shape[2]
    for k, back in enumerate((gate_back, up_back)):
        term = contract(x, back, 0, 0).astype(bf16)
        for quarter in range(4):
            gu_ref[place(jnp.int32(quarter)), k] = term[quarter * rows : (quarter + 1) * rows]
    d_ref[place(i)] = contract(act, g, 0, 0).astype(bf16)

    @pl.when(i == steps - 1)
    def _():
        eo_ref[...] = eo_s[...].astype(bf16)
        ib_ref[...] = ib_s[...].astype(bf16)


def expert(x, g, wg, wu, wd):
    slots, model = x.shape
    inner = wg.shape[1]
    steps = 4
    tile = inner // steps
    quarter = model // 4
    shape = jax.ShapeDtypeStruct
    whole = lambda dims: pl.BlockSpec(dims, lambda i: (0,) * len(dims))
    return pl.pallas_call(
        functools.partial(expert_body, steps),
        grid=(steps,),
        out_shape=[
            shape((slots, model), bf16),
            shape((slots, model), bf16),
            shape((4, 2, quarter, inner), bf16),
            shape((4, tile, model), bf16),
        ],
        in_specs=[
            whole((slots, model)),
            whole((slots, model)),
            pl.BlockSpec((model, tile), lambda i: (0, i)),
            pl.BlockSpec((model, tile), lambda i: (0, i)),
            pl.BlockSpec((tile, model), lambda i: (i, 0)),
        ],
        out_specs=[
            whole((slots, model)),
            whole((slots, model)),
            pl.BlockSpec((4, 2, quarter, tile), lambda i: (0, 0, 0, i)),
            whole((4, tile, model)),
        ],
        scratch_shapes=[pltpu.VMEM((slots, model), f32)] * 2,
        cost_estimate=pl.CostEstimate(flops=6 * 10**9, bytes_accessed=2 * 10**7, transcendentals=4 * 10**5),
        name="ffn",
    )(x, g, wg, wu, wd)


def head_columns(h, shape, axis):
    return lax.broadcasted_iota(jnp.int32, shape, axis) // HEAD_DIM == h


def allowed(block, key_blk, qpos, qstart, prompt):
    kpos = block * key_blk + lax.broadcasted_iota(jnp.int32, (key_blk, qpos.shape[1]), 0)
    return (kpos <= qpos) & ((kpos >= qstart) | (kpos < prompt))


def attend_body(lines, heads, info_ref, q_ref, kv_ref, qinfo_ref, o_ref, low_ref, lse_ref, k_s, vt_s, acc_s, ml_s, qm_s):
    shard = lax.axis_index(SH)
    rows, width = q_ref.shape[1:]
    blocks = vt_s.shape[0]
    key_blk = vt_s.shape[2]
    prompt = info_ref[0]

    @pl.loop(0, blocks)
    def _(j):
        at = pl.ds(pl.multiple_of(j * key_blk, key_blk), key_blk)
        k_s[at, :] = kv_ref[at, :width]
        vt_s[j] = jnp.transpose(kv_ref[at, width:].astype(f32)).astype(bf16)

    @pl.loop(0, lines)
    def _(line):
        start = (line * 4 + shard) * rows
        queries = q_ref[line].astype(f32) * HEAD_DIM**-0.5
        qpos = start + lax.broadcasted_iota(jnp.int32, (1, rows), 1)
        qstart = qinfo_ref[line, 0:1, :]
        first = info_ref[1 + line]
        for h in range(heads):
            qm_s[h] = jnp.where(head_columns(h, queries.shape, 1), queries, 0.0).astype(bf16)
        acc_s[...] = jnp.zeros_like(acc_s)
        for h in range(heads):
            ml_s[h, 0:1, :] = jnp.full((1, rows), neg_fill, f32)
            ml_s[h, 1:2, :] = jnp.zeros((1, rows), f32)

        @pl.loop(0, (start + rows + key_blk - 1) // key_blk)
        def _(j):
            @pl.when((j * key_blk < prompt) | ((j + 1) * key_blk > first))
            def _():
                keys = k_s[pl.ds(pl.multiple_of(j * key_blk, key_blk), key_blk), :]
                ok = allowed(j, key_blk, qpos, qstart, prompt)
                for h in range(heads):
                    scores = jnp.where(ok, contract(keys, qm_s[h], 1, 1), neg_fill)
                    old = ml_s[h, 0:1, :]
                    new = jnp.maximum(old, jnp.max(scores, axis=0, keepdims=True))
                    probs = jnp.exp(scores - new)
                    scale = jnp.exp(old - new)
                    ml_s[h, 0:1, :] = new
                    ml_s[h, 1:2, :] = ml_s[h, 1:2, :] * scale + jnp.sum(
                        probs, axis=0, keepdims=True
                    )
                    part = slice(h * HEAD_DIM, (h + 1) * HEAD_DIM)
                    acc_s[part, :] = acc_s[part, :] * scale + jnp.dot(
                        vt_s[j, part, :], probs.astype(bf16), preferred_element_type=f32
                    )

        for h in range(heads):
            part = slice(h * HEAD_DIM, (h + 1) * HEAD_DIM)
            total = ml_s[h, 1:2, :]
            acc_s[part, :] = acc_s[part, :] / total
            lse_ref[line, h : h + 1, :] = ml_s[h, 0:1, :] + jnp.log(total)
        result = jnp.transpose(acc_s[...])
        o_ref[line] = result
        low_ref[line] = result.astype(bf16)


def attend(info, q, kv, qinfo):
    lines, rows, width = q.shape
    heads = width // HEAD_DIM
    length = kv.shape[0]
    key_blk = KEY_BLK
    shape = jax.ShapeDtypeStruct
    return pl.pallas_call(
        functools.partial(attend_body, lines, heads),
        out_shape=[
            shape((lines, rows, width), f32),
            shape((lines, rows, width), bf16),
            shape((lines, 8, rows), f32),
        ],
        in_specs=[SM, VM, VM, VM],
        out_specs=[VM] * 3,
        scratch_shapes=[
            pltpu.VMEM((length, width), bf16),
            pltpu.VMEM((length // key_blk, width, key_blk), bf16),
            pltpu.VMEM((width, rows), f32),
            pltpu.VMEM((heads, 8, rows), f32),
            pltpu.VMEM((heads, rows, width), bf16),
        ],
        cost_estimate=pl.CostEstimate(flops=2 * 10**9, bytes_accessed=8 * 10**6, transcendentals=4 * 10**6),
        name="attend",
    )(info, q, kv, qinfo)


def attend_back_body(lines, heads, info_ref, q_ref, kv_ref, qinfo_ref, o_ref, lse_ref, back_ref, dq_ref, dkv_ref, k_s, v_s, dk_s, dv_s, dq_s, qm_s, bm_s, delta_s):
    shard = lax.axis_index(SH)
    rows, width = q_ref.shape[1:]
    key_blk = KEY_BLK
    blocks = k_s.shape[0] // key_blk
    prompt = info_ref[0]

    @pl.loop(0, blocks)
    def _(j):
        at = pl.ds(pl.multiple_of(j * key_blk, key_blk), key_blk)
        k_s[at, :] = kv_ref[at, :width]
        v_s[at, :] = kv_ref[at, width:]
        dk_s[at, :] = jnp.zeros((key_blk, width), f32)
        dv_s[at, :] = jnp.zeros((key_blk, width), f32)

    @pl.loop(0, lines)
    def _(line):
        start = (line * 4 + shard) * rows
        queries = q_ref[line].astype(f32) * HEAD_DIM**-0.5
        back = back_ref[line].astype(f32)
        qpos = start + lax.broadcasted_iota(jnp.int32, (1, rows), 1)
        qstart = qinfo_ref[line, 0:1, :]
        first = info_ref[1 + line]
        picks = (
            lax.broadcasted_iota(jnp.int32, (8, width), 1) // HEAD_DIM
            == lax.broadcasted_iota(jnp.int32, (8, width), 0)
        ).astype(f32)
        delta_s[...] = contract(picks, back * o_ref[line], 1, 1, HIGH)
        for h in range(heads):
            mine = head_columns(h, queries.shape, 1)
            qm_s[h] = jnp.where(mine, queries, 0.0).astype(bf16)
            bm_s[h] = jnp.where(mine, back, 0.0).astype(bf16)
        dq_s[...] = jnp.zeros_like(dq_s)

        @pl.loop(0, (start + rows + key_blk - 1) // key_blk)
        def _(j):
            @pl.when((j * key_blk < prompt) | ((j + 1) * key_blk > first))
            def _():
                at = pl.ds(pl.multiple_of(j * key_blk, key_blk), key_blk)
                keys, values = k_s[at, :], v_s[at, :]
                ok = allowed(j, key_blk, qpos, qstart, prompt)
                dk = jnp.zeros((key_blk, width), f32)
                dv = jnp.zeros((key_blk, width), f32)
                for h in range(heads):
                    scores = contract(keys, qm_s[h], 1, 1)
                    probs = jnp.where(ok, jnp.exp(scores - lse_ref[line, h : h + 1, :]), 0.0)
                    grads = contract(values, bm_s[h], 1, 1)
                    slow = (probs * (grads - delta_s[h : h + 1, :])).astype(bf16)
                    dv = dv + jnp.dot(probs.astype(bf16), bm_s[h], preferred_element_type=f32)
                    dk = dk + jnp.dot(slow, qm_s[h], preferred_element_type=f32)
                    dq_s[h] += contract(slow, keys, 0, 0)
                dk_s[at, :] += dk
                dv_s[at, :] += dv

        total = jnp.zeros(queries.shape, f32)
        for h in range(heads):
            total = jnp.where(head_columns(h, queries.shape, 1), dq_s[h], total)
        dq_ref[line] = (total * HEAD_DIM**-0.5).astype(bf16)

    @pl.loop(0, lines)
    def _(line):
        for piece in range(4):
            at = pl.ds(pl.multiple_of((line * 4 + piece) * rows, rows), rows)
            dkv_ref[piece, line, :, :width] = dk_s[at, :].astype(bf16)
            dkv_ref[piece, line, :, width:] = dv_s[at, :].astype(bf16)


def attend_back(info, q, kv, qinfo, o, lse, back):
    lines, rows, width = q.shape
    heads = width // HEAD_DIM
    length = kv.shape[0]
    shape = jax.ShapeDtypeStruct
    return pl.pallas_call(
        functools.partial(attend_back_body, lines, heads),
        out_shape=[
            shape((lines, rows, width), bf16),
            shape((4, lines, rows, 2 * width), bf16),
        ],
        in_specs=[SM] + [VM] * 6,
        out_specs=[VM] * 2,
        scratch_shapes=[
            pltpu.VMEM((length, width), bf16),
            pltpu.VMEM((length, width), bf16),
            pltpu.VMEM((length, width), f32),
            pltpu.VMEM((length, width), f32),
            pltpu.VMEM((heads, rows, width), f32),
            pltpu.VMEM((heads, rows, width), bf16),
            pltpu.VMEM((heads, rows, width), bf16),
            pltpu.VMEM((8, rows), f32),
        ],
        cost_estimate=pl.CostEstimate(flops=5 * 10**9, bytes_accessed=12 * 10**6, transcendentals=4 * 10**6),
        name="attend_back",
    )(info, q, kv, qinfo, o, lse, back)


def swap(x, axis, partner):
    return lax.ppermute(x, axis, [(i, partner(i)) for i in range(lax.axis_size(axis))])


def over_group(mine):
    n = lax.axis_size(GR)
    if n == 2:
        return mine.astype(f32) + swap(mine, GR, lambda i: 1 - i).astype(f32)
    return jnp.sum(lax.all_gather(mine, GR).astype(f32), axis=0)


def fast_shards(
    hidden_in,
    segment_ids,
    routes,
    attn_gain,
    w_query,
    w_key,
    w_value,
    w_out,
    moe_gain,
    w_router,
    const_mix,
    const_vec,
    w_gate,
    w_up,
    w_down,
    out_grad,
):
    rows, model = hidden_in.shape
    lines = lax.axis_size(EX)
    line, shard = lax.axis_index(EX), lax.axis_index(SH)
    width = model // lines
    seg = segment_ids[0]
    length = seg.shape[0]

    w_mine = lax.dynamic_slice_in_dim(
        jnp.stack([w_query, w_key, w_value]), line * width, width, axis=2
    )
    hidden_all, w_cols = run_parts(
        [exchange(EX, GATHER, hidden_in), exchange(SH, GATHER, w_mine)], 0, "gather_in"
    )
    w_heads = w_cols.swapaxes(0, 1).reshape(3, model, width)
    inputs_all = hidden_all.reshape(lines * rows, model).astype(f32)
    inv_all = lax.rsqrt(jnp.mean(inputs_all * inputs_all, axis=1, keepdims=True) + norm_eps)
    attn_in = (inputs_all * inv_all * attn_gain).astype(bf16)
    q = jnp.dot(attn_in, w_heads[0], preferred_element_type=f32).astype(bf16)
    w_kv = jnp.concatenate([w_heads[1], w_heads[2]], axis=1)
    kv = jnp.dot(attn_in, w_kv, preferred_element_type=f32).astype(bf16)
    q = q.reshape(lines, rows, width)
    (kv_all,) = run_parts([tree_gather(kv.reshape(lines, rows, 2 * width))], 1, "gather_kv")
    kv_all = kv_all.reshape(length, 2 * width)

    own_seg = jnp.take(seg.reshape(lines, 4, rows), shard, axis=1)
    qstart = jnp.sum(
        (seg[None, None, :] < own_seg[:, :, None]).astype(jnp.int32), axis=2, dtype=jnp.int32
    )
    prompt = jnp.sum((seg == 0).astype(jnp.int32), dtype=jnp.int32)
    info = jnp.concatenate([prompt[None], qstart[:, 0]])
    qinfo = jnp.broadcast_to(qstart[:, None, :], (lines, 8, rows))
    attn_vec, attn_low_heads, lse = attend(info, q, kv_all, qinfo)
    attn_parts, wo_full = run_parts(
        [exchange(EX, SWAP, attn_low_heads), tree_gather(w_out[None])], 2, "heads_out"
    )
    wo_full = wo_full.reshape(model, model)
    attn_low = attn_parts.swapaxes(0, 1).reshape(rows, model)

    inputs = hidden_in.astype(f32)
    resid_one = inputs + jnp.dot(attn_low, wo_full, preferred_element_type=f32)
    inv_two = lax.rsqrt(jnp.mean(resid_one * resid_one, axis=1, keepdims=True) + norm_eps)
    normed_two = resid_one * inv_two
    moe_in = normed_two * moe_gain
    moe_low = moe_in.astype(bf16)
    n_ids = w_router.shape[1]
    ids = jnp.arange(n_ids, dtype=jnp.int32)
    hot = (routes[:, :, None] == ids).astype(f32)
    small_w = jnp.concatenate([w_router, const_mix], axis=1)
    small = dense32(moe_in, small_w)
    chosen = jnp.sum(hot * small[:, None, :n_ids], axis=2)
    gate_probs = jax.nn.softmax(chosen, axis=1)
    mix_alpha = jax.nn.softmax(small[:, n_ids:].reshape(rows, 2, 2), axis=2)
    ffn_mask = (routes < lines).astype(f32)
    copy_mask = (routes == lines + 1).astype(f32)
    const_mask = hot[:, :, lines + 2 : lines + 4]
    copy_gate = jnp.sum(gate_probs * copy_mask, axis=1)
    const_gate = jnp.sum(gate_probs[:, :, None] * const_mask, axis=1)
    ffn_gate = gate_probs * ffn_mask
    before = (jnp.arange(rows)[:, None] > jnp.arange(rows)[None, :]).astype(bf16)
    earlier = jnp.dot(before, jnp.sum(hot, axis=1).astype(bf16), preferred_element_type=f32)
    slot_num = jnp.sum(hot * earlier[:, None, :], axis=2).astype(jnp.int32)
    slot = jnp.where(routes < lines, routes * CAP + slot_num, -1)
    slots = lines * CAP
    sits = slot[:, :, None] == jnp.arange(slots, dtype=jnp.int32)
    sit_gate = jnp.sum(jnp.where(sits, ffn_gate[:, :, None], 0.0), axis=(0, 1))
    place = [sits[:, k].astype(bf16) for k in range(2)]
    either = place[0] + place[1]
    send_rows = contract(either, moe_low, 0, 0).astype(bf16)
    grad_send = (contract(either, out_grad, 0, 0) * sit_gate[:, None]).astype(bf16)
    recv_rows, recv_grads, weights = run_parts(
        [
            exchange(EX, SWAP, send_rows.reshape(lines, CAP, model)),
            exchange(EX, SWAP, grad_send.reshape(lines, CAP, model)),
            tree_gather(jnp.stack([w_query, w_key, w_value])),
        ],
        3,
        "dispatch",
    )
    weights = weights.reshape(3, model, model)

    expert_out, input_back, gate_up, down = expert(
        recv_rows.reshape(slots, model), recv_grads.reshape(slots, model), w_gate[0], w_up[0], w_down[0]
    )
    returned, input_ret, gu_here, gu_there, d_here, d_there = run_parts(
        [
            exchange(EX, SWAP, expert_out.reshape(lines, CAP, model)),
            exchange(EX, SWAP, input_back.reshape(lines, CAP, model)),
            core_sum(gate_up),
            core_sum(down),
        ],
        4,
        "combine",
    )
    gu_far = swap(gu_there, SH, lambda i: i ^ 2)
    d_far = swap(d_there, SH, lambda i: i ^ 2)

    returned = returned.reshape(slots, model)
    route_out = jnp.stack(
        [jnp.dot(place[k], returned, preferred_element_type=f32) for k in range(2)], axis=1
    )
    ffn_in_grad = jnp.dot(either, input_ret.reshape(slots, model), preferred_element_type=f32)
    const_rows = mix_alpha[:, :, 0:1] * moe_in[:, None, :] + mix_alpha[:, :, 1:2] * const_vec[None]
    moe_sum = (
        jnp.sum(ffn_gate[:, :, None] * route_out, axis=1)
        + copy_gate[:, None] * moe_in
        + jnp.sum(const_gate[:, :, None] * const_rows, axis=1)
    )
    layer_out = (resid_one + moe_sum).astype(bf16)
    upstream = out_grad.astype(f32)
    route_dot = jnp.sum(upstream[:, None, :] * route_out, axis=2)
    copy_dot = jnp.sum(upstream * moe_in, axis=1)
    const_dot = jnp.sum(upstream[:, None, :] * const_rows, axis=2)
    gate_back_r = (
        ffn_mask * route_dot
        + copy_mask * copy_dot[:, None]
        + jnp.sum(const_mask * const_dot[:, None, :], axis=2)
    )
    chosen_grad = gate_probs * (
        gate_back_r - jnp.sum(gate_probs * gate_back_r, axis=1, keepdims=True)
    )
    logit_grad = jnp.sum(chosen_grad[:, :, None] * hot, axis=1)
    up_dot_vec = jnp.sum(upstream[:, None, :] * const_vec[None], axis=2)
    alpha_grad = jnp.stack(
        [const_gate * copy_dot[:, None], const_gate * up_dot_vec], axis=2
    )
    mix_back = (
        mix_alpha * (alpha_grad - jnp.sum(mix_alpha * alpha_grad, axis=2, keepdims=True))
    ).reshape(rows, 4)
    vec_scale = mix_alpha[:, :, 1] * const_gate
    small_back = jnp.concatenate([logit_grad, mix_back], axis=1)
    moe_in_grad = (
        ffn_in_grad
        + (copy_gate + jnp.sum(mix_alpha[:, :, 0] * const_gate, axis=1))[:, None] * upstream
        + dense32(small_back, small_w.T)
    )
    moe_gain_grad = jnp.sum(moe_in_grad * normed_two, axis=0)
    small_grad = contract(small_back, moe_in, 0, 0, HIGH)
    vec_grad = contract(vec_scale, upstream, 0, 0, HIGH)
    resid_grad = upstream + rms_back(resid_one, inv_two, moe_gain, moe_in_grad)
    branch_low = resid_grad.astype(bf16)
    attn_back = contract(branch_low, wo_full, 1, 1).astype(bf16)
    attn_back = attn_back.reshape(rows, lines, width).swapaxes(0, 1)
    (back_heads,) = run_parts([exchange(EX, SWAP, attn_back)], 5, "heads_back")
    own = rows // lines
    out_term = contract(attn_low, branch_low, 0, 0).astype(bf16)
    out_term = out_term.reshape(lines, 4, own, model).swapaxes(0, 1)
    packed = jnp.concatenate([moe_gain_grad[None], vec_grad, small_grad], axis=0)
    packed = jnp.pad(packed, ((0, -packed.shape[0] % 8), (0, 0)))

    dq, dkv = attend_back(info, q, kv_all, qinfo, attn_vec, lse, back_heads)
    gu_mine = (gu_here.astype(f32) + gu_far.astype(f32)).astype(bf16)
    d_mine = (d_here.astype(f32) + d_far.astype(f32)).astype(bf16)
    dkv, gu_mine, d_mine = lax.optimization_barrier((dkv, gu_mine, d_mine))
    gate_up_part, down_part = over_group(gu_mine), over_group(d_mine)
    input_grad, qkv_part, out_part, packed, gain_sum = run_parts(
        [
            tail(
                dkv, dq, attn_in, weights, out_term, packed, hidden_in, resid_grad, attn_gain[None]
            )
        ],
        6,
        "tail",
        pl.CostEstimate(flops=2 * 10**10, bytes_accessed=10**8, transcendentals=0),
    )
    return (
        layer_out,
        input_grad,
        gain_sum[0],
        qkv_part[0],
        qkv_part[1],
        qkv_part[2],
        out_part,
        packed[0],
        packed[3 : 3 + n_ids].T,
        packed[3 + n_ids : 7 + n_ids].T,
        packed[1:3],
        gate_up_part[0][None],
        gate_up_part[1][None],
        down_part[None],
    )


def solution(mesh):
    placed = (
        P((GR, EX, SH), None),
        P(GR, None),
        P((GR, EX, SH), None),
        P(),
        P(SH, None),
        P(SH, None),
        P(SH, None),
        P(SH, None),
        P(),
        P(),
        P(),
        P(),
        P(EX, None, None),
        P(EX, None, None),
        P(EX, None, None),
        P((GR, EX, SH), None),
    )
    sizes = dict(mesh.shape)
    lines = sizes[EX]
    fast = sizes[SH] == 4 and lines == 4 and HEADS % lines == 0
    return jax.shard_map(
        fast_shards if fast else shards,
        mesh=mesh,
        in_specs=placed,
        out_specs=(
            P((GR, EX, SH), None),
            P((GR, EX, SH), None),
            P(),
            P((EX, SH), None),
            P((EX, SH), None),
            P((EX, SH), None),
            P((EX, SH), None),
            P(),
            P(),
            P(),
            P(),
            P(EX, SH, None),
            P(EX, SH, None),
            P(EX, SH, None),
        ),
        check_vma=False,
    )
```

```python
import functools

import jax
import jax.numpy as jnp
from jax import lax
from jax.experimental import pallas as pl
from jax.experimental.pallas import tpu as pltpu
from jax.sharding import PartitionSpec as P

HEADS = 12
HEAD_DIM = 64
CAP = 48
KEY_BLK = 256
EX, SH, GR = ("expert", "shard", "group")
GATHER, GATHER_SUM, SWAP, SWAP_SUM = range(4)


neg_fill = -1e30
norm_eps = 1e-05
bf16 = jnp.bfloat16
f32 = jnp.float32
VM = pl.BlockSpec(memory_space=pltpu.VMEM)
SM = pl.BlockSpec(memory_space=pltpu.SMEM)
HIGH = lax.Precision.HIGHEST


def contract(a, b, da, db, precision=None):
    return lax.dot_general(
        a, b, (((da,), (db,)), ((), ())), preferred_element_type=f32, precision=precision
    )


def dense32(left_side, right_side):
    return jnp.dot(left_side, right_side, precision=lax.Precision.HIGHEST)


def allowed_mask(query_pos, query_seg, key_pos, key_seg):
    same_doc = (key_seg[None, :] == query_seg[:, None]) | (key_seg[None, :] == 0)
    return same_doc & (key_pos[None, :] <= query_pos[:, None])


def rms_back(inputs, inverse, gain_vec, upstream):
    scaled = upstream * gain_vec
    return inverse * scaled - inputs * inverse**3 * jnp.mean(scaled * inputs, axis=1, keepdims=True)


def block_scores(query_blk, keys_blk, score_scale):
    return (
        jnp.einsum("qhd,khd->hqk", query_blk, keys_blk, preferred_element_type=jnp.float32)
        * score_scale
    )


def grad_pieces(
    query_blk, back_blk, keys_blk, values_blk, norm_blk, delta_blk, key_mask, score_scale
):
    scores = block_scores(query_blk, keys_blk, score_scale)
    prob_rows = jnp.where(key_mask[None], jnp.exp(scores - norm_blk[:, :, None]), 0.0)
    prob_grad = jnp.einsum("qhd,khd->hqk", back_blk, values_blk, preferred_element_type=jnp.float32)
    score_low = (prob_rows * (prob_grad - delta_blk[:, :, None])).astype(jnp.bfloat16)
    return (prob_rows.astype(jnp.bfloat16), score_low)


def shards(
    hidden_in,
    segment_ids,
    routes,
    attn_gain,
    w_query,
    w_key,
    w_value,
    w_out,
    moe_gain,
    w_router,
    const_mix,
    const_vec,
    w_gate,
    w_up,
    w_down,
    out_grad,
):
    tok_rows, model_width = hidden_in.shape
    score_scale = HEAD_DIM ** (-0.5)
    inner_rank = lax.axis_index((EX, SH))
    seg_group = segment_ids[0]
    group_len = seg_group.shape[0]
    key_block = min(512, group_len)
    num_blocks = group_len // key_block
    row_start = inner_rank * tok_rows
    own_pos = row_start + jnp.arange(tok_rows, dtype=jnp.int32)
    own_seg = lax.dynamic_slice_in_dim(seg_group, row_start, tok_rows)
    wq_full, wk_full, wv_full, wo_full = (
        lax.all_gather(w_query, SH, axis=0, tiled=True),
        lax.all_gather(w_key, SH, axis=0, tiled=True),
        lax.all_gather(w_value, SH, axis=0, tiled=True),
        lax.all_gather(w_out, SH, axis=0, tiled=True),
    )
    inputs = hidden_in.astype(jnp.float32)
    inv_one = lax.rsqrt(jnp.mean(inputs * inputs, axis=1, keepdims=True) + norm_eps)
    normed_one = inputs * inv_one
    attn_in = (normed_one * attn_gain).astype(jnp.bfloat16)
    queries = jnp.dot(attn_in, wq_full, preferred_element_type=jnp.float32).astype(jnp.bfloat16)
    keys_own = jnp.dot(attn_in, wk_full, preferred_element_type=jnp.float32).astype(jnp.bfloat16)
    values_own = jnp.dot(attn_in, wv_full, preferred_element_type=jnp.float32).astype(jnp.bfloat16)
    keys_all, values_all = (
        lax.all_gather(keys_own, (EX, SH), axis=0, tiled=True),
        lax.all_gather(values_own, (EX, SH), axis=0, tiled=True),
    )
    query_heads = queries.reshape(tok_rows, HEADS, HEAD_DIM)

    def fetch_block(source, block_index):
        return lax.dynamic_slice_in_dim(source, block_index * key_block, key_block).reshape(
            key_block, HEADS, HEAD_DIM
        )

    def block_mask(block_index):
        key_pos = block_index * key_block + jnp.arange(key_block, dtype=jnp.int32)
        key_seg = lax.dynamic_slice_in_dim(seg_group, block_index * key_block, key_block)
        return allowed_mask(own_pos, own_seg, key_pos, key_seg)

    def stats_step(carry_now, block_index):
        key_mask = block_mask(block_index)

        def stats_live_block(carry_in):
            row_max, row_sum = carry_in
            scores = jnp.where(
                key_mask[None],
                block_scores(query_heads, fetch_block(keys_all, block_index), score_scale),
                neg_fill,
            )
            new_max = jnp.maximum(row_max, jnp.max(scores, axis=2))
            weights = jnp.where(key_mask[None], jnp.exp(scores - new_max[:, :, None]), 0.0)
            return (new_max, row_sum * jnp.exp(row_max - new_max) + jnp.sum(weights, axis=2))

        return (
            lax.cond(jnp.any(key_mask), stats_live_block, lambda carry_in: carry_in, carry_now),
            None,
        )

    start_max = jnp.full((HEADS, tok_rows), neg_fill, jnp.float32)
    row_max, row_sum = lax.scan(
        stats_step, (start_max, jnp.zeros_like(start_max)), jnp.arange(num_blocks)
    )[0]
    log_norm = row_max + jnp.log(row_sum)

    def output_step(running, block_index):
        key_mask = block_mask(block_index)

        def output_live_block(carry_in):
            scores = block_scores(query_heads, fetch_block(keys_all, block_index), score_scale)
            prob_rows = jnp.where(
                key_mask[None], jnp.exp(scores - log_norm[:, :, None]), 0.0
            ).astype(jnp.bfloat16)
            return carry_in + jnp.einsum(
                "hqk,khd->qhd",
                prob_rows,
                fetch_block(values_all, block_index),
                preferred_element_type=jnp.float32,
            )

        return (
            lax.cond(jnp.any(key_mask), output_live_block, lambda carry_in: carry_in, running),
            None,
        )

    zero_heads = jnp.zeros((tok_rows, HEADS, HEAD_DIM), jnp.float32)
    attn_sum = lax.scan(output_step, zero_heads, jnp.arange(num_blocks))[0]
    attn_low = attn_sum.reshape(tok_rows, model_width).astype(jnp.bfloat16)
    resid_one = inputs + jnp.dot(attn_low, wo_full, preferred_element_type=jnp.float32)
    inv_two = lax.rsqrt(jnp.mean(resid_one * resid_one, axis=1, keepdims=True) + norm_eps)
    normed_two = resid_one * inv_two
    moe_in = normed_two * moe_gain
    moe_low = moe_in.astype(jnp.bfloat16)
    n_ids = w_router.shape[1]
    local_experts = w_gate.shape[0]
    owners = lax.axis_size(EX)
    ffn_count = local_experts * owners
    id_table = jnp.arange(n_ids, dtype=jnp.int32)
    route_hot = (routes[:, :, None] == id_table).astype(jnp.float32)
    logits = dense32(moe_in, w_router)
    chosen = jnp.einsum("rkn,rn->rk", route_hot, logits, precision=lax.Precision.HIGHEST)
    gate_probs = jax.nn.softmax(chosen, axis=1)
    mix_alpha = jax.nn.softmax(dense32(moe_in, const_mix).reshape(tok_rows, 2, 2), axis=2)
    const_rows = mix_alpha[:, :, 0:1] * moe_in[:, None, :] + mix_alpha[:, :, 1:2] * const_vec[None]
    ffn_mask = (routes < ffn_count).astype(jnp.float32)
    copy_mask = (routes == ffn_count + 1).astype(jnp.float32)
    const_mask = (routes[:, :, None] == ffn_count + 2 + jnp.arange(2, dtype=jnp.int32)).astype(
        jnp.float32
    )
    copy_gate = jnp.sum(gate_probs * copy_mask, axis=1)
    const_gate = jnp.sum(gate_probs[:, :, None] * const_mask, axis=1)
    ffn_gate = gate_probs * ffn_mask
    flat_ids = routes.reshape(-1)
    id_hot = (flat_ids[:, None] == id_table).astype(jnp.int32)
    earlier = jnp.cumsum(id_hot, axis=0, dtype=jnp.int32) - id_hot
    slot_num = jnp.sum(earlier * id_hot, axis=1, dtype=jnp.int32)
    slot_total = ffn_count * CAP
    slot_of_route = jnp.where(flat_ids < ffn_count, flat_ids * CAP + slot_num, slot_total)
    route_count = flat_ids.shape[0]
    route_of_slot = (
        jnp.zeros(slot_total + 1, jnp.int32)
        .at[slot_of_route]
        .set(jnp.arange(route_count, dtype=jnp.int32))[:slot_total]
    )
    slot_used = jnp.zeros(slot_total + 1, jnp.bool_).at[slot_of_route].set(True)[:slot_total]
    send_rows = jnp.where(
        slot_used[:, None], moe_low[route_of_slot // 2], jnp.zeros((), jnp.bfloat16)
    )
    recv_rows = lax.all_to_all(
        send_rows.reshape(owners, local_experts * CAP, model_width),
        EX,
        split_axis=0,
        concat_axis=0,
        tiled=True,
    )
    expert_in = recv_rows.reshape(owners, local_experts, CAP, model_width)
    gate_pre = jnp.einsum("sjcd,jdf->sjcf", expert_in, w_gate, preferred_element_type=jnp.float32)
    up_pre = jnp.einsum("sjcd,jdf->sjcf", expert_in, w_up, preferred_element_type=jnp.float32)
    gate_sigmoid = jax.nn.sigmoid(gate_pre)
    hidden_act = (gate_pre * gate_sigmoid * up_pre).astype(jnp.bfloat16)
    expert_out = jnp.einsum(
        "sjcf,jfd->sjcd", hidden_act, w_down, preferred_element_type=jnp.float32
    ).astype(jnp.bfloat16)
    returned = lax.all_to_all(
        expert_out.reshape(owners, local_experts * CAP, model_width),
        EX,
        split_axis=0,
        concat_axis=0,
        tiled=True,
    )
    padded_out = jnp.concatenate(
        [returned.reshape(slot_total, model_width), jnp.zeros((1, model_width), jnp.bfloat16)],
        axis=0,
    )
    route_out = padded_out[slot_of_route].astype(jnp.float32).reshape(tok_rows, 2, model_width)
    moe_sum = (
        jnp.sum(ffn_gate[:, :, None] * route_out, axis=1)
        + copy_gate[:, None] * moe_in
        + jnp.sum(const_gate[:, :, None] * const_rows, axis=1)
    )
    layer_out = (resid_one + moe_sum).astype(jnp.bfloat16)
    upstream = out_grad.astype(jnp.float32)
    route_dot = jnp.sum(upstream[:, None, :] * route_out, axis=2)
    copy_dot = jnp.sum(upstream * moe_in, axis=1)
    const_dot = jnp.sum(upstream[:, None, :] * const_rows, axis=2)
    gate_back_r = (
        ffn_mask * route_dot
        + copy_mask * copy_dot[:, None]
        + jnp.sum(const_mask * const_dot[:, None, :], axis=2)
    )
    chosen_grad = gate_probs * (
        gate_back_r - jnp.sum(gate_probs * gate_back_r, axis=1, keepdims=True)
    )
    logit_grad = jnp.einsum("rk,rkn->rn", chosen_grad, route_hot, precision=lax.Precision.HIGHEST)
    const_up = const_gate[:, :, None] * upstream[:, None, :]
    alpha_grad = jnp.stack(
        [
            jnp.sum(const_up * moe_in[:, None, :], axis=2),
            jnp.sum(const_up * const_vec[None], axis=2),
        ],
        axis=2,
    )
    mix_back = (
        mix_alpha * (alpha_grad - jnp.sum(mix_alpha * alpha_grad, axis=2, keepdims=True))
    ).reshape(tok_rows, 4)
    vec_grad = jnp.sum(mix_alpha[:, :, 1:2] * const_up, axis=0)
    route_weight = ffn_gate.reshape(-1)
    grad_send = (route_weight[route_of_slot][:, None] * upstream[route_of_slot // 2]).astype(
        jnp.bfloat16
    )
    grad_send = jnp.where(slot_used[:, None], grad_send, jnp.zeros((), jnp.bfloat16))
    grad_recv = lax.all_to_all(
        grad_send.reshape(owners, local_experts * CAP, model_width),
        EX,
        split_axis=0,
        concat_axis=0,
        tiled=True,
    )
    grad_recv = grad_recv.reshape(owners, local_experts, CAP, model_width)
    hidden_grad = jnp.einsum(
        "sjcd,jfd->sjcf", grad_recv, w_down, preferred_element_type=jnp.float32
    )
    down_term = jnp.einsum(
        "sjcf,sjcd->jfd", hidden_act, grad_recv, preferred_element_type=jnp.float32
    )
    gate_back = (
        hidden_grad * up_pre * gate_sigmoid * (1.0 + gate_pre * (1.0 - gate_sigmoid))
    ).astype(jnp.bfloat16)
    up_back = (hidden_grad * gate_pre * gate_sigmoid).astype(jnp.bfloat16)
    gate_term = jnp.einsum(
        "sjcd,sjcf->jdf", expert_in, gate_back, preferred_element_type=jnp.float32
    )
    up_term = jnp.einsum("sjcd,sjcf->jdf", expert_in, up_back, preferred_element_type=jnp.float32)
    input_back = (
        jnp.einsum("sjcf,jdf->sjcd", gate_back, w_gate, preferred_element_type=jnp.float32)
        + jnp.einsum("sjcf,jdf->sjcd", up_back, w_up, preferred_element_type=jnp.float32)
    ).astype(jnp.bfloat16)
    input_ret = lax.all_to_all(
        input_back.reshape(owners, local_experts * CAP, model_width),
        EX,
        split_axis=0,
        concat_axis=0,
        tiled=True,
    )
    padded_in = jnp.concatenate(
        [input_ret.reshape(slot_total, model_width), jnp.zeros((1, model_width), jnp.bfloat16)],
        axis=0,
    )
    ffn_in_grad = jnp.sum(
        padded_in[slot_of_route].astype(jnp.float32).reshape(tok_rows, 2, model_width), axis=1
    )
    moe_in_grad = (
        ffn_in_grad
        + copy_gate[:, None] * upstream
        + jnp.sum(mix_alpha[:, :, 0:1] * const_up, axis=1)
        + dense32(mix_back, const_mix.T)
        + dense32(logit_grad, w_router.T)
    )
    moe_gain_grad = jnp.sum(moe_in_grad * normed_two, axis=0)
    router_grad = dense32(moe_in.T, logit_grad)
    mix_grad = dense32(moe_in.T, mix_back)
    resid_grad = upstream + rms_back(resid_one, inv_two, moe_gain, moe_in_grad)
    branch_low = resid_grad.astype(jnp.bfloat16)
    out_proj_term = jnp.dot(attn_low.T, branch_low, preferred_element_type=jnp.float32)
    attn_back = jnp.dot(branch_low, wo_full.T, preferred_element_type=jnp.float32).astype(
        jnp.bfloat16
    )
    back_heads = attn_back.reshape(tok_rows, HEADS, HEAD_DIM)
    row_delta = jnp.sum(back_heads.astype(jnp.float32) * attn_sum, axis=2).T

    def back_step(query_acc, block_index):
        key_mask = block_mask(block_index)
        keys_blk = fetch_block(keys_all, block_index)
        values_blk = fetch_block(values_all, block_index)

        def back_live_block(running):
            prob_low, score_low = grad_pieces(
                query_heads,
                back_heads,
                keys_blk,
                values_blk,
                log_norm,
                row_delta,
                key_mask,
                score_scale,
            )
            value_part = jnp.einsum(
                "hqk,qhd->khd", prob_low, back_heads, preferred_element_type=jnp.float32
            )
            key_part = (
                jnp.einsum(
                    "hqk,qhd->khd", score_low, query_heads, preferred_element_type=jnp.float32
                )
                * score_scale
            )
            running = (
                running
                + jnp.einsum(
                    "hqk,khd->qhd", score_low, keys_blk, preferred_element_type=jnp.float32
                )
                * score_scale
            )
            return (
                running,
                (
                    key_part.reshape(key_block, model_width),
                    value_part.reshape(key_block, model_width),
                ),
            )

        def dead_block(running):
            empty_rows = jnp.zeros((key_block, model_width), jnp.float32)
            return (running, (empty_rows, empty_rows))

        return lax.cond(jnp.any(key_mask), back_live_block, dead_block, query_acc)

    query_grad32, key_terms = lax.scan(back_step, zero_heads, jnp.arange(num_blocks))
    key_grad32, value_grad32 = (
        lax.psum_scatter(
            key_terms[0].reshape(group_len, model_width).astype(jnp.bfloat16),
            (EX, SH),
            scatter_dimension=0,
            tiled=True,
        ).astype(jnp.float32),
        lax.psum_scatter(
            key_terms[1].reshape(group_len, model_width).astype(jnp.bfloat16),
            (EX, SH),
            scatter_dimension=0,
            tiled=True,
        ).astype(jnp.float32),
    )
    query_low = query_grad32.reshape(tok_rows, model_width).astype(jnp.bfloat16)
    key_low = key_grad32.astype(jnp.bfloat16)
    value_low = value_grad32.astype(jnp.bfloat16)
    query_term = jnp.dot(attn_in.T, query_low, preferred_element_type=jnp.float32)
    key_term = jnp.dot(attn_in.T, key_low, preferred_element_type=jnp.float32)
    value_term = jnp.dot(attn_in.T, value_low, preferred_element_type=jnp.float32)
    attn_in_grad = (
        jnp.dot(query_low, wq_full.T, preferred_element_type=jnp.float32)
        + jnp.dot(key_low, wk_full.T, preferred_element_type=jnp.float32)
        + jnp.dot(value_low, wv_full.T, preferred_element_type=jnp.float32)
    )
    attn_gain_grad = jnp.sum(attn_in_grad * normed_one, axis=0)
    input_grad = resid_grad + rms_back(inputs, inv_one, attn_gain, attn_in_grad)
    query_part, key_part_w, value_part_w, out_part = (
        lax.psum_scatter(
            query_term.astype(jnp.bfloat16), (EX, SH), scatter_dimension=0, tiled=True
        ).astype(jnp.float32),
        lax.psum_scatter(
            key_term.astype(jnp.bfloat16), (EX, SH), scatter_dimension=0, tiled=True
        ).astype(jnp.float32),
        lax.psum_scatter(
            value_term.astype(jnp.bfloat16), (EX, SH), scatter_dimension=0, tiled=True
        ).astype(jnp.float32),
        lax.psum_scatter(
            out_proj_term.astype(jnp.bfloat16), (EX, SH), scatter_dimension=0, tiled=True
        ).astype(jnp.float32),
    )
    gate_part, up_part, down_part = (
        lax.psum_scatter(
            gate_term.astype(jnp.bfloat16), SH, scatter_dimension=1, tiled=True
        ).astype(jnp.float32),
        lax.psum_scatter(
            up_term.astype(jnp.bfloat16), SH, scatter_dimension=1, tiled=True
        ).astype(jnp.float32),
        lax.psum_scatter(
            down_term.astype(jnp.bfloat16), SH, scatter_dimension=1, tiled=True
        ).astype(jnp.float32),
    )
    summed = (
        lax.psum(query_part.astype(jnp.bfloat16), GR).astype(jnp.float32),
        lax.psum(key_part_w.astype(jnp.bfloat16), GR).astype(jnp.float32),
        lax.psum(value_part_w.astype(jnp.bfloat16), GR).astype(jnp.float32),
        lax.psum(out_part.astype(jnp.bfloat16), GR).astype(jnp.float32),
        lax.psum(gate_part.astype(jnp.bfloat16), GR).astype(jnp.float32),
        lax.psum(up_part.astype(jnp.bfloat16), GR).astype(jnp.float32),
        lax.psum(down_part.astype(jnp.bfloat16), GR).astype(jnp.float32),
    )
    small_sums = lax.psum(
        (attn_gain_grad, moe_gain_grad, router_grad, mix_grad, vec_grad),
        (GR, EX, SH),
    )
    return (
        layer_out,
        input_grad,
        small_sums[0],
        summed[0],
        summed[1],
        summed[2],
        summed[3],
        small_sums[1],
        small_sums[2],
        small_sums[3],
        small_sums[4],
        summed[4],
        summed[5],
        summed[6],
    )


def greet(peers):
    barrier = pltpu.get_barrier_semaphore()
    for axis, peer in peers:
        pl.semaphore_signal(
            barrier, inc=1, device_id={axis: peer}, device_id_type=pl.DeviceIdType.MESH
        )
    pl.semaphore_wait(barrier, len(peers))


def send(src, dst, sems, index, axis, peer):
    copy = pltpu.make_async_remote_copy(
        src_ref=src,
        dst_ref=dst,
        send_sem=sems.at[0, index],
        recv_sem=sems.at[1, index],
        device_id={axis: peer},
        device_id_type=pl.DeviceIdType.MESH,
    )
    copy.start()
    return copy


def shard_peers():
    me = lax.axis_index(SH)
    side, core = me // 2, lax.rem(me, 2)
    return me, side, core, 2 * side + 1 - core, 2 * (1 - side) + core


class Part:
    def __init__(self, axes, ins, outs, scratch, copies, phases, specs=None):
        self.axes, self.ins, self.outs, self.scratch = axes, ins, outs, scratch
        self.copies, self.phases = copies, phases
        self.specs = specs or [VM] * len(ins)


def run_parts(parts, collective_id, name=None, cost=None):
    ins = sum([p.ins for p in parts], [])
    outs = sum([p.outs for p in parts], [])
    scratch = sum([p.scratch for p in parts], [])
    copies = sum(p.copies for p in parts)
    axes = sorted(set(sum([list(p.axes) for p in parts], [])))

    def body(*refs):
        sems = refs[-1]
        in_refs, out_refs = list(refs[: len(ins)]), list(refs[len(ins) : len(ins) + len(outs)])
        scr = list(refs[len(ins) + len(outs) : -1])
        peers = []
        for axis in axes:
            me, n = lax.axis_index(axis), lax.axis_size(axis)
            peers += [(axis, lax.rem(me + d, n)) for d in range(1, n)]
        greet(peers)
        base, running = 0, []
        for p in parts:
            take = lambda pool, k: [pool.pop(0) for _ in range(k)]
            refs_p = (take(in_refs, len(p.ins)), take(out_refs, len(p.outs)), take(scr, len(p.scratch)))
            counter = [base]

            def go(src, dst, axis, peer, counter=counter):
                counter[0] += 1
                return send(src, dst, sems, counter[0] - 1, axis, peer)

            running.append(p.phases(*refs_p, go))
            base += p.copies
        while running:
            running = [r for r in running if next(r, True) is None]

    return pl.pallas_call(
        body,
        out_shape=outs,
        in_specs=sum([p.specs for p in parts], []),
        out_specs=[VM] * len(outs),
        scratch_shapes=scratch + [pltpu.SemaphoreType.DMA((2, copies))],
        compiler_params=pltpu.CompilerParams(collective_id=collective_id, has_side_effects=True),
        cost_estimate=cost,
        name=name,
    )(*ins)


def start_swap(go, src, land, axis, gather):
    me, n = lax.axis_index(axis), lax.axis_size(axis)
    started = []
    for d in range(1, n):
        peer = lax.rem(me + d, n)
        started.append(go(src if gather else src.at[peer], land.at[me], axis, peer))
    land[me] = src[...] if gather else src[me]
    return started


def total_of(land, n):
    total = land[0].astype(f32)
    for j in range(1, n):
        total = total + land[j].astype(f32)
    return total


def exchange(axis, kind, x):
    n = lax.axis_size(axis)
    gather, summed = kind in (GATHER, GATHER_SUM), kind in (GATHER_SUM, SWAP_SUM)
    piece = x.shape if gather else x.shape[1:]
    shape = jax.ShapeDtypeStruct
    outs = [shape(piece, f32) if summed else shape((n,) + piece, x.dtype)]
    scratch = [pltpu.VMEM((n,) + piece, x.dtype)] if summed else []

    def phases(ins, outs, scr, go):
        land = scr[0] if summed else outs[0]
        started = start_swap(go, ins[0], land, axis, gather)
        yield
        for copy in started:
            copy.wait()
        if summed:
            outs[0][...] = total_of(land, n)

    return Part([axis], [x], outs, scratch, n - 1, phases)


def tree_gather(x):
    lines = x.shape[0]
    cuts = [(0, lines // 2), (lines // 2, lines)] if lines > 1 else [(0, 1)]
    cuts = [pl.ds(lo, hi - lo) for lo, hi in cuts]

    def phases(ins, outs, scr, go):
        x_ref, out_ref = ins[0], outs[0]
        me, _, _, near, far = shard_peers()
        across = [go(x_ref.at[c], out_ref.at[c, me], SH, far) for c in cuts]
        own = go(x_ref, out_ref.at[:, me], SH, near)
        out_ref[:, me] = x_ref[...]
        yield
        handed = []
        for c, copy in zip(cuts, across):
            copy.wait_recv()
            handed.append(go(out_ref.at[c, far], out_ref.at[c, far], SH, near))
        yield
        for copy in across:
            copy.wait_send()
        own.wait()
        for copy in handed:
            copy.wait()

    shape = (lines, 4) + x.shape[1:]
    return Part([SH], [x], [jax.ShapeDtypeStruct(shape, x.dtype)], [], 2 * len(cuts) + 1, phases)


def core_sum(x):
    piece = x.shape[1:]
    shape = jax.ShapeDtypeStruct

    def phases(ins, outs, scr, go):
        x_ref, (here, there), (land, kept, sems) = ins[0], outs, scr
        near = shard_peers()[3]
        sent = [go(x_ref.at[3], land.at[1], SH, near), go(x_ref.at[2], land.at[0], SH, near)]
        local = [pltpu.make_async_copy(x_ref.at[k], kept.at[k], sems.at[k]) for k in range(2)]
        for copy in local:
            copy.start()
        yield
        for k, out in ((1, there), (0, here)):
            sent[1 - k].wait()
            local[k].wait()
            out[...] = (kept[k].astype(f32) + land[k].astype(f32)).astype(bf16)

    return Part(
        [SH],
        [x],
        [shape(piece, bf16)] * 2,
        [pltpu.VMEM((2,) + piece, bf16)] * 2 + [pltpu.SemaphoreType.DMA((2,))],
        2,
        phases,
        [pl.BlockSpec(memory_space=pl.ANY)],
    )


class Tree:
    copies = 3

    @staticmethod
    def scratch(piece):
        return [pltpu.VMEM((2,) + piece, bf16)] + [pltpu.VMEM(piece, bf16)] * 2

    def __init__(self, x, scr, go):
        self.x, (self.land, self.mine, self.got), self.go = x, scr, go
        self.me, self.side, self.core, self.near, self.far = shard_peers()
        other = 2 * (1 - self.side) + 1 - self.core
        self.first = [
            go(x.at[other], self.land.at[0], SH, self.near),
            go(x.at[self.near], self.land.at[1], SH, self.near),
        ]

    def across(self):
        self.first[0].wait_recv()
        self.mine[...] = (self.x[self.far].astype(f32) + self.land[0].astype(f32)).astype(bf16)
        self.second = self.go(self.mine, self.got, SH, self.far)

    def result(self):
        self.first[1].wait_recv()
        total = self.x[self.me].astype(f32) + self.land[1].astype(f32)
        self.second.wait_recv()
        return total + self.got[...].astype(f32)

    def close(self):
        for copy in (*self.first, self.second):
            copy.wait_send()


def column(x, k):
    return x[:, k : k + 1]


def core_share(go, own, far, out):
    me, _, _, near, other = shard_peers()
    sent = [go(own, out.at[:, me], SH, near), go(far, out.at[:, other], SH, near)]
    out[:, me] = own[...]
    out[:, other] = far[...]
    return sent


def route(heads, hidden, gain, small_w, routes, out_grad, wo, wo_far, w3, w3_far, n_ids):
    lines, rows, width = heads.shape
    model = lines * width
    slots = lines * CAP
    shape = jax.ShapeDtypeStruct

    def phases(ins, outs, scr, go):
        heads_ref, hid_ref, gain_ref, small_ref, routes_ref, up_ref, wo_ref, wof_ref, w3_ref, w3f_ref = ins
        rows_out, grads_out, w3_all, wo_all, resid_ref, table_ref, place_ref, low_ref = outs
        land, rows_s, grads_s = scr
        swaps = start_swap(go, heads_ref, land, EX, False)
        swaps += core_share(go, wo_ref, wof_ref, wo_all)
        shares = core_share(go, w3_ref, w3f_ref, w3_all)
        ids = routes_ref[...]
        lane = lax.broadcasted_iota(jnp.int32, (rows, 128), 1)
        hot = [lane == column(ids, k) for k in range(2)]
        before = (
            lax.broadcasted_iota(jnp.int32, (rows, rows), 0)
            > lax.broadcasted_iota(jnp.int32, (rows, rows), 1)
        ).astype(bf16)
        named = jnp.where(hot[0] | hot[1], 1.0, 0.0).astype(bf16)
        earlier = jnp.dot(before, named, preferred_element_type=f32)
        slot_at = lax.broadcasted_iota(jnp.int32, (rows, slots), 1).astype(f32)
        place = []
        for k in range(2):
            number = jnp.sum(jnp.where(hot[k], earlier, 0.0), axis=1, keepdims=True)
            wanted = column(ids, k).astype(f32) * CAP + number
            wanted = jnp.where(column(ids, k) < lines, wanted, -1.0)
            place.append(jnp.where(slot_at == wanted, 1.0, 0.0))
            place_ref[k] = place[k].astype(bf16)
        either = (place[0] + place[1]).astype(bf16)
        up_rows = contract(either, up_ref[...], 0, 0)
        for copy in swaps:
            copy.wait()
        for line in range(lines):
            low_ref[:, line * width : (line + 1) * width] = land[line]
        w_out = wo_all[...].reshape(model, model)
        resid = hid_ref[...].astype(f32) + jnp.dot(
            low_ref[...], w_out, preferred_element_type=f32
        )
        resid_ref[...] = resid
        inv = lax.rsqrt(jnp.mean(resid * resid, axis=1, keepdims=True) + norm_eps)
        moe_in = resid * inv * gain_ref[...]
        rows_s[...] = contract(either, moe_in.astype(bf16), 0, 0).astype(bf16).reshape(
            lines, CAP, model
        )
        row_swap = start_swap(go, rows_s, rows_out, EX, False)
        small = jnp.dot(moe_in, small_ref[...], preferred_element_type=f32, precision=HIGH)
        chosen = [jnp.sum(jnp.where(h, small, 0.0), axis=1, keepdims=True) for h in hot]
        top = jnp.maximum(chosen[0], chosen[1])
        powers = [jnp.exp(c - top) for c in chosen]
        gates = [p / (powers[0] + powers[1]) for p in powers]
        weight = place[0] * gates[0] + place[1] * gates[1]
        weight = contract(weight, jnp.ones((rows, 128), f32), 0, 0, HIGH)[:, 0:1]
        grads_s[...] = (up_rows * weight).astype(bf16).reshape(lines, CAP, model)
        grad_swap = start_swap(go, grads_s, grads_out, EX, False)
        table = jnp.zeros((rows, 128), f32)
        entries = list(gates)
        for j in range(2):
            pair = [column(small, n_ids + 2 * j + k) for k in range(2)]
            top = jnp.maximum(pair[0], pair[1])
            powers = [jnp.exp(c - top) for c in pair]
            entries += [p / (powers[0] + powers[1]) for p in powers]
        entries += [column(ids, k).astype(f32) for k in range(2)]
        for k, entry in enumerate(entries):
            table = jnp.where(lane == k, entry, table)
        table_ref[...] = table
        for copy in row_swap + grad_swap + shares:
            copy.wait()
        yield

    ins = [heads, hidden, gain, small_w, routes, out_grad, wo, wo_far, w3, w3_far]
    outs = [
        shape((lines, CAP, model), bf16),
        shape((lines, CAP, model), bf16),
        shape((3, 4, model // 4, model), bf16),
        shape((1, 4, model // 4, model), bf16),
        shape((rows, model), f32),
        shape((rows, 128), f32),
        shape((2, rows, slots), bf16),
        shape((rows, model), bf16),
    ]
    scratch = [pltpu.VMEM((lines, rows, width), bf16)] + [pltpu.VMEM((lines, CAP, model), bf16)] * 2
    return Part([EX, SH], ins, outs, scratch, 3 * (lines - 1) + 4, phases)


def to_heads(returned, input_ret, place, table, resid, low, out_grad, gain, small_t, const_vec, wo, n_ids):
    rows, model = resid.shape
    lines = returned.shape[0]
    width = model // lines
    own = rows // lines
    slots = lines * CAP
    shape = jax.ShapeDtypeStruct

    def phases(ins, outs, scr, go):
        ret_ref, iret_ref, place_ref, table_ref, resid_ref, low_ref, up_ref, gain_ref, st_ref, vec_ref, wo_ref = ins
        heads_out, layer_ref, rgrad_ref, term_ref, packed_ref = outs
        (back_s,) = scr
        table = table_ref[...]
        gates = [column(table, k) for k in range(2)]
        alpha = [[column(table, 2 + 2 * j + k) for k in range(2)] for j in range(2)]
        ids = [column(table, 6 + k) for k in range(2)]
        vecs = [vec_ref[j : j + 1, :] for j in range(2)]
        resid = resid_ref[...]
        upstream = up_ref[...].astype(f32)
        inv = lax.rsqrt(jnp.mean(resid * resid, axis=1, keepdims=True) + norm_eps)
        normed = resid * inv
        moe_in = normed * gain_ref[...]
        returned = ret_ref[...].reshape(slots, model)
        total = lambda x: jnp.sum(x, axis=1, keepdims=True)
        flag = lambda x: jnp.where(x, 1.0, 0.0)
        copy_dot = total(upstream * moe_in)
        vec_dot = [total(upstream * v) for v in vecs]
        const_dot = [alpha[j][0] * copy_dot + alpha[j][1] * vec_dot[j] for j in range(2)]
        output = resid
        backs = []
        copy_gate = jnp.zeros((rows, 1), f32)
        const_gate = [jnp.zeros((rows, 1), f32) for _ in range(2)]
        for k in range(2):
            rows_k = jnp.dot(place_ref[k], returned, preferred_element_type=f32)
            is_ffn, is_copy = flag(ids[k] < lines), flag(ids[k] == lines + 1)
            is_const = [flag(ids[k] == lines + 2 + j) for j in range(2)]
            output = output + (gates[k] * is_ffn) * rows_k
            backs.append(
                is_ffn * total(upstream * rows_k)
                + is_copy * copy_dot
                + is_const[0] * const_dot[0]
                + is_const[1] * const_dot[1]
            )
            copy_gate = copy_gate + gates[k] * is_copy
            const_gate = [const_gate[j] + gates[k] * is_const[j] for j in range(2)]
        through = copy_gate + const_gate[0] * alpha[0][0] + const_gate[1] * alpha[1][0]
        output = output + through * moe_in
        for j in range(2):
            output = output + (const_gate[j] * alpha[j][1]) * vecs[j]
        layer_ref[...] = output.astype(bf16)
        mean_back = gates[0] * backs[0] + gates[1] * backs[1]
        lane = lax.broadcasted_iota(jnp.int32, (rows, 128), 1)
        lane_f = lane.astype(f32)
        small = jnp.zeros((rows, 128), f32)
        for k in range(2):
            small = jnp.where(lane_f == ids[k], gates[k] * (backs[k] - mean_back), small)
        for j in range(2):
            grads = [const_gate[j] * copy_dot, const_gate[j] * vec_dot[j]]
            mean = alpha[j][0] * grads[0] + alpha[j][1] * grads[1]
            for k in range(2):
                small = jnp.where(
                    lane == n_ids + 2 * j + k, alpha[j][k] * (grads[k] - mean), small
                )
            small = jnp.where(lane == n_ids + 4 + j, alpha[j][1] * const_gate[j], small)
        either = place_ref[0] + place_ref[1]
        moe_grad = (
            jnp.dot(either, iret_ref[...].reshape(slots, model), preferred_element_type=f32)
            + through * upstream
            + jnp.dot(small, st_ref[...], preferred_element_type=f32, precision=HIGH)
        )
        resid_grad = upstream + rms_back(resid, inv, gain_ref[...], moe_grad)
        branch = resid_grad.astype(bf16)
        back = contract(branch, wo_ref[...], 1, 1).astype(bf16)
        for line in range(lines):
            back_s[line] = back[:, line * width : (line + 1) * width]
        swaps = start_swap(go, back_s, heads_out, EX, False)
        rgrad_ref[...] = resid_grad
        packed_ref[...] = jnp.zeros_like(packed_ref)
        packed_ref[0:1] = jnp.sum(moe_grad * normed, axis=0, keepdims=True)
        small_grad = contract(small, moe_in, 0, 0, HIGH)
        vec_grad = contract(small, upstream, 0, 0, HIGH)
        packed_ref[1:3] = vec_grad[n_ids + 4 : n_ids + 6]
        packed_ref[3 : 7 + n_ids] = small_grad[: n_ids + 4]
        term = contract(low_ref[...], branch, 0, 0).astype(bf16)
        for line in range(lines):
            for piece in range(4):
                at = (line * 4 + piece) * own
                term_ref[piece, line] = term[at : at + own]
        for copy in swaps:
            copy.wait()
        yield

    ins = [returned, input_ret, place, table, resid, low, out_grad, gain, small_t, const_vec, wo]
    outs = [
        shape((lines, rows, width), bf16),
        shape((rows, model), bf16),
        shape((rows, model), f32),
        shape((4, lines, own, model), bf16),
        shape((-(-(7 + n_ids) // 8) * 8, model), f32),
    ]
    return Part([EX], ins, outs, [pltpu.VMEM((lines, rows, width), bf16)], lines - 1, phases)


def tail(dkv, dq, attn_in, weights, out_term, packed, hidden, resid_grad, gain, n_ids):
    lines, rows, width = dq.shape
    model = lines * width
    own = rows // lines
    groups = lax.axis_size(GR)
    shape = jax.ShapeDtypeStruct
    vmem = pltpu.VMEM
    tok = lines * rows
    dkv_piece, q_piece = (lines, rows, 2 * width), (lines, own, width)
    kv_piece, o_piece = (lines, own, 2 * width), (lines, own, model)
    part_dims = (width, 2 * width, model)

    def phases(ins, outs, scr, go):
        dkv_ref, dq_ref, attn_ref, w_ref, o_ref, packed_ref, hid_ref, resid_ref, gain_ref = ins
        input_ref, q_out, k_out, v_out, out_out, gain_out, mgain_out, vec_out, rout_out, mix_out = outs
        scr = list(scr)
        take = lambda k: [scr.pop(0) for _ in range(k)]
        kv_scr, q_scr, kvw_scr, o_scr = take(3), take(3), take(3), take(3)
        own_kv, q_t, kv_t, dq_all, dkv_all, dq_full = take(6)
        sums, lands, halves, gots = take(3), take(3), take(3), take(3)
        pk_l, pk_s, pk_g = take(3)
        mid_l, mid_s = take(2)
        gn_l, gn_s, gn_g, gn_0, gn_1, gn_2 = take(6)
        me = lax.axis_index(SH)

        kv_tree = Tree(dkv_ref, kv_scr, go)
        dq_swap = start_swap(go, dq_ref, dq_all, EX, False)
        o_tree = Tree(o_ref, o_scr, go)
        pk1 = start_swap(go, packed_ref, pk_l, EX, True)

        def term(rows_ref, out):
            value = contract(attn_ref[...], rows_ref[...].reshape(tok, rows_ref.shape[-1]), 0, 0)
            value = value.astype(bf16)
            for line in range(lines):
                for piece in range(4):
                    at = (line * 4 + piece) * own
                    out[piece, line] = value[at : at + own]

        kv_tree.across()
        term(dq_ref, q_t)
        o_tree.across()
        q_tree = Tree(q_t, q_scr, go)
        trees = [q_tree, None, o_tree]

        def lines_out(k):
            sums[k][...] = trees[k].result().astype(bf16)
            return start_swap(go, sums[k], lands[k], EX, False)

        own_kv[...] = kv_tree.result().astype(bf16)
        dkv_swap = start_swap(go, own_kv, dkv_all, EX, False)
        o_lines = lines_out(2)
        q_tree.across()
        term(own_kv, kv_t)
        kvw_tree = Tree(kv_t, kvw_scr, go)
        trees[1] = kvw_tree
        for copy in pk1:
            copy.wait()
        mid_l[...] = total_of(pk_l, lines)
        pk2 = start_swap(go, mid_l, pk_s, SH, True)
        kvw_tree.across()
        q_lines = lines_out(0)
        for copy in dq_swap:
            copy.wait()
        for line in range(lines):
            dq_full[:, line * width : (line + 1) * width] = dq_all[line]
        grad = contract(dq_full[...], w_ref[0], 1, 1)
        for copy in pk2:
            copy.wait()
        mid_s[...] = total_of(pk_s, 4)
        pk3 = start_swap(go, mid_s, pk_g, GR, True)
        kv_lines = lines_out(1)
        for copy in dkv_swap:
            copy.wait()
        for half in range(2):
            for line in range(lines):
                dq_full[:, line * width : (line + 1) * width] = dkv_all[
                    line, :, half * width : (half + 1) * width
                ]
            grad = grad + contract(dq_full[...], w_ref[1 + half], 1, 1)
        inputs = hid_ref[...].astype(f32)
        inv = lax.rsqrt(jnp.mean(inputs * inputs, axis=1, keepdims=True) + norm_eps)
        normed = inputs * inv
        gn_0[...] = jnp.sum((grad * normed).reshape(rows // 8, 8, model), axis=0)
        gn1 = start_swap(go, gn_0, gn_l, EX, True)
        input_ref[...] = resid_ref[...] + rms_back(inputs, inv, gain_ref[...], grad)
        swaps = [None] * 3
        for k, copies in ((2, o_lines), (0, q_lines)):
            for copy in copies:
                copy.wait()
            if k == 2:
                halves[k][...] = total_of(lands[k], lines).astype(bf16)
            else:
                halves[k][...] = lands[k][...]
            swaps[k] = start_swap(go, halves[k], gots[k], GR, True)
        for copy in gn1:
            copy.wait()
        gn_1[...] = total_of(gn_l, lines)
        gn2 = start_swap(go, gn_1, gn_s, SH, True)
        for copy in kv_lines:
            copy.wait()
        halves[1][...] = lands[1][...]
        swaps[1] = start_swap(go, halves[1], gots[1], GR, True)
        for copy in gn2:
            copy.wait()
        gn_2[...] = total_of(gn_s, 4)
        gn3 = start_swap(go, gn_2, gn_g, GR, True)
        for copy in pk3:
            copy.wait()
        small = total_of(pk_g, groups)
        mgain_out[...] = small[0:1]
        vec_out[...] = small[1:3]
        turned = jnp.transpose(small)
        rout_out[...] = turned[:, 3 : 3 + n_ids]
        mix_out[...] = turned[:, 3 + n_ids : 7 + n_ids]
        for k in (2, 0, 1):
            for copy in swaps[k]:
                copy.wait()
            value = total_of(gots[k], groups)
            if k == 2:
                out_out[...] = value
            elif k == 0:
                for line in range(lines):
                    q_out[:, line * width : (line + 1) * width] = value[line]
            else:
                for half, out in ((0, k_out), (1, v_out)):
                    for line in range(lines):
                        out[:, line * width : (line + 1) * width] = value[
                            line, :, half * width : (half + 1) * width
                        ]
        for copy in gn3:
            copy.wait()
        gain_out[...] = jnp.sum(total_of(gn_g, groups), axis=0, keepdims=True)
        for tree in (kv_tree, o_tree, q_tree, kvw_tree):
            tree.close()
        yield

    pieces = [(lines, own, d) for d in part_dims]
    got_pieces = pieces[:2] + [(own, model)]
    scratch = Tree.scratch(dkv_piece) + Tree.scratch(q_piece) + Tree.scratch(kv_piece)
    scratch += Tree.scratch(o_piece)
    scratch += [
        vmem(dkv_piece, bf16),
        vmem((4,) + q_piece, bf16),
        vmem((4,) + kv_piece, bf16),
        vmem((lines, rows, width), bf16),
        vmem((lines, rows, 2 * width), bf16),
        vmem((rows, model), bf16),
    ]
    scratch += [vmem(p, bf16) for p in pieces] + [vmem(p, bf16) for p in pieces]
    scratch += [vmem(p, bf16) for p in got_pieces] + [vmem((groups,) + p, bf16) for p in got_pieces]
    scratch += [vmem((n,) + packed.shape, f32) for n in (lines, 4, groups)]
    scratch += [vmem(packed.shape, f32)] * 2
    scratch += [vmem((n, 8, model), f32) for n in (lines, 4, groups)] + [vmem((8, model), f32)] * 3
    copies = 4 * Tree.copies + 7 * (lines - 1) + 2 * 3 + 5 * (groups - 1)
    outs = [
        shape((rows, model), f32),
        shape((own, model), f32),
        shape((own, model), f32),
        shape((own, model), f32),
        shape((own, model), f32),
        shape((1, model), f32),
        shape((1, model), f32),
        shape((2, model), f32),
        shape((model, n_ids), f32),
        shape((model, 4), f32),
    ]
    ins = [dkv, dq, attn_in, weights, out_term, packed, hidden, resid_grad, gain]
    return Part([EX, SH, GR], ins, outs, scratch, copies, phases)


def expert_body(steps, x_ref, g_ref, wg_ref, wu_ref, wd_ref, eo_ref, ib_ref, ga_ref, up_ref, d_ref, eo_s, ib_s):
    i = pl.program_id(0)
    me, side, core, _, _ = shard_peers()

    @pl.when(i == 0)
    def _():
        eo_s[...] = jnp.zeros_like(eo_s)
        ib_s[...] = jnp.zeros_like(ib_s)

    x, g = x_ref[...], g_ref[...]
    wg, wu, wd = wg_ref[...], wu_ref[...], wd_ref[...]
    gate_pre = jnp.dot(x, wg, preferred_element_type=f32)
    up_pre = jnp.dot(x, wu, preferred_element_type=f32)
    hidden_grad = contract(g, wd, 1, 1)
    gate_sigmoid = jax.nn.sigmoid(gate_pre)
    act = (gate_pre * gate_sigmoid * up_pre).astype(bf16)
    gate_back = (
        hidden_grad * up_pre * gate_sigmoid * (1.0 + gate_pre * (1.0 - gate_sigmoid))
    ).astype(bf16)
    up_back = (hidden_grad * gate_pre * gate_sigmoid).astype(bf16)
    eo_s[...] += jnp.dot(act, wd, preferred_element_type=f32)
    ib_s[...] += contract(gate_back, wg, 1, 1) + contract(up_back, wu, 1, 1)

    def place(quarter):
        return 2 * lax.rem(lax.rem(quarter, 2) + core, 2) + lax.rem(quarter // 2 + side, 2)

    rows = ga_ref.shape[1]
    for ref, back in ((ga_ref, gate_back), (up_ref, up_back)):
        term = contract(x, back, 0, 0).astype(bf16)
        for quarter in range(4):
            ref[place(jnp.int32(quarter))] = term[quarter * rows : (quarter + 1) * rows]
    d_ref[place(i)] = contract(act, g, 0, 0).astype(bf16)

    @pl.when(i == steps - 1)
    def _():
        eo_ref[...] = eo_s[...].astype(bf16)
        ib_ref[...] = ib_s[...].astype(bf16)


def expert(x, g, wg, wu, wd):
    slots, model = x.shape
    inner = wg.shape[1]
    steps = 4
    tile = inner // steps
    quarter = model // 4
    shape = jax.ShapeDtypeStruct
    whole = lambda dims: pl.BlockSpec(dims, lambda i: (0,) * len(dims))
    return pl.pallas_call(
        functools.partial(expert_body, steps),
        grid=(steps,),
        out_shape=[
            shape((slots, model), bf16),
            shape((slots, model), bf16),
            shape((4, quarter, inner), bf16),
            shape((4, quarter, inner), bf16),
            shape((4, tile, model), bf16),
        ],
        in_specs=[
            whole((slots, model)),
            whole((slots, model)),
            pl.BlockSpec((model, tile), lambda i: (0, i)),
            pl.BlockSpec((model, tile), lambda i: (0, i)),
            pl.BlockSpec((tile, model), lambda i: (i, 0)),
        ],
        out_specs=[
            whole((slots, model)),
            whole((slots, model)),
            pl.BlockSpec((4, quarter, tile), lambda i: (0, 0, i)),
            pl.BlockSpec((4, quarter, tile), lambda i: (0, 0, i)),
            whole((4, tile, model)),
        ],
        scratch_shapes=[pltpu.VMEM((slots, model), f32)] * 2,
        cost_estimate=pl.CostEstimate(flops=6 * 10**9, bytes_accessed=2 * 10**7, transcendentals=4 * 10**5),
        name="ffn",
    )(x, g, wg, wu, wd)


def head_columns(h, shape, axis):
    return lax.broadcasted_iota(jnp.int32, shape, axis) // HEAD_DIM == h


def allowed(block, key_blk, qpos, qstart, prompt):
    kpos = block * key_blk + lax.broadcasted_iota(jnp.int32, (key_blk, qpos.shape[1]), 0)
    return (kpos <= qpos) & ((kpos >= qstart) | (kpos < prompt))


def attend_body(lines, heads, info_ref, q_ref, kv_ref, qinfo_ref, o_ref, low_ref, lse_ref, k_s, vt_s, acc_s, ml_s, qm_s):
    shard = lax.axis_index(SH)
    rows, width = q_ref.shape[1:]
    blocks = vt_s.shape[0]
    key_blk = vt_s.shape[2]
    prompt = info_ref[0]

    @pl.loop(0, blocks)
    def _(j):
        at = pl.ds(pl.multiple_of(j * key_blk, key_blk), key_blk)
        k_s[at, :] = kv_ref[at, :width]
        vt_s[j] = jnp.transpose(kv_ref[at, width:].astype(f32)).astype(bf16)

    @pl.loop(0, lines)
    def _(line):
        start = (line * 4 + shard) * rows
        queries = q_ref[line].astype(f32) * HEAD_DIM**-0.5
        qpos = start + lax.broadcasted_iota(jnp.int32, (1, rows), 1)
        qstart = qinfo_ref[line, 0:1, :]
        first = info_ref[1 + line]
        for h in range(heads):
            qm_s[h] = jnp.where(head_columns(h, queries.shape, 1), queries, 0.0).astype(bf16)
        acc_s[...] = jnp.zeros_like(acc_s)
        for h in range(heads):
            ml_s[h, 0:1, :] = jnp.full((1, rows), neg_fill, f32)
            ml_s[h, 1:2, :] = jnp.zeros((1, rows), f32)

        @pl.loop(0, (start + rows + key_blk - 1) // key_blk)
        def _(j):
            @pl.when((j * key_blk < prompt) | ((j + 1) * key_blk > first))
            def _():
                keys = k_s[pl.ds(pl.multiple_of(j * key_blk, key_blk), key_blk), :]
                ok = allowed(j, key_blk, qpos, qstart, prompt)
                for h in range(heads):
                    scores = jnp.where(ok, contract(keys, qm_s[h], 1, 1), neg_fill)
                    old = ml_s[h, 0:1, :]
                    new = jnp.maximum(old, jnp.max(scores, axis=0, keepdims=True))
                    probs = jnp.exp(scores - new)
                    scale = jnp.exp(old - new)
                    ml_s[h, 0:1, :] = new
                    ml_s[h, 1:2, :] = ml_s[h, 1:2, :] * scale + jnp.sum(
                        probs, axis=0, keepdims=True
                    )
                    part = slice(h * HEAD_DIM, (h + 1) * HEAD_DIM)
                    acc_s[part, :] = acc_s[part, :] * scale + jnp.dot(
                        vt_s[j, part, :], probs.astype(bf16), preferred_element_type=f32
                    )

        for h in range(heads):
            part = slice(h * HEAD_DIM, (h + 1) * HEAD_DIM)
            total = ml_s[h, 1:2, :]
            acc_s[part, :] = acc_s[part, :] / total
            lse_ref[line, h : h + 1, :] = ml_s[h, 0:1, :] + jnp.log(total)
        result = jnp.transpose(acc_s[...])
        o_ref[line] = result
        low_ref[line] = result.astype(bf16)


def attend(info, q, kv, qinfo):
    lines, rows, width = q.shape
    heads = width // HEAD_DIM
    length = kv.shape[0]
    key_blk = KEY_BLK
    shape = jax.ShapeDtypeStruct
    return pl.pallas_call(
        functools.partial(attend_body, lines, heads),
        out_shape=[
            shape((lines, rows, width), f32),
            shape((lines, rows, width), bf16),
            shape((lines, 8, rows), f32),
        ],
        in_specs=[SM, VM, VM, VM],
        out_specs=[VM] * 3,
        scratch_shapes=[
            pltpu.VMEM((length, width), bf16),
            pltpu.VMEM((length // key_blk, width, key_blk), bf16),
            pltpu.VMEM((width, rows), f32),
            pltpu.VMEM((heads, 8, rows), f32),
            pltpu.VMEM((heads, rows, width), bf16),
        ],
        cost_estimate=pl.CostEstimate(flops=2 * 10**9, bytes_accessed=8 * 10**6, transcendentals=4 * 10**6),
        name="attend",
    )(info, q, kv, qinfo)


def attend_back_body(lines, heads, info_ref, q_ref, kv_ref, qinfo_ref, o_ref, lse_ref, back_ref, dq_ref, dkv_ref, k_s, v_s, dk_s, dv_s, dq_s, qm_s, bm_s, delta_s):
    shard = lax.axis_index(SH)
    rows, width = q_ref.shape[1:]
    key_blk = KEY_BLK
    blocks = k_s.shape[0] // key_blk
    prompt = info_ref[0]

    @pl.loop(0, blocks)
    def _(j):
        at = pl.ds(pl.multiple_of(j * key_blk, key_blk), key_blk)
        k_s[at, :] = kv_ref[at, :width]
        v_s[at, :] = kv_ref[at, width:]
        dk_s[at, :] = jnp.zeros((key_blk, width), f32)
        dv_s[at, :] = jnp.zeros((key_blk, width), f32)

    @pl.loop(0, lines)
    def _(line):
        start = (line * 4 + shard) * rows
        queries = q_ref[line].astype(f32) * HEAD_DIM**-0.5
        back = back_ref[line].astype(f32)
        qpos = start + lax.broadcasted_iota(jnp.int32, (1, rows), 1)
        qstart = qinfo_ref[line, 0:1, :]
        first = info_ref[1 + line]
        picks = (
            lax.broadcasted_iota(jnp.int32, (8, width), 1) // HEAD_DIM
            == lax.broadcasted_iota(jnp.int32, (8, width), 0)
        ).astype(f32)
        delta_s[...] = contract(picks, back * o_ref[line], 1, 1, HIGH)
        for h in range(heads):
            mine = head_columns(h, queries.shape, 1)
            qm_s[h] = jnp.where(mine, queries, 0.0).astype(bf16)
            bm_s[h] = jnp.where(mine, back, 0.0).astype(bf16)
        dq_s[...] = jnp.zeros_like(dq_s)

        @pl.loop(0, (start + rows + key_blk - 1) // key_blk)
        def _(j):
            @pl.when((j * key_blk < prompt) | ((j + 1) * key_blk > first))
            def _():
                at = pl.ds(pl.multiple_of(j * key_blk, key_blk), key_blk)
                keys, values = k_s[at, :], v_s[at, :]
                ok = allowed(j, key_blk, qpos, qstart, prompt)
                dk = jnp.zeros((key_blk, width), f32)
                dv = jnp.zeros((key_blk, width), f32)
                for h in range(heads):
                    scores = contract(keys, qm_s[h], 1, 1)
                    probs = jnp.where(ok, jnp.exp(scores - lse_ref[line, h : h + 1, :]), 0.0)
                    grads = contract(values, bm_s[h], 1, 1)
                    slow = (probs * (grads - delta_s[h : h + 1, :])).astype(bf16)
                    dv = dv + jnp.dot(probs.astype(bf16), bm_s[h], preferred_element_type=f32)
                    dk = dk + jnp.dot(slow, qm_s[h], preferred_element_type=f32)
                    dq_s[h] += contract(slow, keys, 0, 0)
                dk_s[at, :] += dk
                dv_s[at, :] += dv

        total = jnp.zeros(queries.shape, f32)
        for h in range(heads):
            total = jnp.where(head_columns(h, queries.shape, 1), dq_s[h], total)
        dq_ref[line] = (total * HEAD_DIM**-0.5).astype(bf16)

    @pl.loop(0, lines)
    def _(line):
        for piece in range(4):
            at = pl.ds(pl.multiple_of((line * 4 + piece) * rows, rows), rows)
            dkv_ref[piece, line, :, :width] = dk_s[at, :].astype(bf16)
            dkv_ref[piece, line, :, width:] = dv_s[at, :].astype(bf16)


def attend_back(info, q, kv, qinfo, o, lse, back):
    lines, rows, width = q.shape
    heads = width // HEAD_DIM
    length = kv.shape[0]
    shape = jax.ShapeDtypeStruct
    return pl.pallas_call(
        functools.partial(attend_back_body, lines, heads),
        out_shape=[
            shape((lines, rows, width), bf16),
            shape((4, lines, rows, 2 * width), bf16),
        ],
        in_specs=[SM] + [VM] * 6,
        out_specs=[VM] * 2,
        scratch_shapes=[
            pltpu.VMEM((length, width), bf16),
            pltpu.VMEM((length, width), bf16),
            pltpu.VMEM((length, width), f32),
            pltpu.VMEM((length, width), f32),
            pltpu.VMEM((heads, rows, width), f32),
            pltpu.VMEM((heads, rows, width), bf16),
            pltpu.VMEM((heads, rows, width), bf16),
            pltpu.VMEM((8, rows), f32),
        ],
        cost_estimate=pl.CostEstimate(flops=5 * 10**9, bytes_accessed=12 * 10**6, transcendentals=4 * 10**6),
        name="attend_back",
    )(info, q, kv, qinfo, o, lse, back)


def swap(x, axis, partner):
    return lax.ppermute(x, axis, [(i, partner(i)) for i in range(lax.axis_size(axis))])


def over_group(mine):
    n = lax.axis_size(GR)
    if n == 2:
        return mine.astype(f32) + swap(mine, GR, lambda i: 1 - i).astype(f32)
    return jnp.sum(lax.all_gather(mine, GR).astype(f32), axis=0)


def fast_shards(
    hidden_in,
    segment_ids,
    routes,
    attn_gain,
    w_query,
    w_key,
    w_value,
    w_out,
    moe_gain,
    w_router,
    const_mix,
    const_vec,
    w_gate,
    w_up,
    w_down,
    out_grad,
):
    rows, model = hidden_in.shape
    lines = lax.axis_size(EX)
    line, shard = lax.axis_index(EX), lax.axis_index(SH)
    width = model // lines
    seg = segment_ids[0]
    length = seg.shape[0]

    w_qkv = jnp.stack([w_query, w_key, w_value])
    w_mine = lax.dynamic_slice_in_dim(w_qkv, line * width, width, axis=2)
    wo_far = swap(w_out, SH, lambda i: i ^ 2)
    w_far = swap(w_qkv, SH, lambda i: i ^ 2)
    hidden_all, w_cols = run_parts(
        [exchange(EX, GATHER, hidden_in), exchange(SH, GATHER, w_mine)], 0, "gather_in"
    )
    w_heads = w_cols.swapaxes(0, 1).reshape(3, model, width)
    inputs_all = hidden_all.reshape(lines * rows, model).astype(f32)
    inv_all = lax.rsqrt(jnp.mean(inputs_all * inputs_all, axis=1, keepdims=True) + norm_eps)
    attn_in = (inputs_all * inv_all * attn_gain).astype(bf16)
    q = jnp.dot(attn_in, w_heads[0], preferred_element_type=f32).astype(bf16)
    w_kv = jnp.concatenate([w_heads[1], w_heads[2]], axis=1)
    kv = jnp.dot(attn_in, w_kv, preferred_element_type=f32).astype(bf16)
    q = q.reshape(lines, rows, width)
    (kv_all,) = run_parts([tree_gather(kv.reshape(lines, rows, 2 * width))], 1, "gather_kv")
    kv_all = kv_all.reshape(length, 2 * width)

    own_seg = jnp.take(seg.reshape(lines, 4, rows), shard, axis=1)
    qstart = jnp.sum(
        (seg[None, None, :] < own_seg[:, :, None]).astype(jnp.int32), axis=2, dtype=jnp.int32
    )
    prompt = jnp.sum((seg == 0).astype(jnp.int32), dtype=jnp.int32)
    info = jnp.concatenate([prompt[None], qstart[:, 0]])
    qinfo = jnp.broadcast_to(qstart[:, None, :], (lines, 8, rows))
    attn_vec, attn_heads, lse = attend(info, q, kv_all, qinfo)
    n_ids = w_router.shape[1]
    small_w = jnp.pad(
        jnp.concatenate([w_router, const_mix], axis=1), ((0, 0), (0, 124 - n_ids))
    )
    gain_two = moe_gain[None]
    recv_rows, recv_grads, weights, wo_full, resid_one, table, place, attn_low = run_parts(
        [
            route(
                attn_heads, hidden_in, gain_two, small_w, routes, out_grad, w_out[None], wo_far[None], w_qkv, w_far, n_ids
            )
        ],
        2,
        "route",
    )
    weights = weights.reshape(3, model, model)
    wo_full = wo_full.reshape(model, model)
    slots = lines * CAP

    expert_out, input_back, *terms = expert(
        recv_rows.reshape(slots, model), recv_grads.reshape(slots, model), w_gate[0], w_up[0], w_down[0]
    )
    returned, input_ret, *sums = run_parts(
        [
            exchange(EX, SWAP, expert_out.reshape(lines, CAP, model)),
            exchange(EX, SWAP, input_back.reshape(lines, CAP, model)),
        ]
        + [core_sum(term) for term in terms],
        4,
        "combine",
    )
    far = [swap(there, SH, lambda i: i ^ 2) for there in sums[1::2]]
    mine = [(x.astype(f32) + y.astype(f32)).astype(bf16) for x, y in zip(sums[0::2], far)]

    back_heads, layer_out, resid_grad, out_term, packed = run_parts(
        [
            to_heads(
                returned, input_ret, place, table, resid_one, attn_low, out_grad, gain_two, small_w.T, const_vec, wo_full, n_ids
            )
        ],
        5,
        "to_heads",
    )
    back_heads, mine[2] = lax.optimization_barrier((back_heads, mine[2]))
    down_part = over_group(mine[2])
    dq, dkv = attend_back(info, q, kv_all, qinfo, attn_vec, lse, back_heads)
    dkv, *mine[:2] = lax.optimization_barrier((dkv, *mine[:2]))
    gate_part, up_part = over_group(mine[0]), over_group(mine[1])
    input_grad, *grads, gain_sum, moe_gain_sum, vec_sum, router_sum, mix_sum = run_parts(
        [
            tail(
                dkv, dq, attn_in, weights, out_term, packed, hidden_in, resid_grad, attn_gain[None], n_ids
            )
        ],
        6,
        "tail",
        pl.CostEstimate(flops=2 * 10**10, bytes_accessed=10**8, transcendentals=0),
    )
    return (
        layer_out,
        input_grad,
        gain_sum[0],
        *grads,
        moe_gain_sum[0],
        router_sum,
        mix_sum,
        vec_sum,
        gate_part[None],
        up_part[None],
        down_part[None],
    )


def solution(mesh):
    placed = (
        P((GR, EX, SH), None),
        P(GR, None),
        P((GR, EX, SH), None),
        P(),
        P(SH, None),
        P(SH, None),
        P(SH, None),
        P(SH, None),
        P(),
        P(),
        P(),
        P(),
        P(EX, None, None),
        P(EX, None, None),
        P(EX, None, None),
        P((GR, EX, SH), None),
    )
    sizes = dict(mesh.shape)
    lines = sizes[EX]
    fast = sizes[SH] == 4 and lines == 4 and HEADS % lines == 0
    return jax.shard_map(
        fast_shards if fast else shards,
        mesh=mesh,
        in_specs=placed,
        out_specs=(
            P((GR, EX, SH), None),
            P((GR, EX, SH), None),
            P(),
            P((EX, SH), None),
            P((EX, SH), None),
            P((EX, SH), None),
            P((EX, SH), None),
            P(),
            P(),
            P(),
            P(),
            P(EX, SH, None),
            P(EX, SH, None),
            P(EX, SH, None),
        ),
        check_vma=False,
    )
```

```python
import functools

import jax
import jax.numpy as jnp
from jax import lax
from jax.experimental import pallas as pl
from jax.experimental.pallas import tpu as pltpu
from jax.sharding import PartitionSpec as P

HEADS = 12
HEAD_DIM = 64
CAP = 48
DOCS = 9
KEY_BLK = 256
EX, SH, GR = ("expert", "shard", "group")
GATHER, GATHER_SUM, SWAP, SWAP_SUM = range(4)


neg_fill = -1e30
norm_eps = 1e-05
bf16 = jnp.bfloat16
f32 = jnp.float32
VM = pl.BlockSpec(memory_space=pltpu.VMEM)
SM = pl.BlockSpec(memory_space=pltpu.SMEM)
HIGH = lax.Precision.HIGHEST


def contract(a, b, da, db, precision=None):
    return lax.dot_general(
        a, b, (((da,), (db,)), ((), ())), preferred_element_type=f32, precision=precision
    )


def dense32(left_side, right_side):
    return jnp.dot(left_side, right_side, precision=lax.Precision.HIGHEST)


def allowed_mask(query_pos, query_seg, key_pos, key_seg):
    same_doc = (key_seg[None, :] == query_seg[:, None]) | (key_seg[None, :] == 0)
    return same_doc & (key_pos[None, :] <= query_pos[:, None])


def rms_back(inputs, inverse, gain_vec, upstream):
    scaled = upstream * gain_vec
    return inverse * scaled - inputs * inverse**3 * jnp.mean(scaled * inputs, axis=1, keepdims=True)


def block_scores(query_blk, keys_blk, score_scale):
    return (
        jnp.einsum("qhd,khd->hqk", query_blk, keys_blk, preferred_element_type=jnp.float32)
        * score_scale
    )


def grad_pieces(
    query_blk, back_blk, keys_blk, values_blk, norm_blk, delta_blk, key_mask, score_scale
):
    scores = block_scores(query_blk, keys_blk, score_scale)
    prob_rows = jnp.where(key_mask[None], jnp.exp(scores - norm_blk[:, :, None]), 0.0)
    prob_grad = jnp.einsum("qhd,khd->hqk", back_blk, values_blk, preferred_element_type=jnp.float32)
    score_low = (prob_rows * (prob_grad - delta_blk[:, :, None])).astype(jnp.bfloat16)
    return (prob_rows.astype(jnp.bfloat16), score_low)


def shards(
    hidden_in,
    segment_ids,
    routes,
    attn_gain,
    w_query,
    w_key,
    w_value,
    w_out,
    moe_gain,
    w_router,
    const_mix,
    const_vec,
    w_gate,
    w_up,
    w_down,
    out_grad,
):
    tok_rows, model_width = hidden_in.shape
    score_scale = HEAD_DIM ** (-0.5)
    inner_rank = lax.axis_index((EX, SH))
    seg_group = segment_ids[0]
    group_len = seg_group.shape[0]
    key_block = min(512, group_len)
    num_blocks = group_len // key_block
    row_start = inner_rank * tok_rows
    own_pos = row_start + jnp.arange(tok_rows, dtype=jnp.int32)
    own_seg = lax.dynamic_slice_in_dim(seg_group, row_start, tok_rows)
    wq_full, wk_full, wv_full, wo_full = (
        lax.all_gather(w_query, SH, axis=0, tiled=True),
        lax.all_gather(w_key, SH, axis=0, tiled=True),
        lax.all_gather(w_value, SH, axis=0, tiled=True),
        lax.all_gather(w_out, SH, axis=0, tiled=True),
    )
    inputs = hidden_in.astype(jnp.float32)
    inv_one = lax.rsqrt(jnp.mean(inputs * inputs, axis=1, keepdims=True) + norm_eps)
    normed_one = inputs * inv_one
    attn_in = (normed_one * attn_gain).astype(jnp.bfloat16)
    queries = jnp.dot(attn_in, wq_full, preferred_element_type=jnp.float32).astype(jnp.bfloat16)
    keys_own = jnp.dot(attn_in, wk_full, preferred_element_type=jnp.float32).astype(jnp.bfloat16)
    values_own = jnp.dot(attn_in, wv_full, preferred_element_type=jnp.float32).astype(jnp.bfloat16)
    keys_all, values_all = (
        lax.all_gather(keys_own, (EX, SH), axis=0, tiled=True),
        lax.all_gather(values_own, (EX, SH), axis=0, tiled=True),
    )
    query_heads = queries.reshape(tok_rows, HEADS, HEAD_DIM)

    def fetch_block(source, block_index):
        return lax.dynamic_slice_in_dim(source, block_index * key_block, key_block).reshape(
            key_block, HEADS, HEAD_DIM
        )

    def block_mask(block_index):
        key_pos = block_index * key_block + jnp.arange(key_block, dtype=jnp.int32)
        key_seg = lax.dynamic_slice_in_dim(seg_group, block_index * key_block, key_block)
        return allowed_mask(own_pos, own_seg, key_pos, key_seg)

    def stats_step(carry_now, block_index):
        key_mask = block_mask(block_index)

        def stats_live_block(carry_in):
            row_max, row_sum = carry_in
            scores = jnp.where(
                key_mask[None],
                block_scores(query_heads, fetch_block(keys_all, block_index), score_scale),
                neg_fill,
            )
            new_max = jnp.maximum(row_max, jnp.max(scores, axis=2))
            weights = jnp.where(key_mask[None], jnp.exp(scores - new_max[:, :, None]), 0.0)
            return (new_max, row_sum * jnp.exp(row_max - new_max) + jnp.sum(weights, axis=2))

        return (
            lax.cond(jnp.any(key_mask), stats_live_block, lambda carry_in: carry_in, carry_now),
            None,
        )

    start_max = jnp.full((HEADS, tok_rows), neg_fill, jnp.float32)
    row_max, row_sum = lax.scan(
        stats_step, (start_max, jnp.zeros_like(start_max)), jnp.arange(num_blocks)
    )[0]
    log_norm = row_max + jnp.log(row_sum)

    def output_step(running, block_index):
        key_mask = block_mask(block_index)

        def output_live_block(carry_in):
            scores = block_scores(query_heads, fetch_block(keys_all, block_index), score_scale)
            prob_rows = jnp.where(
                key_mask[None], jnp.exp(scores - log_norm[:, :, None]), 0.0
            ).astype(jnp.bfloat16)
            return carry_in + jnp.einsum(
                "hqk,khd->qhd",
                prob_rows,
                fetch_block(values_all, block_index),
                preferred_element_type=jnp.float32,
            )

        return (
            lax.cond(jnp.any(key_mask), output_live_block, lambda carry_in: carry_in, running),
            None,
        )

    zero_heads = jnp.zeros((tok_rows, HEADS, HEAD_DIM), jnp.float32)
    attn_sum = lax.scan(output_step, zero_heads, jnp.arange(num_blocks))[0]
    attn_low = attn_sum.reshape(tok_rows, model_width).astype(jnp.bfloat16)
    resid_one = inputs + jnp.dot(attn_low, wo_full, preferred_element_type=jnp.float32)
    inv_two = lax.rsqrt(jnp.mean(resid_one * resid_one, axis=1, keepdims=True) + norm_eps)
    normed_two = resid_one * inv_two
    moe_in = normed_two * moe_gain
    moe_low = moe_in.astype(jnp.bfloat16)
    n_ids = w_router.shape[1]
    local_experts = w_gate.shape[0]
    owners = lax.axis_size(EX)
    ffn_count = local_experts * owners
    id_table = jnp.arange(n_ids, dtype=jnp.int32)
    route_hot = (routes[:, :, None] == id_table).astype(jnp.float32)
    logits = dense32(moe_in, w_router)
    chosen = jnp.einsum("rkn,rn->rk", route_hot, logits, precision=lax.Precision.HIGHEST)
    gate_probs = jax.nn.softmax(chosen, axis=1)
    mix_alpha = jax.nn.softmax(dense32(moe_in, const_mix).reshape(tok_rows, 2, 2), axis=2)
    const_rows = mix_alpha[:, :, 0:1] * moe_in[:, None, :] + mix_alpha[:, :, 1:2] * const_vec[None]
    ffn_mask = (routes < ffn_count).astype(jnp.float32)
    copy_mask = (routes == ffn_count + 1).astype(jnp.float32)
    const_mask = (routes[:, :, None] == ffn_count + 2 + jnp.arange(2, dtype=jnp.int32)).astype(
        jnp.float32
    )
    copy_gate = jnp.sum(gate_probs * copy_mask, axis=1)
    const_gate = jnp.sum(gate_probs[:, :, None] * const_mask, axis=1)
    ffn_gate = gate_probs * ffn_mask
    flat_ids = routes.reshape(-1)
    id_hot = (flat_ids[:, None] == id_table).astype(jnp.int32)
    earlier = jnp.cumsum(id_hot, axis=0, dtype=jnp.int32) - id_hot
    slot_num = jnp.sum(earlier * id_hot, axis=1, dtype=jnp.int32)
    slot_total = ffn_count * CAP
    slot_of_route = jnp.where(flat_ids < ffn_count, flat_ids * CAP + slot_num, slot_total)
    route_count = flat_ids.shape[0]
    route_of_slot = (
        jnp.zeros(slot_total + 1, jnp.int32)
        .at[slot_of_route]
        .set(jnp.arange(route_count, dtype=jnp.int32))[:slot_total]
    )
    slot_used = jnp.zeros(slot_total + 1, jnp.bool_).at[slot_of_route].set(True)[:slot_total]
    send_rows = jnp.where(
        slot_used[:, None], moe_low[route_of_slot // 2], jnp.zeros((), jnp.bfloat16)
    )
    recv_rows = lax.all_to_all(
        send_rows.reshape(owners, local_experts * CAP, model_width),
        EX,
        split_axis=0,
        concat_axis=0,
        tiled=True,
    )
    expert_in = recv_rows.reshape(owners, local_experts, CAP, model_width)
    gate_pre = jnp.einsum("sjcd,jdf->sjcf", expert_in, w_gate, preferred_element_type=jnp.float32)
    up_pre = jnp.einsum("sjcd,jdf->sjcf", expert_in, w_up, preferred_element_type=jnp.float32)
    gate_sigmoid = jax.nn.sigmoid(gate_pre)
    hidden_act = (gate_pre * gate_sigmoid * up_pre).astype(jnp.bfloat16)
    expert_out = jnp.einsum(
        "sjcf,jfd->sjcd", hidden_act, w_down, preferred_element_type=jnp.float32
    ).astype(jnp.bfloat16)
    returned = lax.all_to_all(
        expert_out.reshape(owners, local_experts * CAP, model_width),
        EX,
        split_axis=0,
        concat_axis=0,
        tiled=True,
    )
    padded_out = jnp.concatenate(
        [returned.reshape(slot_total, model_width), jnp.zeros((1, model_width), jnp.bfloat16)],
        axis=0,
    )
    route_out = padded_out[slot_of_route].astype(jnp.float32).reshape(tok_rows, 2, model_width)
    moe_sum = (
        jnp.sum(ffn_gate[:, :, None] * route_out, axis=1)
        + copy_gate[:, None] * moe_in
        + jnp.sum(const_gate[:, :, None] * const_rows, axis=1)
    )
    layer_out = (resid_one + moe_sum).astype(jnp.bfloat16)
    upstream = out_grad.astype(jnp.float32)
    route_dot = jnp.sum(upstream[:, None, :] * route_out, axis=2)
    copy_dot = jnp.sum(upstream * moe_in, axis=1)
    const_dot = jnp.sum(upstream[:, None, :] * const_rows, axis=2)
    gate_back_r = (
        ffn_mask * route_dot
        + copy_mask * copy_dot[:, None]
        + jnp.sum(const_mask * const_dot[:, None, :], axis=2)
    )
    chosen_grad = gate_probs * (
        gate_back_r - jnp.sum(gate_probs * gate_back_r, axis=1, keepdims=True)
    )
    logit_grad = jnp.einsum("rk,rkn->rn", chosen_grad, route_hot, precision=lax.Precision.HIGHEST)
    const_up = const_gate[:, :, None] * upstream[:, None, :]
    alpha_grad = jnp.stack(
        [
            jnp.sum(const_up * moe_in[:, None, :], axis=2),
            jnp.sum(const_up * const_vec[None], axis=2),
        ],
        axis=2,
    )
    mix_back = (
        mix_alpha * (alpha_grad - jnp.sum(mix_alpha * alpha_grad, axis=2, keepdims=True))
    ).reshape(tok_rows, 4)
    vec_grad = jnp.sum(mix_alpha[:, :, 1:2] * const_up, axis=0)
    route_weight = ffn_gate.reshape(-1)
    grad_send = (route_weight[route_of_slot][:, None] * upstream[route_of_slot // 2]).astype(
        jnp.bfloat16
    )
    grad_send = jnp.where(slot_used[:, None], grad_send, jnp.zeros((), jnp.bfloat16))
    grad_recv = lax.all_to_all(
        grad_send.reshape(owners, local_experts * CAP, model_width),
        EX,
        split_axis=0,
        concat_axis=0,
        tiled=True,
    )
    grad_recv = grad_recv.reshape(owners, local_experts, CAP, model_width)
    hidden_grad = jnp.einsum(
        "sjcd,jfd->sjcf", grad_recv, w_down, preferred_element_type=jnp.float32
    )
    down_term = jnp.einsum(
        "sjcf,sjcd->jfd", hidden_act, grad_recv, preferred_element_type=jnp.float32
    )
    gate_back = (
        hidden_grad * up_pre * gate_sigmoid * (1.0 + gate_pre * (1.0 - gate_sigmoid))
    ).astype(jnp.bfloat16)
    up_back = (hidden_grad * gate_pre * gate_sigmoid).astype(jnp.bfloat16)
    gate_term = jnp.einsum(
        "sjcd,sjcf->jdf", expert_in, gate_back, preferred_element_type=jnp.float32
    )
    up_term = jnp.einsum("sjcd,sjcf->jdf", expert_in, up_back, preferred_element_type=jnp.float32)
    input_back = (
        jnp.einsum("sjcf,jdf->sjcd", gate_back, w_gate, preferred_element_type=jnp.float32)
        + jnp.einsum("sjcf,jdf->sjcd", up_back, w_up, preferred_element_type=jnp.float32)
    ).astype(jnp.bfloat16)
    input_ret = lax.all_to_all(
        input_back.reshape(owners, local_experts * CAP, model_width),
        EX,
        split_axis=0,
        concat_axis=0,
        tiled=True,
    )
    padded_in = jnp.concatenate(
        [input_ret.reshape(slot_total, model_width), jnp.zeros((1, model_width), jnp.bfloat16)],
        axis=0,
    )
    ffn_in_grad = jnp.sum(
        padded_in[slot_of_route].astype(jnp.float32).reshape(tok_rows, 2, model_width), axis=1
    )
    moe_in_grad = (
        ffn_in_grad
        + copy_gate[:, None] * upstream
        + jnp.sum(mix_alpha[:, :, 0:1] * const_up, axis=1)
        + dense32(mix_back, const_mix.T)
        + dense32(logit_grad, w_router.T)
    )
    moe_gain_grad = jnp.sum(moe_in_grad * normed_two, axis=0)
    router_grad = dense32(moe_in.T, logit_grad)
    mix_grad = dense32(moe_in.T, mix_back)
    resid_grad = upstream + rms_back(resid_one, inv_two, moe_gain, moe_in_grad)
    branch_low = resid_grad.astype(jnp.bfloat16)
    out_proj_term = jnp.dot(attn_low.T, branch_low, preferred_element_type=jnp.float32)
    attn_back = jnp.dot(branch_low, wo_full.T, preferred_element_type=jnp.float32).astype(
        jnp.bfloat16
    )
    back_heads = attn_back.reshape(tok_rows, HEADS, HEAD_DIM)
    row_delta = jnp.sum(back_heads.astype(jnp.float32) * attn_sum, axis=2).T

    def back_step(query_acc, block_index):
        key_mask = block_mask(block_index)
        keys_blk = fetch_block(keys_all, block_index)
        values_blk = fetch_block(values_all, block_index)

        def back_live_block(running):
            prob_low, score_low = grad_pieces(
                query_heads,
                back_heads,
                keys_blk,
                values_blk,
                log_norm,
                row_delta,
                key_mask,
                score_scale,
            )
            value_part = jnp.einsum(
                "hqk,qhd->khd", prob_low, back_heads, preferred_element_type=jnp.float32
            )
            key_part = (
                jnp.einsum(
                    "hqk,qhd->khd", score_low, query_heads, preferred_element_type=jnp.float32
                )
                * score_scale
            )
            running = (
                running
                + jnp.einsum(
                    "hqk,khd->qhd", score_low, keys_blk, preferred_element_type=jnp.float32
                )
                * score_scale
            )
            return (
                running,
                (
                    key_part.reshape(key_block, model_width),
                    value_part.reshape(key_block, model_width),
                ),
            )

        def dead_block(running):
            empty_rows = jnp.zeros((key_block, model_width), jnp.float32)
            return (running, (empty_rows, empty_rows))

        return lax.cond(jnp.any(key_mask), back_live_block, dead_block, query_acc)

    query_grad32, key_terms = lax.scan(back_step, zero_heads, jnp.arange(num_blocks))
    key_grad32, value_grad32 = (
        lax.psum_scatter(
            key_terms[0].reshape(group_len, model_width).astype(jnp.bfloat16),
            (EX, SH),
            scatter_dimension=0,
            tiled=True,
        ).astype(jnp.float32),
        lax.psum_scatter(
            key_terms[1].reshape(group_len, model_width).astype(jnp.bfloat16),
            (EX, SH),
            scatter_dimension=0,
            tiled=True,
        ).astype(jnp.float32),
    )
    query_low = query_grad32.reshape(tok_rows, model_width).astype(jnp.bfloat16)
    key_low = key_grad32.astype(jnp.bfloat16)
    value_low = value_grad32.astype(jnp.bfloat16)
    query_term = jnp.dot(attn_in.T, query_low, preferred_element_type=jnp.float32)
    key_term = jnp.dot(attn_in.T, key_low, preferred_element_type=jnp.float32)
    value_term = jnp.dot(attn_in.T, value_low, preferred_element_type=jnp.float32)
    attn_in_grad = (
        jnp.dot(query_low, wq_full.T, preferred_element_type=jnp.float32)
        + jnp.dot(key_low, wk_full.T, preferred_element_type=jnp.float32)
        + jnp.dot(value_low, wv_full.T, preferred_element_type=jnp.float32)
    )
    attn_gain_grad = jnp.sum(attn_in_grad * normed_one, axis=0)
    input_grad = resid_grad + rms_back(inputs, inv_one, attn_gain, attn_in_grad)
    query_part, key_part_w, value_part_w, out_part = (
        lax.psum_scatter(
            query_term.astype(jnp.bfloat16), (EX, SH), scatter_dimension=0, tiled=True
        ).astype(jnp.float32),
        lax.psum_scatter(
            key_term.astype(jnp.bfloat16), (EX, SH), scatter_dimension=0, tiled=True
        ).astype(jnp.float32),
        lax.psum_scatter(
            value_term.astype(jnp.bfloat16), (EX, SH), scatter_dimension=0, tiled=True
        ).astype(jnp.float32),
        lax.psum_scatter(
            out_proj_term.astype(jnp.bfloat16), (EX, SH), scatter_dimension=0, tiled=True
        ).astype(jnp.float32),
    )
    gate_part, up_part, down_part = (
        lax.psum_scatter(
            gate_term.astype(jnp.bfloat16), SH, scatter_dimension=1, tiled=True
        ).astype(jnp.float32),
        lax.psum_scatter(
            up_term.astype(jnp.bfloat16), SH, scatter_dimension=1, tiled=True
        ).astype(jnp.float32),
        lax.psum_scatter(
            down_term.astype(jnp.bfloat16), SH, scatter_dimension=1, tiled=True
        ).astype(jnp.float32),
    )
    summed = (
        lax.psum(query_part.astype(jnp.bfloat16), GR).astype(jnp.float32),
        lax.psum(key_part_w.astype(jnp.bfloat16), GR).astype(jnp.float32),
        lax.psum(value_part_w.astype(jnp.bfloat16), GR).astype(jnp.float32),
        lax.psum(out_part.astype(jnp.bfloat16), GR).astype(jnp.float32),
        lax.psum(gate_part.astype(jnp.bfloat16), GR).astype(jnp.float32),
        lax.psum(up_part.astype(jnp.bfloat16), GR).astype(jnp.float32),
        lax.psum(down_part.astype(jnp.bfloat16), GR).astype(jnp.float32),
    )
    small_sums = lax.psum(
        (attn_gain_grad, moe_gain_grad, router_grad, mix_grad, vec_grad),
        (GR, EX, SH),
    )
    return (
        layer_out,
        input_grad,
        small_sums[0],
        summed[0],
        summed[1],
        summed[2],
        summed[3],
        small_sums[1],
        small_sums[2],
        small_sums[3],
        small_sums[4],
        summed[4],
        summed[5],
        summed[6],
    )


def greet(peers):
    barrier = pltpu.get_barrier_semaphore()
    for axis, peer in peers:
        pl.semaphore_signal(
            barrier, inc=1, device_id={axis: peer}, device_id_type=pl.DeviceIdType.MESH
        )
    pl.semaphore_wait(barrier, len(peers))


def send(src, dst, sems, index, axis, peer):
    copy = pltpu.make_async_remote_copy(
        src_ref=src,
        dst_ref=dst,
        send_sem=sems.at[0, index],
        recv_sem=sems.at[1, index],
        device_id={axis: peer},
        device_id_type=pl.DeviceIdType.MESH,
    )
    copy.start()
    return copy


def shard_peers():
    me = lax.axis_index(SH)
    side, core = me // 2, lax.rem(me, 2)
    return me, side, core, 2 * side + 1 - core, 2 * (1 - side) + core


class Part:
    def __init__(self, axes, ins, outs, scratch, copies, phases, specs=None):
        self.axes, self.ins, self.outs, self.scratch = axes, ins, outs, scratch
        self.copies, self.phases = copies, phases
        self.specs = specs or [VM] * len(ins)


def run_parts(parts, collective_id, name=None, cost=None):
    ins = sum([p.ins for p in parts], [])
    outs = sum([p.outs for p in parts], [])
    scratch = sum([p.scratch for p in parts], [])
    copies = sum(p.copies for p in parts)
    axes = sorted(set(sum([list(p.axes) for p in parts], [])))

    def body(*refs):
        sems = refs[-1]
        in_refs, out_refs = list(refs[: len(ins)]), list(refs[len(ins) : len(ins) + len(outs)])
        scr = list(refs[len(ins) + len(outs) : -1])
        peers = []
        for axis in axes:
            me, n = lax.axis_index(axis), lax.axis_size(axis)
            peers += [(axis, lax.rem(me + d, n)) for d in range(1, n)]
        greet(peers)
        base, running = 0, []
        for p in parts:
            take = lambda pool, k: [pool.pop(0) for _ in range(k)]
            refs_p = (take(in_refs, len(p.ins)), take(out_refs, len(p.outs)), take(scr, len(p.scratch)))
            counter = [base]

            def go(src, dst, axis, peer, counter=counter):
                counter[0] += 1
                return send(src, dst, sems, counter[0] - 1, axis, peer)

            running.append(p.phases(*refs_p, go))
            base += p.copies
        while running:
            running = [r for r in running if next(r, True) is None]

    return pl.pallas_call(
        body,
        out_shape=outs,
        in_specs=sum([p.specs for p in parts], []),
        out_specs=[VM] * len(outs),
        scratch_shapes=scratch + [pltpu.SemaphoreType.DMA((2, copies))],
        compiler_params=pltpu.CompilerParams(collective_id=collective_id, has_side_effects=True),
        cost_estimate=cost,
        name=name,
    )(*ins)


def start_swap(go, src, land, axis, gather):
    me, n = lax.axis_index(axis), lax.axis_size(axis)
    started = []
    for d in range(1, n):
        peer = lax.rem(me + d, n)
        started.append(go(src if gather else src.at[peer], land.at[me], axis, peer))
    land[me] = src[...] if gather else src[me]
    return started


def total_of(land, n):
    total = land[0].astype(f32)
    for j in range(1, n):
        total = total + land[j].astype(f32)
    return total


def exchange(axis, kind, x):
    n = lax.axis_size(axis)
    gather, summed = kind in (GATHER, GATHER_SUM), kind in (GATHER_SUM, SWAP_SUM)
    piece = x.shape if gather else x.shape[1:]
    shape = jax.ShapeDtypeStruct
    outs = [shape(piece, f32) if summed else shape((n,) + piece, x.dtype)]
    scratch = [pltpu.VMEM((n,) + piece, x.dtype)] if summed else []

    def phases(ins, outs, scr, go):
        land = scr[0] if summed else outs[0]
        started = start_swap(go, ins[0], land, axis, gather)
        yield
        for copy in started:
            copy.wait()
        if summed:
            outs[0][...] = total_of(land, n)

    return Part([axis], [x], outs, scratch, n - 1, phases)


def tree_gather(x):
    lines = x.shape[0]
    cuts = [(0, lines // 2), (lines // 2, lines)] if lines > 1 else [(0, 1)]
    cuts = [pl.ds(lo, hi - lo) for lo, hi in cuts]

    def phases(ins, outs, scr, go):
        x_ref, out_ref = ins[0], outs[0]
        me, _, _, near, far = shard_peers()
        across = [go(x_ref.at[c], out_ref.at[c, me], SH, far) for c in cuts]
        own = go(x_ref, out_ref.at[:, me], SH, near)
        out_ref[:, me] = x_ref[...]
        yield
        handed = []
        for c, copy in zip(cuts, across):
            copy.wait_recv()
            handed.append(go(out_ref.at[c, far], out_ref.at[c, far], SH, near))
        yield
        for copy in across:
            copy.wait_send()
        own.wait()
        for copy in handed:
            copy.wait()

    shape = (lines, 4) + x.shape[1:]
    return Part([SH], [x], [jax.ShapeDtypeStruct(shape, x.dtype)], [], 2 * len(cuts) + 1, phases)


def core_sum(x):
    piece = x.shape[1:]
    shape = jax.ShapeDtypeStruct

    def phases(ins, outs, scr, go):
        x_ref, (here, there), (land, kept, sems) = ins[0], outs, scr
        near = shard_peers()[3]
        sent = [go(x_ref.at[3], land.at[1], SH, near), go(x_ref.at[2], land.at[0], SH, near)]
        local = [pltpu.make_async_copy(x_ref.at[k], kept.at[k], sems.at[k]) for k in range(2)]
        for copy in local:
            copy.start()
        yield
        for k, out in ((1, there), (0, here)):
            sent[1 - k].wait()
            local[k].wait()
            out[...] = (kept[k].astype(f32) + land[k].astype(f32)).astype(bf16)

    return Part(
        [SH],
        [x],
        [shape(piece, bf16)] * 2,
        [pltpu.VMEM((2,) + piece, bf16)] * 2 + [pltpu.SemaphoreType.DMA((2,))],
        2,
        phases,
        [pl.BlockSpec(memory_space=pl.ANY)],
    )


class Tree:
    copies = 3

    @staticmethod
    def scratch(piece):
        return [pltpu.VMEM((2,) + piece, bf16)] + [pltpu.VMEM(piece, bf16)] * 2

    def __init__(self, x, scr, go):
        self.x, (self.land, self.mine, self.got), self.go = x, scr, go
        self.me, self.side, self.core, self.near, self.far = shard_peers()
        other = 2 * (1 - self.side) + 1 - self.core
        self.first = [
            go(x.at[other], self.land.at[0], SH, self.near),
            go(x.at[self.near], self.land.at[1], SH, self.near),
        ]

    def across(self):
        self.first[0].wait_recv()
        self.mine[...] = (self.x[self.far].astype(f32) + self.land[0].astype(f32)).astype(bf16)
        self.second = self.go(self.mine, self.got, SH, self.far)

    def result(self):
        self.first[1].wait_recv()
        total = self.x[self.me].astype(f32) + self.land[1].astype(f32)
        self.second.wait_recv()
        return total + self.got[...].astype(f32)

    def close(self):
        for copy in (*self.first, self.second):
            copy.wait_send()


def front(hidden, w_mine, gain):
    rows, model = hidden.shape
    lines = lax.axis_size(EX)
    width = model // lines
    shape = jax.ShapeDtypeStruct
    last = lines - 1

    def body(hid_ref, w_ref, gain_ref, attn_ref, q_ref, kv_ref, land, w_all, kv_own, sems):
        line_me = lax.axis_index(EX)
        me, _, _, near, far = shard_peers()
        left, right = jnp.maximum(line_me - 1, 0), jnp.minimum(line_me + 1, last)
        greet(
            [(EX, lax.rem(line_me + d, lines)) for d in range(1, lines)]
            + [(SH, lax.rem(me + d, 4)) for d in range(1, 4)]
        )

        def copy(src, dst, index, axis, peer):
            return pltpu.make_async_remote_copy(
                src_ref=src,
                dst_ref=dst,
                send_sem=sems.at[0, index],
                recv_sem=sems.at[1, index],
                device_id={axis: peer},
                device_id_type=pl.DeviceIdType.MESH,
            )

        def relay(step, way):
            block = line_me - step if way == 0 else line_me + step
            block = jnp.clip(block, 0, last)
            src = hid_ref if step == 0 else land.at[block]
            return copy(src, land.at[block], last * way + step, EX, right if way == 0 else left)

        def sends(step, way):
            if way == 0:
                return (line_me < last) & (line_me - step >= 0)
            return (line_me > 0) & (line_me + step <= last)

        def comes(step, way):
            return line_me - 1 - step >= 0 if way == 0 else line_me + 1 + step <= last

        def source(step, way):
            line = line_me - 1 - step if way == 0 else line_me + 1 + step
            return jnp.clip(line, 0, last)

        def arrival(step, way):
            line = source(step, way)
            return copy(land.at[line], land.at[line], last * way + step, EX, right if way == 0 else left)

        base = 2 * last
        for way in range(2):

            @pl.when(sends(0, way))
            def _():
                relay(0, way).start()

        w_far = copy(w_ref, w_all.at[me], base, SH, far)
        w_near = copy(w_ref, w_all.at[me], base + 1, SH, near)
        w_pass = copy(w_all.at[far], w_all.at[far], base + 2, SH, near)
        w_far.start()
        w_near.start()
        w_all[me] = w_ref[...]
        base += 3
        kv_far = lambda line: copy(kv_own.at[line], kv_ref.at[line, me], base + line, SH, far)
        kv_near = lambda line: copy(
            kv_own.at[line], kv_ref.at[line, me], base + lines + line, SH, near
        )
        kv_pass = lambda line: copy(
            kv_ref.at[line, far], kv_ref.at[line, far], base + 2 * lines + line, SH, near
        )

        def project(line, x):
            inputs = x.astype(f32)
            inv = lax.rsqrt(jnp.mean(inputs * inputs, axis=1, keepdims=True) + norm_eps)
            attn_in = (inputs * inv * gain_ref[...]).astype(bf16)
            attn_ref[line] = attn_in
            value = jnp.dot(
                attn_in, w_all[...].reshape(model, 3 * width), preferred_element_type=f32
            ).astype(bf16)
            kv_own[line] = value[:, : 2 * width]
            kv_far(line).start()
            kv_near(line).start()
            kv_ref[line, me] = value[:, : 2 * width]
            q_ref[line] = value[:, 2 * width :]

        def hand(line):
            kv_far(line).wait_recv()
            kv_pass(line).start()

        w_far.wait_recv()
        w_pass.start()
        w_near.wait_recv()
        w_pass.wait_recv()
        project(line_me, hid_ref[...])
        for step in range(last):
            for way in range(2):

                @pl.when(comes(step, way))
                def _():
                    arrival(step, way).wait_recv()

                if step + 1 < last:

                    @pl.when(sends(step + 1, way))
                    def _():
                        relay(step + 1, way).start()

            for way in range(2):

                @pl.when(comes(step, way))
                def _():
                    line = source(step, way)
                    project(line, land[line])

            if step == 0:
                hand(line_me)
            else:
                for way in range(2):

                    @pl.when(comes(step - 1, way))
                    def _():
                        hand(source(step - 1, way))

        for way in range(2):

            @pl.when(comes(last - 1, way))
            def _():
                hand(source(last - 1, way))

        for way in range(2):
            for step in range(last):

                @pl.when(sends(step, way))
                def _():
                    relay(step, way).wait_send()

        w_far.wait_send()
        w_near.wait_send()
        w_pass.wait_send()
        for line in range(lines):
            kv_far(line).wait_send()
            kv_near(line).wait()
            kv_pass(line).wait()

    return pl.pallas_call(
        body,
        out_shape=[
            shape((lines, rows, model), bf16),
            shape((lines, rows, width), bf16),
            shape((lines, 4, rows, 2 * width), bf16),
        ],
        in_specs=[VM] * 3,
        out_specs=[VM] * 3,
        scratch_shapes=[
            pltpu.VMEM((lines, rows, model), bf16),
            pltpu.VMEM((4, rows, 3 * width), bf16),
            pltpu.VMEM((lines, rows, 2 * width), bf16),
            pltpu.SemaphoreType.DMA((2, 2 * last + 3 + 3 * lines)),
        ],
        compiler_params=pltpu.CompilerParams(collective_id=0, has_side_effects=True),
        name="front",
    )(hidden, w_mine, gain)


def column(x, k):
    return x[:, k : k + 1]


def core_share(go, own, far, out):
    me, _, _, near, other = shard_peers()
    sent = [go(own, out.at[:, me], SH, near), go(far, out.at[:, other], SH, near)]
    out[:, me] = own[...]
    out[:, other] = far[...]
    return sent


def route(heads, hidden, gain, small_w, routes, out_grad, wo, wo_far, w3, w3_far, n_ids):
    lines, rows, width = heads.shape
    model = lines * width
    slots = lines * CAP
    shape = jax.ShapeDtypeStruct

    def phases(ins, outs, scr, go):
        heads_ref, hid_ref, gain_ref, small_ref, routes_ref, up_ref, wo_ref, wof_ref, w3_ref, w3f_ref = ins
        rows_out, grads_out, w3_all, wo_all, resid_ref, table_ref, place_ref, low_ref = outs
        land, rows_s, grads_s = scr
        swaps = start_swap(go, heads_ref, land, EX, False)
        swaps += core_share(go, wo_ref, wof_ref, wo_all)
        shares = core_share(go, w3_ref, w3f_ref, w3_all)
        ids = routes_ref[...]
        lane = lax.broadcasted_iota(jnp.int32, (rows, 128), 1)
        hot = [lane == column(ids, k) for k in range(2)]
        before = (
            lax.broadcasted_iota(jnp.int32, (rows, rows), 0)
            > lax.broadcasted_iota(jnp.int32, (rows, rows), 1)
        ).astype(bf16)
        named = jnp.where(hot[0] | hot[1], 1.0, 0.0).astype(bf16)
        earlier = jnp.dot(before, named, preferred_element_type=f32)
        slot_at = lax.broadcasted_iota(jnp.int32, (rows, slots), 1).astype(f32)
        place = []
        for k in range(2):
            number = jnp.sum(jnp.where(hot[k], earlier, 0.0), axis=1, keepdims=True)
            wanted = column(ids, k).astype(f32) * CAP + number
            wanted = jnp.where(column(ids, k) < lines, wanted, -1.0)
            place.append(jnp.where(slot_at == wanted, 1.0, 0.0))
            place_ref[k] = place[k].astype(bf16)
        either = (place[0] + place[1]).astype(bf16)
        up_rows = contract(either, up_ref[...], 0, 0)
        for copy in swaps:
            copy.wait()
        for line in range(lines):
            low_ref[:, line * width : (line + 1) * width] = land[line]
        w_out = wo_all[...].reshape(model, model)
        resid = hid_ref[...].astype(f32) + jnp.dot(
            low_ref[...], w_out, preferred_element_type=f32
        )
        resid_ref[...] = resid
        inv = lax.rsqrt(jnp.mean(resid * resid, axis=1, keepdims=True) + norm_eps)
        moe_in = resid * inv * gain_ref[...]
        rows_s[...] = contract(either, moe_in.astype(bf16), 0, 0).astype(bf16).reshape(
            lines, CAP, model
        )
        row_swap = start_swap(go, rows_s, rows_out, EX, False)
        small = jnp.dot(moe_in, small_ref[...], preferred_element_type=f32, precision=HIGH)
        chosen = [jnp.sum(jnp.where(h, small, 0.0), axis=1, keepdims=True) for h in hot]
        top = jnp.maximum(chosen[0], chosen[1])
        powers = [jnp.exp(c - top) for c in chosen]
        gates = [p / (powers[0] + powers[1]) for p in powers]
        weight = place[0] * gates[0] + place[1] * gates[1]
        weight = contract(weight, jnp.ones((rows, 128), f32), 0, 0, HIGH)[:, 0:1]
        grads_s[...] = (up_rows * weight).astype(bf16).reshape(lines, CAP, model)
        grad_swap = start_swap(go, grads_s, grads_out, EX, False)
        table = jnp.zeros((rows, 128), f32)
        entries = list(gates)
        for j in range(2):
            pair = [column(small, n_ids + 2 * j + k) for k in range(2)]
            top = jnp.maximum(pair[0], pair[1])
            powers = [jnp.exp(c - top) for c in pair]
            entries += [p / (powers[0] + powers[1]) for p in powers]
        entries += [column(ids, k).astype(f32) for k in range(2)]
        for k, entry in enumerate(entries):
            table = jnp.where(lane == k, entry, table)
        table_ref[...] = table
        for copy in row_swap + grad_swap + shares:
            copy.wait()
        yield

    ins = [heads, hidden, gain, small_w, routes, out_grad, wo, wo_far, w3, w3_far]
    outs = [
        shape((lines, CAP, model), bf16),
        shape((lines, CAP, model), bf16),
        shape((3, 4, model // 4, model), bf16),
        shape((1, 4, model // 4, model), bf16),
        shape((rows, model), f32),
        shape((rows, 128), f32),
        shape((2, rows, slots), bf16),
        shape((rows, model), bf16),
    ]
    scratch = [pltpu.VMEM((lines, rows, width), bf16)] + [pltpu.VMEM((lines, CAP, model), bf16)] * 2
    return Part([EX, SH], ins, outs, scratch, 3 * (lines - 1) + 4, phases)


def to_heads(returned, input_ret, place, table, resid, low, out_grad, gain, small_t, const_vec, wo, n_ids):
    rows, model = resid.shape
    lines = returned.shape[0]
    width = model // lines
    own = rows // lines
    slots = lines * CAP
    shape = jax.ShapeDtypeStruct

    def phases(ins, outs, scr, go):
        ret_ref, iret_ref, place_ref, table_ref, resid_ref, low_ref, up_ref, gain_ref, st_ref, vec_ref, wo_ref = ins
        heads_out, layer_ref, rgrad_ref, term_ref, packed_ref = outs
        (back_s,) = scr
        table = table_ref[...]
        gates = [column(table, k) for k in range(2)]
        alpha = [[column(table, 2 + 2 * j + k) for k in range(2)] for j in range(2)]
        ids = [column(table, 6 + k) for k in range(2)]
        vecs = [vec_ref[j : j + 1, :] for j in range(2)]
        resid = resid_ref[...]
        upstream = up_ref[...].astype(f32)
        inv = lax.rsqrt(jnp.mean(resid * resid, axis=1, keepdims=True) + norm_eps)
        normed = resid * inv
        moe_in = normed * gain_ref[...]
        returned = ret_ref[...].reshape(slots, model)
        total = lambda x: jnp.sum(x, axis=1, keepdims=True)
        flag = lambda x: jnp.where(x, 1.0, 0.0)
        copy_dot = total(upstream * moe_in)
        vec_dot = [total(upstream * v) for v in vecs]
        const_dot = [alpha[j][0] * copy_dot + alpha[j][1] * vec_dot[j] for j in range(2)]
        output = resid
        backs = []
        copy_gate = jnp.zeros((rows, 1), f32)
        const_gate = [jnp.zeros((rows, 1), f32) for _ in range(2)]
        for k in range(2):
            rows_k = jnp.dot(place_ref[k], returned, preferred_element_type=f32)
            is_ffn, is_copy = flag(ids[k] < lines), flag(ids[k] == lines + 1)
            is_const = [flag(ids[k] == lines + 2 + j) for j in range(2)]
            output = output + (gates[k] * is_ffn) * rows_k
            backs.append(
                is_ffn * total(upstream * rows_k)
                + is_copy * copy_dot
                + is_const[0] * const_dot[0]
                + is_const[1] * const_dot[1]
            )
            copy_gate = copy_gate + gates[k] * is_copy
            const_gate = [const_gate[j] + gates[k] * is_const[j] for j in range(2)]
        through = copy_gate + const_gate[0] * alpha[0][0] + const_gate[1] * alpha[1][0]
        output = output + through * moe_in
        for j in range(2):
            output = output + (const_gate[j] * alpha[j][1]) * vecs[j]
        layer_ref[...] = output.astype(bf16)
        mean_back = gates[0] * backs[0] + gates[1] * backs[1]
        lane = lax.broadcasted_iota(jnp.int32, (rows, 128), 1)
        lane_f = lane.astype(f32)
        small = jnp.zeros((rows, 128), f32)
        for k in range(2):
            small = jnp.where(lane_f == ids[k], gates[k] * (backs[k] - mean_back), small)
        for j in range(2):
            grads = [const_gate[j] * copy_dot, const_gate[j] * vec_dot[j]]
            mean = alpha[j][0] * grads[0] + alpha[j][1] * grads[1]
            for k in range(2):
                small = jnp.where(
                    lane == n_ids + 2 * j + k, alpha[j][k] * (grads[k] - mean), small
                )
            small = jnp.where(lane == n_ids + 4 + j, alpha[j][1] * const_gate[j], small)
        either = place_ref[0] + place_ref[1]
        moe_grad = (
            jnp.dot(either, iret_ref[...].reshape(slots, model), preferred_element_type=f32)
            + through * upstream
            + jnp.dot(small, st_ref[...], preferred_element_type=f32, precision=HIGH)
        )
        resid_grad = upstream + rms_back(resid, inv, gain_ref[...], moe_grad)
        branch = resid_grad.astype(bf16)
        back = contract(branch, wo_ref[...], 1, 1).astype(bf16)
        for line in range(lines):
            back_s[line] = back[:, line * width : (line + 1) * width]
        swaps = start_swap(go, back_s, heads_out, EX, False)
        rgrad_ref[...] = resid_grad
        packed_ref[...] = jnp.zeros_like(packed_ref)
        packed_ref[0:1] = jnp.sum(moe_grad * normed, axis=0, keepdims=True)
        small_grad = contract(small, moe_in, 0, 0, HIGH)
        vec_grad = contract(small, upstream, 0, 0, HIGH)
        packed_ref[1:3] = vec_grad[n_ids + 4 : n_ids + 6]
        packed_ref[3 : 7 + n_ids] = small_grad[: n_ids + 4]
        term = contract(low_ref[...], branch, 0, 0).astype(bf16)
        for line in range(lines):
            for piece in range(4):
                at = (line * 4 + piece) * own
                term_ref[piece, line] = term[at : at + own]
        for copy in swaps:
            copy.wait()
        yield

    ins = [returned, input_ret, place, table, resid, low, out_grad, gain, small_t, const_vec, wo]
    outs = [
        shape((lines, rows, width), bf16),
        shape((rows, model), bf16),
        shape((rows, model), f32),
        shape((4, lines, own, model), bf16),
        shape((-(-(7 + n_ids) // 8) * 8, model), f32),
    ]
    return Part([EX], ins, outs, [pltpu.VMEM((lines, rows, width), bf16)], lines - 1, phases)


def tail(dkv, dq, attn_in, weights, out_term, packed, hidden, resid_grad, gain):
    lines, rows, width = dq.shape
    model = lines * width
    own = rows // lines
    groups = lax.axis_size(GR)
    shape = jax.ShapeDtypeStruct
    vmem = pltpu.VMEM
    tok = lines * rows
    dkv_piece, q_piece = (lines, rows, 2 * width), (lines, own, width)
    kv_piece, o_piece = (lines, own, 2 * width), (lines, own, model)
    part_dims = (width, 2 * width, model)

    def phases(ins, outs, scr, go):
        dkv_ref, dq_ref, attn_ref, w_ref, o_ref, packed_ref, hid_ref, resid_ref, gain_ref = ins
        input_ref, q_out, kv_out, out_out, packed_out, gain_out = outs
        scr = list(scr)
        take = lambda k: [scr.pop(0) for _ in range(k)]
        kv_scr, q_scr, kvw_scr, o_scr = take(3), take(3), take(3), take(3)
        own_kv, q_t, kv_t, dq_all, dkv_all, dq_full = take(6)
        sums, lands, halves, gots = take(3), take(3), take(3), take(3)
        pk_l, pk_s, pk_g = take(3)
        mid_l, mid_s = take(2)
        gn_l, gn_s, gn_g, gn_0, gn_1, gn_2 = take(6)
        me = lax.axis_index(SH)

        kv_tree = Tree(dkv_ref, kv_scr, go)
        dq_swap = start_swap(go, dq_ref, dq_all, EX, False)
        o_tree = Tree(o_ref, o_scr, go)
        pk1 = start_swap(go, packed_ref, pk_l, EX, True)

        def term(rows_ref, out):
            value = contract(attn_ref[...], rows_ref[...].reshape(tok, rows_ref.shape[-1]), 0, 0)
            value = value.astype(bf16)
            for line in range(lines):
                for piece in range(4):
                    at = (line * 4 + piece) * own
                    out[piece, line] = value[at : at + own]

        kv_tree.across()
        term(dq_ref, q_t)
        o_tree.across()
        q_tree = Tree(q_t, q_scr, go)
        trees = [q_tree, None, o_tree]

        def lines_out(k):
            sums[k][...] = trees[k].result().astype(bf16)
            return start_swap(go, sums[k], lands[k], EX, False)

        own_kv[...] = kv_tree.result().astype(bf16)
        dkv_swap = start_swap(go, own_kv, dkv_all, EX, False)
        o_lines = lines_out(2)
        q_tree.across()
        term(own_kv, kv_t)
        kvw_tree = Tree(kv_t, kvw_scr, go)
        trees[1] = kvw_tree
        for copy in pk1:
            copy.wait()
        mid_l[...] = total_of(pk_l, lines)
        pk2 = start_swap(go, mid_l, pk_s, SH, True)
        kvw_tree.across()
        q_lines = lines_out(0)
        for copy in dq_swap:
            copy.wait()
        for line in range(lines):
            dq_full[:, line * width : (line + 1) * width] = dq_all[line]
        grad = contract(dq_full[...], w_ref[0], 1, 1)
        for copy in pk2:
            copy.wait()
        mid_s[...] = total_of(pk_s, 4)
        pk3 = start_swap(go, mid_s, pk_g, GR, True)
        kv_lines = lines_out(1)
        for copy in dkv_swap:
            copy.wait()
        for half in range(2):
            for line in range(lines):
                dq_full[:, line * width : (line + 1) * width] = dkv_all[
                    line, :, half * width : (half + 1) * width
                ]
            grad = grad + contract(dq_full[...], w_ref[1 + half], 1, 1)
        inputs = hid_ref[...].astype(f32)
        inv = lax.rsqrt(jnp.mean(inputs * inputs, axis=1, keepdims=True) + norm_eps)
        normed = inputs * inv
        gn_0[...] = jnp.sum((grad * normed).reshape(rows // 8, 8, model), axis=0)
        gn1 = start_swap(go, gn_0, gn_l, EX, True)
        input_ref[...] = resid_ref[...] + rms_back(inputs, inv, gain_ref[...], grad)
        swaps = [None] * 3
        for k, copies in ((2, o_lines), (0, q_lines)):
            for copy in copies:
                copy.wait()
            if k == 2:
                halves[k][...] = total_of(lands[k], lines).astype(bf16)
            else:
                halves[k][...] = lands[k][...]
            swaps[k] = start_swap(go, halves[k], gots[k], GR, True)
        for copy in gn1:
            copy.wait()
        gn_1[...] = total_of(gn_l, lines)
        gn2 = start_swap(go, gn_1, gn_s, SH, True)
        for copy in kv_lines:
            copy.wait()
        halves[1][...] = lands[1][...]
        swaps[1] = start_swap(go, halves[1], gots[1], GR, True)
        for copy in gn2:
            copy.wait()
        gn_2[...] = total_of(gn_s, 4)
        gn3 = start_swap(go, gn_2, gn_g, GR, True)
        for copy in pk3:
            copy.wait()
        packed_out[...] = total_of(pk_g, groups)
        for k, out in ((2, out_out), (0, q_out), (1, kv_out)):
            for copy in swaps[k]:
                copy.wait()
            out[...] = total_of(gots[k], groups)
        for copy in gn3:
            copy.wait()
        gain_out[...] = total_of(gn_g, groups)
        for tree in (kv_tree, o_tree, q_tree, kvw_tree):
            tree.close()
        yield

    pieces = [(lines, own, d) for d in part_dims]
    got_pieces = pieces[:2] + [(own, model)]
    scratch = Tree.scratch(dkv_piece) + Tree.scratch(q_piece) + Tree.scratch(kv_piece)
    scratch += Tree.scratch(o_piece)
    scratch += [
        vmem(dkv_piece, bf16),
        vmem((4,) + q_piece, bf16),
        vmem((4,) + kv_piece, bf16),
        vmem((lines, rows, width), bf16),
        vmem((lines, rows, 2 * width), bf16),
        vmem((rows, model), bf16),
    ]
    scratch += [vmem(p, bf16) for p in pieces] + [vmem(p, bf16) for p in pieces]
    scratch += [vmem(p, bf16) for p in got_pieces] + [vmem((groups,) + p, bf16) for p in got_pieces]
    scratch += [vmem((n,) + packed.shape, f32) for n in (lines, 4, groups)]
    scratch += [vmem(packed.shape, f32)] * 2
    scratch += [vmem((n, 8, model), f32) for n in (lines, 4, groups)] + [vmem((8, model), f32)] * 3
    copies = 4 * Tree.copies + 7 * (lines - 1) + 2 * 3 + 5 * (groups - 1)
    outs = [
        shape((rows, model), f32),
        shape((lines, own, width), f32),
        shape((lines, own, 2 * width), f32),
        shape((own, model), f32),
        shape(packed.shape, f32),
        shape((8, model), f32),
    ]
    ins = [dkv, dq, attn_in, weights, out_term, packed, hidden, resid_grad, gain]
    return Part([EX, SH, GR], ins, outs, scratch, copies, phases)


def expert_body(steps, x_ref, g_ref, wg_ref, wu_ref, wd_ref, eo_ref, ib_ref, ga_ref, up_ref, d_ref, eo_s, ib_s):
    i = pl.program_id(0)
    me, side, core, _, _ = shard_peers()

    @pl.when(i == 0)
    def _():
        eo_s[...] = jnp.zeros_like(eo_s)
        ib_s[...] = jnp.zeros_like(ib_s)

    x, g = x_ref[...], g_ref[...]
    wg, wu, wd = wg_ref[...], wu_ref[...], wd_ref[...]
    gate_pre = jnp.dot(x, wg, preferred_element_type=f32)
    up_pre = jnp.dot(x, wu, preferred_element_type=f32)
    hidden_grad = contract(g, wd, 1, 1)
    gate_sigmoid = jax.nn.sigmoid(gate_pre)
    act = (gate_pre * gate_sigmoid * up_pre).astype(bf16)
    gate_back = (
        hidden_grad * up_pre * gate_sigmoid * (1.0 + gate_pre * (1.0 - gate_sigmoid))
    ).astype(bf16)
    up_back = (hidden_grad * gate_pre * gate_sigmoid).astype(bf16)
    eo_s[...] += jnp.dot(act, wd, preferred_element_type=f32)
    ib_s[...] += contract(gate_back, wg, 1, 1) + contract(up_back, wu, 1, 1)

    def place(quarter):
        return 2 * lax.rem(lax.rem(quarter, 2) + core, 2) + lax.rem(quarter // 2 + side, 2)

    rows = ga_ref.shape[1]
    for ref, back in ((ga_ref, gate_back), (up_ref, up_back)):
        term = contract(x, back, 0, 0).astype(bf16)
        for quarter in range(4):
            ref[place(jnp.int32(quarter))] = term[quarter * rows : (quarter + 1) * rows]
    d_ref[place(i)] = contract(act, g, 0, 0).astype(bf16)

    @pl.when(i == steps - 1)
    def _():
        eo_ref[...] = eo_s[...].astype(bf16)
        ib_ref[...] = ib_s[...].astype(bf16)


def expert(x, g, wg, wu, wd):
    slots, model = x.shape
    inner = wg.shape[1]
    steps = 4
    tile = inner // steps
    quarter = model // 4
    shape = jax.ShapeDtypeStruct
    whole = lambda dims: pl.BlockSpec(dims, lambda i: (0,) * len(dims))
    return pl.pallas_call(
        functools.partial(expert_body, steps),
        grid=(steps,),
        out_shape=[
            shape((slots, model), bf16),
            shape((slots, model), bf16),
            shape((4, quarter, inner), bf16),
            shape((4, quarter, inner), bf16),
            shape((4, tile, model), bf16),
        ],
        in_specs=[
            whole((slots, model)),
            whole((slots, model)),
            pl.BlockSpec((model, tile), lambda i: (0, i)),
            pl.BlockSpec((model, tile), lambda i: (0, i)),
            pl.BlockSpec((tile, model), lambda i: (i, 0)),
        ],
        out_specs=[
            whole((slots, model)),
            whole((slots, model)),
            pl.BlockSpec((4, quarter, tile), lambda i: (0, 0, i)),
            pl.BlockSpec((4, quarter, tile), lambda i: (0, 0, i)),
            whole((4, tile, model)),
        ],
        scratch_shapes=[pltpu.VMEM((slots, model), f32)] * 2,
        cost_estimate=pl.CostEstimate(flops=6 * 10**9, bytes_accessed=2 * 10**7, transcendentals=4 * 10**5),
        name="ffn",
    )(x, g, wg, wu, wd)


def head_columns(h, shape, axis):
    return lax.broadcasted_iota(jnp.int32, shape, axis) // HEAD_DIM == h


def allowed(block, key_blk, qpos, qstart, prompt):
    kpos = block * key_blk + lax.broadcasted_iota(jnp.int32, (key_blk, qpos.shape[1]), 0)
    return (kpos <= qpos) & ((kpos >= qstart) | (kpos < prompt))


def doc_start(block, info_ref, qinfo_ref):
    docs = qinfo_ref[pl.ds(block, 1), :]
    starts = jnp.zeros(docs.shape, jnp.int32)
    for doc in range(1, DOCS):
        starts = jnp.where(docs == doc, info_ref[doc], starts)
    return starts, info_ref[info_ref[DOCS + block]]


def attend_body(lines, heads, info_ref, q_ref, kv_ref, qinfo_ref, o_ref, low_ref, lse_ref, k_s, vt_s, acc_s, ml_s, qm_s):
    shard = lax.axis_index(SH)
    rows, width = q_ref.shape[1:]
    blocks = vt_s.shape[0]
    key_blk = vt_s.shape[2]
    prompt = info_ref[1]

    @pl.loop(0, blocks)
    def _(j):
        at = pl.ds(pl.multiple_of(j * key_blk, key_blk), key_blk)
        k_s[at, :] = kv_ref[at, :width]
        vt_s[j] = jnp.transpose(kv_ref[at, width:].astype(f32)).astype(bf16)

    @pl.loop(0, lines)
    def _(line):
        start = (line * 4 + shard) * rows
        queries = q_ref[line].astype(f32) * HEAD_DIM**-0.5
        qpos = start + lax.broadcasted_iota(jnp.int32, (1, rows), 1)
        qstart, first = doc_start(line * 4 + shard, info_ref, qinfo_ref)
        for h in range(heads):
            qm_s[h] = jnp.where(head_columns(h, queries.shape, 1), queries, 0.0).astype(bf16)
        acc_s[...] = jnp.zeros_like(acc_s)
        for h in range(heads):
            ml_s[h, 0:1, :] = jnp.full((1, rows), neg_fill, f32)
            ml_s[h, 1:2, :] = jnp.zeros((1, rows), f32)

        @pl.loop(0, (start + rows + key_blk - 1) // key_blk)
        def _(j):
            @pl.when((j * key_blk < prompt) | ((j + 1) * key_blk > first))
            def _():
                keys = k_s[pl.ds(pl.multiple_of(j * key_blk, key_blk), key_blk), :]
                ok = allowed(j, key_blk, qpos, qstart, prompt)
                for h in range(heads):
                    scores = jnp.where(ok, contract(keys, qm_s[h], 1, 1), neg_fill)
                    old = ml_s[h, 0:1, :]
                    new = jnp.maximum(old, jnp.max(scores, axis=0, keepdims=True))
                    probs = jnp.exp(scores - new)
                    scale = jnp.exp(old - new)
                    ml_s[h, 0:1, :] = new
                    ml_s[h, 1:2, :] = ml_s[h, 1:2, :] * scale + jnp.sum(
                        probs, axis=0, keepdims=True
                    )
                    part = slice(h * HEAD_DIM, (h + 1) * HEAD_DIM)
                    acc_s[part, :] = acc_s[part, :] * scale + jnp.dot(
                        vt_s[j, part, :], probs.astype(bf16), preferred_element_type=f32
                    )

        for h in range(heads):
            part = slice(h * HEAD_DIM, (h + 1) * HEAD_DIM)
            total = ml_s[h, 1:2, :]
            acc_s[part, :] = acc_s[part, :] / total
            lse_ref[line, h : h + 1, :] = ml_s[h, 0:1, :] + jnp.log(total)
        result = jnp.transpose(acc_s[...])
        o_ref[line] = result
        low_ref[line] = result.astype(bf16)


def attend(info, q, kv, qinfo):
    lines, rows, width = q.shape
    heads = width // HEAD_DIM
    length = kv.shape[0]
    key_blk = KEY_BLK
    shape = jax.ShapeDtypeStruct
    return pl.pallas_call(
        functools.partial(attend_body, lines, heads),
        out_shape=[
            shape((lines, rows, width), f32),
            shape((lines, rows, width), bf16),
            shape((lines, 8, rows), f32),
        ],
        in_specs=[SM, VM, VM, VM],
        out_specs=[VM] * 3,
        scratch_shapes=[
            pltpu.VMEM((length, width), bf16),
            pltpu.VMEM((length // key_blk, width, key_blk), bf16),
            pltpu.VMEM((width, rows), f32),
            pltpu.VMEM((heads, 8, rows), f32),
            pltpu.VMEM((heads, rows, width), bf16),
        ],
        cost_estimate=pl.CostEstimate(flops=2 * 10**9, bytes_accessed=8 * 10**6, transcendentals=4 * 10**6),
        name="attend",
    )(info, q, kv, qinfo)


def attend_back_body(lines, heads, info_ref, q_ref, kv_ref, qinfo_ref, o_ref, lse_ref, back_ref, dq_ref, dkv_ref, k_s, v_s, dk_s, dv_s, dq_s, qm_s, bm_s, delta_s):
    shard = lax.axis_index(SH)
    rows, width = q_ref.shape[1:]
    key_blk = KEY_BLK
    blocks = k_s.shape[0] // key_blk
    prompt = info_ref[1]

    @pl.loop(0, blocks)
    def _(j):
        at = pl.ds(pl.multiple_of(j * key_blk, key_blk), key_blk)
        k_s[at, :] = kv_ref[at, :width]
        v_s[at, :] = kv_ref[at, width:]
        dk_s[at, :] = jnp.zeros((key_blk, width), f32)
        dv_s[at, :] = jnp.zeros((key_blk, width), f32)

    @pl.loop(0, lines)
    def _(line):
        start = (line * 4 + shard) * rows
        queries = q_ref[line].astype(f32) * HEAD_DIM**-0.5
        back = back_ref[line].astype(f32)
        qpos = start + lax.broadcasted_iota(jnp.int32, (1, rows), 1)
        qstart, first = doc_start(line * 4 + shard, info_ref, qinfo_ref)
        picks = (
            lax.broadcasted_iota(jnp.int32, (8, width), 1) // HEAD_DIM
            == lax.broadcasted_iota(jnp.int32, (8, width), 0)
        ).astype(f32)
        delta_s[...] = contract(picks, back * o_ref[line], 1, 1, HIGH)
        for h in range(heads):
            mine = head_columns(h, queries.shape, 1)
            qm_s[h] = jnp.where(mine, queries, 0.0).astype(bf16)
            bm_s[h] = jnp.where(mine, back, 0.0).astype(bf16)
        dq_s[...] = jnp.zeros_like(dq_s)

        @pl.loop(0, (start + rows + key_blk - 1) // key_blk)
        def _(j):
            @pl.when((j * key_blk < prompt) | ((j + 1) * key_blk > first))
            def _():
                at = pl.ds(pl.multiple_of(j * key_blk, key_blk), key_blk)
                keys, values = k_s[at, :], v_s[at, :]
                ok = allowed(j, key_blk, qpos, qstart, prompt)
                dk = jnp.zeros((key_blk, width), f32)
                dv = jnp.zeros((key_blk, width), f32)
                for h in range(heads):
                    scores = contract(keys, qm_s[h], 1, 1)
                    probs = jnp.where(ok, jnp.exp(scores - lse_ref[line, h : h + 1, :]), 0.0)
                    grads = contract(values, bm_s[h], 1, 1)
                    slow = (probs * (grads - delta_s[h : h + 1, :])).astype(bf16)
                    dv = dv + jnp.dot(probs.astype(bf16), bm_s[h], preferred_element_type=f32)
                    dk = dk + jnp.dot(slow, qm_s[h], preferred_element_type=f32)
                    dq_s[h] += contract(slow, keys, 0, 0)
                dk_s[at, :] += dk
                dv_s[at, :] += dv

        total = jnp.zeros(queries.shape, f32)
        for h in range(heads):
            total = jnp.where(head_columns(h, queries.shape, 1), dq_s[h], total)
        dq_ref[line] = (total * HEAD_DIM**-0.5).astype(bf16)

    @pl.loop(0, lines)
    def _(line):
        for piece in range(4):
            at = pl.ds(pl.multiple_of((line * 4 + piece) * rows, rows), rows)
            dkv_ref[piece, line, :, :width] = dk_s[at, :].astype(bf16)
            dkv_ref[piece, line, :, width:] = dv_s[at, :].astype(bf16)


def attend_back(info, q, kv, qinfo, o, lse, back):
    lines, rows, width = q.shape
    heads = width // HEAD_DIM
    length = kv.shape[0]
    shape = jax.ShapeDtypeStruct
    return pl.pallas_call(
        functools.partial(attend_back_body, lines, heads),
        out_shape=[
            shape((lines, rows, width), bf16),
            shape((4, lines, rows, 2 * width), bf16),
        ],
        in_specs=[SM] + [VM] * 6,
        out_specs=[VM] * 2,
        scratch_shapes=[
            pltpu.VMEM((length, width), bf16),
            pltpu.VMEM((length, width), bf16),
            pltpu.VMEM((length, width), f32),
            pltpu.VMEM((length, width), f32),
            pltpu.VMEM((heads, rows, width), f32),
            pltpu.VMEM((heads, rows, width), bf16),
            pltpu.VMEM((heads, rows, width), bf16),
            pltpu.VMEM((8, rows), f32),
        ],
        cost_estimate=pl.CostEstimate(flops=5 * 10**9, bytes_accessed=12 * 10**6, transcendentals=4 * 10**6),
        name="attend_back",
    )(info, q, kv, qinfo, o, lse, back)


def finale_body(lines, n_ids, *refs):
    ins, outs = refs[:13], refs[13:]
    for k in range(3):
        outs[k][...] = ins[k][...].astype(f32) + ins[3 + k][...].astype(f32)
    for k in range(2):
        outs[3 + k][...] = ins[6 + k][...]

    @pl.when(pl.program_id(0) == 0)
    def _():
        q_sum, kv_sum, out_sum, small_ref, gain_ref = ins[8:]
        q_out, k_out, v_out, out_out, gain_out, mgain_out, vec_out, rout_out, mix_out = outs[5:]
        width = q_sum.shape[2]
        for line in range(lines):
            at = slice(line * width, (line + 1) * width)
            q_out[:, at] = q_sum[line]
            k_out[:, at] = kv_sum[line, :, :width]
            v_out[:, at] = kv_sum[line, :, width:]
        out_out[...] = out_sum[...]
        gain_out[...] = jnp.sum(gain_ref[...], axis=0)
        small = small_ref[...]
        mgain_out[...] = jnp.sum(small[0:1], axis=0)
        vec_out[...] = small[1:3]
        turned = jnp.transpose(small)
        rout_out[...] = turned[:, 3 : 3 + n_ids]
        mix_out[...] = turned[:, 3 + n_ids : 7 + n_ids]


def finale(mine, far, input_grad, layer_out, sums, n_ids):
    steps = 4
    shape = jax.ShapeDtypeStruct
    own, model = sums[2].shape
    lines = sums[0].shape[0]

    def tiled(dims, dim):
        block = tuple(d // steps if k == dim else d for k, d in enumerate(dims))
        return pl.BlockSpec(block, lambda i: tuple(i if k == dim else 0 for k in range(2)))

    def whole(dims):
        return pl.BlockSpec(dims, lambda i: (0,) * len(dims))

    wide = [tiled(mine[0].shape, 1), tiled(mine[1].shape, 1), tiled(mine[2].shape, 0)]
    rows = [tiled(input_grad.shape, 0), tiled(layer_out.shape, 0)]
    small = [(own, model)] * 4 + [(model,), (model,), (2, model), (model, n_ids), (model, 4)]
    return pl.pallas_call(
        functools.partial(finale_body, lines, n_ids),
        grid=(steps,),
        out_shape=[shape(m.shape, f32) for m in mine]
        + [shape(input_grad.shape, f32), shape(layer_out.shape, bf16)]
        + [shape(d, f32) for d in small],
        in_specs=wide + wide + rows + [whole(x.shape) for x in sums],
        out_specs=wide + rows + [whole(d) for d in small],
        cost_estimate=pl.CostEstimate(flops=10**7, bytes_accessed=10**7, transcendentals=0),
        name="finale",
    )(*mine, *far, input_grad, layer_out, *sums)


def swap(x, axis, partner):
    return lax.ppermute(x, axis, [(i, partner(i)) for i in range(lax.axis_size(axis))])


def fast_shards(
    hidden_in,
    segment_ids,
    routes,
    attn_gain,
    w_query,
    w_key,
    w_value,
    w_out,
    moe_gain,
    w_router,
    const_mix,
    const_vec,
    w_gate,
    w_up,
    w_down,
    out_grad,
):
    rows, model = hidden_in.shape
    lines = lax.axis_size(EX)
    line, shard = lax.axis_index(EX), lax.axis_index(SH)
    width = model // lines
    seg = segment_ids[0]
    length = seg.shape[0]

    w_qkv = jnp.stack([w_query, w_key, w_value])
    w_mine = lax.dynamic_slice_in_dim(w_qkv, line * width, width, axis=2)
    w_mine = jnp.concatenate([w_mine[1], w_mine[2], w_mine[0]], axis=1)
    attn_in, q, kv_all = front(hidden_in, w_mine, attn_gain[None])
    attn_in = attn_in.reshape(lines * rows, model)
    kv_all, w_out_b, w_qkv = lax.optimization_barrier((kv_all, w_out, w_qkv))
    wo_far = swap(w_out_b, SH, lambda i: i ^ 2)
    w_far = swap(w_qkv, SH, lambda i: i ^ 2)
    kv_all = kv_all.reshape(length, 2 * width)
    starts = jnp.sum(
        (seg[None, :] < jnp.arange(DOCS, dtype=jnp.int32)[:, None]).astype(jnp.int32),
        axis=1,
        dtype=jnp.int32,
    )
    qinfo = seg.reshape(length // rows, rows)
    info = jnp.concatenate([starts, qinfo[:, 0]])
    attn_vec, attn_heads, lse = attend(info, q, kv_all, qinfo)
    n_ids = w_router.shape[1]
    small_w = jnp.pad(
        jnp.concatenate([w_router, const_mix], axis=1), ((0, 0), (0, 124 - n_ids))
    )
    gain_two = moe_gain[None]
    recv_rows, recv_grads, weights, wo_full, resid_one, table, place, attn_low = run_parts(
        [
            route(
                attn_heads, hidden_in, gain_two, small_w, routes, out_grad, w_out[None], wo_far[None], w_qkv, w_far, n_ids
            )
        ],
        2,
        "route",
    )
    weights = weights.reshape(3, model, model)
    wo_full = wo_full.reshape(model, model)
    slots = lines * CAP

    expert_out, input_back, *terms = expert(
        recv_rows.reshape(slots, model), recv_grads.reshape(slots, model), w_gate[0], w_up[0], w_down[0]
    )
    returned, input_ret, *sums = run_parts(
        [
            exchange(EX, SWAP, expert_out.reshape(lines, CAP, model)),
            exchange(EX, SWAP, input_back.reshape(lines, CAP, model)),
        ]
        + [core_sum(term) for term in terms],
        4,
        "combine",
    )
    far = [swap(there, SH, lambda i: i ^ 2) for there in sums[1::2]]
    mine = [(x.astype(f32) + y.astype(f32)).astype(bf16) for x, y in zip(sums[0::2], far)]

    back_heads, layer_out, resid_grad, out_term, packed = run_parts(
        [
            to_heads(
                returned, input_ret, place, table, resid_one, attn_low, out_grad, gain_two, small_w.T, const_vec, wo_full, n_ids
            )
        ],
        5,
        "to_heads",
    )
    back_heads, mine[2] = lax.optimization_barrier((back_heads, mine[2]))
    cross = lambda x: swap(x, GR, lambda i: 1 - i)
    down_far = cross(mine[2])
    dq, dkv = attend_back(info, q, kv_all, qinfo, attn_vec, lse, back_heads)
    dkv, *mine[:2] = lax.optimization_barrier((dkv, *mine[:2]))
    group_far = [cross(mine[0]), cross(mine[1]), down_far]
    input_grad, *sums = run_parts(
        [
            tail(
                dkv, dq, attn_in, weights, out_term, packed, hidden_in, resid_grad, attn_gain[None]
            )
        ],
        6,
        "tail",
        pl.CostEstimate(flops=2 * 10**10, bytes_accessed=10**8, transcendentals=0),
    )
    gate, up, down, input_grad, layer_out, *grads, gain, gain_two, vecs, router, mix = finale(
        mine, group_far, input_grad, layer_out, sums, n_ids
    )
    return (
        layer_out,
        input_grad,
        gain,
        *grads,
        gain_two,
        router,
        mix,
        vecs,
        gate[None],
        up[None],
        down[None],
    )


def solution(mesh):
    placed = (
        P((GR, EX, SH), None),
        P(GR, None),
        P((GR, EX, SH), None),
        P(),
        P(SH, None),
        P(SH, None),
        P(SH, None),
        P(SH, None),
        P(),
        P(),
        P(),
        P(),
        P(EX, None, None),
        P(EX, None, None),
        P(EX, None, None),
        P((GR, EX, SH), None),
    )
    sizes = dict(mesh.shape)
    lines = sizes[EX]
    fast = (sizes[GR], sizes[SH], lines) == (2, 4, 4)
    return jax.shard_map(
        fast_shards if fast else shards,
        mesh=mesh,
        in_specs=placed,
        out_specs=(
            P((GR, EX, SH), None),
            P((GR, EX, SH), None),
            P(),
            P((EX, SH), None),
            P((EX, SH), None),
            P((EX, SH), None),
            P((EX, SH), None),
            P(),
            P(),
            P(),
            P(),
            P(EX, SH, None),
            P(EX, SH, None),
            P(EX, SH, None),
        ),
        check_vma=False,
    )
```

```python
import functools

import jax
import jax.numpy as jnp
from jax import lax
from jax.experimental import pallas as pl
from jax.experimental.pallas import tpu as pltpu
from jax.sharding import PartitionSpec as P

HEADS = 12
HEAD_DIM = 64
CAP = 48
DOCS = 9
KEY_BLK = 256
EX, SH, GR = ("expert", "shard", "group")
GATHER, GATHER_SUM, SWAP, SWAP_SUM = range(4)


neg_fill = -1e30
norm_eps = 1e-05
bf16 = jnp.bfloat16
f32 = jnp.float32
VM = pl.BlockSpec(memory_space=pltpu.VMEM)
SM = pl.BlockSpec(memory_space=pltpu.SMEM)
HIGH = lax.Precision.HIGHEST


def contract(a, b, da, db, precision=None):
    return lax.dot_general(
        a, b, (((da,), (db,)), ((), ())), preferred_element_type=f32, precision=precision
    )


def dense32(left_side, right_side):
    return jnp.dot(left_side, right_side, precision=lax.Precision.HIGHEST)


def allowed_mask(query_pos, query_seg, key_pos, key_seg):
    same_doc = (key_seg[None, :] == query_seg[:, None]) | (key_seg[None, :] == 0)
    return same_doc & (key_pos[None, :] <= query_pos[:, None])


def rms_back(inputs, inverse, gain_vec, upstream):
    scaled = upstream * gain_vec
    return inverse * scaled - inputs * inverse**3 * jnp.mean(scaled * inputs, axis=1, keepdims=True)


def block_scores(query_blk, keys_blk, score_scale):
    return (
        jnp.einsum("qhd,khd->hqk", query_blk, keys_blk, preferred_element_type=jnp.float32)
        * score_scale
    )


def grad_pieces(
    query_blk, back_blk, keys_blk, values_blk, norm_blk, delta_blk, key_mask, score_scale
):
    scores = block_scores(query_blk, keys_blk, score_scale)
    prob_rows = jnp.where(key_mask[None], jnp.exp(scores - norm_blk[:, :, None]), 0.0)
    prob_grad = jnp.einsum("qhd,khd->hqk", back_blk, values_blk, preferred_element_type=jnp.float32)
    score_low = (prob_rows * (prob_grad - delta_blk[:, :, None])).astype(jnp.bfloat16)
    return (prob_rows.astype(jnp.bfloat16), score_low)


def shards(
    hidden_in,
    segment_ids,
    routes,
    attn_gain,
    w_query,
    w_key,
    w_value,
    w_out,
    moe_gain,
    w_router,
    const_mix,
    const_vec,
    w_gate,
    w_up,
    w_down,
    out_grad,
):
    tok_rows, model_width = hidden_in.shape
    score_scale = HEAD_DIM ** (-0.5)
    inner_rank = lax.axis_index((EX, SH))
    seg_group = segment_ids[0]
    group_len = seg_group.shape[0]
    key_block = min(512, group_len)
    num_blocks = group_len // key_block
    row_start = inner_rank * tok_rows
    own_pos = row_start + jnp.arange(tok_rows, dtype=jnp.int32)
    own_seg = lax.dynamic_slice_in_dim(seg_group, row_start, tok_rows)
    wq_full, wk_full, wv_full, wo_full = (
        lax.all_gather(w_query, SH, axis=0, tiled=True),
        lax.all_gather(w_key, SH, axis=0, tiled=True),
        lax.all_gather(w_value, SH, axis=0, tiled=True),
        lax.all_gather(w_out, SH, axis=0, tiled=True),
    )
    inputs = hidden_in.astype(jnp.float32)
    inv_one = lax.rsqrt(jnp.mean(inputs * inputs, axis=1, keepdims=True) + norm_eps)
    normed_one = inputs * inv_one
    attn_in = (normed_one * attn_gain).astype(jnp.bfloat16)
    queries = jnp.dot(attn_in, wq_full, preferred_element_type=jnp.float32).astype(jnp.bfloat16)
    keys_own = jnp.dot(attn_in, wk_full, preferred_element_type=jnp.float32).astype(jnp.bfloat16)
    values_own = jnp.dot(attn_in, wv_full, preferred_element_type=jnp.float32).astype(jnp.bfloat16)
    keys_all, values_all = (
        lax.all_gather(keys_own, (EX, SH), axis=0, tiled=True),
        lax.all_gather(values_own, (EX, SH), axis=0, tiled=True),
    )
    query_heads = queries.reshape(tok_rows, HEADS, HEAD_DIM)

    def fetch_block(source, block_index):
        return lax.dynamic_slice_in_dim(source, block_index * key_block, key_block).reshape(
            key_block, HEADS, HEAD_DIM
        )

    def block_mask(block_index):
        key_pos = block_index * key_block + jnp.arange(key_block, dtype=jnp.int32)
        key_seg = lax.dynamic_slice_in_dim(seg_group, block_index * key_block, key_block)
        return allowed_mask(own_pos, own_seg, key_pos, key_seg)

    def stats_step(carry_now, block_index):
        key_mask = block_mask(block_index)

        def stats_live_block(carry_in):
            row_max, row_sum = carry_in
            scores = jnp.where(
                key_mask[None],
                block_scores(query_heads, fetch_block(keys_all, block_index), score_scale),
                neg_fill,
            )
            new_max = jnp.maximum(row_max, jnp.max(scores, axis=2))
            weights = jnp.where(key_mask[None], jnp.exp(scores - new_max[:, :, None]), 0.0)
            return (new_max, row_sum * jnp.exp(row_max - new_max) + jnp.sum(weights, axis=2))

        return (
            lax.cond(jnp.any(key_mask), stats_live_block, lambda carry_in: carry_in, carry_now),
            None,
        )

    start_max = jnp.full((HEADS, tok_rows), neg_fill, jnp.float32)
    row_max, row_sum = lax.scan(
        stats_step, (start_max, jnp.zeros_like(start_max)), jnp.arange(num_blocks)
    )[0]
    log_norm = row_max + jnp.log(row_sum)

    def output_step(running, block_index):
        key_mask = block_mask(block_index)

        def output_live_block(carry_in):
            scores = block_scores(query_heads, fetch_block(keys_all, block_index), score_scale)
            prob_rows = jnp.where(
                key_mask[None], jnp.exp(scores - log_norm[:, :, None]), 0.0
            ).astype(jnp.bfloat16)
            return carry_in + jnp.einsum(
                "hqk,khd->qhd",
                prob_rows,
                fetch_block(values_all, block_index),
                preferred_element_type=jnp.float32,
            )

        return (
            lax.cond(jnp.any(key_mask), output_live_block, lambda carry_in: carry_in, running),
            None,
        )

    zero_heads = jnp.zeros((tok_rows, HEADS, HEAD_DIM), jnp.float32)
    attn_sum = lax.scan(output_step, zero_heads, jnp.arange(num_blocks))[0]
    attn_low = attn_sum.reshape(tok_rows, model_width).astype(jnp.bfloat16)
    resid_one = inputs + jnp.dot(attn_low, wo_full, preferred_element_type=jnp.float32)
    inv_two = lax.rsqrt(jnp.mean(resid_one * resid_one, axis=1, keepdims=True) + norm_eps)
    normed_two = resid_one * inv_two
    moe_in = normed_two * moe_gain
    moe_low = moe_in.astype(jnp.bfloat16)
    n_ids = w_router.shape[1]
    local_experts = w_gate.shape[0]
    owners = lax.axis_size(EX)
    ffn_count = local_experts * owners
    id_table = jnp.arange(n_ids, dtype=jnp.int32)
    route_hot = (routes[:, :, None] == id_table).astype(jnp.float32)
    logits = dense32(moe_in, w_router)
    chosen = jnp.einsum("rkn,rn->rk", route_hot, logits, precision=lax.Precision.HIGHEST)
    gate_probs = jax.nn.softmax(chosen, axis=1)
    mix_alpha = jax.nn.softmax(dense32(moe_in, const_mix).reshape(tok_rows, 2, 2), axis=2)
    const_rows = mix_alpha[:, :, 0:1] * moe_in[:, None, :] + mix_alpha[:, :, 1:2] * const_vec[None]
    ffn_mask = (routes < ffn_count).astype(jnp.float32)
    copy_mask = (routes == ffn_count + 1).astype(jnp.float32)
    const_mask = (routes[:, :, None] == ffn_count + 2 + jnp.arange(2, dtype=jnp.int32)).astype(
        jnp.float32
    )
    copy_gate = jnp.sum(gate_probs * copy_mask, axis=1)
    const_gate = jnp.sum(gate_probs[:, :, None] * const_mask, axis=1)
    ffn_gate = gate_probs * ffn_mask
    flat_ids = routes.reshape(-1)
    id_hot = (flat_ids[:, None] == id_table).astype(jnp.int32)
    earlier = jnp.cumsum(id_hot, axis=0, dtype=jnp.int32) - id_hot
    slot_num = jnp.sum(earlier * id_hot, axis=1, dtype=jnp.int32)
    slot_total = ffn_count * CAP
    slot_of_route = jnp.where(flat_ids < ffn_count, flat_ids * CAP + slot_num, slot_total)
    route_count = flat_ids.shape[0]
    route_of_slot = (
        jnp.zeros(slot_total + 1, jnp.int32)
        .at[slot_of_route]
        .set(jnp.arange(route_count, dtype=jnp.int32))[:slot_total]
    )
    slot_used = jnp.zeros(slot_total + 1, jnp.bool_).at[slot_of_route].set(True)[:slot_total]
    send_rows = jnp.where(
        slot_used[:, None], moe_low[route_of_slot // 2], jnp.zeros((), jnp.bfloat16)
    )
    recv_rows = lax.all_to_all(
        send_rows.reshape(owners, local_experts * CAP, model_width),
        EX,
        split_axis=0,
        concat_axis=0,
        tiled=True,
    )
    expert_in = recv_rows.reshape(owners, local_experts, CAP, model_width)
    gate_pre = jnp.einsum("sjcd,jdf->sjcf", expert_in, w_gate, preferred_element_type=jnp.float32)
    up_pre = jnp.einsum("sjcd,jdf->sjcf", expert_in, w_up, preferred_element_type=jnp.float32)
    gate_sigmoid = jax.nn.sigmoid(gate_pre)
    hidden_act = (gate_pre * gate_sigmoid * up_pre).astype(jnp.bfloat16)
    expert_out = jnp.einsum(
        "sjcf,jfd->sjcd", hidden_act, w_down, preferred_element_type=jnp.float32
    ).astype(jnp.bfloat16)
    returned = lax.all_to_all(
        expert_out.reshape(owners, local_experts * CAP, model_width),
        EX,
        split_axis=0,
        concat_axis=0,
        tiled=True,
    )
    padded_out = jnp.concatenate(
        [returned.reshape(slot_total, model_width), jnp.zeros((1, model_width), jnp.bfloat16)],
        axis=0,
    )
    route_out = padded_out[slot_of_route].astype(jnp.float32).reshape(tok_rows, 2, model_width)
    moe_sum = (
        jnp.sum(ffn_gate[:, :, None] * route_out, axis=1)
        + copy_gate[:, None] * moe_in
        + jnp.sum(const_gate[:, :, None] * const_rows, axis=1)
    )
    layer_out = (resid_one + moe_sum).astype(jnp.bfloat16)
    upstream = out_grad.astype(jnp.float32)
    route_dot = jnp.sum(upstream[:, None, :] * route_out, axis=2)
    copy_dot = jnp.sum(upstream * moe_in, axis=1)
    const_dot = jnp.sum(upstream[:, None, :] * const_rows, axis=2)
    gate_back_r = (
        ffn_mask * route_dot
        + copy_mask * copy_dot[:, None]
        + jnp.sum(const_mask * const_dot[:, None, :], axis=2)
    )
    chosen_grad = gate_probs * (
        gate_back_r - jnp.sum(gate_probs * gate_back_r, axis=1, keepdims=True)
    )
    logit_grad = jnp.einsum("rk,rkn->rn", chosen_grad, route_hot, precision=lax.Precision.HIGHEST)
    const_up = const_gate[:, :, None] * upstream[:, None, :]
    alpha_grad = jnp.stack(
        [
            jnp.sum(const_up * moe_in[:, None, :], axis=2),
            jnp.sum(const_up * const_vec[None], axis=2),
        ],
        axis=2,
    )
    mix_back = (
        mix_alpha * (alpha_grad - jnp.sum(mix_alpha * alpha_grad, axis=2, keepdims=True))
    ).reshape(tok_rows, 4)
    vec_grad = jnp.sum(mix_alpha[:, :, 1:2] * const_up, axis=0)
    route_weight = ffn_gate.reshape(-1)
    grad_send = (route_weight[route_of_slot][:, None] * upstream[route_of_slot // 2]).astype(
        jnp.bfloat16
    )
    grad_send = jnp.where(slot_used[:, None], grad_send, jnp.zeros((), jnp.bfloat16))
    grad_recv = lax.all_to_all(
        grad_send.reshape(owners, local_experts * CAP, model_width),
        EX,
        split_axis=0,
        concat_axis=0,
        tiled=True,
    )
    grad_recv = grad_recv.reshape(owners, local_experts, CAP, model_width)
    hidden_grad = jnp.einsum(
        "sjcd,jfd->sjcf", grad_recv, w_down, preferred_element_type=jnp.float32
    )
    down_term = jnp.einsum(
        "sjcf,sjcd->jfd", hidden_act, grad_recv, preferred_element_type=jnp.float32
    )
    gate_back = (
        hidden_grad * up_pre * gate_sigmoid * (1.0 + gate_pre * (1.0 - gate_sigmoid))
    ).astype(jnp.bfloat16)
    up_back = (hidden_grad * gate_pre * gate_sigmoid).astype(jnp.bfloat16)
    gate_term = jnp.einsum(
        "sjcd,sjcf->jdf", expert_in, gate_back, preferred_element_type=jnp.float32
    )
    up_term = jnp.einsum("sjcd,sjcf->jdf", expert_in, up_back, preferred_element_type=jnp.float32)
    input_back = (
        jnp.einsum("sjcf,jdf->sjcd", gate_back, w_gate, preferred_element_type=jnp.float32)
        + jnp.einsum("sjcf,jdf->sjcd", up_back, w_up, preferred_element_type=jnp.float32)
    ).astype(jnp.bfloat16)
    input_ret = lax.all_to_all(
        input_back.reshape(owners, local_experts * CAP, model_width),
        EX,
        split_axis=0,
        concat_axis=0,
        tiled=True,
    )
    padded_in = jnp.concatenate(
        [input_ret.reshape(slot_total, model_width), jnp.zeros((1, model_width), jnp.bfloat16)],
        axis=0,
    )
    ffn_in_grad = jnp.sum(
        padded_in[slot_of_route].astype(jnp.float32).reshape(tok_rows, 2, model_width), axis=1
    )
    moe_in_grad = (
        ffn_in_grad
        + copy_gate[:, None] * upstream
        + jnp.sum(mix_alpha[:, :, 0:1] * const_up, axis=1)
        + dense32(mix_back, const_mix.T)
        + dense32(logit_grad, w_router.T)
    )
    moe_gain_grad = jnp.sum(moe_in_grad * normed_two, axis=0)
    router_grad = dense32(moe_in.T, logit_grad)
    mix_grad = dense32(moe_in.T, mix_back)
    resid_grad = upstream + rms_back(resid_one, inv_two, moe_gain, moe_in_grad)
    branch_low = resid_grad.astype(jnp.bfloat16)
    out_proj_term = jnp.dot(attn_low.T, branch_low, preferred_element_type=jnp.float32)
    attn_back = jnp.dot(branch_low, wo_full.T, preferred_element_type=jnp.float32).astype(
        jnp.bfloat16
    )
    back_heads = attn_back.reshape(tok_rows, HEADS, HEAD_DIM)
    row_delta = jnp.sum(back_heads.astype(jnp.float32) * attn_sum, axis=2).T

    def back_step(query_acc, block_index):
        key_mask = block_mask(block_index)
        keys_blk = fetch_block(keys_all, block_index)
        values_blk = fetch_block(values_all, block_index)

        def back_live_block(running):
            prob_low, score_low = grad_pieces(
                query_heads,
                back_heads,
                keys_blk,
                values_blk,
                log_norm,
                row_delta,
                key_mask,
                score_scale,
            )
            value_part = jnp.einsum(
                "hqk,qhd->khd", prob_low, back_heads, preferred_element_type=jnp.float32
            )
            key_part = (
                jnp.einsum(
                    "hqk,qhd->khd", score_low, query_heads, preferred_element_type=jnp.float32
                )
                * score_scale
            )
            running = (
                running
                + jnp.einsum(
                    "hqk,khd->qhd", score_low, keys_blk, preferred_element_type=jnp.float32
                )
                * score_scale
            )
            return (
                running,
                (
                    key_part.reshape(key_block, model_width),
                    value_part.reshape(key_block, model_width),
                ),
            )

        def dead_block(running):
            empty_rows = jnp.zeros((key_block, model_width), jnp.float32)
            return (running, (empty_rows, empty_rows))

        return lax.cond(jnp.any(key_mask), back_live_block, dead_block, query_acc)

    query_grad32, key_terms = lax.scan(back_step, zero_heads, jnp.arange(num_blocks))
    key_grad32, value_grad32 = (
        lax.psum_scatter(
            key_terms[0].reshape(group_len, model_width).astype(jnp.bfloat16),
            (EX, SH),
            scatter_dimension=0,
            tiled=True,
        ).astype(jnp.float32),
        lax.psum_scatter(
            key_terms[1].reshape(group_len, model_width).astype(jnp.bfloat16),
            (EX, SH),
            scatter_dimension=0,
            tiled=True,
        ).astype(jnp.float32),
    )
    query_low = query_grad32.reshape(tok_rows, model_width).astype(jnp.bfloat16)
    key_low = key_grad32.astype(jnp.bfloat16)
    value_low = value_grad32.astype(jnp.bfloat16)
    query_term = jnp.dot(attn_in.T, query_low, preferred_element_type=jnp.float32)
    key_term = jnp.dot(attn_in.T, key_low, preferred_element_type=jnp.float32)
    value_term = jnp.dot(attn_in.T, value_low, preferred_element_type=jnp.float32)
    attn_in_grad = (
        jnp.dot(query_low, wq_full.T, preferred_element_type=jnp.float32)
        + jnp.dot(key_low, wk_full.T, preferred_element_type=jnp.float32)
        + jnp.dot(value_low, wv_full.T, preferred_element_type=jnp.float32)
    )
    attn_gain_grad = jnp.sum(attn_in_grad * normed_one, axis=0)
    input_grad = resid_grad + rms_back(inputs, inv_one, attn_gain, attn_in_grad)
    query_part, key_part_w, value_part_w, out_part = (
        lax.psum_scatter(
            query_term.astype(jnp.bfloat16), (EX, SH), scatter_dimension=0, tiled=True
        ).astype(jnp.float32),
        lax.psum_scatter(
            key_term.astype(jnp.bfloat16), (EX, SH), scatter_dimension=0, tiled=True
        ).astype(jnp.float32),
        lax.psum_scatter(
            value_term.astype(jnp.bfloat16), (EX, SH), scatter_dimension=0, tiled=True
        ).astype(jnp.float32),
        lax.psum_scatter(
            out_proj_term.astype(jnp.bfloat16), (EX, SH), scatter_dimension=0, tiled=True
        ).astype(jnp.float32),
    )
    gate_part, up_part, down_part = (
        lax.psum_scatter(
            gate_term.astype(jnp.bfloat16), SH, scatter_dimension=1, tiled=True
        ).astype(jnp.float32),
        lax.psum_scatter(
            up_term.astype(jnp.bfloat16), SH, scatter_dimension=1, tiled=True
        ).astype(jnp.float32),
        lax.psum_scatter(
            down_term.astype(jnp.bfloat16), SH, scatter_dimension=1, tiled=True
        ).astype(jnp.float32),
    )
    summed = (
        lax.psum(query_part.astype(jnp.bfloat16), GR).astype(jnp.float32),
        lax.psum(key_part_w.astype(jnp.bfloat16), GR).astype(jnp.float32),
        lax.psum(value_part_w.astype(jnp.bfloat16), GR).astype(jnp.float32),
        lax.psum(out_part.astype(jnp.bfloat16), GR).astype(jnp.float32),
        lax.psum(gate_part.astype(jnp.bfloat16), GR).astype(jnp.float32),
        lax.psum(up_part.astype(jnp.bfloat16), GR).astype(jnp.float32),
        lax.psum(down_part.astype(jnp.bfloat16), GR).astype(jnp.float32),
    )
    small_sums = lax.psum(
        (attn_gain_grad, moe_gain_grad, router_grad, mix_grad, vec_grad),
        (GR, EX, SH),
    )
    return (
        layer_out,
        input_grad,
        small_sums[0],
        summed[0],
        summed[1],
        summed[2],
        summed[3],
        small_sums[1],
        small_sums[2],
        small_sums[3],
        small_sums[4],
        summed[4],
        summed[5],
        summed[6],
    )


def greet(peers):
    barrier = pltpu.get_barrier_semaphore()
    for axis, peer in peers:
        pl.semaphore_signal(
            barrier, inc=1, device_id={axis: peer}, device_id_type=pl.DeviceIdType.MESH
        )
    pl.semaphore_wait(barrier, len(peers))


def send(src, dst, sems, index, axis, peer):
    copy = pltpu.make_async_remote_copy(
        src_ref=src,
        dst_ref=dst,
        send_sem=sems.at[0, index],
        recv_sem=sems.at[1, index],
        device_id={axis: peer},
        device_id_type=pl.DeviceIdType.MESH,
    )
    copy.start()
    return copy


def shard_peers():
    me = lax.axis_index(SH)
    side, core = me // 2, lax.rem(me, 2)
    return me, side, core, 2 * side + 1 - core, 2 * (1 - side) + core


class Part:
    def __init__(self, axes, ins, outs, scratch, copies, phases, specs=None):
        self.axes, self.ins, self.outs, self.scratch = axes, ins, outs, scratch
        self.copies, self.phases = copies, phases
        self.specs = specs or [VM] * len(ins)


def run_parts(parts, collective_id, name=None, cost=None):
    ins = sum([p.ins for p in parts], [])
    outs = sum([p.outs for p in parts], [])
    scratch = sum([p.scratch for p in parts], [])
    copies = sum(p.copies for p in parts)
    axes = sorted(set(sum([list(p.axes) for p in parts], [])))

    def body(*refs):
        sems = refs[-1]
        in_refs, out_refs = list(refs[: len(ins)]), list(refs[len(ins) : len(ins) + len(outs)])
        scr = list(refs[len(ins) + len(outs) : -1])
        peers = []
        for axis in axes:
            me, n = lax.axis_index(axis), lax.axis_size(axis)
            peers += [(axis, lax.rem(me + d, n)) for d in range(1, n)]
        greet(peers)
        base, running = 0, []
        for p in parts:
            take = lambda pool, k: [pool.pop(0) for _ in range(k)]
            refs_p = (take(in_refs, len(p.ins)), take(out_refs, len(p.outs)), take(scr, len(p.scratch)))
            counter = [base]

            def go(src, dst, axis, peer, counter=counter):
                counter[0] += 1
                return send(src, dst, sems, counter[0] - 1, axis, peer)

            running.append(p.phases(*refs_p, go))
            base += p.copies
        while running:
            running = [r for r in running if next(r, True) is None]

    return pl.pallas_call(
        body,
        out_shape=outs,
        in_specs=sum([p.specs for p in parts], []),
        out_specs=[VM] * len(outs),
        scratch_shapes=scratch + [pltpu.SemaphoreType.DMA((2, copies))],
        compiler_params=pltpu.CompilerParams(collective_id=collective_id, has_side_effects=True),
        cost_estimate=cost,
        name=name,
    )(*ins)


def start_swap(go, src, land, axis, gather):
    me, n = lax.axis_index(axis), lax.axis_size(axis)
    started = []
    for d in range(1, n):
        peer = lax.rem(me + d, n)
        started.append(go(src if gather else src.at[peer], land.at[me], axis, peer))
    land[me] = src[...] if gather else src[me]
    return started


def total_of(land, n):
    total = land[0].astype(f32)
    for j in range(1, n):
        total = total + land[j].astype(f32)
    return total


def exchange(axis, kind, x):
    n = lax.axis_size(axis)
    gather, summed = kind in (GATHER, GATHER_SUM), kind in (GATHER_SUM, SWAP_SUM)
    piece = x.shape if gather else x.shape[1:]
    shape = jax.ShapeDtypeStruct
    outs = [shape(piece, f32) if summed else shape((n,) + piece, x.dtype)]
    scratch = [pltpu.VMEM((n,) + piece, x.dtype)] if summed else []

    def phases(ins, outs, scr, go):
        land = scr[0] if summed else outs[0]
        started = start_swap(go, ins[0], land, axis, gather)
        yield
        for copy in started:
            copy.wait()
        if summed:
            outs[0][...] = total_of(land, n)

    return Part([axis], [x], outs, scratch, n - 1, phases)


def tree_gather(x):
    lines = x.shape[0]
    cuts = [(0, lines // 2), (lines // 2, lines)] if lines > 1 else [(0, 1)]
    cuts = [pl.ds(lo, hi - lo) for lo, hi in cuts]

    def phases(ins, outs, scr, go):
        x_ref, out_ref = ins[0], outs[0]
        me, _, _, near, far = shard_peers()
        across = [go(x_ref.at[c], out_ref.at[c, me], SH, far) for c in cuts]
        own = go(x_ref, out_ref.at[:, me], SH, near)
        out_ref[:, me] = x_ref[...]
        yield
        handed = []
        for c, copy in zip(cuts, across):
            copy.wait_recv()
            handed.append(go(out_ref.at[c, far], out_ref.at[c, far], SH, near))
        yield
        for copy in across:
            copy.wait_send()
        own.wait()
        for copy in handed:
            copy.wait()

    shape = (lines, 4) + x.shape[1:]
    return Part([SH], [x], [jax.ShapeDtypeStruct(shape, x.dtype)], [], 2 * len(cuts) + 1, phases)


def core_sum(x):
    piece = x.shape[1:]
    shape = jax.ShapeDtypeStruct

    def phases(ins, outs, scr, go):
        x_ref, (here, there), (land, kept, sems) = ins[0], outs, scr
        near = shard_peers()[3]
        sent = [go(x_ref.at[3], land.at[1], SH, near), go(x_ref.at[2], land.at[0], SH, near)]
        local = [pltpu.make_async_copy(x_ref.at[k], kept.at[k], sems.at[k]) for k in range(2)]
        for copy in local:
            copy.start()
        yield
        for k, out in ((1, there), (0, here)):
            sent[1 - k].wait()
            local[k].wait()
            out[...] = (kept[k].astype(f32) + land[k].astype(f32)).astype(bf16)

    return Part(
        [SH],
        [x],
        [shape(piece, bf16)] * 2,
        [pltpu.VMEM((2,) + piece, bf16)] * 2 + [pltpu.SemaphoreType.DMA((2,))],
        2,
        phases,
        [pl.BlockSpec(memory_space=pl.ANY)],
    )


class Tree:
    copies = 3

    @staticmethod
    def scratch(piece):
        return [pltpu.VMEM((2,) + piece, bf16)] + [pltpu.VMEM(piece, bf16)] * 2

    def __init__(self, x, scr, go):
        self.x, (self.land, self.mine, self.got), self.go = x, scr, go
        self.me, self.side, self.core, self.near, self.far = shard_peers()
        other = 2 * (1 - self.side) + 1 - self.core
        self.first = [
            go(x.at[other], self.land.at[0], SH, self.near),
            go(x.at[self.near], self.land.at[1], SH, self.near),
        ]

    def across(self):
        self.first[0].wait_recv()
        self.mine[...] = (self.x[self.far].astype(f32) + self.land[0].astype(f32)).astype(bf16)
        self.second = self.go(self.mine, self.got, SH, self.far)

    def result(self):
        self.first[1].wait_recv()
        total = self.x[self.me].astype(f32) + self.land[1].astype(f32)
        self.second.wait_recv()
        return total + self.got[...].astype(f32)

    def close(self):
        for copy in (*self.first, self.second):
            copy.wait_send()


def slot_places(ids, lines, slots):
    rows = ids.shape[0]
    lane = lax.broadcasted_iota(jnp.int32, (rows, 128), 1)
    hot = [lane == column(ids, k) for k in range(2)]
    before = (
        lax.broadcasted_iota(jnp.int32, (rows, rows), 0)
        > lax.broadcasted_iota(jnp.int32, (rows, rows), 1)
    ).astype(bf16)
    named = jnp.where(hot[0] | hot[1], 1.0, 0.0).astype(bf16)
    earlier = jnp.dot(before, named, preferred_element_type=f32)
    slot_at = lax.broadcasted_iota(jnp.int32, (rows, slots), 1).astype(f32)
    place = []
    for k in range(2):
        number = jnp.sum(jnp.where(hot[k], earlier, 0.0), axis=1, keepdims=True)
        wanted = column(ids, k).astype(f32) * CAP + number
        wanted = jnp.where(column(ids, k) < lines, wanted, -1.0)
        place.append(jnp.where(slot_at == wanted, 1.0, 0.0))
    return place


def front(hidden, w_mine, gain, routes, out_grad):
    rows, model = hidden.shape
    lines = lax.axis_size(EX)
    width = model // lines
    shape = jax.ShapeDtypeStruct
    last = lines - 1

    slots = lines * CAP

    def body(hid_ref, w_ref, gain_ref, ids_ref, up_ref, attn_ref, q_ref, kv_ref, place_ref, rows_out, land, w_all, kv_own, rows_s, sems):
        line_me = lax.axis_index(EX)
        me, _, _, near, far = shard_peers()
        left, right = jnp.maximum(line_me - 1, 0), jnp.minimum(line_me + 1, last)
        greet(
            [(EX, lax.rem(line_me + d, lines)) for d in range(1, lines)]
            + [(SH, lax.rem(me + d, 4)) for d in range(1, 4)]
        )

        def copy(src, dst, index, axis, peer):
            return pltpu.make_async_remote_copy(
                src_ref=src,
                dst_ref=dst,
                send_sem=sems.at[0, index],
                recv_sem=sems.at[1, index],
                device_id={axis: peer},
                device_id_type=pl.DeviceIdType.MESH,
            )

        def relay(step, way):
            block = line_me - step if way == 0 else line_me + step
            block = jnp.clip(block, 0, last)
            src = hid_ref if step == 0 else land.at[block]
            return copy(src, land.at[block], last * way + step, EX, right if way == 0 else left)

        def sends(step, way):
            if way == 0:
                return (line_me < last) & (line_me - step >= 0)
            return (line_me > 0) & (line_me + step <= last)

        def comes(step, way):
            return line_me - 1 - step >= 0 if way == 0 else line_me + 1 + step <= last

        def source(step, way):
            line = line_me - 1 - step if way == 0 else line_me + 1 + step
            return jnp.clip(line, 0, last)

        def arrival(step, way):
            line = source(step, way)
            return copy(land.at[line], land.at[line], last * way + step, EX, right if way == 0 else left)

        base = 2 * last
        for way in range(2):

            @pl.when(sends(0, way))
            def _():
                relay(0, way).start()

        w_far = copy(w_ref, w_all.at[me], base, SH, far)
        w_near = copy(w_ref, w_all.at[me], base + 1, SH, near)
        w_pass = copy(w_all.at[far], w_all.at[far], base + 2, SH, near)
        w_far.start()
        w_near.start()
        w_all[me] = w_ref[...]
        ids = ids_ref[...]
        place = slot_places(ids, lines, slots)
        for k in range(2):
            place_ref[k] = place[k].astype(bf16)
        either = (place[0] + place[1]).astype(bf16)
        rows_s[...] = contract(either, up_ref[...], 0, 0).astype(bf16).reshape(lines, CAP, model)
        base += 3
        kv_far = lambda line: copy(kv_own.at[line], kv_ref.at[line, me], base + line, SH, far)
        kv_near = lambda line: copy(
            kv_own.at[line], kv_ref.at[line, me], base + lines + line, SH, near
        )
        kv_pass = lambda line: copy(
            kv_ref.at[line, far], kv_ref.at[line, far], base + 2 * lines + line, SH, near
        )

        def project(line, x):
            inputs = x.astype(f32)
            inv = lax.rsqrt(jnp.mean(inputs * inputs, axis=1, keepdims=True) + norm_eps)
            attn_in = (inputs * inv * gain_ref[...]).astype(bf16)
            attn_ref[line] = attn_in
            value = jnp.dot(
                attn_in, w_all[...].reshape(model, 3 * width), preferred_element_type=f32
            ).astype(bf16)
            kv_own[line] = value[:, : 2 * width]
            kv_far(line).start()
            kv_near(line).start()
            kv_ref[line, me] = value[:, : 2 * width]
            q_ref[line] = value[:, 2 * width :]

        def hand(line):
            kv_far(line).wait_recv()
            kv_pass(line).start()

        w_far.wait_recv()
        w_pass.start()
        w_near.wait_recv()
        w_pass.wait_recv()
        project(line_me, hid_ref[...])
        for step in range(last):
            for way in range(2):

                @pl.when(comes(step, way))
                def _():
                    arrival(step, way).wait_recv()

                if step + 1 < last:

                    @pl.when(sends(step + 1, way))
                    def _():
                        relay(step + 1, way).start()

            for way in range(2):

                @pl.when(comes(step, way))
                def _():
                    line = source(step, way)
                    project(line, land[line])

            if step == last - 2:
                first = base + 3 * lines
                ups = []
                for d in range(1, lines):
                    peer = lax.rem(line_me + d, lines)
                    ups.append(copy(rows_s.at[peer], rows_out.at[line_me], first + d - 1, EX, peer))
                    ups[-1].start()
                rows_out[line_me] = rows_s[line_me]
            if step == 0:
                hand(line_me)
            else:
                for way in range(2):

                    @pl.when(comes(step - 1, way))
                    def _():
                        hand(source(step - 1, way))

        for way in range(2):

            @pl.when(comes(last - 1, way))
            def _():
                hand(source(last - 1, way))

        for way in range(2):
            for step in range(last):

                @pl.when(sends(step, way))
                def _():
                    relay(step, way).wait_send()

        w_far.wait_send()
        w_near.wait_send()
        w_pass.wait_send()
        for line in range(lines):
            kv_far(line).wait_send()
            kv_near(line).wait()
            kv_pass(line).wait()
        for up in ups:
            up.wait()

    return pl.pallas_call(
        body,
        out_shape=[
            shape((lines, rows, model), bf16),
            shape((lines, rows, width), bf16),
            shape((lines, 4, rows, 2 * width), bf16),
            shape((2, rows, slots), bf16),
            shape((lines, CAP, model), bf16),
        ],
        in_specs=[VM] * 5,
        out_specs=[VM] * 5,
        scratch_shapes=[
            pltpu.VMEM((lines, rows, model), bf16),
            pltpu.VMEM((4, rows, 3 * width), bf16),
            pltpu.VMEM((lines, rows, 2 * width), bf16),
            pltpu.VMEM((lines, CAP, model), bf16),
            pltpu.SemaphoreType.DMA((2, 3 * last + 3 + 3 * lines)),
        ],
        compiler_params=pltpu.CompilerParams(collective_id=0, has_side_effects=True),
        name="front",
    )(hidden, w_mine, gain, routes, out_grad)


def column(x, k):
    return x[:, k : k + 1]


def core_share(go, own, far, out):
    me, _, _, near, other = shard_peers()
    sent = [go(own, out.at[:, me], SH, near), go(far, out.at[:, other], SH, near)]
    out[:, me] = own[...]
    out[:, other] = far[...]
    return sent


def route(heads, hidden, gain, small_w, routes, place, wo, wo_far, n_ids):
    lines, rows, width = heads.shape
    model = lines * width
    slots = lines * CAP
    shape = jax.ShapeDtypeStruct

    def phases(ins, outs, scr, go):
        heads_ref, hid_ref, gain_ref, small_ref, routes_ref, place_ref, wo_ref, wof_ref = ins
        rows_out, wo_all, resid_ref, table_ref, low_ref = outs
        land, rows_s = scr
        swaps = start_swap(go, heads_ref, land, EX, False)
        swaps += core_share(go, wo_ref, wof_ref, wo_all)
        ids = routes_ref[...]
        lane = lax.broadcasted_iota(jnp.int32, (rows, 128), 1)
        hot = [lane == column(ids, k) for k in range(2)]
        place = [place_ref[k].astype(f32) for k in range(2)]
        either = place_ref[0] + place_ref[1]
        for copy in swaps:
            copy.wait()
        for line in range(lines):
            low_ref[:, line * width : (line + 1) * width] = land[line]
        w_out = wo_all[...].reshape(model, model)
        resid = hid_ref[...].astype(f32) + jnp.dot(
            low_ref[...], w_out, preferred_element_type=f32
        )
        resid_ref[...] = resid
        inv = lax.rsqrt(jnp.mean(resid * resid, axis=1, keepdims=True) + norm_eps)
        moe_in = resid * inv * gain_ref[...]
        small = jnp.dot(moe_in, small_ref[...], preferred_element_type=f32, precision=HIGH)
        chosen = [jnp.sum(jnp.where(h, small, 0.0), axis=1, keepdims=True) for h in hot]
        top = jnp.maximum(chosen[0], chosen[1])
        powers = [jnp.exp(c - top) for c in chosen]
        gates = [p / (powers[0] + powers[1]) for p in powers]
        weight = place[0] * gates[0] + place[1] * gates[1]
        weight = contract(weight, jnp.ones((rows, 128), f32), 0, 0, HIGH)[:, 0:1]
        high = weight.astype(bf16)
        low = (weight - high.astype(f32)).astype(bf16)
        slot_lane = lax.broadcasted_iota(jnp.int32, (slots, 128), 1)
        extra = jnp.where(slot_lane == 0, high, jnp.where(slot_lane == 1, low, jnp.zeros_like(low)))
        rows_s[:, :, :model] = (
            contract(either, moe_in.astype(bf16), 0, 0).astype(bf16).reshape(lines, CAP, model)
        )
        rows_s[:, :, model:] = extra.reshape(lines, CAP, 128)
        row_swap = start_swap(go, rows_s, rows_out, EX, False)
        table = jnp.zeros((rows, 128), f32)
        entries = list(gates)
        for j in range(2):
            pair = [column(small, n_ids + 2 * j + k) for k in range(2)]
            top = jnp.maximum(pair[0], pair[1])
            powers = [jnp.exp(c - top) for c in pair]
            entries += [p / (powers[0] + powers[1]) for p in powers]
        entries += [column(ids, k).astype(f32) for k in range(2)]
        for k, entry in enumerate(entries):
            table = jnp.where(lane == k, entry, table)
        table_ref[...] = table
        for copy in row_swap:
            copy.wait()
        yield

    ins = [heads, hidden, gain, small_w, routes, place, wo, wo_far]
    outs = [
        shape((lines, CAP, model + 128), bf16),
        shape((1, 4, model // 4, model), bf16),
        shape((rows, model), f32),
        shape((rows, 128), f32),
        shape((rows, model), bf16),
    ]
    scratch = [
        pltpu.VMEM((lines, rows, width), bf16),
        pltpu.VMEM((lines, CAP, model + 128), bf16),
    ]
    return Part([EX, SH], ins, outs, scratch, 2 * (lines - 1) + 2, phases)


def share_weights(own, far):
    def phases(ins, outs, scr, go):
        copies = core_share(go, ins[0], ins[1], outs[0])
        yield
        for copy in copies:
            copy.wait()

    dims = (own.shape[0], 4) + own.shape[1:]
    return Part([SH], [own, far], [jax.ShapeDtypeStruct(dims, bf16)], [], 2, phases)


def to_heads(returned, input_ret, place, table, resid, low, out_grad, gain, small_t, const_vec, wo, n_ids):
    rows, model = resid.shape
    lines = returned.shape[0]
    width = model // lines
    own = rows // lines
    slots = lines * CAP
    shape = jax.ShapeDtypeStruct

    def phases(ins, outs, scr, go):
        ret_ref, iret_ref, place_ref, table_ref, resid_ref, low_ref, up_ref, gain_ref, st_ref, vec_ref, wo_ref = ins
        heads_out, layer_ref, rgrad_ref, term_ref, packed_ref = outs
        (back_s,) = scr
        table = table_ref[...]
        gates = [column(table, k) for k in range(2)]
        alpha = [[column(table, 2 + 2 * j + k) for k in range(2)] for j in range(2)]
        ids = [column(table, 6 + k) for k in range(2)]
        vecs = [vec_ref[j : j + 1, :] for j in range(2)]
        resid = resid_ref[...]
        upstream = up_ref[...].astype(f32)
        inv = lax.rsqrt(jnp.mean(resid * resid, axis=1, keepdims=True) + norm_eps)
        normed = resid * inv
        moe_in = normed * gain_ref[...]
        returned = ret_ref[...].reshape(slots, model)
        total = lambda x: jnp.sum(x, axis=1, keepdims=True)
        flag = lambda x: jnp.where(x, 1.0, 0.0)
        copy_dot = total(upstream * moe_in)
        vec_dot = [total(upstream * v) for v in vecs]
        const_dot = [alpha[j][0] * copy_dot + alpha[j][1] * vec_dot[j] for j in range(2)]
        output = resid
        backs = []
        copy_gate = jnp.zeros((rows, 1), f32)
        const_gate = [jnp.zeros((rows, 1), f32) for _ in range(2)]
        for k in range(2):
            rows_k = jnp.dot(place_ref[k], returned, preferred_element_type=f32)
            is_ffn, is_copy = flag(ids[k] < lines), flag(ids[k] == lines + 1)
            is_const = [flag(ids[k] == lines + 2 + j) for j in range(2)]
            output = output + (gates[k] * is_ffn) * rows_k
            backs.append(
                is_ffn * total(upstream * rows_k)
                + is_copy * copy_dot
                + is_const[0] * const_dot[0]
                + is_const[1] * const_dot[1]
            )
            copy_gate = copy_gate + gates[k] * is_copy
            const_gate = [const_gate[j] + gates[k] * is_const[j] for j in range(2)]
        through = copy_gate + const_gate[0] * alpha[0][0] + const_gate[1] * alpha[1][0]
        output = output + through * moe_in
        for j in range(2):
            output = output + (const_gate[j] * alpha[j][1]) * vecs[j]
        layer_ref[...] = output.astype(bf16)
        mean_back = gates[0] * backs[0] + gates[1] * backs[1]
        lane = lax.broadcasted_iota(jnp.int32, (rows, 128), 1)
        lane_f = lane.astype(f32)
        small = jnp.zeros((rows, 128), f32)
        for k in range(2):
            small = jnp.where(lane_f == ids[k], gates[k] * (backs[k] - mean_back), small)
        for j in range(2):
            grads = [const_gate[j] * copy_dot, const_gate[j] * vec_dot[j]]
            mean = alpha[j][0] * grads[0] + alpha[j][1] * grads[1]
            for k in range(2):
                small = jnp.where(
                    lane == n_ids + 2 * j + k, alpha[j][k] * (grads[k] - mean), small
                )
            small = jnp.where(lane == n_ids + 4 + j, alpha[j][1] * const_gate[j], small)
        either = place_ref[0] + place_ref[1]
        moe_grad = (
            jnp.dot(either, iret_ref[...].reshape(slots, model), preferred_element_type=f32)
            + through * upstream
            + jnp.dot(small, st_ref[...], preferred_element_type=f32, precision=HIGH)
        )
        resid_grad = upstream + rms_back(resid, inv, gain_ref[...], moe_grad)
        branch = resid_grad.astype(bf16)
        back = contract(branch, wo_ref[...], 1, 1).astype(bf16)
        for line in range(lines):
            back_s[line] = back[:, line * width : (line + 1) * width]
        swaps = start_swap(go, back_s, heads_out, EX, False)
        rgrad_ref[...] = resid_grad
        packed_ref[...] = jnp.zeros_like(packed_ref)
        packed_ref[0:1] = jnp.sum(moe_grad * normed, axis=0, keepdims=True)
        small_grad = contract(small, moe_in, 0, 0, HIGH)
        vec_grad = contract(small, upstream, 0, 0, HIGH)
        packed_ref[1:3] = vec_grad[n_ids + 4 : n_ids + 6]
        packed_ref[3 : 7 + n_ids] = small_grad[: n_ids + 4]
        term = contract(low_ref[...], branch, 0, 0).astype(bf16)
        for line in range(lines):
            for piece in range(4):
                at = (line * 4 + piece) * own
                term_ref[piece, line] = term[at : at + own]
        for copy in swaps:
            copy.wait()
        yield

    ins = [returned, input_ret, place, table, resid, low, out_grad, gain, small_t, const_vec, wo]
    outs = [
        shape((lines, rows, width), bf16),
        shape((rows, model), bf16),
        shape((rows, model), f32),
        shape((4, lines, own, model), bf16),
        shape((-(-(7 + n_ids) // 8) * 8, model), f32),
    ]
    return Part([EX], ins, outs, [pltpu.VMEM((lines, rows, width), bf16)], lines - 1, phases)


def tail(dkv, dq, attn_in, weights, out_term, packed, hidden, resid_grad, gain):
    lines, rows, width = dq.shape
    model = lines * width
    own = rows // lines
    groups = lax.axis_size(GR)
    shape = jax.ShapeDtypeStruct
    vmem = pltpu.VMEM
    tok = lines * rows
    few = lines // 2
    dkv_piece, q_piece = (few, rows, 2 * width), (lines, own, width)
    kv_piece, o_piece = (lines, own, 2 * width), (lines, own, model)
    part_dims = (width, 2 * width, model)

    def phases(ins, outs, scr, go):
        lo_ref, hi_ref, dq_ref, attn_ref, w_ref, o_ref, packed_ref, hid_ref, resid_ref, gain_ref = ins
        input_ref, q_out, kv_out, out_out, packed_out, gain_out = outs
        scr = list(scr)
        take = lambda k: [scr.pop(0) for _ in range(k)]
        lo_scr, hi_scr, q_scr, kvw_scr, o_scr = take(3), take(3), take(3), take(3), take(3)
        own_kv, q_t, kv_t, dq_all, dkv_all, dq_full = take(6)
        kv_sems = take(1)[0]
        sums, lands, halves, gots = take(3), take(3), take(3), take(3)
        pk_l, pk_s, pk_g = take(3)
        mid_l, mid_s = take(2)
        gn_l, gn_s, gn_g, gn_0, gn_1, gn_2 = take(6)
        me = lax.axis_index(SH)

        line_me = lax.axis_index(EX)
        kv_trees = [Tree(lo_ref, lo_scr, go), Tree(hi_ref, hi_scr, go)]

        def kv_copy(sender, target):
            return pltpu.make_async_remote_copy(
                src_ref=own_kv.at[target],
                dst_ref=dkv_all.at[sender],
                send_sem=kv_sems.at[0, target],
                recv_sem=kv_sems.at[1, sender],
                device_id={EX: target},
                device_id_type=pl.DeviceIdType.MESH,
            )

        def push_kv(k):
            own_kv[k * few : (k + 1) * few] = kv_trees[k].result().astype(bf16)
            for target in range(k * few, (k + 1) * few):

                @pl.when(line_me != target)
                def _():
                    kv_copy(line_me, jnp.int32(target)).start()

                @pl.when(line_me == target)
                def _():
                    dkv_all[target] = own_kv[target]

        dq_swap = start_swap(go, dq_ref, dq_all, EX, False)
        o_tree = Tree(o_ref, o_scr, go)
        pk1 = start_swap(go, packed_ref, pk_l, EX, True)

        def term(rows_ref, out):
            value = contract(attn_ref[...], rows_ref[...].reshape(tok, rows_ref.shape[-1]), 0, 0)
            value = value.astype(bf16)
            for line in range(lines):
                for piece in range(4):
                    at = (line * 4 + piece) * own
                    out[piece, line] = value[at : at + own]

        for tree in kv_trees:
            tree.across()
        term(dq_ref, q_t)
        o_tree.across()
        q_tree = Tree(q_t, q_scr, go)
        trees = [q_tree, None, o_tree]

        def lines_out(k):
            sums[k][...] = trees[k].result().astype(bf16)
            return start_swap(go, sums[k], lands[k], EX, False)

        push_kv(0)
        push_kv(1)
        o_lines = lines_out(2)
        q_tree.across()
        term(own_kv, kv_t)
        kvw_tree = Tree(kv_t, kvw_scr, go)
        trees[1] = kvw_tree
        for copy in pk1:
            copy.wait()
        mid_l[...] = total_of(pk_l, lines)
        pk2 = start_swap(go, mid_l, pk_s, SH, True)
        kvw_tree.across()
        q_lines = lines_out(0)
        for copy in dq_swap:
            copy.wait()
        for line in range(lines):
            dq_full[:, line * width : (line + 1) * width] = dq_all[line]
        grad = contract(dq_full[...], w_ref[0], 1, 1)
        for copy in pk2:
            copy.wait()
        mid_s[...] = total_of(pk_s, 4)
        pk3 = start_swap(go, mid_s, pk_g, GR, True)
        kv_lines = lines_out(1)
        for other in range(lines):

            @pl.when(line_me != other)
            def _():
                kv_copy(jnp.int32(other), line_me).wait_recv()
                kv_copy(line_me, jnp.int32(other)).wait_send()

        for half in range(2):
            for line in range(lines):
                dq_full[:, line * width : (line + 1) * width] = dkv_all[
                    line, :, half * width : (half + 1) * width
                ]
            grad = grad + contract(dq_full[...], w_ref[1 + half], 1, 1)
        inputs = hid_ref[...].astype(f32)
        inv = lax.rsqrt(jnp.mean(inputs * inputs, axis=1, keepdims=True) + norm_eps)
        normed = inputs * inv
        gn_0[...] = jnp.sum(grad * normed, axis=0, keepdims=True)
        gn1 = start_swap(go, gn_0, gn_l, EX, True)
        input_ref[...] = resid_ref[...] + rms_back(inputs, inv, gain_ref[...], grad)
        swaps = [None] * 3
        for k, copies in ((2, o_lines), (0, q_lines)):
            for copy in copies:
                copy.wait()
            if k == 2:
                halves[k][...] = total_of(lands[k], lines).astype(bf16)
            else:
                halves[k][...] = lands[k][...]
            swaps[k] = start_swap(go, halves[k], gots[k], GR, True)
        for copy in gn1:
            copy.wait()
        gn_1[...] = total_of(gn_l, lines)
        gn2 = start_swap(go, gn_1, gn_s, SH, True)
        for copy in kv_lines:
            copy.wait()
        halves[1][...] = lands[1][...]
        swaps[1] = start_swap(go, halves[1], gots[1], GR, True)
        for copy in gn2:
            copy.wait()
        gn_2[...] = total_of(gn_s, 4)
        gn3 = start_swap(go, gn_2, gn_g, GR, True)
        for copy in pk3:
            copy.wait()
        packed_out[...] = total_of(pk_g, groups)
        for k, out in ((2, out_out), (0, q_out), (1, kv_out)):
            for copy in swaps[k]:
                copy.wait()
            out[...] = total_of(gots[k], groups)
        for copy in gn3:
            copy.wait()
        gain_out[...] = total_of(gn_g, groups)
        for tree in (*kv_trees, o_tree, q_tree, kvw_tree):
            tree.close()
        yield

    pieces = [(lines, own, d) for d in part_dims]
    got_pieces = pieces[:2] + [(own, model)]
    scratch = Tree.scratch(dkv_piece) * 2 + Tree.scratch(q_piece) + Tree.scratch(kv_piece)
    scratch += Tree.scratch(o_piece)
    scratch += [
        vmem((lines, rows, 2 * width), bf16),
        vmem((4,) + q_piece, bf16),
        vmem((4,) + kv_piece, bf16),
        vmem((lines, rows, width), bf16),
        vmem((lines, rows, 2 * width), bf16),
        vmem((rows, model), bf16),
        pltpu.SemaphoreType.DMA((2, lines)),
    ]
    scratch += [vmem(p, bf16) for p in pieces] + [vmem(p, bf16) for p in pieces]
    scratch += [vmem(p, bf16) for p in got_pieces] + [vmem((groups,) + p, bf16) for p in got_pieces]
    scratch += [vmem((n,) + packed.shape, f32) for n in (lines, 4, groups)]
    scratch += [vmem(packed.shape, f32)] * 2
    scratch += [vmem((n, 1, model), f32) for n in (lines, 4, groups)] + [vmem((1, model), f32)] * 3
    copies = 5 * Tree.copies + 6 * (lines - 1) + 2 * 3 + 5 * (groups - 1)
    outs = [
        shape((rows, model), f32),
        shape((lines, own, width), f32),
        shape((lines, own, 2 * width), f32),
        shape((own, model), f32),
        shape(packed.shape, f32),
        shape((1, model), f32),
    ]
    ins = [*dkv, dq, attn_in, weights, out_term, packed, hidden, resid_grad, gain]
    return Part([EX, SH, GR], ins, outs, scratch, copies, phases)


def expert_body(steps, x_ref, g_ref, wg_ref, wu_ref, wd_ref, eo_ref, ib_ref, ga_ref, up_ref, d_ref, eo_s, ib_s, g_s):
    i = pl.program_id(0)
    me, side, core, _, _ = shard_peers()

    @pl.when(i == 0)
    def _():
        eo_s[...] = jnp.zeros_like(eo_s)
        ib_s[...] = jnp.zeros_like(ib_s)
        model = g_ref.shape[1]
        high, low = x_ref[:, model : model + 1], x_ref[:, model + 1 : model + 2]
        gate = high.astype(f32) + low.astype(f32)
        g_s[...] = (g_ref[...].astype(f32) * gate).astype(bf16)

    x, g = x_ref[:, : g_ref.shape[1]], g_s[...]
    wg, wu, wd = wg_ref[...], wu_ref[...], wd_ref[...]
    gate_pre = jnp.dot(x, wg, preferred_element_type=f32)
    up_pre = jnp.dot(x, wu, preferred_element_type=f32)
    hidden_grad = contract(g, wd, 1, 1)
    gate_sigmoid = jax.nn.sigmoid(gate_pre)
    act = (gate_pre * gate_sigmoid * up_pre).astype(bf16)
    gate_back = (
        hidden_grad * up_pre * gate_sigmoid * (1.0 + gate_pre * (1.0 - gate_sigmoid))
    ).astype(bf16)
    up_back = (hidden_grad * gate_pre * gate_sigmoid).astype(bf16)
    eo_s[...] += jnp.dot(act, wd, preferred_element_type=f32)
    ib_s[...] += contract(gate_back, wg, 1, 1) + contract(up_back, wu, 1, 1)

    def place(quarter):
        return 2 * lax.rem(lax.rem(quarter, 2) + core, 2) + lax.rem(quarter // 2 + side, 2)

    rows = ga_ref.shape[1]
    for ref, back in ((ga_ref, gate_back), (up_ref, up_back)):
        term = contract(x, back, 0, 0).astype(bf16)
        for quarter in range(4):
            ref[place(jnp.int32(quarter))] = term[quarter * rows : (quarter + 1) * rows]
    d_ref[place(i)] = contract(act, g, 0, 0).astype(bf16)

    @pl.when(i == steps - 1)
    def _():
        eo_ref[...] = eo_s[...].astype(bf16)
        ib_ref[...] = ib_s[...].astype(bf16)


def expert(x, g, wg, wu, wd):
    slots, model = g.shape
    inner = wg.shape[1]
    steps = 4
    tile = inner // steps
    quarter = model // 4
    shape = jax.ShapeDtypeStruct
    whole = lambda dims: pl.BlockSpec(dims, lambda i: (0,) * len(dims))
    return pl.pallas_call(
        functools.partial(expert_body, steps),
        grid=(steps,),
        out_shape=[
            shape((slots, model), bf16),
            shape((slots, model), bf16),
            shape((4, quarter, inner), bf16),
            shape((4, quarter, inner), bf16),
            shape((4, tile, model), bf16),
        ],
        in_specs=[
            whole(x.shape),
            whole((slots, model)),
            pl.BlockSpec((model, tile), lambda i: (0, i)),
            pl.BlockSpec((model, tile), lambda i: (0, i)),
            pl.BlockSpec((tile, model), lambda i: (i, 0)),
        ],
        out_specs=[
            whole((slots, model)),
            whole((slots, model)),
            pl.BlockSpec((4, quarter, tile), lambda i: (0, 0, i)),
            pl.BlockSpec((4, quarter, tile), lambda i: (0, 0, i)),
            whole((4, tile, model)),
        ],
        scratch_shapes=[pltpu.VMEM((slots, model), f32)] * 2 + [pltpu.VMEM((slots, model), bf16)],
        cost_estimate=pl.CostEstimate(flops=6 * 10**9, bytes_accessed=2 * 10**7, transcendentals=4 * 10**5),
        name="ffn",
    )(x, g, wg, wu, wd)


def head_columns(h, shape, axis):
    return lax.broadcasted_iota(jnp.int32, shape, axis) // HEAD_DIM == h


def allowed(block, key_blk, qpos, qstart, prompt):
    kpos = block * key_blk + lax.broadcasted_iota(jnp.int32, (key_blk, qpos.shape[1]), 0)
    return (kpos <= qpos) & ((kpos >= qstart) | (kpos < prompt))


def doc_start(block, info_ref, qinfo_ref):
    docs = qinfo_ref[pl.ds(block, 1), :]
    starts = jnp.zeros(docs.shape, jnp.int32)
    for doc in range(1, DOCS):
        starts = jnp.where(docs == doc, info_ref[doc], starts)
    return starts, info_ref[info_ref[DOCS + block]]


def attend_body(lines, heads, info_ref, q_ref, kv_ref, qinfo_ref, o_ref, low_ref, lse_ref, k_s, vt_s, acc_s, ml_s, qm_s):
    shard = lax.axis_index(SH)
    rows, width = q_ref.shape[1:]
    blocks = vt_s.shape[0]
    key_blk = vt_s.shape[2]
    prompt = info_ref[1]

    @pl.loop(0, blocks)
    def _(j):
        at = pl.ds(pl.multiple_of(j * key_blk, key_blk), key_blk)
        k_s[at, :] = kv_ref[at, :width]
        vt_s[j] = jnp.transpose(kv_ref[at, width:].astype(f32)).astype(bf16)

    @pl.loop(0, lines)
    def _(line):
        start = (line * 4 + shard) * rows
        queries = q_ref[line].astype(f32) * HEAD_DIM**-0.5
        qpos = start + lax.broadcasted_iota(jnp.int32, (1, rows), 1)
        qstart, first = doc_start(line * 4 + shard, info_ref, qinfo_ref)
        for h in range(heads):
            qm_s[h] = jnp.where(head_columns(h, queries.shape, 1), queries, 0.0).astype(bf16)
        acc_s[...] = jnp.zeros_like(acc_s)
        for h in range(heads):
            ml_s[h, 0:1, :] = jnp.full((1, rows), neg_fill, f32)
            ml_s[h, 1:2, :] = jnp.zeros((1, rows), f32)

        @pl.loop(0, (start + rows + key_blk - 1) // key_blk)
        def _(j):
            @pl.when((j * key_blk < prompt) | ((j + 1) * key_blk > first))
            def _():
                keys = k_s[pl.ds(pl.multiple_of(j * key_blk, key_blk), key_blk), :]
                ok = allowed(j, key_blk, qpos, qstart, prompt)
                for h in range(heads):
                    scores = jnp.where(ok, contract(keys, qm_s[h], 1, 1), neg_fill)
                    old = ml_s[h, 0:1, :]
                    new = jnp.maximum(old, jnp.max(scores, axis=0, keepdims=True))
                    probs = jnp.exp(scores - new)
                    scale = jnp.exp(old - new)
                    ml_s[h, 0:1, :] = new
                    ml_s[h, 1:2, :] = ml_s[h, 1:2, :] * scale + jnp.sum(
                        probs, axis=0, keepdims=True
                    )
                    part = slice(h * HEAD_DIM, (h + 1) * HEAD_DIM)
                    acc_s[part, :] = acc_s[part, :] * scale + jnp.dot(
                        vt_s[j, part, :], probs.astype(bf16), preferred_element_type=f32
                    )

        for h in range(heads):
            part = slice(h * HEAD_DIM, (h + 1) * HEAD_DIM)
            total = ml_s[h, 1:2, :]
            acc_s[part, :] = acc_s[part, :] / total
            lse_ref[line, h : h + 1, :] = ml_s[h, 0:1, :] + jnp.log(total)
        result = jnp.transpose(acc_s[...])
        o_ref[line] = result
        low_ref[line] = result.astype(bf16)


def attend(info, q, kv, qinfo):
    lines, rows, width = q.shape
    heads = width // HEAD_DIM
    length = kv.shape[0]
    key_blk = KEY_BLK
    shape = jax.ShapeDtypeStruct
    return pl.pallas_call(
        functools.partial(attend_body, lines, heads),
        out_shape=[
            shape((lines, rows, width), f32),
            shape((lines, rows, width), bf16),
            shape((lines, 8, rows), f32),
        ],
        in_specs=[SM, VM, VM, VM],
        out_specs=[VM] * 3,
        scratch_shapes=[
            pltpu.VMEM((length, width), bf16),
            pltpu.VMEM((length // key_blk, width, key_blk), bf16),
            pltpu.VMEM((width, rows), f32),
            pltpu.VMEM((heads, 8, rows), f32),
            pltpu.VMEM((heads, rows, width), bf16),
        ],
        cost_estimate=pl.CostEstimate(flops=2 * 10**9, bytes_accessed=8 * 10**6, transcendentals=4 * 10**6),
        name="attend",
    )(info, q, kv, qinfo)


def attend_back_body(lines, heads, info_ref, q_ref, kv_ref, qinfo_ref, o_ref, lse_ref, back_ref, dq_ref, dkv_lo, dkv_hi, k_s, v_s, dk_s, dv_s, dq_s, qm_s, bm_s, delta_s):
    shard = lax.axis_index(SH)
    rows, width = q_ref.shape[1:]
    key_blk = KEY_BLK
    blocks = k_s.shape[0] // key_blk
    prompt = info_ref[1]

    @pl.loop(0, blocks)
    def _(j):
        at = pl.ds(pl.multiple_of(j * key_blk, key_blk), key_blk)
        k_s[at, :] = kv_ref[at, :width]
        v_s[at, :] = kv_ref[at, width:]
        dk_s[at, :] = jnp.zeros((key_blk, width), f32)
        dv_s[at, :] = jnp.zeros((key_blk, width), f32)

    @pl.loop(0, lines)
    def _(line):
        start = (line * 4 + shard) * rows
        queries = q_ref[line].astype(f32) * HEAD_DIM**-0.5
        back = back_ref[line].astype(f32)
        qpos = start + lax.broadcasted_iota(jnp.int32, (1, rows), 1)
        qstart, first = doc_start(line * 4 + shard, info_ref, qinfo_ref)
        picks = (
            lax.broadcasted_iota(jnp.int32, (8, width), 1) // HEAD_DIM
            == lax.broadcasted_iota(jnp.int32, (8, width), 0)
        ).astype(f32)
        delta_s[...] = contract(picks, back * o_ref[line], 1, 1, HIGH)
        for h in range(heads):
            mine = head_columns(h, queries.shape, 1)
            qm_s[h] = jnp.where(mine, queries, 0.0).astype(bf16)
            bm_s[h] = jnp.where(mine, back, 0.0).astype(bf16)
        dq_s[...] = jnp.zeros_like(dq_s)

        @pl.loop(0, (start + rows + key_blk - 1) // key_blk)
        def _(j):
            @pl.when((j * key_blk < prompt) | ((j + 1) * key_blk > first))
            def _():
                at = pl.ds(pl.multiple_of(j * key_blk, key_blk), key_blk)
                keys, values = k_s[at, :], v_s[at, :]
                ok = allowed(j, key_blk, qpos, qstart, prompt)
                dk = jnp.zeros((key_blk, width), f32)
                dv = jnp.zeros((key_blk, width), f32)
                for h in range(heads):
                    scores = contract(keys, qm_s[h], 1, 1)
                    probs = jnp.where(ok, jnp.exp(scores - lse_ref[line, h : h + 1, :]), 0.0)
                    grads = contract(values, bm_s[h], 1, 1)
                    slow = (probs * (grads - delta_s[h : h + 1, :])).astype(bf16)
                    dv = dv + jnp.dot(probs.astype(bf16), bm_s[h], preferred_element_type=f32)
                    dk = dk + jnp.dot(slow, qm_s[h], preferred_element_type=f32)
                    dq_s[h] += contract(slow, keys, 0, 0)
                dk_s[at, :] += dk
                dv_s[at, :] += dv

        total = jnp.zeros(queries.shape, f32)
        for h in range(heads):
            total = jnp.where(head_columns(h, queries.shape, 1), dq_s[h], total)
        dq_ref[line] = (total * HEAD_DIM**-0.5).astype(bf16)

    half = lines // 2
    for k, ref in enumerate((dkv_lo, dkv_hi)):

        @pl.loop(0, half)
        def _(line):
            for piece in range(4):
                at = ((k * half + line) * 4 + piece) * rows
                at = pl.ds(pl.multiple_of(at, rows), rows)
                ref[piece, line, :, :width] = dk_s[at, :].astype(bf16)
                ref[piece, line, :, width:] = dv_s[at, :].astype(bf16)


def attend_back(info, q, kv, qinfo, o, lse, back):
    lines, rows, width = q.shape
    heads = width // HEAD_DIM
    length = kv.shape[0]
    shape = jax.ShapeDtypeStruct
    return pl.pallas_call(
        functools.partial(attend_back_body, lines, heads),
        out_shape=[
            shape((lines, rows, width), bf16),
            shape((4, lines // 2, rows, 2 * width), bf16),
            shape((4, lines // 2, rows, 2 * width), bf16),
        ],
        in_specs=[SM] + [VM] * 6,
        out_specs=[VM] * 3,
        scratch_shapes=[
            pltpu.VMEM((length, width), bf16),
            pltpu.VMEM((length, width), bf16),
            pltpu.VMEM((length, width), f32),
            pltpu.VMEM((length, width), f32),
            pltpu.VMEM((heads, rows, width), f32),
            pltpu.VMEM((heads, rows, width), bf16),
            pltpu.VMEM((heads, rows, width), bf16),
            pltpu.VMEM((8, rows), f32),
        ],
        cost_estimate=pl.CostEstimate(flops=5 * 10**9, bytes_accessed=12 * 10**6, transcendentals=4 * 10**6),
        name="attend_back",
    )(info, q, kv, qinfo, o, lse, back)


def finale_body(lines, n_ids, *refs):
    ins, outs = refs[:13], refs[13:]
    for k in range(3):
        outs[k][...] = ins[k][...].astype(f32) + ins[3 + k][...].astype(f32)
    for k in range(2):
        outs[3 + k][...] = ins[6 + k][...]

    @pl.when(pl.program_id(0) == 0)
    def _():
        q_sum, kv_sum, out_sum, small_ref, gain_ref = ins[8:]
        q_out, k_out, v_out, out_out, gain_out, mgain_out, vec_out, rout_out, mix_out = outs[5:]
        width = q_sum.shape[2]
        for line in range(lines):
            at = slice(line * width, (line + 1) * width)
            q_out[:, at] = q_sum[line]
            k_out[:, at] = kv_sum[line, :, :width]
            v_out[:, at] = kv_sum[line, :, width:]
        out_out[...] = out_sum[...]
        gain_out[...] = jnp.sum(gain_ref[...], axis=0)
        small = small_ref[...]
        mgain_out[...] = jnp.sum(small[0:1], axis=0)
        vec_out[...] = small[1:3]
        turned = jnp.transpose(small)
        rout_out[...] = turned[:, 3 : 3 + n_ids]
        mix_out[...] = turned[:, 3 + n_ids : 7 + n_ids]


def finale(mine, far, input_grad, layer_out, sums, n_ids):
    steps = 4
    shape = jax.ShapeDtypeStruct
    own, model = sums[2].shape
    lines = sums[0].shape[0]

    def tiled(dims, dim):
        block = tuple(d // steps if k == dim else d for k, d in enumerate(dims))
        return pl.BlockSpec(block, lambda i: tuple(i if k == dim else 0 for k in range(2)))

    def whole(dims):
        return pl.BlockSpec(dims, lambda i: (0,) * len(dims))

    wide = [tiled(mine[0].shape, 1), tiled(mine[1].shape, 1), tiled(mine[2].shape, 0)]
    rows = [tiled(input_grad.shape, 0), tiled(layer_out.shape, 0)]
    small = [(own, model)] * 4 + [(model,), (model,), (2, model), (model, n_ids), (model, 4)]
    return pl.pallas_call(
        functools.partial(finale_body, lines, n_ids),
        grid=(steps,),
        out_shape=[shape(m.shape, f32) for m in mine]
        + [shape(input_grad.shape, f32), shape(layer_out.shape, bf16)]
        + [shape(d, f32) for d in small],
        in_specs=wide + wide + rows + [whole(x.shape) for x in sums],
        out_specs=wide + rows + [whole(d) for d in small],
        cost_estimate=pl.CostEstimate(flops=10**7, bytes_accessed=10**7, transcendentals=0),
        name="finale",
    )(*mine, *far, input_grad, layer_out, *sums)


def swap(x, axis, partner):
    return lax.ppermute(x, axis, [(i, partner(i)) for i in range(lax.axis_size(axis))])


def fast_shards(
    hidden_in,
    segment_ids,
    routes,
    attn_gain,
    w_query,
    w_key,
    w_value,
    w_out,
    moe_gain,
    w_router,
    const_mix,
    const_vec,
    w_gate,
    w_up,
    w_down,
    out_grad,
):
    rows, model = hidden_in.shape
    lines = lax.axis_size(EX)
    line, shard = lax.axis_index(EX), lax.axis_index(SH)
    width = model // lines
    seg = segment_ids[0]
    length = seg.shape[0]

    w_qkv = jnp.stack([w_query, w_key, w_value])
    w_mine = lax.dynamic_slice_in_dim(w_qkv, line * width, width, axis=2)
    w_mine = jnp.concatenate([w_mine[1], w_mine[2], w_mine[0]], axis=1)
    attn_in, q, kv_all, place, recv_grads = front(
        hidden_in, w_mine, attn_gain[None], routes, out_grad
    )
    attn_in = attn_in.reshape(lines * rows, model)
    kv_all, w_out_b, w_qkv = lax.optimization_barrier((kv_all, w_out, w_qkv))
    wo_far = swap(w_out_b, SH, lambda i: i ^ 2)
    w_far = swap(w_qkv, SH, lambda i: i ^ 2)
    kv_all = kv_all.reshape(length, 2 * width)
    starts = jnp.sum(
        (seg[None, :] < jnp.arange(DOCS, dtype=jnp.int32)[:, None]).astype(jnp.int32),
        axis=1,
        dtype=jnp.int32,
    )
    qinfo = seg.reshape(length // rows, rows)
    info = jnp.concatenate([starts, qinfo[:, 0]])
    attn_vec, attn_heads, lse = attend(info, q, kv_all, qinfo)
    n_ids = w_router.shape[1]
    small_w = jnp.pad(
        jnp.concatenate([w_router, const_mix], axis=1), ((0, 0), (0, 124 - n_ids))
    )
    gain_two = moe_gain[None]
    recv_rows, wo_full, resid_one, table, attn_low = run_parts(
        [
            route(
                attn_heads, hidden_in, gain_two, small_w, routes, place, w_out[None], wo_far[None], n_ids
            )
        ],
        2,
        "route",
    )
    wo_full = wo_full.reshape(model, model)
    slots = lines * CAP

    expert_out, input_back, *terms = expert(
        recv_rows.reshape(slots, model + 128), recv_grads.reshape(slots, model), w_gate[0], w_up[0], w_down[0]
    )
    returned, input_ret, weights, *sums = run_parts(
        [
            exchange(EX, SWAP, expert_out.reshape(lines, CAP, model)),
            exchange(EX, SWAP, input_back.reshape(lines, CAP, model)),
            share_weights(w_qkv, w_far),
        ]
        + [core_sum(term) for term in terms],
        4,
        "combine",
    )
    weights = weights.reshape(3, model, model)
    far = [swap(there, SH, lambda i: i ^ 2) for there in sums[1::2]]
    mine = [(x.astype(f32) + y.astype(f32)).astype(bf16) for x, y in zip(sums[0::2], far)]

    back_heads, layer_out, resid_grad, out_term, packed = run_parts(
        [
            to_heads(
                returned, input_ret, place, table, resid_one, attn_low, out_grad, gain_two, small_w.T, const_vec, wo_full, n_ids
            )
        ],
        5,
        "to_heads",
    )
    back_heads, mine[2] = lax.optimization_barrier((back_heads, mine[2]))
    cross = lambda x: swap(x, GR, lambda i: 1 - i)
    down_far = cross(mine[2])
    dq, *dkv = attend_back(info, q, kv_all, qinfo, attn_vec, lse, back_heads)
    *dkv, mine[0], mine[1] = lax.optimization_barrier((*dkv, *mine[:2]))
    group_far = [cross(mine[0]), cross(mine[1]), down_far]
    input_grad, *sums = run_parts(
        [
            tail(
                dkv, dq, attn_in, weights, out_term, packed, hidden_in, resid_grad, attn_gain[None]
            )
        ],
        6,
        "tail",
        pl.CostEstimate(flops=2 * 10**10, bytes_accessed=10**8, transcendentals=0),
    )
    gate, up, down, input_grad, layer_out, *grads, gain, gain_two, vecs, router, mix = finale(
        mine, group_far, input_grad, layer_out, sums, n_ids
    )
    return (
        layer_out,
        input_grad,
        gain,
        *grads,
        gain_two,
        router,
        mix,
        vecs,
        gate[None],
        up[None],
        down[None],
    )


def solution(mesh):
    placed = (
        P((GR, EX, SH), None),
        P(GR, None),
        P((GR, EX, SH), None),
        P(),
        P(SH, None),
        P(SH, None),
        P(SH, None),
        P(SH, None),
        P(),
        P(),
        P(),
        P(),
        P(EX, None, None),
        P(EX, None, None),
        P(EX, None, None),
        P((GR, EX, SH), None),
    )
    sizes = dict(mesh.shape)
    lines = sizes[EX]
    fast = (sizes[GR], sizes[SH], lines) == (2, 4, 4)
    return jax.shard_map(
        fast_shards if fast else shards,
        mesh=mesh,
        in_specs=placed,
        out_specs=(
            P((GR, EX, SH), None),
            P((GR, EX, SH), None),
            P(),
            P((EX, SH), None),
            P((EX, SH), None),
            P((EX, SH), None),
            P((EX, SH), None),
            P(),
            P(),
            P(),
            P(),
            P(EX, SH, None),
            P(EX, SH, None),
            P(EX, SH, None),
        ),
        check_vma=False,
    )
```

```python
import functools

import jax
import jax.numpy as jnp
from jax import lax
from jax.experimental import pallas as pl
from jax.experimental.pallas import tpu as pltpu
from jax.sharding import PartitionSpec as P

HEADS = 12
HEAD_DIM = 64
CAP = 48
DOCS = 9
KEY_BLK = 256
KEY_BACK = 768
EX, SH, GR = ("expert", "shard", "group")
GATHER, GATHER_SUM, SWAP, SWAP_SUM = range(4)


neg_fill = -1e30
norm_eps = 1e-05
bf16 = jnp.bfloat16
f32 = jnp.float32
VM = pl.BlockSpec(memory_space=pltpu.VMEM)
SM = pl.BlockSpec(memory_space=pltpu.SMEM)
HIGH = lax.Precision.HIGHEST


def contract(a, b, da, db, precision=None):
    return lax.dot_general(
        a, b, (((da,), (db,)), ((), ())), preferred_element_type=f32, precision=precision
    )


def dense32(left_side, right_side):
    return jnp.dot(left_side, right_side, precision=lax.Precision.HIGHEST)


def allowed_mask(query_pos, query_seg, key_pos, key_seg):
    same_doc = (key_seg[None, :] == query_seg[:, None]) | (key_seg[None, :] == 0)
    return same_doc & (key_pos[None, :] <= query_pos[:, None])


def rms_back(inputs, inverse, gain_vec, upstream):
    scaled = upstream * gain_vec
    return inverse * scaled - inputs * inverse**3 * jnp.mean(scaled * inputs, axis=1, keepdims=True)


def block_scores(query_blk, keys_blk, score_scale):
    return (
        jnp.einsum("qhd,khd->hqk", query_blk, keys_blk, preferred_element_type=jnp.float32)
        * score_scale
    )


def grad_pieces(
    query_blk, back_blk, keys_blk, values_blk, norm_blk, delta_blk, key_mask, score_scale
):
    scores = block_scores(query_blk, keys_blk, score_scale)
    prob_rows = jnp.where(key_mask[None], jnp.exp(scores - norm_blk[:, :, None]), 0.0)
    prob_grad = jnp.einsum("qhd,khd->hqk", back_blk, values_blk, preferred_element_type=jnp.float32)
    score_low = (prob_rows * (prob_grad - delta_blk[:, :, None])).astype(jnp.bfloat16)
    return (prob_rows.astype(jnp.bfloat16), score_low)


def shards(
    hidden_in,
    segment_ids,
    routes,
    attn_gain,
    w_query,
    w_key,
    w_value,
    w_out,
    moe_gain,
    w_router,
    const_mix,
    const_vec,
    w_gate,
    w_up,
    w_down,
    out_grad,
):
    tok_rows, model_width = hidden_in.shape
    score_scale = HEAD_DIM ** (-0.5)
    inner_rank = lax.axis_index((EX, SH))
    seg_group = segment_ids[0]
    group_len = seg_group.shape[0]
    key_block = min(512, group_len)
    num_blocks = group_len // key_block
    row_start = inner_rank * tok_rows
    own_pos = row_start + jnp.arange(tok_rows, dtype=jnp.int32)
    own_seg = lax.dynamic_slice_in_dim(seg_group, row_start, tok_rows)
    wq_full, wk_full, wv_full, wo_full = (
        lax.all_gather(w_query, SH, axis=0, tiled=True),
        lax.all_gather(w_key, SH, axis=0, tiled=True),
        lax.all_gather(w_value, SH, axis=0, tiled=True),
        lax.all_gather(w_out, SH, axis=0, tiled=True),
    )
    inputs = hidden_in.astype(jnp.float32)
    inv_one = lax.rsqrt(jnp.mean(inputs * inputs, axis=1, keepdims=True) + norm_eps)
    normed_one = inputs * inv_one
    attn_in = (normed_one * attn_gain).astype(jnp.bfloat16)
    queries = jnp.dot(attn_in, wq_full, preferred_element_type=jnp.float32).astype(jnp.bfloat16)
    keys_own = jnp.dot(attn_in, wk_full, preferred_element_type=jnp.float32).astype(jnp.bfloat16)
    values_own = jnp.dot(attn_in, wv_full, preferred_element_type=jnp.float32).astype(jnp.bfloat16)
    keys_all, values_all = (
        lax.all_gather(keys_own, (EX, SH), axis=0, tiled=True),
        lax.all_gather(values_own, (EX, SH), axis=0, tiled=True),
    )
    query_heads = queries.reshape(tok_rows, HEADS, HEAD_DIM)

    def fetch_block(source, block_index):
        return lax.dynamic_slice_in_dim(source, block_index * key_block, key_block).reshape(
            key_block, HEADS, HEAD_DIM
        )

    def block_mask(block_index):
        key_pos = block_index * key_block + jnp.arange(key_block, dtype=jnp.int32)
        key_seg = lax.dynamic_slice_in_dim(seg_group, block_index * key_block, key_block)
        return allowed_mask(own_pos, own_seg, key_pos, key_seg)

    def stats_step(carry_now, block_index):
        key_mask = block_mask(block_index)

        def stats_live_block(carry_in):
            row_max, row_sum = carry_in
            scores = jnp.where(
                key_mask[None],
                block_scores(query_heads, fetch_block(keys_all, block_index), score_scale),
                neg_fill,
            )
            new_max = jnp.maximum(row_max, jnp.max(scores, axis=2))
            weights = jnp.where(key_mask[None], jnp.exp(scores - new_max[:, :, None]), 0.0)
            return (new_max, row_sum * jnp.exp(row_max - new_max) + jnp.sum(weights, axis=2))

        return (
            lax.cond(jnp.any(key_mask), stats_live_block, lambda carry_in: carry_in, carry_now),
            None,
        )

    start_max = jnp.full((HEADS, tok_rows), neg_fill, jnp.float32)
    row_max, row_sum = lax.scan(
        stats_step, (start_max, jnp.zeros_like(start_max)), jnp.arange(num_blocks)
    )[0]
    log_norm = row_max + jnp.log(row_sum)

    def output_step(running, block_index):
        key_mask = block_mask(block_index)

        def output_live_block(carry_in):
            scores = block_scores(query_heads, fetch_block(keys_all, block_index), score_scale)
            prob_rows = jnp.where(
                key_mask[None], jnp.exp(scores - log_norm[:, :, None]), 0.0
            ).astype(jnp.bfloat16)
            return carry_in + jnp.einsum(
                "hqk,khd->qhd",
                prob_rows,
                fetch_block(values_all, block_index),
                preferred_element_type=jnp.float32,
            )

        return (
            lax.cond(jnp.any(key_mask), output_live_block, lambda carry_in: carry_in, running),
            None,
        )

    zero_heads = jnp.zeros((tok_rows, HEADS, HEAD_DIM), jnp.float32)
    attn_sum = lax.scan(output_step, zero_heads, jnp.arange(num_blocks))[0]
    attn_low = attn_sum.reshape(tok_rows, model_width).astype(jnp.bfloat16)
    resid_one = inputs + jnp.dot(attn_low, wo_full, preferred_element_type=jnp.float32)
    inv_two = lax.rsqrt(jnp.mean(resid_one * resid_one, axis=1, keepdims=True) + norm_eps)
    normed_two = resid_one * inv_two
    moe_in = normed_two * moe_gain
    moe_low = moe_in.astype(jnp.bfloat16)
    n_ids = w_router.shape[1]
    local_experts = w_gate.shape[0]
    owners = lax.axis_size(EX)
    ffn_count = local_experts * owners
    id_table = jnp.arange(n_ids, dtype=jnp.int32)
    route_hot = (routes[:, :, None] == id_table).astype(jnp.float32)
    logits = dense32(moe_in, w_router)
    chosen = jnp.einsum("rkn,rn->rk", route_hot, logits, precision=lax.Precision.HIGHEST)
    gate_probs = jax.nn.softmax(chosen, axis=1)
    mix_alpha = jax.nn.softmax(dense32(moe_in, const_mix).reshape(tok_rows, 2, 2), axis=2)
    const_rows = mix_alpha[:, :, 0:1] * moe_in[:, None, :] + mix_alpha[:, :, 1:2] * const_vec[None]
    ffn_mask = (routes < ffn_count).astype(jnp.float32)
    copy_mask = (routes == ffn_count + 1).astype(jnp.float32)
    const_mask = (routes[:, :, None] == ffn_count + 2 + jnp.arange(2, dtype=jnp.int32)).astype(
        jnp.float32
    )
    copy_gate = jnp.sum(gate_probs * copy_mask, axis=1)
    const_gate = jnp.sum(gate_probs[:, :, None] * const_mask, axis=1)
    ffn_gate = gate_probs * ffn_mask
    flat_ids = routes.reshape(-1)
    id_hot = (flat_ids[:, None] == id_table).astype(jnp.int32)
    earlier = jnp.cumsum(id_hot, axis=0, dtype=jnp.int32) - id_hot
    slot_num = jnp.sum(earlier * id_hot, axis=1, dtype=jnp.int32)
    slot_total = ffn_count * CAP
    slot_of_route = jnp.where(flat_ids < ffn_count, flat_ids * CAP + slot_num, slot_total)
    route_count = flat_ids.shape[0]
    route_of_slot = (
        jnp.zeros(slot_total + 1, jnp.int32)
        .at[slot_of_route]
        .set(jnp.arange(route_count, dtype=jnp.int32))[:slot_total]
    )
    slot_used = jnp.zeros(slot_total + 1, jnp.bool_).at[slot_of_route].set(True)[:slot_total]
    send_rows = jnp.where(
        slot_used[:, None], moe_low[route_of_slot // 2], jnp.zeros((), jnp.bfloat16)
    )
    recv_rows = lax.all_to_all(
        send_rows.reshape(owners, local_experts * CAP, model_width),
        EX,
        split_axis=0,
        concat_axis=0,
        tiled=True,
    )
    expert_in = recv_rows.reshape(owners, local_experts, CAP, model_width)
    gate_pre = jnp.einsum("sjcd,jdf->sjcf", expert_in, w_gate, preferred_element_type=jnp.float32)
    up_pre = jnp.einsum("sjcd,jdf->sjcf", expert_in, w_up, preferred_element_type=jnp.float32)
    gate_sigmoid = jax.nn.sigmoid(gate_pre)
    hidden_act = (gate_pre * gate_sigmoid * up_pre).astype(jnp.bfloat16)
    expert_out = jnp.einsum(
        "sjcf,jfd->sjcd", hidden_act, w_down, preferred_element_type=jnp.float32
    ).astype(jnp.bfloat16)
    returned = lax.all_to_all(
        expert_out.reshape(owners, local_experts * CAP, model_width),
        EX,
        split_axis=0,
        concat_axis=0,
        tiled=True,
    )
    padded_out = jnp.concatenate(
        [returned.reshape(slot_total, model_width), jnp.zeros((1, model_width), jnp.bfloat16)],
        axis=0,
    )
    route_out = padded_out[slot_of_route].astype(jnp.float32).reshape(tok_rows, 2, model_width)
    moe_sum = (
        jnp.sum(ffn_gate[:, :, None] * route_out, axis=1)
        + copy_gate[:, None] * moe_in
        + jnp.sum(const_gate[:, :, None] * const_rows, axis=1)
    )
    layer_out = (resid_one + moe_sum).astype(jnp.bfloat16)
    upstream = out_grad.astype(jnp.float32)
    route_dot = jnp.sum(upstream[:, None, :] * route_out, axis=2)
    copy_dot = jnp.sum(upstream * moe_in, axis=1)
    const_dot = jnp.sum(upstream[:, None, :] * const_rows, axis=2)
    gate_back_r = (
        ffn_mask * route_dot
        + copy_mask * copy_dot[:, None]
        + jnp.sum(const_mask * const_dot[:, None, :], axis=2)
    )
    chosen_grad = gate_probs * (
        gate_back_r - jnp.sum(gate_probs * gate_back_r, axis=1, keepdims=True)
    )
    logit_grad = jnp.einsum("rk,rkn->rn", chosen_grad, route_hot, precision=lax.Precision.HIGHEST)
    const_up = const_gate[:, :, None] * upstream[:, None, :]
    alpha_grad = jnp.stack(
        [
            jnp.sum(const_up * moe_in[:, None, :], axis=2),
            jnp.sum(const_up * const_vec[None], axis=2),
        ],
        axis=2,
    )
    mix_back = (
        mix_alpha * (alpha_grad - jnp.sum(mix_alpha * alpha_grad, axis=2, keepdims=True))
    ).reshape(tok_rows, 4)
    vec_grad = jnp.sum(mix_alpha[:, :, 1:2] * const_up, axis=0)
    route_weight = ffn_gate.reshape(-1)
    grad_send = (route_weight[route_of_slot][:, None] * upstream[route_of_slot // 2]).astype(
        jnp.bfloat16
    )
    grad_send = jnp.where(slot_used[:, None], grad_send, jnp.zeros((), jnp.bfloat16))
    grad_recv = lax.all_to_all(
        grad_send.reshape(owners, local_experts * CAP, model_width),
        EX,
        split_axis=0,
        concat_axis=0,
        tiled=True,
    )
    grad_recv = grad_recv.reshape(owners, local_experts, CAP, model_width)
    hidden_grad = jnp.einsum(
        "sjcd,jfd->sjcf", grad_recv, w_down, preferred_element_type=jnp.float32
    )
    down_term = jnp.einsum(
        "sjcf,sjcd->jfd", hidden_act, grad_recv, preferred_element_type=jnp.float32
    )
    gate_back = (
        hidden_grad * up_pre * gate_sigmoid * (1.0 + gate_pre * (1.0 - gate_sigmoid))
    ).astype(jnp.bfloat16)
    up_back = (hidden_grad * gate_pre * gate_sigmoid).astype(jnp.bfloat16)
    gate_term = jnp.einsum(
        "sjcd,sjcf->jdf", expert_in, gate_back, preferred_element_type=jnp.float32
    )
    up_term = jnp.einsum("sjcd,sjcf->jdf", expert_in, up_back, preferred_element_type=jnp.float32)
    input_back = (
        jnp.einsum("sjcf,jdf->sjcd", gate_back, w_gate, preferred_element_type=jnp.float32)
        + jnp.einsum("sjcf,jdf->sjcd", up_back, w_up, preferred_element_type=jnp.float32)
    ).astype(jnp.bfloat16)
    input_ret = lax.all_to_all(
        input_back.reshape(owners, local_experts * CAP, model_width),
        EX,
        split_axis=0,
        concat_axis=0,
        tiled=True,
    )
    padded_in = jnp.concatenate(
        [input_ret.reshape(slot_total, model_width), jnp.zeros((1, model_width), jnp.bfloat16)],
        axis=0,
    )
    ffn_in_grad = jnp.sum(
        padded_in[slot_of_route].astype(jnp.float32).reshape(tok_rows, 2, model_width), axis=1
    )
    moe_in_grad = (
        ffn_in_grad
        + copy_gate[:, None] * upstream
        + jnp.sum(mix_alpha[:, :, 0:1] * const_up, axis=1)
        + dense32(mix_back, const_mix.T)
        + dense32(logit_grad, w_router.T)
    )
    moe_gain_grad = jnp.sum(moe_in_grad * normed_two, axis=0)
    router_grad = dense32(moe_in.T, logit_grad)
    mix_grad = dense32(moe_in.T, mix_back)
    resid_grad = upstream + rms_back(resid_one, inv_two, moe_gain, moe_in_grad)
    branch_low = resid_grad.astype(jnp.bfloat16)
    out_proj_term = jnp.dot(attn_low.T, branch_low, preferred_element_type=jnp.float32)
    attn_back = jnp.dot(branch_low, wo_full.T, preferred_element_type=jnp.float32).astype(
        jnp.bfloat16
    )
    back_heads = attn_back.reshape(tok_rows, HEADS, HEAD_DIM)
    row_delta = jnp.sum(back_heads.astype(jnp.float32) * attn_sum, axis=2).T

    def back_step(query_acc, block_index):
        key_mask = block_mask(block_index)
        keys_blk = fetch_block(keys_all, block_index)
        values_blk = fetch_block(values_all, block_index)

        def back_live_block(running):
            prob_low, score_low = grad_pieces(
                query_heads,
                back_heads,
                keys_blk,
                values_blk,
                log_norm,
                row_delta,
                key_mask,
                score_scale,
            )
            value_part = jnp.einsum(
                "hqk,qhd->khd", prob_low, back_heads, preferred_element_type=jnp.float32
            )
            key_part = (
                jnp.einsum(
                    "hqk,qhd->khd", score_low, query_heads, preferred_element_type=jnp.float32
                )
                * score_scale
            )
            running = (
                running
                + jnp.einsum(
                    "hqk,khd->qhd", score_low, keys_blk, preferred_element_type=jnp.float32
                )
                * score_scale
            )
            return (
                running,
                (
                    key_part.reshape(key_block, model_width),
                    value_part.reshape(key_block, model_width),
                ),
            )

        def dead_block(running):
            empty_rows = jnp.zeros((key_block, model_width), jnp.float32)
            return (running, (empty_rows, empty_rows))

        return lax.cond(jnp.any(key_mask), back_live_block, dead_block, query_acc)

    query_grad32, key_terms = lax.scan(back_step, zero_heads, jnp.arange(num_blocks))
    key_grad32, value_grad32 = (
        lax.psum_scatter(
            key_terms[0].reshape(group_len, model_width).astype(jnp.bfloat16),
            (EX, SH),
            scatter_dimension=0,
            tiled=True,
        ).astype(jnp.float32),
        lax.psum_scatter(
            key_terms[1].reshape(group_len, model_width).astype(jnp.bfloat16),
            (EX, SH),
            scatter_dimension=0,
            tiled=True,
        ).astype(jnp.float32),
    )
    query_low = query_grad32.reshape(tok_rows, model_width).astype(jnp.bfloat16)
    key_low = key_grad32.astype(jnp.bfloat16)
    value_low = value_grad32.astype(jnp.bfloat16)
    query_term = jnp.dot(attn_in.T, query_low, preferred_element_type=jnp.float32)
    key_term = jnp.dot(attn_in.T, key_low, preferred_element_type=jnp.float32)
    value_term = jnp.dot(attn_in.T, value_low, preferred_element_type=jnp.float32)
    attn_in_grad = (
        jnp.dot(query_low, wq_full.T, preferred_element_type=jnp.float32)
        + jnp.dot(key_low, wk_full.T, preferred_element_type=jnp.float32)
        + jnp.dot(value_low, wv_full.T, preferred_element_type=jnp.float32)
    )
    attn_gain_grad = jnp.sum(attn_in_grad * normed_one, axis=0)
    input_grad = resid_grad + rms_back(inputs, inv_one, attn_gain, attn_in_grad)
    query_part, key_part_w, value_part_w, out_part = (
        lax.psum_scatter(
            query_term.astype(jnp.bfloat16), (EX, SH), scatter_dimension=0, tiled=True
        ).astype(jnp.float32),
        lax.psum_scatter(
            key_term.astype(jnp.bfloat16), (EX, SH), scatter_dimension=0, tiled=True
        ).astype(jnp.float32),
        lax.psum_scatter(
            value_term.astype(jnp.bfloat16), (EX, SH), scatter_dimension=0, tiled=True
        ).astype(jnp.float32),
        lax.psum_scatter(
            out_proj_term.astype(jnp.bfloat16), (EX, SH), scatter_dimension=0, tiled=True
        ).astype(jnp.float32),
    )
    gate_part, up_part, down_part = (
        lax.psum_scatter(
            gate_term.astype(jnp.bfloat16), SH, scatter_dimension=1, tiled=True
        ).astype(jnp.float32),
        lax.psum_scatter(
            up_term.astype(jnp.bfloat16), SH, scatter_dimension=1, tiled=True
        ).astype(jnp.float32),
        lax.psum_scatter(
            down_term.astype(jnp.bfloat16), SH, scatter_dimension=1, tiled=True
        ).astype(jnp.float32),
    )
    summed = (
        lax.psum(query_part.astype(jnp.bfloat16), GR).astype(jnp.float32),
        lax.psum(key_part_w.astype(jnp.bfloat16), GR).astype(jnp.float32),
        lax.psum(value_part_w.astype(jnp.bfloat16), GR).astype(jnp.float32),
        lax.psum(out_part.astype(jnp.bfloat16), GR).astype(jnp.float32),
        lax.psum(gate_part.astype(jnp.bfloat16), GR).astype(jnp.float32),
        lax.psum(up_part.astype(jnp.bfloat16), GR).astype(jnp.float32),
        lax.psum(down_part.astype(jnp.bfloat16), GR).astype(jnp.float32),
    )
    small_sums = lax.psum(
        (attn_gain_grad, moe_gain_grad, router_grad, mix_grad, vec_grad),
        (GR, EX, SH),
    )
    return (
        layer_out,
        input_grad,
        small_sums[0],
        summed[0],
        summed[1],
        summed[2],
        summed[3],
        small_sums[1],
        small_sums[2],
        small_sums[3],
        small_sums[4],
        summed[4],
        summed[5],
        summed[6],
    )


def greet(peers):
    barrier = pltpu.get_barrier_semaphore()
    for axis, peer in peers:
        pl.semaphore_signal(
            barrier, inc=1, device_id={axis: peer}, device_id_type=pl.DeviceIdType.MESH
        )
    pl.semaphore_wait(barrier, len(peers))


def send(src, dst, sems, index, axis, peer):
    copy = pltpu.make_async_remote_copy(
        src_ref=src,
        dst_ref=dst,
        send_sem=sems.at[0, index],
        recv_sem=sems.at[1, index],
        device_id={axis: peer},
        device_id_type=pl.DeviceIdType.MESH,
    )
    copy.start()
    return copy


def shard_peers():
    me = lax.axis_index(SH)
    side, core = me // 2, lax.rem(me, 2)
    return me, side, core, 2 * side + 1 - core, 2 * (1 - side) + core


class Part:
    def __init__(self, axes, ins, outs, scratch, copies, phases, specs=None):
        self.axes, self.ins, self.outs, self.scratch = axes, ins, outs, scratch
        self.copies, self.phases = copies, phases
        self.specs = specs or [VM] * len(ins)


def run_parts(parts, collective_id, name=None, cost=None):
    ins = sum([p.ins for p in parts], [])
    outs = sum([p.outs for p in parts], [])
    scratch = sum([p.scratch for p in parts], [])
    copies = sum(p.copies for p in parts)
    axes = sorted(set(sum([list(p.axes) for p in parts], [])))

    def body(*refs):
        sems = refs[-1]
        in_refs, out_refs = list(refs[: len(ins)]), list(refs[len(ins) : len(ins) + len(outs)])
        scr = list(refs[len(ins) + len(outs) : -1])
        peers = []
        for axis in axes:
            me, n = lax.axis_index(axis), lax.axis_size(axis)
            peers += [(axis, lax.rem(me + d, n)) for d in range(1, n)]
        greet(peers)
        base, running = 0, []
        for p in parts:
            take = lambda pool, k: [pool.pop(0) for _ in range(k)]
            refs_p = (take(in_refs, len(p.ins)), take(out_refs, len(p.outs)), take(scr, len(p.scratch)))
            counter = [base]

            def go(src, dst, axis, peer, counter=counter):
                counter[0] += 1
                return send(src, dst, sems, counter[0] - 1, axis, peer)

            running.append(p.phases(*refs_p, go))
            base += p.copies
        while running:
            running = [r for r in running if next(r, True) is None]

    return pl.pallas_call(
        body,
        out_shape=outs,
        in_specs=sum([p.specs for p in parts], []),
        out_specs=[VM] * len(outs),
        scratch_shapes=scratch + [pltpu.SemaphoreType.DMA((2, copies))],
        compiler_params=pltpu.CompilerParams(collective_id=collective_id, has_side_effects=True),
        cost_estimate=cost,
        name=name,
    )(*ins)


def start_swap(go, src, land, axis, gather):
    me, n = lax.axis_index(axis), lax.axis_size(axis)
    started = []
    for d in range(1, n):
        peer = lax.rem(me + d, n)
        started.append(go(src if gather else src.at[peer], land.at[me], axis, peer))
    land[me] = src[...] if gather else src[me]
    return started


def total_of(land, n):
    total = land[0].astype(f32)
    for j in range(1, n):
        total = total + land[j].astype(f32)
    return total


def exchange(axis, kind, x):
    n = lax.axis_size(axis)
    gather, summed = kind in (GATHER, GATHER_SUM), kind in (GATHER_SUM, SWAP_SUM)
    piece = x.shape if gather else x.shape[1:]
    shape = jax.ShapeDtypeStruct
    outs = [shape(piece, f32) if summed else shape((n,) + piece, x.dtype)]
    scratch = [pltpu.VMEM((n,) + piece, x.dtype)] if summed else []

    def phases(ins, outs, scr, go):
        land = scr[0] if summed else outs[0]
        started = start_swap(go, ins[0], land, axis, gather)
        yield
        for copy in started:
            copy.wait()
        if summed:
            outs[0][...] = total_of(land, n)

    return Part([axis], [x], outs, scratch, n - 1, phases)


def tree_gather(x):
    lines = x.shape[0]
    cuts = [(0, lines // 2), (lines // 2, lines)] if lines > 1 else [(0, 1)]
    cuts = [pl.ds(lo, hi - lo) for lo, hi in cuts]

    def phases(ins, outs, scr, go):
        x_ref, out_ref = ins[0], outs[0]
        me, _, _, near, far = shard_peers()
        across = [go(x_ref.at[c], out_ref.at[c, me], SH, far) for c in cuts]
        own = go(x_ref, out_ref.at[:, me], SH, near)
        out_ref[:, me] = x_ref[...]
        yield
        handed = []
        for c, copy in zip(cuts, across):
            copy.wait_recv()
            handed.append(go(out_ref.at[c, far], out_ref.at[c, far], SH, near))
        yield
        for copy in across:
            copy.wait_send()
        own.wait()
        for copy in handed:
            copy.wait()

    shape = (lines, 4) + x.shape[1:]
    return Part([SH], [x], [jax.ShapeDtypeStruct(shape, x.dtype)], [], 2 * len(cuts) + 1, phases)


def core_sum(x):
    piece = x.shape[1:]
    shape = jax.ShapeDtypeStruct

    def phases(ins, outs, scr, go):
        x_ref, (here, there), (land, kept, sems) = ins[0], outs, scr
        near = shard_peers()[3]
        sent = [go(x_ref.at[3], land.at[1], SH, near), go(x_ref.at[2], land.at[0], SH, near)]
        local = [pltpu.make_async_copy(x_ref.at[k], kept.at[k], sems.at[k]) for k in range(2)]
        for copy in local:
            copy.start()
        yield
        for k, out in ((1, there), (0, here)):
            sent[1 - k].wait()
            local[k].wait()
            out[...] = (kept[k].astype(f32) + land[k].astype(f32)).astype(bf16)

    return Part(
        [SH],
        [x],
        [shape(piece, bf16)] * 2,
        [pltpu.VMEM((2,) + piece, bf16)] * 2 + [pltpu.SemaphoreType.DMA((2,))],
        2,
        phases,
        [pl.BlockSpec(memory_space=pl.ANY)],
    )


class Tree:
    copies = 3

    @staticmethod
    def scratch(piece):
        return [pltpu.VMEM((2,) + piece, bf16)] + [pltpu.VMEM(piece, bf16)] * 2

    def __init__(self, x, scr, go):
        self.x, (self.land, self.mine, self.got), self.go = x, scr, go
        self.me, self.side, self.core, self.near, self.far = shard_peers()
        other = 2 * (1 - self.side) + 1 - self.core
        self.first = [
            go(x.at[other], self.land.at[0], SH, self.near),
            go(x.at[self.near], self.land.at[1], SH, self.near),
        ]

    def across(self):
        self.first[0].wait_recv()
        self.mine[...] = (self.x[self.far].astype(f32) + self.land[0].astype(f32)).astype(bf16)
        self.second = self.go(self.mine, self.got, SH, self.far)

    def result(self):
        self.first[1].wait_recv()
        total = self.x[self.me].astype(f32) + self.land[1].astype(f32)
        self.second.wait_recv()
        return total + self.got[...].astype(f32)

    def close(self):
        for copy in (*self.first, self.second):
            copy.wait_send()


def turned_ids(ids_ref):
    ids = ids_ref[...].astype(f32)
    return jnp.transpose(jnp.concatenate([ids] * 4, axis=0)).astype(jnp.int32)


def slot_places(ids, lines, slots):
    rows = ids.shape[0]
    lane = lax.broadcasted_iota(jnp.int32, (rows, 128), 1)
    hot = [lane == column(ids, k) for k in range(2)]
    before = (
        lax.broadcasted_iota(jnp.int32, (rows, rows), 0)
        > lax.broadcasted_iota(jnp.int32, (rows, rows), 1)
    ).astype(bf16)
    named = jnp.where(hot[0] | hot[1], 1.0, 0.0).astype(bf16)
    earlier = jnp.dot(before, named, preferred_element_type=f32)
    slot_at = lax.broadcasted_iota(jnp.int32, (rows, slots), 1).astype(f32)
    place = []
    for k in range(2):
        number = jnp.sum(jnp.where(hot[k], earlier, 0.0), axis=1, keepdims=True)
        wanted = column(ids, k).astype(f32) * CAP + number
        wanted = jnp.where(column(ids, k) < lines, wanted, -1.0)
        place.append(jnp.where(slot_at == wanted, 1.0, 0.0))
    return place


def front(hidden, w_mine, gain, routes, out_grad):
    rows, model = hidden.shape
    lines = lax.axis_size(EX)
    width = model // lines
    shape = jax.ShapeDtypeStruct
    last = lines - 1

    slots = lines * CAP

    def body(hid_ref, w_ref, gain_ref, ids_ref, up_ref, attn_ref, q_ref, kv_ref, place_ref, rows_out, land, w_all, kv_own, rows_s, sems):
        line_me = lax.axis_index(EX)
        me, _, _, near, far = shard_peers()
        left, right = jnp.maximum(line_me - 1, 0), jnp.minimum(line_me + 1, last)
        greet(
            [(EX, lax.rem(line_me + d, lines)) for d in range(1, lines)]
            + [(SH, lax.rem(me + d, 4)) for d in range(1, 4)]
        )

        def copy(src, dst, index, axis, peer):
            return pltpu.make_async_remote_copy(
                src_ref=src,
                dst_ref=dst,
                send_sem=sems.at[0, index],
                recv_sem=sems.at[1, index],
                device_id={axis: peer},
                device_id_type=pl.DeviceIdType.MESH,
            )

        def relay(step, way):
            block = line_me - step if way == 0 else line_me + step
            block = jnp.clip(block, 0, last)
            src = hid_ref if step == 0 else land.at[block]
            return copy(src, land.at[block], last * way + step, EX, right if way == 0 else left)

        def sends(step, way):
            if way == 0:
                return (line_me < last) & (line_me - step >= 0)
            return (line_me > 0) & (line_me + step <= last)

        def comes(step, way):
            return line_me - 1 - step >= 0 if way == 0 else line_me + 1 + step <= last

        def source(step, way):
            line = line_me - 1 - step if way == 0 else line_me + 1 + step
            return jnp.clip(line, 0, last)

        def arrival(step, way):
            line = source(step, way)
            return copy(land.at[line], land.at[line], last * way + step, EX, right if way == 0 else left)

        base = 2 * last
        for way in range(2):

            @pl.when(sends(0, way))
            def _():
                relay(0, way).start()

        w_far = copy(w_ref, w_all.at[me], base, SH, far)
        w_near = copy(w_ref, w_all.at[me], base + 1, SH, near)
        w_pass = copy(w_all.at[far], w_all.at[far], base + 2, SH, near)
        w_far.start()
        w_near.start()
        w_all[me] = w_ref[...]
        ids = turned_ids(ids_ref)
        place = slot_places(ids, lines, slots)
        for k in range(2):
            place_ref[k] = place[k].astype(bf16)
        either = (place[0] + place[1]).astype(bf16)
        rows_s[...] = contract(either, up_ref[...], 0, 0).astype(bf16).reshape(lines, CAP, model)
        base += 3
        kv_far = lambda line: copy(kv_own.at[line], kv_ref.at[line, me], base + line, SH, far)
        kv_near = lambda line: copy(
            kv_own.at[line], kv_ref.at[line, me], base + lines + line, SH, near
        )
        kv_pass = lambda line: copy(
            kv_ref.at[line, far], kv_ref.at[line, far], base + 2 * lines + line, SH, near
        )

        def project(line, x):
            inputs = x.astype(f32)
            inv = lax.rsqrt(jnp.mean(inputs * inputs, axis=1, keepdims=True) + norm_eps)
            attn_in = (inputs * inv * gain_ref[...][None]).astype(bf16)
            attn_ref[line] = attn_in
            value = jnp.dot(
                attn_in, w_all[...].reshape(model, 3 * width), preferred_element_type=f32
            ).astype(bf16)
            kv_own[line] = value[:, : 2 * width]
            kv_far(line).start()
            kv_near(line).start()
            kv_ref[line, me] = value[:, : 2 * width]
            q_ref[line] = value[:, 2 * width :]

        def hand(line):
            kv_far(line).wait_recv()
            kv_pass(line).start()

        w_far.wait_recv()
        w_pass.start()
        w_near.wait_recv()
        w_pass.wait_recv()
        project(line_me, hid_ref[...])
        for step in range(last):
            for way in range(2):

                @pl.when(comes(step, way))
                def _():
                    arrival(step, way).wait_recv()

                if step + 1 < last:

                    @pl.when(sends(step + 1, way))
                    def _():
                        relay(step + 1, way).start()

            for way in range(2):

                @pl.when(comes(step, way))
                def _():
                    line = source(step, way)
                    project(line, land[line])

            if step == last - 2:
                first = base + 3 * lines
                ups = []
                for d in range(1, lines):
                    peer = lax.rem(line_me + d, lines)
                    ups.append(copy(rows_s.at[peer], rows_out.at[line_me], first + d - 1, EX, peer))
                    ups[-1].start()
                rows_out[line_me] = rows_s[line_me]
            if step == 0:
                hand(line_me)
            else:
                for way in range(2):

                    @pl.when(comes(step - 1, way))
                    def _():
                        hand(source(step - 1, way))

        for way in range(2):

            @pl.when(comes(last - 1, way))
            def _():
                hand(source(last - 1, way))

        for way in range(2):
            for step in range(last):

                @pl.when(sends(step, way))
                def _():
                    relay(step, way).wait_send()

        w_far.wait_send()
        w_near.wait_send()
        w_pass.wait_send()
        for line in range(lines):
            kv_far(line).wait_send()
            kv_near(line).wait()
            kv_pass(line).wait()
        for up in ups:
            up.wait()

    return pl.pallas_call(
        body,
        out_shape=[
            shape((lines, rows, model), bf16),
            shape((lines, rows, width), bf16),
            shape((lines, 4, rows, 2 * width), bf16),
            shape((2, rows, slots), bf16),
            shape((lines, CAP, model), bf16),
        ],
        in_specs=[VM] * 5,
        out_specs=[VM] * 5,
        scratch_shapes=[
            pltpu.VMEM((lines, rows, model), bf16),
            pltpu.VMEM((4, rows, 3 * width), bf16),
            pltpu.VMEM((lines, rows, 2 * width), bf16),
            pltpu.VMEM((lines, CAP, model), bf16),
            pltpu.SemaphoreType.DMA((2, 3 * last + 3 + 3 * lines)),
        ],
        compiler_params=pltpu.CompilerParams(collective_id=0, has_side_effects=True),
        name="front",
    )(hidden, w_mine, gain, routes, out_grad)


def column(x, k):
    return x[:, k : k + 1]


def core_share(go, own, far, out):
    me, _, _, near, other = shard_peers()
    sent = [go(own, out.at[:, me], SH, near), go(far, out.at[:, other], SH, near)]
    out[:, me] = own[...]
    out[:, other] = far[...]
    return sent


def route(heads, hidden, gain, small_w, routes, place, wo, wo_far, n_ids):
    lines, rows, width = heads.shape
    model = lines * width
    slots = lines * CAP
    shape = jax.ShapeDtypeStruct

    def phases(ins, outs, scr, go):
        heads_ref, hid_ref, gain_ref, small_ref, routes_ref, place_ref, wo_ref, wof_ref = ins
        rows_out, wo_all, resid_ref, table_ref, low_ref = outs
        land, rows_s = scr
        swaps = start_swap(go, heads_ref, land, EX, False)
        swaps += core_share(go, wo_ref, wof_ref, wo_all)
        ids = turned_ids(routes_ref)
        lane = lax.broadcasted_iota(jnp.int32, (rows, 128), 1)
        hot = [lane == column(ids, k) for k in range(2)]
        place = [place_ref[k].astype(f32) for k in range(2)]
        either = place_ref[0] + place_ref[1]
        for copy in swaps:
            copy.wait()
        for line in range(lines):
            low_ref[:, line * width : (line + 1) * width] = land[line]
        w_out = wo_all[...].reshape(model, model)
        resid = hid_ref[...].astype(f32) + jnp.dot(
            low_ref[...], w_out, preferred_element_type=f32
        )
        resid_ref[...] = resid
        inv = lax.rsqrt(jnp.mean(resid * resid, axis=1, keepdims=True) + norm_eps)
        moe_in = resid * inv * gain_ref[...][None]
        small = jnp.dot(moe_in, small_ref[...], preferred_element_type=f32, precision=HIGH)
        chosen = [jnp.sum(jnp.where(h, small, 0.0), axis=1, keepdims=True) for h in hot]
        top = jnp.maximum(chosen[0], chosen[1])
        powers = [jnp.exp(c - top) for c in chosen]
        gates = [p / (powers[0] + powers[1]) for p in powers]
        weight = place[0] * gates[0] + place[1] * gates[1]
        weight = contract(weight, jnp.ones((rows, 128), f32), 0, 0, HIGH)[:, 0:1]
        high = weight.astype(bf16)
        low = (weight - high.astype(f32)).astype(bf16)
        slot_lane = lax.broadcasted_iota(jnp.int32, (slots, 128), 1)
        extra = jnp.where(slot_lane == 0, high, jnp.where(slot_lane == 1, low, jnp.zeros_like(low)))
        rows_s[:, :, :model] = (
            contract(either, moe_in.astype(bf16), 0, 0).astype(bf16).reshape(lines, CAP, model)
        )
        rows_s[:, :, model:] = extra.reshape(lines, CAP, 128)
        row_swap = start_swap(go, rows_s, rows_out, EX, False)
        table = jnp.zeros((rows, 128), f32)
        entries = list(gates)
        for j in range(2):
            pair = [column(small, n_ids + 2 * j + k) for k in range(2)]
            top = jnp.maximum(pair[0], pair[1])
            powers = [jnp.exp(c - top) for c in pair]
            entries += [p / (powers[0] + powers[1]) for p in powers]
        entries += [column(ids, k).astype(f32) for k in range(2)]
        for k, entry in enumerate(entries):
            table = jnp.where(lane == k, entry, table)
        table_ref[...] = table
        for copy in row_swap:
            copy.wait()
        yield

    ins = [heads, hidden, gain, small_w, routes, place, wo, wo_far]
    outs = [
        shape((lines, CAP, model + 128), bf16),
        shape((1, 4, model // 4, model), bf16),
        shape((rows, model), f32),
        shape((rows, 128), f32),
        shape((rows, model), bf16),
    ]
    scratch = [
        pltpu.VMEM((lines, rows, width), bf16),
        pltpu.VMEM((lines, CAP, model + 128), bf16),
    ]
    return Part([EX, SH], ins, outs, scratch, 2 * (lines - 1) + 2, phases)


def share_weights(own, far):
    def phases(ins, outs, scr, go):
        copies = core_share(go, ins[0], ins[1], outs[0])
        yield
        for copy in copies:
            copy.wait()

    dims = (own.shape[0], 4) + own.shape[1:]
    return Part([SH], [own, far], [jax.ShapeDtypeStruct(dims, bf16)], [], 2, phases)


def to_heads(returned, input_ret, place, table, resid, low, out_grad, gain, small_t, const_vec, wo, n_ids):
    rows, model = resid.shape
    lines = returned.shape[0]
    width = model // lines
    own = rows // lines
    slots = lines * CAP
    shape = jax.ShapeDtypeStruct

    def phases(ins, outs, scr, go):
        ret_ref, iret_ref, place_ref, table_ref, resid_ref, low_ref, up_ref, gain_ref, st_ref, vec_ref, wo_ref = ins
        heads_out, layer_ref, rgrad_ref, term_ref, packed_ref = outs
        (back_s,) = scr
        table = table_ref[...]
        gates = [column(table, k) for k in range(2)]
        alpha = [[column(table, 2 + 2 * j + k) for k in range(2)] for j in range(2)]
        ids = [column(table, 6 + k) for k in range(2)]
        vecs = [vec_ref[j : j + 1, :] for j in range(2)]
        resid = resid_ref[...]
        upstream = up_ref[...].astype(f32)
        inv = lax.rsqrt(jnp.mean(resid * resid, axis=1, keepdims=True) + norm_eps)
        normed = resid * inv
        moe_in = normed * gain_ref[...][None]
        returned = ret_ref[...].reshape(slots, model)
        total = lambda x: jnp.sum(x, axis=1, keepdims=True)
        flag = lambda x: jnp.where(x, 1.0, 0.0)
        copy_dot = total(upstream * moe_in)
        vec_dot = [total(upstream * v) for v in vecs]
        const_dot = [alpha[j][0] * copy_dot + alpha[j][1] * vec_dot[j] for j in range(2)]
        output = resid
        backs = []
        copy_gate = jnp.zeros((rows, 1), f32)
        const_gate = [jnp.zeros((rows, 1), f32) for _ in range(2)]
        for k in range(2):
            rows_k = jnp.dot(place_ref[k], returned, preferred_element_type=f32)
            is_ffn, is_copy = flag(ids[k] < lines), flag(ids[k] == lines + 1)
            is_const = [flag(ids[k] == lines + 2 + j) for j in range(2)]
            output = output + (gates[k] * is_ffn) * rows_k
            backs.append(
                is_ffn * total(upstream * rows_k)
                + is_copy * copy_dot
                + is_const[0] * const_dot[0]
                + is_const[1] * const_dot[1]
            )
            copy_gate = copy_gate + gates[k] * is_copy
            const_gate = [const_gate[j] + gates[k] * is_const[j] for j in range(2)]
        through = copy_gate + const_gate[0] * alpha[0][0] + const_gate[1] * alpha[1][0]
        output = output + through * moe_in
        for j in range(2):
            output = output + (const_gate[j] * alpha[j][1]) * vecs[j]
        layer_ref[...] = output.astype(bf16)
        mean_back = gates[0] * backs[0] + gates[1] * backs[1]
        lane = lax.broadcasted_iota(jnp.int32, (rows, 128), 1)
        lane_f = lane.astype(f32)
        small = jnp.zeros((rows, 128), f32)
        for k in range(2):
            small = jnp.where(lane_f == ids[k], gates[k] * (backs[k] - mean_back), small)
        for j in range(2):
            grads = [const_gate[j] * copy_dot, const_gate[j] * vec_dot[j]]
            mean = alpha[j][0] * grads[0] + alpha[j][1] * grads[1]
            for k in range(2):
                small = jnp.where(
                    lane == n_ids + 2 * j + k, alpha[j][k] * (grads[k] - mean), small
                )
            small = jnp.where(lane == n_ids + 4 + j, alpha[j][1] * const_gate[j], small)
        either = place_ref[0] + place_ref[1]
        moe_grad = (
            jnp.dot(either, iret_ref[...].reshape(slots, model), preferred_element_type=f32)
            + through * upstream
            + jnp.dot(small, st_ref[...], preferred_element_type=f32, precision=HIGH)
        )
        resid_grad = upstream + rms_back(resid, inv, gain_ref[...][None], moe_grad)
        branch = resid_grad.astype(bf16)
        back = contract(branch, wo_ref[...], 1, 1).astype(bf16)
        for line in range(lines):
            back_s[line] = back[:, line * width : (line + 1) * width]
        swaps = start_swap(go, back_s, heads_out, EX, False)
        rgrad_ref[...] = resid_grad
        packed_ref[...] = jnp.zeros_like(packed_ref)
        packed_ref[0:1] = jnp.sum(moe_grad * normed, axis=0, keepdims=True)
        small_grad = contract(small, moe_in, 0, 0, HIGH)
        vec_grad = contract(small, upstream, 0, 0, HIGH)
        packed_ref[1:3] = vec_grad[n_ids + 4 : n_ids + 6]
        packed_ref[3 : 7 + n_ids] = small_grad[: n_ids + 4]
        term = contract(low_ref[...], branch, 0, 0).astype(bf16)
        for line in range(lines):
            for piece in range(4):
                at = (line * 4 + piece) * own
                term_ref[piece, line] = term[at : at + own]
        for copy in swaps:
            copy.wait()
        yield

    ins = [returned, input_ret, place, table, resid, low, out_grad, gain, small_t, const_vec, wo]
    outs = [
        shape((lines, rows, width), bf16),
        shape((rows, model), bf16),
        shape((rows, model), f32),
        shape((4, lines, own, model), bf16),
        shape((-(-(7 + n_ids) // 8) * 8, model), f32),
    ]
    return Part([EX], ins, outs, [pltpu.VMEM((lines, rows, width), bf16)], lines - 1, phases)


def tail(dkv, dq, attn_in, weights, out_term, packed, hidden, resid_grad, gain, pairs):
    lines, rows, width = dq.shape
    model = lines * width
    own = rows // lines
    groups = lax.axis_size(GR)
    shape = jax.ShapeDtypeStruct
    vmem = pltpu.VMEM
    tok = lines * rows
    few = lines // 2
    dkv_piece, q_piece = (few, rows, 2 * width), (lines, own, width)
    kv_piece, o_piece = (lines, own, 2 * width), (lines, own, model)
    part_dims = (width, 2 * width, model)

    def phases(ins, outs, scr, go):
        lo_ref, hi_ref, dq_ref, attn_ref, w_ref, o_ref, packed_ref, hid_ref, resid_ref, gain_ref = ins[:10]
        input_ref, q_out, kv_out, out_out, packed_out, gain_out = outs[:6]
        scr = list(scr)
        take = lambda k: [scr.pop(0) for _ in range(k)]
        lo_scr, hi_scr, q_scr, kvw_scr, o_scr = take(3), take(3), take(3), take(3), take(3)
        own_kv, q_t, kv_t, dq_all, dkv_all, dq_full = take(6)
        kv_sems = take(1)[0]
        sums, lands, halves, gots = take(3), take(3), take(3), take(3)
        pk_l, pk_s, pk_g = take(3)
        mid_l, mid_s = take(2)
        gn_l, gn_s, gn_g, gn_0, gn_1, gn_2 = take(6)
        me = lax.axis_index(SH)

        line_me, group_me = lax.axis_index(EX), lax.axis_index(GR)
        kv_trees = [Tree(lo_ref, lo_scr, go), Tree(hi_ref, hi_scr, go)]

        def kv_copy(sender, target):
            return pltpu.make_async_remote_copy(
                src_ref=own_kv.at[target],
                dst_ref=dkv_all.at[sender],
                send_sem=kv_sems.at[0, target],
                recv_sem=kv_sems.at[1, sender],
                device_id={EX: target},
                device_id_type=pl.DeviceIdType.MESH,
            )

        def push_kv(k):
            own_kv[k * few : (k + 1) * few] = kv_trees[k].result().astype(bf16)
            for target in range(k * few, (k + 1) * few):

                @pl.when(line_me != target)
                def _():
                    kv_copy(line_me, jnp.int32(target)).start()

                @pl.when(line_me == target)
                def _():
                    dkv_all[target] = own_kv[target]

        dq_swap = start_swap(go, dq_ref, dq_all, EX, False)
        o_tree = Tree(o_ref, o_scr, go)
        pk1 = start_swap(go, packed_ref, pk_l, EX, True)
        wide = []
        for k in range(len(pairs)):
            mine, other = outs[6 + 2 * k : 8 + 2 * k]
            here, there = ins[10 + 2 * k : 12 + 2 * k]
            mine[...] = (here[...].astype(f32) + there[...].astype(f32)).astype(bf16)
            wide.append(go(mine, other, GR, lax.rem(group_me + 1, groups)))

        def term(rows_ref, out):
            value = contract(attn_ref[...], rows_ref[...].reshape(tok, rows_ref.shape[-1]), 0, 0)
            value = value.astype(bf16)
            for line in range(lines):
                for piece in range(4):
                    at = (line * 4 + piece) * own
                    out[piece, line] = value[at : at + own]

        for tree in kv_trees:
            tree.across()
        term(dq_ref, q_t)
        o_tree.across()
        q_tree = Tree(q_t, q_scr, go)
        trees = [q_tree, None, o_tree]

        def lines_out(k):
            sums[k][...] = trees[k].result().astype(bf16)
            return start_swap(go, sums[k], lands[k], EX, False)

        push_kv(0)
        push_kv(1)
        o_lines = lines_out(2)
        q_tree.across()
        term(own_kv, kv_t)
        kvw_tree = Tree(kv_t, kvw_scr, go)
        trees[1] = kvw_tree
        for copy in pk1:
            copy.wait()
        mid_l[...] = total_of(pk_l, lines)
        pk2 = start_swap(go, mid_l, pk_s, SH, True)
        kvw_tree.across()
        q_lines = lines_out(0)
        for copy in dq_swap:
            copy.wait()
        for line in range(lines):
            dq_full[:, line * width : (line + 1) * width] = dq_all[line]
        grad = contract(dq_full[...], w_ref[0], 1, 1)
        for copy in pk2:
            copy.wait()
        mid_s[...] = total_of(pk_s, 4)
        pk3 = start_swap(go, mid_s, pk_g, GR, True)
        kv_lines = lines_out(1)
        for other in range(lines):

            @pl.when(line_me != other)
            def _():
                kv_copy(jnp.int32(other), line_me).wait_recv()
                kv_copy(line_me, jnp.int32(other)).wait_send()

        for half in range(2):
            for line in range(lines):
                dq_full[:, line * width : (line + 1) * width] = dkv_all[
                    line, :, half * width : (half + 1) * width
                ]
            grad = grad + contract(dq_full[...], w_ref[1 + half], 1, 1)
        inputs = hid_ref[...].astype(f32)
        inv = lax.rsqrt(jnp.mean(inputs * inputs, axis=1, keepdims=True) + norm_eps)
        normed = inputs * inv
        gn_0[...] = jnp.sum(grad * normed, axis=0, keepdims=True)
        gn1 = start_swap(go, gn_0, gn_l, EX, True)
        input_ref[...] = resid_ref[...] + rms_back(inputs, inv, gain_ref[...][None], grad)
        swaps = [None] * 3
        for k, copies in ((2, o_lines), (0, q_lines)):
            for copy in copies:
                copy.wait()
            if k == 2:
                halves[k][...] = total_of(lands[k], lines).astype(bf16)
            else:
                halves[k][...] = lands[k][...]
            swaps[k] = start_swap(go, halves[k], gots[k], GR, True)
        for copy in gn1:
            copy.wait()
        gn_1[...] = total_of(gn_l, lines)
        gn2 = start_swap(go, gn_1, gn_s, SH, True)
        for copy in kv_lines:
            copy.wait()
        halves[1][...] = lands[1][...]
        swaps[1] = start_swap(go, halves[1], gots[1], GR, True)
        for copy in gn2:
            copy.wait()
        gn_2[...] = total_of(gn_s, 4)
        gn3 = start_swap(go, gn_2, gn_g, GR, True)
        for copy in pk3:
            copy.wait()
        packed_out[...] = total_of(pk_g, groups)
        for k, out in ((2, out_out), (0, q_out), (1, kv_out)):
            for copy in swaps[k]:
                copy.wait()
            out[...] = total_of(gots[k], groups)
        for copy in gn3:
            copy.wait()
        gain_out[...] = total_of(gn_g, groups)
        for copy in wide:
            copy.wait()
        for tree in (*kv_trees, o_tree, q_tree, kvw_tree):
            tree.close()
        yield

    pieces = [(lines, own, d) for d in part_dims]
    got_pieces = pieces[:2] + [(own, model)]
    scratch = Tree.scratch(dkv_piece) * 2 + Tree.scratch(q_piece) + Tree.scratch(kv_piece)
    scratch += Tree.scratch(o_piece)
    scratch += [
        vmem((lines, rows, 2 * width), bf16),
        vmem((4,) + q_piece, bf16),
        vmem((4,) + kv_piece, bf16),
        vmem((lines, rows, width), bf16),
        vmem((lines, rows, 2 * width), bf16),
        vmem((rows, model), bf16),
        pltpu.SemaphoreType.DMA((2, lines)),
    ]
    scratch += [vmem(p, bf16) for p in pieces] + [vmem(p, bf16) for p in pieces]
    scratch += [vmem(p, bf16) for p in got_pieces] + [vmem((groups,) + p, bf16) for p in got_pieces]
    scratch += [vmem((n,) + packed.shape, f32) for n in (lines, 4, groups)]
    scratch += [vmem(packed.shape, f32)] * 2
    scratch += [vmem((n, 1, model), f32) for n in (lines, 4, groups)] + [vmem((1, model), f32)] * 3
    copies = len(pairs) + 5 * Tree.copies + 6 * (lines - 1) + 2 * 3 + 5 * (groups - 1)
    outs = [
        shape((rows, model), f32),
        shape((lines, own, width), f32),
        shape((lines, own, 2 * width), f32),
        shape((own, model), f32),
        shape(packed.shape, f32),
        shape((1, model), f32),
    ] + [shape(x.shape, bf16) for pair in pairs for x in pair]
    ins = [*dkv, dq, attn_in, weights, out_term, packed, hidden, resid_grad, gain]
    ins += [x for pair in pairs for x in pair]
    return Part([EX, SH, GR], ins, outs, scratch, copies, phases)


def expert_body(steps, x_ref, g_ref, wg_ref, wu_ref, wd_ref, eo_ref, ib_ref, ga_ref, up_ref, d_ref, eo_s, ib_s, g_s):
    i = pl.program_id(0)
    me, side, core, _, _ = shard_peers()

    @pl.when(i == 0)
    def _():
        eo_s[...] = jnp.zeros_like(eo_s)
        ib_s[...] = jnp.zeros_like(ib_s)
        model = g_ref.shape[1]
        high, low = x_ref[:, model : model + 1], x_ref[:, model + 1 : model + 2]
        gate = high.astype(f32) + low.astype(f32)
        g_s[...] = (g_ref[...].astype(f32) * gate).astype(bf16)

    x, g = x_ref[:, : g_ref.shape[1]], g_s[...]
    wg, wu, wd = wg_ref[...], wu_ref[...], wd_ref[...]
    gate_pre = jnp.dot(x, wg, preferred_element_type=f32)
    up_pre = jnp.dot(x, wu, preferred_element_type=f32)
    hidden_grad = contract(g, wd, 1, 1)
    gate_sigmoid = jax.nn.sigmoid(gate_pre)
    act = (gate_pre * gate_sigmoid * up_pre).astype(bf16)
    gate_back = (
        hidden_grad * up_pre * gate_sigmoid * (1.0 + gate_pre * (1.0 - gate_sigmoid))
    ).astype(bf16)
    up_back = (hidden_grad * gate_pre * gate_sigmoid).astype(bf16)
    eo_s[...] += jnp.dot(act, wd, preferred_element_type=f32)
    ib_s[...] += contract(gate_back, wg, 1, 1) + contract(up_back, wu, 1, 1)

    def place(quarter):
        return 2 * lax.rem(lax.rem(quarter, 2) + core, 2) + lax.rem(quarter // 2 + side, 2)

    rows = ga_ref.shape[1]
    for ref, back in ((ga_ref, gate_back), (up_ref, up_back)):
        term = contract(x, back, 0, 0).astype(bf16)
        for quarter in range(4):
            ref[place(jnp.int32(quarter))] = term[quarter * rows : (quarter + 1) * rows]
    d_ref[place(i)] = contract(act, g, 0, 0).astype(bf16)

    @pl.when(i == steps - 1)
    def _():
        eo_ref[...] = eo_s[...].astype(bf16)
        ib_ref[...] = ib_s[...].astype(bf16)


def expert(x, g, wg, wu, wd):
    slots, model = g.shape
    inner = wg.shape[1]
    steps = 4
    tile = inner // steps
    quarter = model // 4
    shape = jax.ShapeDtypeStruct
    whole = lambda dims: pl.BlockSpec(dims, lambda i: (0,) * len(dims))
    return pl.pallas_call(
        functools.partial(expert_body, steps),
        grid=(steps,),
        out_shape=[
            shape((slots, model), bf16),
            shape((slots, model), bf16),
            shape((4, quarter, inner), bf16),
            shape((4, quarter, inner), bf16),
            shape((4, tile, model), bf16),
        ],
        in_specs=[
            whole(x.shape),
            whole((slots, model)),
            pl.BlockSpec((model, tile), lambda i: (0, i)),
            pl.BlockSpec((model, tile), lambda i: (0, i)),
            pl.BlockSpec((tile, model), lambda i: (i, 0)),
        ],
        out_specs=[
            whole((slots, model)),
            whole((slots, model)),
            pl.BlockSpec((4, quarter, tile), lambda i: (0, 0, i)),
            pl.BlockSpec((4, quarter, tile), lambda i: (0, 0, i)),
            whole((4, tile, model)),
        ],
        scratch_shapes=[pltpu.VMEM((slots, model), f32)] * 2 + [pltpu.VMEM((slots, model), bf16)],
        cost_estimate=pl.CostEstimate(flops=6 * 10**9, bytes_accessed=2 * 10**7, transcendentals=4 * 10**5),
        name="ffn",
    )(x, g, wg, wu, wd)


def head_columns(h, shape, axis):
    return lax.broadcasted_iota(jnp.int32, shape, axis) // HEAD_DIM == h


def allowed(block, key_blk, qpos, qstart, prompt):
    kpos = block * key_blk + lax.broadcasted_iota(jnp.int32, (key_blk, qpos.shape[1]), 0)
    return (kpos <= qpos) & ((kpos >= qstart) | (kpos < prompt))


def doc_start(block, info_ref, qinfo_ref):
    docs = qinfo_ref[pl.ds(block, 1), :]
    starts = jnp.zeros(docs.shape, jnp.int32)
    for doc in range(1, DOCS):
        starts = jnp.where(docs == doc, info_ref[doc], starts)
    return starts, info_ref[info_ref[DOCS + block]]


def attend_body(lines, heads, info_ref, q_ref, kv_ref, qinfo_ref, o_ref, low_ref, lse_ref, k_s, vt_s, acc_s, ml_s, qm_s):
    shard = lax.axis_index(SH)
    rows, width = q_ref.shape[1:]
    blocks = vt_s.shape[0]
    key_blk = vt_s.shape[2]
    prompt = info_ref[1]

    @pl.loop(0, blocks)
    def _(j):
        at = pl.ds(pl.multiple_of(j * key_blk, key_blk), key_blk)
        k_s[at, :] = kv_ref[at, :width]
        vt_s[j] = jnp.transpose(kv_ref[at, width:].astype(f32)).astype(bf16)

    @pl.loop(0, lines)
    def _(line):
        start = (line * 4 + shard) * rows
        queries = q_ref[line].astype(f32) * HEAD_DIM**-0.5
        qpos = start + lax.broadcasted_iota(jnp.int32, (1, rows), 1)
        qstart, first = doc_start(line * 4 + shard, info_ref, qinfo_ref)
        for h in range(heads):
            qm_s[h] = jnp.where(head_columns(h, queries.shape, 1), queries, 0.0).astype(bf16)
        acc_s[...] = jnp.zeros_like(acc_s)
        for h in range(heads):
            ml_s[h, 0:1, :] = jnp.full((1, rows), neg_fill, f32)
            ml_s[h, 1:2, :] = jnp.zeros((1, rows), f32)

        @pl.loop(0, (start + rows + key_blk - 1) // key_blk)
        def _(j):
            @pl.when((j * key_blk < prompt) | ((j + 1) * key_blk > first))
            def _():
                keys = k_s[pl.ds(pl.multiple_of(j * key_blk, key_blk), key_blk), :]
                ok = allowed(j, key_blk, qpos, qstart, prompt)
                for h in range(heads):
                    scores = jnp.where(ok, contract(keys, qm_s[h], 1, 1), neg_fill)
                    old = ml_s[h, 0:1, :]
                    new = jnp.maximum(old, jnp.max(scores, axis=0, keepdims=True))
                    probs = jnp.exp(scores - new)
                    scale = jnp.exp(old - new)
                    ml_s[h, 0:1, :] = new
                    ml_s[h, 1:2, :] = ml_s[h, 1:2, :] * scale + jnp.sum(
                        probs, axis=0, keepdims=True
                    )
                    part = slice(h * HEAD_DIM, (h + 1) * HEAD_DIM)
                    acc_s[part, :] = acc_s[part, :] * scale + jnp.dot(
                        vt_s[j, part, :], probs.astype(bf16), preferred_element_type=f32
                    )

        for h in range(heads):
            part = slice(h * HEAD_DIM, (h + 1) * HEAD_DIM)
            total = ml_s[h, 1:2, :]
            acc_s[part, :] = acc_s[part, :] / total
            lse_ref[line, h : h + 1, :] = ml_s[h, 0:1, :] + jnp.log(total)
        result = jnp.transpose(acc_s[...])
        o_ref[line] = result
        low_ref[line] = result.astype(bf16)


def attend(info, q, kv, qinfo):
    lines, rows, width = q.shape
    heads = width // HEAD_DIM
    length = kv.shape[0]
    key_blk = KEY_BLK
    shape = jax.ShapeDtypeStruct
    return pl.pallas_call(
        functools.partial(attend_body, lines, heads),
        out_shape=[
            shape((lines, rows, width), f32),
            shape((lines, rows, width), bf16),
            shape((lines, 8, rows), f32),
        ],
        in_specs=[SM, VM, VM, VM],
        out_specs=[VM] * 3,
        scratch_shapes=[
            pltpu.VMEM((length, width), bf16),
            pltpu.VMEM((length // key_blk, width, key_blk), bf16),
            pltpu.VMEM((width, rows), f32),
            pltpu.VMEM((heads, 8, rows), f32),
            pltpu.VMEM((heads, rows, width), bf16),
        ],
        cost_estimate=pl.CostEstimate(flops=2 * 10**9, bytes_accessed=8 * 10**6, transcendentals=4 * 10**6),
        name="attend",
    )(info, q, kv, qinfo)


def attend_back_body(lines, heads, info_ref, q_ref, kv_ref, qinfo_ref, o_ref, lse_ref, back_ref, dq_ref, dkv_lo, dkv_hi, k_s, v_s, dk_s, dv_s, dq_s, qm_s, bm_s, delta_s):
    shard = lax.axis_index(SH)
    rows, width = q_ref.shape[1:]
    key_blk = KEY_BACK
    blocks = k_s.shape[0] // key_blk
    prompt = info_ref[1]

    @pl.loop(0, blocks)
    def _(j):
        at = pl.ds(pl.multiple_of(j * key_blk, key_blk), key_blk)
        k_s[at, :] = kv_ref[at, :width]
        v_s[at, :] = kv_ref[at, width:]
        dk_s[at, :] = jnp.zeros((key_blk, width), f32)
        dv_s[at, :] = jnp.zeros((key_blk, width), f32)

    @pl.loop(0, lines)
    def _(line):
        start = (line * 4 + shard) * rows
        queries = q_ref[line].astype(f32) * HEAD_DIM**-0.5
        back = back_ref[line].astype(f32)
        qpos = start + lax.broadcasted_iota(jnp.int32, (1, rows), 1)
        qstart, first = doc_start(line * 4 + shard, info_ref, qinfo_ref)
        picks = (
            lax.broadcasted_iota(jnp.int32, (8, width), 1) // HEAD_DIM
            == lax.broadcasted_iota(jnp.int32, (8, width), 0)
        ).astype(f32)
        delta_s[...] = contract(picks, back * o_ref[line], 1, 1, HIGH)
        for h in range(heads):
            mine = head_columns(h, queries.shape, 1)
            qm_s[h] = jnp.where(mine, queries, 0.0).astype(bf16)
            bm_s[h] = jnp.where(mine, back, 0.0).astype(bf16)
        dq_s[...] = jnp.zeros_like(dq_s)

        @pl.loop(0, (start + rows + key_blk - 1) // key_blk)
        def _(j):
            @pl.when((j * key_blk < prompt) | ((j + 1) * key_blk > first))
            def _():
                at = pl.ds(pl.multiple_of(j * key_blk, key_blk), key_blk)
                keys, values = k_s[at, :], v_s[at, :]
                ok = allowed(j, key_blk, qpos, qstart, prompt)
                dk = jnp.zeros((key_blk, width), f32)
                dv = jnp.zeros((key_blk, width), f32)
                for h in range(heads):
                    scores = contract(keys, qm_s[h], 1, 1)
                    probs = jnp.where(ok, jnp.exp(scores - lse_ref[line, h : h + 1, :]), 0.0)
                    grads = contract(values, bm_s[h], 1, 1)
                    slow = (probs * (grads - delta_s[h : h + 1, :])).astype(bf16)
                    dv = dv + jnp.dot(probs.astype(bf16), bm_s[h], preferred_element_type=f32)
                    dk = dk + jnp.dot(slow, qm_s[h], preferred_element_type=f32)
                    dq_s[h] += contract(slow, keys, 0, 0)
                dk_s[at, :] += dk
                dv_s[at, :] += dv

        total = jnp.zeros(queries.shape, f32)
        for h in range(heads):
            total = jnp.where(head_columns(h, queries.shape, 1), dq_s[h], total)
        dq_ref[line] = (total * HEAD_DIM**-0.5).astype(bf16)

    half = lines // 2
    for k, ref in enumerate((dkv_lo, dkv_hi)):

        @pl.loop(0, half)
        def _(line):
            for piece in range(4):
                at = ((k * half + line) * 4 + piece) * rows
                at = pl.ds(pl.multiple_of(at, rows), rows)
                ref[piece, line, :, :width] = dk_s[at, :].astype(bf16)
                ref[piece, line, :, width:] = dv_s[at, :].astype(bf16)


def attend_back(info, q, kv, qinfo, o, lse, back):
    lines, rows, width = q.shape
    heads = width // HEAD_DIM
    length = kv.shape[0]
    shape = jax.ShapeDtypeStruct
    return pl.pallas_call(
        functools.partial(attend_back_body, lines, heads),
        out_shape=[
            shape((lines, rows, width), bf16),
            shape((4, lines // 2, rows, 2 * width), bf16),
            shape((4, lines // 2, rows, 2 * width), bf16),
        ],
        in_specs=[SM] + [VM] * 6,
        out_specs=[VM] * 3,
        scratch_shapes=[
            pltpu.VMEM((length, width), bf16),
            pltpu.VMEM((length, width), bf16),
            pltpu.VMEM((length, width), f32),
            pltpu.VMEM((length, width), f32),
            pltpu.VMEM((heads, rows, width), f32),
            pltpu.VMEM((heads, rows, width), bf16),
            pltpu.VMEM((heads, rows, width), bf16),
            pltpu.VMEM((8, rows), f32),
        ],
        cost_estimate=pl.CostEstimate(flops=5 * 10**9, bytes_accessed=12 * 10**6, transcendentals=4 * 10**6),
        name="attend_back",
    )(info, q, kv, qinfo, o, lse, back)


def finale_body(lines, n_ids, *refs):
    ins, outs = refs[:13], refs[13:]
    for k in range(3):
        outs[k][...] = ins[k][...].astype(f32) + ins[3 + k][...].astype(f32)
    for k in range(2):
        outs[3 + k][...] = ins[6 + k][...]

    @pl.when(pl.program_id(0) == 0)
    def _():
        q_sum, kv_sum, out_sum, small_ref, gain_ref = ins[8:]
        q_out, k_out, v_out, out_out, gain_out, mgain_out, vec_out, rout_out, mix_out = outs[5:]
        width = q_sum.shape[2]
        for line in range(lines):
            at = slice(line * width, (line + 1) * width)
            q_out[:, at] = q_sum[line]
            k_out[:, at] = kv_sum[line, :, :width]
            v_out[:, at] = kv_sum[line, :, width:]
        out_out[...] = out_sum[...]
        gain_out[...] = jnp.sum(gain_ref[...], axis=0)
        small = small_ref[...]
        mgain_out[...] = jnp.sum(small[0:1], axis=0)
        vec_out[...] = small[1:3]
        rout_out[...] = small[3 : 3 + n_ids]
        mix_out[...] = small[3 + n_ids : 7 + n_ids]


def finale(mine, far, input_grad, layer_out, sums, n_ids):
    steps = 4
    shape = jax.ShapeDtypeStruct
    own, model = sums[2].shape
    lines = sums[0].shape[0]

    def tiled(dims, dim):
        block = tuple(d // steps if k == dim else d for k, d in enumerate(dims))
        return pl.BlockSpec(block, lambda i: tuple(i if k == dim else 0 for k in range(2)))

    def whole(dims):
        return pl.BlockSpec(dims, lambda i: (0,) * len(dims))

    wide = [tiled(mine[0].shape, 1), tiled(mine[1].shape, 1), tiled(mine[2].shape, 0)]
    rows = [tiled(input_grad.shape, 0), tiled(layer_out.shape, 0)]
    small = [(own, model)] * 4 + [(model,), (model,), (2, model), (n_ids, model), (4, model)]
    return pl.pallas_call(
        functools.partial(finale_body, lines, n_ids),
        grid=(steps,),
        out_shape=[shape(m.shape, f32) for m in mine]
        + [shape(input_grad.shape, f32), shape(layer_out.shape, bf16)]
        + [shape(d, f32) for d in small],
        in_specs=wide + wide + rows + [whole(x.shape) for x in sums],
        out_specs=wide + rows + [whole(d) for d in small],
        cost_estimate=pl.CostEstimate(flops=10**7, bytes_accessed=10**7, transcendentals=0),
        name="finale",
    )(*mine, *far, input_grad, layer_out, *sums)


def swap(x, axis, partner):
    return lax.ppermute(x, axis, [(i, partner(i)) for i in range(lax.axis_size(axis))])


def fast_shards(
    hidden_in,
    segment_ids,
    routes,
    attn_gain,
    w_query,
    w_key,
    w_value,
    w_out,
    moe_gain,
    w_router,
    const_mix,
    const_vec,
    w_gate,
    w_up,
    w_down,
    out_grad,
):
    rows, model = hidden_in.shape
    lines = lax.axis_size(EX)
    line, shard = lax.axis_index(EX), lax.axis_index(SH)
    width = model // lines
    seg = segment_ids[0]
    length = seg.shape[0]

    w_qkv = jnp.stack([w_query, w_key, w_value])
    w_mine = lax.dynamic_slice_in_dim(w_qkv, line * width, width, axis=2)
    w_mine = jnp.concatenate([w_mine[1], w_mine[2], w_mine[0]], axis=1)
    attn_in, q, kv_all, place, recv_grads = front(
        hidden_in, w_mine, attn_gain, routes.T, out_grad
    )
    attn_in = attn_in.reshape(lines * rows, model)
    kv_all, w_out_b, w_qkv = lax.optimization_barrier((kv_all, w_out, w_qkv))
    wo_far = swap(w_out_b, SH, lambda i: i ^ 2)
    w_far = swap(w_qkv, SH, lambda i: i ^ 2)
    kv_all = kv_all.reshape(length, 2 * width)
    starts = jnp.sum(
        (seg[None, :] < jnp.arange(DOCS, dtype=jnp.int32)[:, None]).astype(jnp.int32),
        axis=1,
        dtype=jnp.int32,
    )
    qinfo = seg.reshape(length // rows, rows)
    info = jnp.concatenate([starts, qinfo[:, 0]])
    attn_vec, attn_heads, lse = attend(info, q, kv_all, qinfo)
    n_ids = w_router.shape[1]
    small_w = jnp.pad(
        jnp.concatenate([w_router, const_mix], axis=1), ((0, 0), (0, 124 - n_ids))
    )
    gain_two = moe_gain
    recv_rows, wo_full, resid_one, table, attn_low = run_parts(
        [
            route(
                attn_heads, hidden_in, gain_two, small_w, routes.T, place, w_out[None], wo_far[None], n_ids
            )
        ],
        2,
        "route",
    )
    wo_full = wo_full.reshape(model, model)
    slots = lines * CAP

    expert_out, input_back, *terms = expert(
        recv_rows.reshape(slots, model + 128), recv_grads.reshape(slots, model), w_gate[0], w_up[0], w_down[0]
    )
    returned, input_ret, weights, *sums = run_parts(
        [
            exchange(EX, SWAP, expert_out.reshape(lines, CAP, model)),
            exchange(EX, SWAP, input_back.reshape(lines, CAP, model)),
            share_weights(w_qkv, w_far),
        ]
        + [core_sum(term) for term in terms],
        4,
        "combine",
    )
    weights = weights.reshape(3, model, model)
    far = [swap(there, SH, lambda i: i ^ 2) for there in sums[1::2]]
    down = (sums[4].astype(f32) + far[2].astype(f32)).astype(bf16)

    back_heads, layer_out, resid_grad, out_term, packed = run_parts(
        [
            to_heads(
                returned, input_ret, place, table, resid_one, attn_low, out_grad, gain_two, small_w.T, const_vec, wo_full, n_ids
            )
        ],
        5,
        "to_heads",
    )
    back_heads, down = lax.optimization_barrier((back_heads, down))
    cross = lambda x: swap(x, GR, lambda i: 1 - i)
    down_far = cross(down)
    dq, *dkv = attend_back(info, q, kv_all, qinfo, attn_vec, lse, back_heads)
    pairs = [(sums[0], far[0]), (sums[2], far[1])]
    input_grad, *parts = run_parts(
        [
            tail(
                dkv, dq, attn_in, weights, out_term, packed, hidden_in, resid_grad, attn_gain, pairs
            )
        ],
        6,
        "tail",
        pl.CostEstimate(flops=2 * 10**10, bytes_accessed=10**8, transcendentals=0),
    )
    gate, up, down, input_grad, layer_out, *grads, gain, gain_two, vecs, router, mix = finale(
        [parts[5], parts[7], down],
        [parts[6], parts[8], down_far],
        input_grad,
        layer_out,
        parts[:5],
        n_ids,
    )
    return (
        layer_out,
        input_grad,
        gain,
        *grads,
        gain_two,
        router.T,
        mix.T,
        vecs,
        gate[None],
        up[None],
        down[None],
    )


def solution(mesh):
    placed = (
        P((GR, EX, SH), None),
        P(GR, None),
        P((GR, EX, SH), None),
        P(),
        P(SH, None),
        P(SH, None),
        P(SH, None),
        P(SH, None),
        P(),
        P(),
        P(),
        P(),
        P(EX, None, None),
        P(EX, None, None),
        P(EX, None, None),
        P((GR, EX, SH), None),
    )
    sizes = dict(mesh.shape)
    lines = sizes[EX]
    fast = (sizes[GR], sizes[SH], lines) == (2, 4, 4)
    return jax.shard_map(
        fast_shards if fast else shards,
        mesh=mesh,
        in_specs=placed,
        out_specs=(
            P((GR, EX, SH), None),
            P((GR, EX, SH), None),
            P(),
            P((EX, SH), None),
            P((EX, SH), None),
            P((EX, SH), None),
            P((EX, SH), None),
            P(),
            P(),
            P(),
            P(),
            P(EX, SH, None),
            P(EX, SH, None),
            P(EX, SH, None),
        ),
        check_vma=False,
    )
```

```python
import functools

import jax
import jax.numpy as jnp
from jax import lax
from jax.experimental import pallas as pl
from jax.experimental.pallas import tpu as pltpu
from jax.sharding import PartitionSpec as P

HEADS = 12
HEAD_DIM = 64
CAP = 48
DOCS = 9
KEY_BLK = 256
KEY_BACK = 768
EX, SH, GR = ("expert", "shard", "group")
GATHER, GATHER_SUM, SWAP, SWAP_SUM = range(4)


neg_fill = -1e30
norm_eps = 1e-05
bf16 = jnp.bfloat16
f32 = jnp.float32
VM = pl.BlockSpec(memory_space=pltpu.VMEM)
SM = pl.BlockSpec(memory_space=pltpu.SMEM)
HIGH = lax.Precision.HIGHEST


def contract(a, b, da, db, precision=None):
    return lax.dot_general(
        a, b, (((da,), (db,)), ((), ())), preferred_element_type=f32, precision=precision
    )


def dense32(left_side, right_side):
    return jnp.dot(left_side, right_side, precision=lax.Precision.HIGHEST)


def allowed_mask(query_pos, query_seg, key_pos, key_seg):
    same_doc = (key_seg[None, :] == query_seg[:, None]) | (key_seg[None, :] == 0)
    return same_doc & (key_pos[None, :] <= query_pos[:, None])


def rms_back(inputs, inverse, gain_vec, upstream):
    scaled = upstream * gain_vec
    return inverse * scaled - inputs * inverse**3 * jnp.mean(scaled * inputs, axis=1, keepdims=True)


def block_scores(query_blk, keys_blk, score_scale):
    return (
        jnp.einsum("qhd,khd->hqk", query_blk, keys_blk, preferred_element_type=jnp.float32)
        * score_scale
    )


def grad_pieces(
    query_blk, back_blk, keys_blk, values_blk, norm_blk, delta_blk, key_mask, score_scale
):
    scores = block_scores(query_blk, keys_blk, score_scale)
    prob_rows = jnp.where(key_mask[None], jnp.exp(scores - norm_blk[:, :, None]), 0.0)
    prob_grad = jnp.einsum("qhd,khd->hqk", back_blk, values_blk, preferred_element_type=jnp.float32)
    score_low = (prob_rows * (prob_grad - delta_blk[:, :, None])).astype(jnp.bfloat16)
    return (prob_rows.astype(jnp.bfloat16), score_low)


def shards(
    hidden_in,
    segment_ids,
    routes,
    attn_gain,
    w_query,
    w_key,
    w_value,
    w_out,
    moe_gain,
    w_router,
    const_mix,
    const_vec,
    w_gate,
    w_up,
    w_down,
    out_grad,
):
    tok_rows, model_width = hidden_in.shape
    score_scale = HEAD_DIM ** (-0.5)
    inner_rank = lax.axis_index((EX, SH))
    seg_group = segment_ids[0]
    group_len = seg_group.shape[0]
    key_block = min(512, group_len)
    num_blocks = group_len // key_block
    row_start = inner_rank * tok_rows
    own_pos = row_start + jnp.arange(tok_rows, dtype=jnp.int32)
    own_seg = lax.dynamic_slice_in_dim(seg_group, row_start, tok_rows)
    wq_full, wk_full, wv_full, wo_full = (
        lax.all_gather(w_query, SH, axis=0, tiled=True),
        lax.all_gather(w_key, SH, axis=0, tiled=True),
        lax.all_gather(w_value, SH, axis=0, tiled=True),
        lax.all_gather(w_out, SH, axis=0, tiled=True),
    )
    inputs = hidden_in.astype(jnp.float32)
    inv_one = lax.rsqrt(jnp.mean(inputs * inputs, axis=1, keepdims=True) + norm_eps)
    normed_one = inputs * inv_one
    attn_in = (normed_one * attn_gain).astype(jnp.bfloat16)
    queries = jnp.dot(attn_in, wq_full, preferred_element_type=jnp.float32).astype(jnp.bfloat16)
    keys_own = jnp.dot(attn_in, wk_full, preferred_element_type=jnp.float32).astype(jnp.bfloat16)
    values_own = jnp.dot(attn_in, wv_full, preferred_element_type=jnp.float32).astype(jnp.bfloat16)
    keys_all, values_all = (
        lax.all_gather(keys_own, (EX, SH), axis=0, tiled=True),
        lax.all_gather(values_own, (EX, SH), axis=0, tiled=True),
    )
    query_heads = queries.reshape(tok_rows, HEADS, HEAD_DIM)

    def fetch_block(source, block_index):
        return lax.dynamic_slice_in_dim(source, block_index * key_block, key_block).reshape(
            key_block, HEADS, HEAD_DIM
        )

    def block_mask(block_index):
        key_pos = block_index * key_block + jnp.arange(key_block, dtype=jnp.int32)
        key_seg = lax.dynamic_slice_in_dim(seg_group, block_index * key_block, key_block)
        return allowed_mask(own_pos, own_seg, key_pos, key_seg)

    def stats_step(carry_now, block_index):
        key_mask = block_mask(block_index)

        def stats_live_block(carry_in):
            row_max, row_sum = carry_in
            scores = jnp.where(
                key_mask[None],
                block_scores(query_heads, fetch_block(keys_all, block_index), score_scale),
                neg_fill,
            )
            new_max = jnp.maximum(row_max, jnp.max(scores, axis=2))
            weights = jnp.where(key_mask[None], jnp.exp(scores - new_max[:, :, None]), 0.0)
            return (new_max, row_sum * jnp.exp(row_max - new_max) + jnp.sum(weights, axis=2))

        return (
            lax.cond(jnp.any(key_mask), stats_live_block, lambda carry_in: carry_in, carry_now),
            None,
        )

    start_max = jnp.full((HEADS, tok_rows), neg_fill, jnp.float32)
    row_max, row_sum = lax.scan(
        stats_step, (start_max, jnp.zeros_like(start_max)), jnp.arange(num_blocks)
    )[0]
    log_norm = row_max + jnp.log(row_sum)

    def output_step(running, block_index):
        key_mask = block_mask(block_index)

        def output_live_block(carry_in):
            scores = block_scores(query_heads, fetch_block(keys_all, block_index), score_scale)
            prob_rows = jnp.where(
                key_mask[None], jnp.exp(scores - log_norm[:, :, None]), 0.0
            ).astype(jnp.bfloat16)
            return carry_in + jnp.einsum(
                "hqk,khd->qhd",
                prob_rows,
                fetch_block(values_all, block_index),
                preferred_element_type=jnp.float32,
            )

        return (
            lax.cond(jnp.any(key_mask), output_live_block, lambda carry_in: carry_in, running),
            None,
        )

    zero_heads = jnp.zeros((tok_rows, HEADS, HEAD_DIM), jnp.float32)
    attn_sum = lax.scan(output_step, zero_heads, jnp.arange(num_blocks))[0]
    attn_low = attn_sum.reshape(tok_rows, model_width).astype(jnp.bfloat16)
    resid_one = inputs + jnp.dot(attn_low, wo_full, preferred_element_type=jnp.float32)
    inv_two = lax.rsqrt(jnp.mean(resid_one * resid_one, axis=1, keepdims=True) + norm_eps)
    normed_two = resid_one * inv_two
    moe_in = normed_two * moe_gain
    moe_low = moe_in.astype(jnp.bfloat16)
    n_ids = w_router.shape[1]
    local_experts = w_gate.shape[0]
    owners = lax.axis_size(EX)
    ffn_count = local_experts * owners
    id_table = jnp.arange(n_ids, dtype=jnp.int32)
    route_hot = (routes[:, :, None] == id_table).astype(jnp.float32)
    logits = dense32(moe_in, w_router)
    chosen = jnp.einsum("rkn,rn->rk", route_hot, logits, precision=lax.Precision.HIGHEST)
    gate_probs = jax.nn.softmax(chosen, axis=1)
    mix_alpha = jax.nn.softmax(dense32(moe_in, const_mix).reshape(tok_rows, 2, 2), axis=2)
    const_rows = mix_alpha[:, :, 0:1] * moe_in[:, None, :] + mix_alpha[:, :, 1:2] * const_vec[None]
    ffn_mask = (routes < ffn_count).astype(jnp.float32)
    copy_mask = (routes == ffn_count + 1).astype(jnp.float32)
    const_mask = (routes[:, :, None] == ffn_count + 2 + jnp.arange(2, dtype=jnp.int32)).astype(
        jnp.float32
    )
    copy_gate = jnp.sum(gate_probs * copy_mask, axis=1)
    const_gate = jnp.sum(gate_probs[:, :, None] * const_mask, axis=1)
    ffn_gate = gate_probs * ffn_mask
    flat_ids = routes.reshape(-1)
    id_hot = (flat_ids[:, None] == id_table).astype(jnp.int32)
    earlier = jnp.cumsum(id_hot, axis=0, dtype=jnp.int32) - id_hot
    slot_num = jnp.sum(earlier * id_hot, axis=1, dtype=jnp.int32)
    slot_total = ffn_count * CAP
    slot_of_route = jnp.where(flat_ids < ffn_count, flat_ids * CAP + slot_num, slot_total)
    route_count = flat_ids.shape[0]
    route_of_slot = (
        jnp.zeros(slot_total + 1, jnp.int32)
        .at[slot_of_route]
        .set(jnp.arange(route_count, dtype=jnp.int32))[:slot_total]
    )
    slot_used = jnp.zeros(slot_total + 1, jnp.bool_).at[slot_of_route].set(True)[:slot_total]
    send_rows = jnp.where(
        slot_used[:, None], moe_low[route_of_slot // 2], jnp.zeros((), jnp.bfloat16)
    )
    recv_rows = lax.all_to_all(
        send_rows.reshape(owners, local_experts * CAP, model_width),
        EX,
        split_axis=0,
        concat_axis=0,
        tiled=True,
    )
    expert_in = recv_rows.reshape(owners, local_experts, CAP, model_width)
    gate_pre = jnp.einsum("sjcd,jdf->sjcf", expert_in, w_gate, preferred_element_type=jnp.float32)
    up_pre = jnp.einsum("sjcd,jdf->sjcf", expert_in, w_up, preferred_element_type=jnp.float32)
    gate_sigmoid = jax.nn.sigmoid(gate_pre)
    hidden_act = (gate_pre * gate_sigmoid * up_pre).astype(jnp.bfloat16)
    expert_out = jnp.einsum(
        "sjcf,jfd->sjcd", hidden_act, w_down, preferred_element_type=jnp.float32
    ).astype(jnp.bfloat16)
    returned = lax.all_to_all(
        expert_out.reshape(owners, local_experts * CAP, model_width),
        EX,
        split_axis=0,
        concat_axis=0,
        tiled=True,
    )
    padded_out = jnp.concatenate(
        [returned.reshape(slot_total, model_width), jnp.zeros((1, model_width), jnp.bfloat16)],
        axis=0,
    )
    route_out = padded_out[slot_of_route].astype(jnp.float32).reshape(tok_rows, 2, model_width)
    moe_sum = (
        jnp.sum(ffn_gate[:, :, None] * route_out, axis=1)
        + copy_gate[:, None] * moe_in
        + jnp.sum(const_gate[:, :, None] * const_rows, axis=1)
    )
    layer_out = (resid_one + moe_sum).astype(jnp.bfloat16)
    upstream = out_grad.astype(jnp.float32)
    route_dot = jnp.sum(upstream[:, None, :] * route_out, axis=2)
    copy_dot = jnp.sum(upstream * moe_in, axis=1)
    const_dot = jnp.sum(upstream[:, None, :] * const_rows, axis=2)
    gate_back_r = (
        ffn_mask * route_dot
        + copy_mask * copy_dot[:, None]
        + jnp.sum(const_mask * const_dot[:, None, :], axis=2)
    )
    chosen_grad = gate_probs * (
        gate_back_r - jnp.sum(gate_probs * gate_back_r, axis=1, keepdims=True)
    )
    logit_grad = jnp.einsum("rk,rkn->rn", chosen_grad, route_hot, precision=lax.Precision.HIGHEST)
    const_up = const_gate[:, :, None] * upstream[:, None, :]
    alpha_grad = jnp.stack(
        [
            jnp.sum(const_up * moe_in[:, None, :], axis=2),
            jnp.sum(const_up * const_vec[None], axis=2),
        ],
        axis=2,
    )
    mix_back = (
        mix_alpha * (alpha_grad - jnp.sum(mix_alpha * alpha_grad, axis=2, keepdims=True))
    ).reshape(tok_rows, 4)
    vec_grad = jnp.sum(mix_alpha[:, :, 1:2] * const_up, axis=0)
    route_weight = ffn_gate.reshape(-1)
    grad_send = (route_weight[route_of_slot][:, None] * upstream[route_of_slot // 2]).astype(
        jnp.bfloat16
    )
    grad_send = jnp.where(slot_used[:, None], grad_send, jnp.zeros((), jnp.bfloat16))
    grad_recv = lax.all_to_all(
        grad_send.reshape(owners, local_experts * CAP, model_width),
        EX,
        split_axis=0,
        concat_axis=0,
        tiled=True,
    )
    grad_recv = grad_recv.reshape(owners, local_experts, CAP, model_width)
    hidden_grad = jnp.einsum(
        "sjcd,jfd->sjcf", grad_recv, w_down, preferred_element_type=jnp.float32
    )
    down_term = jnp.einsum(
        "sjcf,sjcd->jfd", hidden_act, grad_recv, preferred_element_type=jnp.float32
    )
    gate_back = (
        hidden_grad * up_pre * gate_sigmoid * (1.0 + gate_pre * (1.0 - gate_sigmoid))
    ).astype(jnp.bfloat16)
    up_back = (hidden_grad * gate_pre * gate_sigmoid).astype(jnp.bfloat16)
    gate_term = jnp.einsum(
        "sjcd,sjcf->jdf", expert_in, gate_back, preferred_element_type=jnp.float32
    )
    up_term = jnp.einsum("sjcd,sjcf->jdf", expert_in, up_back, preferred_element_type=jnp.float32)
    input_back = (
        jnp.einsum("sjcf,jdf->sjcd", gate_back, w_gate, preferred_element_type=jnp.float32)
        + jnp.einsum("sjcf,jdf->sjcd", up_back, w_up, preferred_element_type=jnp.float32)
    ).astype(jnp.bfloat16)
    input_ret = lax.all_to_all(
        input_back.reshape(owners, local_experts * CAP, model_width),
        EX,
        split_axis=0,
        concat_axis=0,
        tiled=True,
    )
    padded_in = jnp.concatenate(
        [input_ret.reshape(slot_total, model_width), jnp.zeros((1, model_width), jnp.bfloat16)],
        axis=0,
    )
    ffn_in_grad = jnp.sum(
        padded_in[slot_of_route].astype(jnp.float32).reshape(tok_rows, 2, model_width), axis=1
    )
    moe_in_grad = (
        ffn_in_grad
        + copy_gate[:, None] * upstream
        + jnp.sum(mix_alpha[:, :, 0:1] * const_up, axis=1)
        + dense32(mix_back, const_mix.T)
        + dense32(logit_grad, w_router.T)
    )
    moe_gain_grad = jnp.sum(moe_in_grad * normed_two, axis=0)
    router_grad = dense32(moe_in.T, logit_grad)
    mix_grad = dense32(moe_in.T, mix_back)
    resid_grad = upstream + rms_back(resid_one, inv_two, moe_gain, moe_in_grad)
    branch_low = resid_grad.astype(jnp.bfloat16)
    out_proj_term = jnp.dot(attn_low.T, branch_low, preferred_element_type=jnp.float32)
    attn_back = jnp.dot(branch_low, wo_full.T, preferred_element_type=jnp.float32).astype(
        jnp.bfloat16
    )
    back_heads = attn_back.reshape(tok_rows, HEADS, HEAD_DIM)
    row_delta = jnp.sum(back_heads.astype(jnp.float32) * attn_sum, axis=2).T

    def back_step(query_acc, block_index):
        key_mask = block_mask(block_index)
        keys_blk = fetch_block(keys_all, block_index)
        values_blk = fetch_block(values_all, block_index)

        def back_live_block(running):
            prob_low, score_low = grad_pieces(
                query_heads,
                back_heads,
                keys_blk,
                values_blk,
                log_norm,
                row_delta,
                key_mask,
                score_scale,
            )
            value_part = jnp.einsum(
                "hqk,qhd->khd", prob_low, back_heads, preferred_element_type=jnp.float32
            )
            key_part = (
                jnp.einsum(
                    "hqk,qhd->khd", score_low, query_heads, preferred_element_type=jnp.float32
                )
                * score_scale
            )
            running = (
                running
                + jnp.einsum(
                    "hqk,khd->qhd", score_low, keys_blk, preferred_element_type=jnp.float32
                )
                * score_scale
            )
            return (
                running,
                (
                    key_part.reshape(key_block, model_width),
                    value_part.reshape(key_block, model_width),
                ),
            )

        def dead_block(running):
            empty_rows = jnp.zeros((key_block, model_width), jnp.float32)
            return (running, (empty_rows, empty_rows))

        return lax.cond(jnp.any(key_mask), back_live_block, dead_block, query_acc)

    query_grad32, key_terms = lax.scan(back_step, zero_heads, jnp.arange(num_blocks))
    key_grad32, value_grad32 = (
        lax.psum_scatter(
            key_terms[0].reshape(group_len, model_width).astype(jnp.bfloat16),
            (EX, SH),
            scatter_dimension=0,
            tiled=True,
        ).astype(jnp.float32),
        lax.psum_scatter(
            key_terms[1].reshape(group_len, model_width).astype(jnp.bfloat16),
            (EX, SH),
            scatter_dimension=0,
            tiled=True,
        ).astype(jnp.float32),
    )
    query_low = query_grad32.reshape(tok_rows, model_width).astype(jnp.bfloat16)
    key_low = key_grad32.astype(jnp.bfloat16)
    value_low = value_grad32.astype(jnp.bfloat16)
    query_term = jnp.dot(attn_in.T, query_low, preferred_element_type=jnp.float32)
    key_term = jnp.dot(attn_in.T, key_low, preferred_element_type=jnp.float32)
    value_term = jnp.dot(attn_in.T, value_low, preferred_element_type=jnp.float32)
    attn_in_grad = (
        jnp.dot(query_low, wq_full.T, preferred_element_type=jnp.float32)
        + jnp.dot(key_low, wk_full.T, preferred_element_type=jnp.float32)
        + jnp.dot(value_low, wv_full.T, preferred_element_type=jnp.float32)
    )
    attn_gain_grad = jnp.sum(attn_in_grad * normed_one, axis=0)
    input_grad = resid_grad + rms_back(inputs, inv_one, attn_gain, attn_in_grad)
    query_part, key_part_w, value_part_w, out_part = (
        lax.psum_scatter(
            query_term.astype(jnp.bfloat16), (EX, SH), scatter_dimension=0, tiled=True
        ).astype(jnp.float32),
        lax.psum_scatter(
            key_term.astype(jnp.bfloat16), (EX, SH), scatter_dimension=0, tiled=True
        ).astype(jnp.float32),
        lax.psum_scatter(
            value_term.astype(jnp.bfloat16), (EX, SH), scatter_dimension=0, tiled=True
        ).astype(jnp.float32),
        lax.psum_scatter(
            out_proj_term.astype(jnp.bfloat16), (EX, SH), scatter_dimension=0, tiled=True
        ).astype(jnp.float32),
    )
    gate_part, up_part, down_part = (
        lax.psum_scatter(
            gate_term.astype(jnp.bfloat16), SH, scatter_dimension=1, tiled=True
        ).astype(jnp.float32),
        lax.psum_scatter(
            up_term.astype(jnp.bfloat16), SH, scatter_dimension=1, tiled=True
        ).astype(jnp.float32),
        lax.psum_scatter(
            down_term.astype(jnp.bfloat16), SH, scatter_dimension=1, tiled=True
        ).astype(jnp.float32),
    )
    summed = (
        lax.psum(query_part.astype(jnp.bfloat16), GR).astype(jnp.float32),
        lax.psum(key_part_w.astype(jnp.bfloat16), GR).astype(jnp.float32),
        lax.psum(value_part_w.astype(jnp.bfloat16), GR).astype(jnp.float32),
        lax.psum(out_part.astype(jnp.bfloat16), GR).astype(jnp.float32),
        lax.psum(gate_part.astype(jnp.bfloat16), GR).astype(jnp.float32),
        lax.psum(up_part.astype(jnp.bfloat16), GR).astype(jnp.float32),
        lax.psum(down_part.astype(jnp.bfloat16), GR).astype(jnp.float32),
    )
    small_sums = lax.psum(
        (attn_gain_grad, moe_gain_grad, router_grad, mix_grad, vec_grad),
        (GR, EX, SH),
    )
    return (
        layer_out,
        input_grad,
        small_sums[0],
        summed[0],
        summed[1],
        summed[2],
        summed[3],
        small_sums[1],
        small_sums[2],
        small_sums[3],
        small_sums[4],
        summed[4],
        summed[5],
        summed[6],
    )


def greet(peers):
    barrier = pltpu.get_barrier_semaphore()
    for axis, peer in peers:
        pl.semaphore_signal(
            barrier, inc=1, device_id={axis: peer}, device_id_type=pl.DeviceIdType.MESH
        )
    pl.semaphore_wait(barrier, len(peers))


def send(src, dst, sems, index, axis, peer):
    copy = pltpu.make_async_remote_copy(
        src_ref=src,
        dst_ref=dst,
        send_sem=sems.at[0, index],
        recv_sem=sems.at[1, index],
        device_id={axis: peer},
        device_id_type=pl.DeviceIdType.MESH,
    )
    copy.start()
    return copy


def shard_peers():
    me = lax.axis_index(SH)
    side, core = me // 2, lax.rem(me, 2)
    return me, side, core, 2 * side + 1 - core, 2 * (1 - side) + core


class Part:
    def __init__(self, axes, ins, outs, scratch, copies, phases, specs=None):
        self.axes, self.ins, self.outs, self.scratch = axes, ins, outs, scratch
        self.copies, self.phases = copies, phases
        self.specs = specs or [VM] * len(ins)


def run_parts(parts, collective_id, name=None, cost=None):
    ins = sum([p.ins for p in parts], [])
    outs = sum([p.outs for p in parts], [])
    scratch = sum([p.scratch for p in parts], [])
    copies = sum(p.copies for p in parts)
    axes = sorted(set(sum([list(p.axes) for p in parts], [])))

    def body(*refs):
        sems = refs[-1]
        in_refs, out_refs = list(refs[: len(ins)]), list(refs[len(ins) : len(ins) + len(outs)])
        scr = list(refs[len(ins) + len(outs) : -1])
        peers = []
        for axis in axes:
            me, n = lax.axis_index(axis), lax.axis_size(axis)
            peers += [(axis, lax.rem(me + d, n)) for d in range(1, n)]
        greet(peers)
        base, running = 0, []
        for p in parts:
            take = lambda pool, k: [pool.pop(0) for _ in range(k)]
            refs_p = (take(in_refs, len(p.ins)), take(out_refs, len(p.outs)), take(scr, len(p.scratch)))
            counter = [base]

            def go(src, dst, axis, peer, counter=counter):
                counter[0] += 1
                return send(src, dst, sems, counter[0] - 1, axis, peer)

            running.append(p.phases(*refs_p, go))
            base += p.copies
        while running:
            running = [r for r in running if next(r, True) is None]

    return pl.pallas_call(
        body,
        out_shape=outs,
        in_specs=sum([p.specs for p in parts], []),
        out_specs=[VM] * len(outs),
        scratch_shapes=scratch + [pltpu.SemaphoreType.DMA((2, copies))],
        compiler_params=pltpu.CompilerParams(collective_id=collective_id, has_side_effects=True),
        cost_estimate=cost,
        name=name,
    )(*ins)


def start_swap(go, src, land, axis, gather):
    me, n = lax.axis_index(axis), lax.axis_size(axis)
    started = []
    for d in range(1, n):
        peer = lax.rem(me + d, n)
        started.append(go(src if gather else src.at[peer], land.at[me], axis, peer))
    land[me] = src[...] if gather else src[me]
    return started


def total_of(land, n):
    total = land[0].astype(f32)
    for j in range(1, n):
        total = total + land[j].astype(f32)
    return total


def exchange(axis, kind, x):
    n = lax.axis_size(axis)
    gather, summed = kind in (GATHER, GATHER_SUM), kind in (GATHER_SUM, SWAP_SUM)
    piece = x.shape if gather else x.shape[1:]
    shape = jax.ShapeDtypeStruct
    outs = [shape(piece, f32) if summed else shape((n,) + piece, x.dtype)]
    scratch = [pltpu.VMEM((n,) + piece, x.dtype)] if summed else []

    def phases(ins, outs, scr, go):
        land = scr[0] if summed else outs[0]
        started = start_swap(go, ins[0], land, axis, gather)
        yield
        for copy in started:
            copy.wait()
        if summed:
            outs[0][...] = total_of(land, n)

    return Part([axis], [x], outs, scratch, n - 1, phases)


def tree_gather(x):
    lines = x.shape[0]
    cuts = [(0, lines // 2), (lines // 2, lines)] if lines > 1 else [(0, 1)]
    cuts = [pl.ds(lo, hi - lo) for lo, hi in cuts]

    def phases(ins, outs, scr, go):
        x_ref, out_ref = ins[0], outs[0]
        me, _, _, near, far = shard_peers()
        across = [go(x_ref.at[c], out_ref.at[c, me], SH, far) for c in cuts]
        own = go(x_ref, out_ref.at[:, me], SH, near)
        out_ref[:, me] = x_ref[...]
        yield
        handed = []
        for c, copy in zip(cuts, across):
            copy.wait_recv()
            handed.append(go(out_ref.at[c, far], out_ref.at[c, far], SH, near))
        yield
        for copy in across:
            copy.wait_send()
        own.wait()
        for copy in handed:
            copy.wait()

    shape = (lines, 4) + x.shape[1:]
    return Part([SH], [x], [jax.ShapeDtypeStruct(shape, x.dtype)], [], 2 * len(cuts) + 1, phases)


def core_sum(x):
    piece = x.shape[1:]
    shape = jax.ShapeDtypeStruct

    def phases(ins, outs, scr, go):
        x_ref, (here, there), (land, kept, sems) = ins[0], outs, scr
        near = shard_peers()[3]
        sent = [go(x_ref.at[3], land.at[1], SH, near), go(x_ref.at[2], land.at[0], SH, near)]
        local = [pltpu.make_async_copy(x_ref.at[k], kept.at[k], sems.at[k]) for k in range(2)]
        for copy in local:
            copy.start()
        yield
        for k, out in ((1, there), (0, here)):
            sent[1 - k].wait()
            local[k].wait()
            out[...] = (kept[k].astype(f32) + land[k].astype(f32)).astype(bf16)

    return Part(
        [SH],
        [x],
        [shape(piece, bf16)] * 2,
        [pltpu.VMEM((2,) + piece, bf16)] * 2 + [pltpu.SemaphoreType.DMA((2,))],
        2,
        phases,
        [pl.BlockSpec(memory_space=pl.ANY)],
    )


class Tree:
    copies = 3

    @staticmethod
    def scratch(piece):
        return [pltpu.VMEM((2,) + piece, bf16)] + [pltpu.VMEM(piece, bf16)] * 2

    def __init__(self, x, scr, go):
        self.x, (self.land, self.mine, self.got), self.go = x, scr, go
        self.me, self.side, self.core, self.near, self.far = shard_peers()
        other = 2 * (1 - self.side) + 1 - self.core
        self.first = [
            go(x.at[other], self.land.at[0], SH, self.near),
            go(x.at[self.near], self.land.at[1], SH, self.near),
        ]

    def across(self):
        self.first[0].wait_recv()
        self.mine[...] = (self.x[self.far].astype(f32) + self.land[0].astype(f32)).astype(bf16)
        self.second = self.go(self.mine, self.got, SH, self.far)

    def result(self):
        self.first[1].wait_recv()
        total = self.x[self.me].astype(f32) + self.land[1].astype(f32)
        self.second.wait_recv()
        return total + self.got[...].astype(f32)

    def close(self):
        for copy in (*self.first, self.second):
            copy.wait_send()


def turned_ids(ids_ref):
    ids = ids_ref[...].astype(f32)
    return jnp.transpose(jnp.concatenate([ids] * 4, axis=0)).astype(jnp.int32)


def slot_places(ids, lines, slots):
    rows = ids.shape[0]
    lane = lax.broadcasted_iota(jnp.int32, (rows, 128), 1)
    hot = [lane == column(ids, k) for k in range(2)]
    before = (
        lax.broadcasted_iota(jnp.int32, (rows, rows), 0)
        > lax.broadcasted_iota(jnp.int32, (rows, rows), 1)
    ).astype(bf16)
    named = jnp.where(hot[0] | hot[1], 1.0, 0.0).astype(bf16)
    earlier = jnp.dot(before, named, preferred_element_type=f32)
    slot_at = lax.broadcasted_iota(jnp.int32, (rows, slots), 1).astype(f32)
    place = []
    for k in range(2):
        number = jnp.sum(jnp.where(hot[k], earlier, 0.0), axis=1, keepdims=True)
        wanted = column(ids, k).astype(f32) * CAP + number
        wanted = jnp.where(column(ids, k) < lines, wanted, -1.0)
        place.append(jnp.where(slot_at == wanted, 1.0, 0.0))
    return place


def front(hidden, w_mine, gain, routes, out_grad, docs):
    rows, model = hidden.shape
    lines = lax.axis_size(EX)
    width = model // lines
    shape = jax.ShapeDtypeStruct
    last = lines - 1

    slots = lines * CAP

    def body(hid_ref, w_ref, gain_ref, ids_ref, up_ref, docs_ref, attn_ref, q_ref, kv_ref, place_ref, rows_out, info_ref, land, w_all, kv_own, rows_s, sems):
        line_me = lax.axis_index(EX)
        me, _, _, near, far = shard_peers()
        left, right = jnp.maximum(line_me - 1, 0), jnp.minimum(line_me + 1, last)
        greet(
            [(EX, lax.rem(line_me + d, lines)) for d in range(1, lines)]
            + [(SH, lax.rem(me + d, 4)) for d in range(1, 4)]
        )

        def copy(src, dst, index, axis, peer):
            return pltpu.make_async_remote_copy(
                src_ref=src,
                dst_ref=dst,
                send_sem=sems.at[0, index],
                recv_sem=sems.at[1, index],
                device_id={axis: peer},
                device_id_type=pl.DeviceIdType.MESH,
            )

        def relay(step, way):
            block = line_me - step if way == 0 else line_me + step
            block = jnp.clip(block, 0, last)
            src = hid_ref if step == 0 else land.at[block]
            return copy(src, land.at[block], last * way + step, EX, right if way == 0 else left)

        def sends(step, way):
            if way == 0:
                return (line_me < last) & (line_me - step >= 0)
            return (line_me > 0) & (line_me + step <= last)

        def comes(step, way):
            return line_me - 1 - step >= 0 if way == 0 else line_me + 1 + step <= last

        def source(step, way):
            line = line_me - 1 - step if way == 0 else line_me + 1 + step
            return jnp.clip(line, 0, last)

        def arrival(step, way):
            line = source(step, way)
            return copy(land.at[line], land.at[line], last * way + step, EX, right if way == 0 else left)

        base = 2 * last
        for way in range(2):

            @pl.when(sends(0, way))
            def _():
                relay(0, way).start()

        w_far = copy(w_ref, w_all.at[me], base, SH, far)
        w_near = copy(w_ref, w_all.at[me], base + 1, SH, near)
        w_pass = copy(w_all.at[far], w_all.at[far], base + 2, SH, near)
        w_far.start()
        w_near.start()
        w_all[me] = w_ref[...]
        docs = docs_ref[...]
        lane = lax.broadcasted_iota(jnp.int32, (docs.shape[0], 128), 1)
        block = lax.broadcasted_iota(jnp.int32, (docs.shape[0], 128), 0)
        table = jnp.where(lane == DOCS + block, jnp.broadcast_to(docs[:, 0:1], lane.shape), 0)
        for doc in range(1, DOCS):
            before = jnp.sum(jnp.where(docs < doc, 1, 0), axis=1, keepdims=True)
            table = table + jnp.where(lane == doc, jnp.broadcast_to(before, lane.shape), 0)
        info_ref[...] = jnp.sum(table, axis=0, keepdims=True)
        ids = turned_ids(ids_ref)
        place = slot_places(ids, lines, slots)
        for k in range(2):
            place_ref[k] = place[k].astype(bf16)
        either = (place[0] + place[1]).astype(bf16)
        rows_s[...] = contract(either, up_ref[...], 0, 0).astype(bf16).reshape(lines, CAP, model)
        base += 3
        kv_far = lambda line: copy(kv_own.at[line], kv_ref.at[line, me], base + line, SH, far)
        kv_near = lambda line: copy(
            kv_own.at[line], kv_ref.at[line, me], base + lines + line, SH, near
        )
        kv_pass = lambda line: copy(
            kv_ref.at[line, far], kv_ref.at[line, far], base + 2 * lines + line, SH, near
        )

        def project(line, x):
            inputs = x.astype(f32)
            inv = lax.rsqrt(jnp.mean(inputs * inputs, axis=1, keepdims=True) + norm_eps)
            attn_in = (inputs * inv * gain_ref[...][None]).astype(bf16)
            attn_ref[line] = attn_in
            value = jnp.dot(
                attn_in, w_all[...].reshape(model, 3 * width), preferred_element_type=f32
            ).astype(bf16)
            kv_own[line] = value[:, : 2 * width]
            kv_far(line).start()
            kv_near(line).start()
            kv_ref[line, me] = value[:, : 2 * width]
            q_ref[line] = value[:, 2 * width :]

        def hand(line):
            kv_far(line).wait_recv()
            kv_pass(line).start()

        w_far.wait_recv()
        w_pass.start()
        w_near.wait_recv()
        w_pass.wait_recv()
        project(line_me, hid_ref[...])
        for step in range(last):
            for way in range(2):

                @pl.when(comes(step, way))
                def _():
                    arrival(step, way).wait_recv()

                if step + 1 < last:

                    @pl.when(sends(step + 1, way))
                    def _():
                        relay(step + 1, way).start()

            for way in range(2):

                @pl.when(comes(step, way))
                def _():
                    line = source(step, way)
                    project(line, land[line])

            if step == last - 2:
                first = base + 3 * lines
                ups = []
                for d in range(1, lines):
                    peer = lax.rem(line_me + d, lines)
                    ups.append(copy(rows_s.at[peer], rows_out.at[line_me], first + d - 1, EX, peer))
                    ups[-1].start()
                rows_out[line_me] = rows_s[line_me]
            if step == 0:
                hand(line_me)
            else:
                for way in range(2):

                    @pl.when(comes(step - 1, way))
                    def _():
                        hand(source(step - 1, way))

        for way in range(2):

            @pl.when(comes(last - 1, way))
            def _():
                hand(source(last - 1, way))

        for way in range(2):
            for step in range(last):

                @pl.when(sends(step, way))
                def _():
                    relay(step, way).wait_send()

        w_far.wait_send()
        w_near.wait_send()
        w_pass.wait_send()
        for line in range(lines):
            kv_far(line).wait_send()
            kv_near(line).wait()
            kv_pass(line).wait()
        for up in ups:
            up.wait()

    return pl.pallas_call(
        body,
        out_shape=[
            shape((lines, rows, model), bf16),
            shape((lines, rows, width), bf16),
            shape((lines, 4, rows, 2 * width), bf16),
            shape((2, rows, slots), bf16),
            shape((lines, CAP, model), bf16),
            shape((1, 128), jnp.int32),
        ],
        in_specs=[VM] * 6,
        out_specs=[VM] * 6,
        scratch_shapes=[
            pltpu.VMEM((lines, rows, model), bf16),
            pltpu.VMEM((4, rows, 3 * width), bf16),
            pltpu.VMEM((lines, rows, 2 * width), bf16),
            pltpu.VMEM((lines, CAP, model), bf16),
            pltpu.SemaphoreType.DMA((2, 3 * last + 3 + 3 * lines)),
        ],
        compiler_params=pltpu.CompilerParams(collective_id=0, has_side_effects=True),
        name="front",
    )(hidden, w_mine, gain, routes, out_grad, docs)


def column(x, k):
    return x[:, k : k + 1]


def core_share(go, own, far, out):
    me, _, _, near, other = shard_peers()
    sent = [go(own, out.at[:, me], SH, near), go(far, out.at[:, other], SH, near)]
    out[:, me] = own[...]
    out[:, other] = far[...]
    return sent


def route(heads, hidden, gain, small_w, routes, place, wo, wo_far, n_ids):
    lines, rows, width = heads.shape
    model = lines * width
    slots = lines * CAP
    shape = jax.ShapeDtypeStruct

    def phases(ins, outs, scr, go):
        heads_ref, hid_ref, gain_ref, small_ref, routes_ref, place_ref, wo_ref, wof_ref = ins
        rows_out, wo_all, resid_ref, table_ref, low_ref = outs
        land, rows_s = scr
        swaps = start_swap(go, heads_ref, land, EX, False)
        swaps += core_share(go, wo_ref, wof_ref, wo_all)
        ids = turned_ids(routes_ref)
        lane = lax.broadcasted_iota(jnp.int32, (rows, 128), 1)
        hot = [lane == column(ids, k) for k in range(2)]
        place = [place_ref[k].astype(f32) for k in range(2)]
        either = place_ref[0] + place_ref[1]
        for copy in swaps:
            copy.wait()
        for line in range(lines):
            low_ref[:, line * width : (line + 1) * width] = land[line]
        w_out = wo_all[...].reshape(model, model)
        resid = hid_ref[...].astype(f32) + jnp.dot(
            low_ref[...], w_out, preferred_element_type=f32
        )
        resid_ref[...] = resid
        inv = lax.rsqrt(jnp.mean(resid * resid, axis=1, keepdims=True) + norm_eps)
        moe_in = resid * inv * gain_ref[...][None]
        small = contract(moe_in, small_ref[...], 1, 1, HIGH)
        chosen = [jnp.sum(jnp.where(h, small, 0.0), axis=1, keepdims=True) for h in hot]
        top = jnp.maximum(chosen[0], chosen[1])
        powers = [jnp.exp(c - top) for c in chosen]
        gates = [p / (powers[0] + powers[1]) for p in powers]
        weight = place[0] * gates[0] + place[1] * gates[1]
        weight = contract(weight, jnp.ones((rows, 128), f32), 0, 0, HIGH)[:, 0:1]
        high = weight.astype(bf16)
        low = (weight - high.astype(f32)).astype(bf16)
        slot_lane = lax.broadcasted_iota(jnp.int32, (slots, 128), 1)
        extra = jnp.where(slot_lane == 0, high, jnp.where(slot_lane == 1, low, jnp.zeros_like(low)))
        rows_s[:, :, :model] = (
            contract(either, moe_in.astype(bf16), 0, 0).astype(bf16).reshape(lines, CAP, model)
        )
        rows_s[:, :, model:] = extra.reshape(lines, CAP, 128)
        row_swap = start_swap(go, rows_s, rows_out, EX, False)
        table = jnp.zeros((rows, 128), f32)
        entries = list(gates)
        for j in range(2):
            pair = [column(small, n_ids + 2 * j + k) for k in range(2)]
            top = jnp.maximum(pair[0], pair[1])
            powers = [jnp.exp(c - top) for c in pair]
            entries += [p / (powers[0] + powers[1]) for p in powers]
        entries += [column(ids, k).astype(f32) for k in range(2)]
        for k, entry in enumerate(entries):
            table = jnp.where(lane == k, entry, table)
        table_ref[...] = table
        for copy in row_swap:
            copy.wait()
        yield

    ins = [heads, hidden, gain, small_w, routes, place, wo, wo_far]
    outs = [
        shape((lines, CAP, model + 128), bf16),
        shape((1, 4, model // 4, model), bf16),
        shape((rows, model), f32),
        shape((rows, 128), f32),
        shape((rows, model), bf16),
    ]
    scratch = [
        pltpu.VMEM((lines, rows, width), bf16),
        pltpu.VMEM((lines, CAP, model + 128), bf16),
    ]
    return Part([EX, SH], ins, outs, scratch, 2 * (lines - 1) + 2, phases)


def share_weights(own, far):
    def phases(ins, outs, scr, go):
        copies = core_share(go, ins[0], ins[1], outs[0])
        yield
        for copy in copies:
            copy.wait()

    dims = (own.shape[0], 4) + own.shape[1:]
    return Part([SH], [own, far], [jax.ShapeDtypeStruct(dims, bf16)], [], 2, phases)


def to_heads(returned, input_ret, place, table, resid, low, out_grad, gain, small_t, const_vec, wo, n_ids):
    rows, model = resid.shape
    lines = returned.shape[0]
    width = model // lines
    own = rows // lines
    slots = lines * CAP
    shape = jax.ShapeDtypeStruct

    def phases(ins, outs, scr, go):
        ret_ref, iret_ref, place_ref, table_ref, resid_ref, low_ref, up_ref, gain_ref, st_ref, vec_ref, wo_ref = ins
        heads_out, layer_ref, rgrad_ref, term_ref, packed_ref = outs
        (back_s,) = scr
        table = table_ref[...]
        gates = [column(table, k) for k in range(2)]
        alpha = [[column(table, 2 + 2 * j + k) for k in range(2)] for j in range(2)]
        ids = [column(table, 6 + k) for k in range(2)]
        vecs = [vec_ref[j : j + 1, :] for j in range(2)]
        resid = resid_ref[...]
        upstream = up_ref[...].astype(f32)
        inv = lax.rsqrt(jnp.mean(resid * resid, axis=1, keepdims=True) + norm_eps)
        normed = resid * inv
        moe_in = normed * gain_ref[...][None]
        returned = ret_ref[...].reshape(slots, model)
        total = lambda x: jnp.sum(x, axis=1, keepdims=True)
        flag = lambda x: jnp.where(x, 1.0, 0.0)
        copy_dot = total(upstream * moe_in)
        vec_dot = [total(upstream * v) for v in vecs]
        const_dot = [alpha[j][0] * copy_dot + alpha[j][1] * vec_dot[j] for j in range(2)]
        output = resid
        backs = []
        copy_gate = jnp.zeros((rows, 1), f32)
        const_gate = [jnp.zeros((rows, 1), f32) for _ in range(2)]
        for k in range(2):
            rows_k = jnp.dot(place_ref[k], returned, preferred_element_type=f32)
            is_ffn, is_copy = flag(ids[k] < lines), flag(ids[k] == lines + 1)
            is_const = [flag(ids[k] == lines + 2 + j) for j in range(2)]
            output = output + (gates[k] * is_ffn) * rows_k
            backs.append(
                is_ffn * total(upstream * rows_k)
                + is_copy * copy_dot
                + is_const[0] * const_dot[0]
                + is_const[1] * const_dot[1]
            )
            copy_gate = copy_gate + gates[k] * is_copy
            const_gate = [const_gate[j] + gates[k] * is_const[j] for j in range(2)]
        through = copy_gate + const_gate[0] * alpha[0][0] + const_gate[1] * alpha[1][0]
        output = output + through * moe_in
        for j in range(2):
            output = output + (const_gate[j] * alpha[j][1]) * vecs[j]
        layer_ref[...] = output.astype(bf16)
        mean_back = gates[0] * backs[0] + gates[1] * backs[1]
        lane = lax.broadcasted_iota(jnp.int32, (rows, 128), 1)
        lane_f = lane.astype(f32)
        small = jnp.zeros((rows, 128), f32)
        for k in range(2):
            small = jnp.where(lane_f == ids[k], gates[k] * (backs[k] - mean_back), small)
        for j in range(2):
            grads = [const_gate[j] * copy_dot, const_gate[j] * vec_dot[j]]
            mean = alpha[j][0] * grads[0] + alpha[j][1] * grads[1]
            for k in range(2):
                small = jnp.where(
                    lane == n_ids + 2 * j + k, alpha[j][k] * (grads[k] - mean), small
                )
            small = jnp.where(lane == n_ids + 4 + j, alpha[j][1] * const_gate[j], small)
        either = place_ref[0] + place_ref[1]
        moe_grad = (
            jnp.dot(either, iret_ref[...].reshape(slots, model), preferred_element_type=f32)
            + through * upstream
            + jnp.dot(small, st_ref[...], preferred_element_type=f32, precision=HIGH)
        )
        resid_grad = upstream + rms_back(resid, inv, gain_ref[...][None], moe_grad)
        branch = resid_grad.astype(bf16)
        back = contract(branch, wo_ref[...], 1, 1).astype(bf16)
        for line in range(lines):
            back_s[line] = back[:, line * width : (line + 1) * width]
        swaps = start_swap(go, back_s, heads_out, EX, False)
        rgrad_ref[...] = resid_grad
        packed_ref[...] = jnp.zeros_like(packed_ref)
        packed_ref[0:1] = jnp.sum(moe_grad * normed, axis=0, keepdims=True)
        small_grad = contract(small, moe_in, 0, 0, HIGH)
        vec_grad = contract(small, upstream, 0, 0, HIGH)
        packed_ref[1:3] = vec_grad[n_ids + 4 : n_ids + 6]
        packed_ref[3 : 7 + n_ids] = small_grad[: n_ids + 4]
        term = contract(low_ref[...], branch, 0, 0).astype(bf16)
        for line in range(lines):
            for piece in range(4):
                at = (line * 4 + piece) * own
                term_ref[piece, line] = term[at : at + own]
        for copy in swaps:
            copy.wait()
        yield

    ins = [returned, input_ret, place, table, resid, low, out_grad, gain, small_t, const_vec, wo]
    outs = [
        shape((lines, rows, width), bf16),
        shape((rows, model), bf16),
        shape((rows, model), f32),
        shape((4, lines, own, model), bf16),
        shape((-(-(7 + n_ids) // 8) * 8, model), f32),
    ]
    return Part([EX], ins, outs, [pltpu.VMEM((lines, rows, width), bf16)], lines - 1, phases)


def tail(dkv, dq, attn_in, weights, out_term, packed, hidden, resid_grad, gain, pairs):
    lines, rows, width = dq.shape
    model = lines * width
    own = rows // lines
    groups = lax.axis_size(GR)
    shape = jax.ShapeDtypeStruct
    vmem = pltpu.VMEM
    tok = lines * rows
    few = lines // 2
    dkv_piece, q_piece = (few, rows, 2 * width), (lines, own, width)
    kv_piece, o_piece = (lines, own, 2 * width), (lines, own, model)
    part_dims = (width, 2 * width, model)

    def phases(ins, outs, scr, go):
        lo_ref, hi_ref, dq_ref, attn_ref, w_ref, o_ref, packed_ref, hid_ref, resid_ref, gain_ref = ins[:10]
        input_ref, q_out, kv_out, out_out, packed_out, gain_out = outs[:6]
        scr = list(scr)
        take = lambda k: [scr.pop(0) for _ in range(k)]
        lo_scr, hi_scr, q_scr, kvw_scr, o_scr = take(3), take(3), take(3), take(3), take(3)
        own_kv, q_t, kv_t, dq_all, dkv_all, dq_full = take(6)
        kv_sems, w_s, w_sem = take(3)
        held = take(2 * len(pairs))
        w_copy = pltpu.make_async_copy(w_ref, w_s, w_sem.at[2 * len(pairs)])
        fetch = [
            pltpu.make_async_copy(ins[10 + k], held[k], w_sem.at[k]) for k in range(2 * len(pairs))
        ]
        for copy in fetch:
            copy.start()
        w_copy.start()
        sums, lands, halves, gots = take(3), take(3), take(3), take(3)
        pk_l, pk_s, pk_g = take(3)
        mid_l, mid_s = take(2)
        gn_l, gn_s, gn_g, gn_0, gn_1, gn_2 = take(6)
        me = lax.axis_index(SH)

        line_me, group_me = lax.axis_index(EX), lax.axis_index(GR)
        kv_trees = [Tree(lo_ref, lo_scr, go), Tree(hi_ref, hi_scr, go)]

        def kv_copy(sender, target):
            return pltpu.make_async_remote_copy(
                src_ref=own_kv.at[target],
                dst_ref=dkv_all.at[sender],
                send_sem=kv_sems.at[0, target],
                recv_sem=kv_sems.at[1, sender],
                device_id={EX: target},
                device_id_type=pl.DeviceIdType.MESH,
            )

        def push_kv(k):
            own_kv[k * few : (k + 1) * few] = kv_trees[k].result().astype(bf16)
            for target in range(k * few, (k + 1) * few):

                @pl.when(line_me != target)
                def _():
                    kv_copy(line_me, jnp.int32(target)).start()

                @pl.when(line_me == target)
                def _():
                    dkv_all[target] = own_kv[target]

        dq_swap = start_swap(go, dq_ref, dq_all, EX, False)
        o_tree = Tree(o_ref, o_scr, go)
        pk1 = start_swap(go, packed_ref, pk_l, EX, True)
        def term(rows_ref, out):
            value = contract(attn_ref[...], rows_ref[...].reshape(tok, rows_ref.shape[-1]), 0, 0)
            value = value.astype(bf16)
            for line in range(lines):
                for piece in range(4):
                    at = (line * 4 + piece) * own
                    out[piece, line] = value[at : at + own]

        for tree in kv_trees:
            tree.across()
        wide = []
        for k in range(len(pairs)):
            mine, other = outs[6 + 2 * k : 8 + 2 * k]
            here, there = held[2 * k : 2 * k + 2]
            fetch[2 * k].wait()
            fetch[2 * k + 1].wait()
            mine[...] = (here[...].astype(f32) + there[...].astype(f32)).astype(bf16)
            wide.append(go(mine, other, GR, lax.rem(group_me + 1, groups)))
        term(dq_ref, q_t)
        o_tree.across()
        q_tree = Tree(q_t, q_scr, go)
        trees = [q_tree, None, o_tree]

        def lines_out(k):
            sums[k][...] = trees[k].result().astype(bf16)
            return start_swap(go, sums[k], lands[k], EX, False)

        push_kv(0)
        push_kv(1)
        o_lines = lines_out(2)
        q_tree.across()
        term(own_kv, kv_t)
        kvw_tree = Tree(kv_t, kvw_scr, go)
        trees[1] = kvw_tree
        for copy in pk1:
            copy.wait()
        mid_l[...] = total_of(pk_l, lines)
        pk2 = start_swap(go, mid_l, pk_s, SH, True)
        kvw_tree.across()
        q_lines = lines_out(0)
        for copy in dq_swap:
            copy.wait()
        for line in range(lines):
            dq_full[:, line * width : (line + 1) * width] = dq_all[line]
        w_copy.wait()
        grad = contract(dq_full[...], w_s[0], 1, 1)
        for copy in pk2:
            copy.wait()
        mid_s[...] = total_of(pk_s, 4)
        pk3 = start_swap(go, mid_s, pk_g, GR, True)
        kv_lines = lines_out(1)
        for other in range(lines):

            @pl.when(line_me != other)
            def _():
                kv_copy(jnp.int32(other), line_me).wait_recv()
                kv_copy(line_me, jnp.int32(other)).wait_send()

        for half in range(2):
            for line in range(lines):
                dq_full[:, line * width : (line + 1) * width] = dkv_all[
                    line, :, half * width : (half + 1) * width
                ]
            grad = grad + contract(dq_full[...], w_s[1 + half], 1, 1)
        inputs = hid_ref[...].astype(f32)
        inv = lax.rsqrt(jnp.mean(inputs * inputs, axis=1, keepdims=True) + norm_eps)
        normed = inputs * inv
        gn_0[...] = jnp.sum(grad * normed, axis=0, keepdims=True)
        gn1 = start_swap(go, gn_0, gn_l, EX, True)
        input_ref[...] = resid_ref[...] + rms_back(inputs, inv, gain_ref[...][None], grad)
        swaps = [None] * 3
        for k, copies in ((2, o_lines), (0, q_lines)):
            for copy in copies:
                copy.wait()
            if k == 2:
                halves[k][...] = total_of(lands[k], lines).astype(bf16)
            else:
                halves[k][...] = lands[k][...]
            swaps[k] = start_swap(go, halves[k], gots[k], GR, True)
        for copy in gn1:
            copy.wait()
        gn_1[...] = total_of(gn_l, lines)
        gn2 = start_swap(go, gn_1, gn_s, SH, True)
        for copy in kv_lines:
            copy.wait()
        halves[1][...] = lands[1][...]
        swaps[1] = start_swap(go, halves[1], gots[1], GR, True)
        for copy in gn2:
            copy.wait()
        gn_2[...] = total_of(gn_s, 4)
        gn3 = start_swap(go, gn_2, gn_g, GR, True)
        for copy in pk3:
            copy.wait()
        packed_out[...] = total_of(pk_g, groups)
        for k, out in ((2, out_out), (0, q_out), (1, kv_out)):
            for copy in swaps[k]:
                copy.wait()
            out[...] = total_of(gots[k], groups)
        for copy in gn3:
            copy.wait()
        gain_out[...] = total_of(gn_g, groups)
        for copy in wide:
            copy.wait()
        for tree in (*kv_trees, o_tree, q_tree, kvw_tree):
            tree.close()
        yield

    pieces = [(lines, own, d) for d in part_dims]
    got_pieces = pieces[:2] + [(own, model)]
    scratch = Tree.scratch(dkv_piece) * 2 + Tree.scratch(q_piece) + Tree.scratch(kv_piece)
    scratch += Tree.scratch(o_piece)
    scratch += [
        vmem((lines, rows, 2 * width), bf16),
        vmem((4,) + q_piece, bf16),
        vmem((4,) + kv_piece, bf16),
        vmem((lines, rows, width), bf16),
        vmem((lines, rows, 2 * width), bf16),
        vmem((rows, model), bf16),
        pltpu.SemaphoreType.DMA((2, lines)),
        vmem(weights.shape, bf16),
        pltpu.SemaphoreType.DMA((2 * len(pairs) + 1,)),
    ]
    scratch += [vmem(x.shape, bf16) for pair in pairs for x in pair]
    scratch += [vmem(p, bf16) for p in pieces] + [vmem(p, bf16) for p in pieces]
    scratch += [vmem(p, bf16) for p in got_pieces] + [vmem((groups,) + p, bf16) for p in got_pieces]
    scratch += [vmem((n,) + packed.shape, f32) for n in (lines, 4, groups)]
    scratch += [vmem(packed.shape, f32)] * 2
    scratch += [vmem((n, 1, model), f32) for n in (lines, 4, groups)] + [vmem((1, model), f32)] * 3
    copies = len(pairs) + 5 * Tree.copies + 6 * (lines - 1) + 2 * 3 + 5 * (groups - 1)
    outs = [
        shape((rows, model), f32),
        shape((lines, own, width), f32),
        shape((lines, own, 2 * width), f32),
        shape((own, model), f32),
        shape(packed.shape, f32),
        shape((1, model), f32),
    ] + [shape(x.shape, bf16) for pair in pairs for x in pair]
    ins = [*dkv, dq, attn_in, weights, out_term, packed, hidden, resid_grad, gain]
    ins += [x for pair in pairs for x in pair]
    hbm = pl.BlockSpec(memory_space=pl.ANY)
    specs = [hbm if x is weights or k >= 10 else VM for k, x in enumerate(ins)]
    return Part([EX, SH, GR], ins, outs, scratch, copies, phases, specs)


def expert_body(steps, x_ref, g_ref, wg_ref, wu_ref, wd_ref, eo_ref, ib_ref, ga_ref, up_ref, d_ref, eo_s, ib_s, g_s, xt_s):
    i = pl.program_id(0)
    me, side, core, _, _ = shard_peers()

    @pl.when(i == 0)
    def _():
        eo_s[...] = jnp.zeros_like(eo_s)
        ib_s[...] = jnp.zeros_like(ib_s)
        model = g_ref.shape[1]
        high, low = x_ref[:, model : model + 1], x_ref[:, model + 1 : model + 2]
        gate = high.astype(f32) + low.astype(f32)
        g_s[...] = (g_ref[...].astype(f32) * gate).astype(bf16)
        xt_s[...] = jnp.transpose(x_ref[:, :model])

    x, g = x_ref[:, : g_ref.shape[1]], g_s[...]
    wg, wu, wd = wg_ref[...], wu_ref[...], wd_ref[...]
    gate_pre = jnp.dot(x, wg, preferred_element_type=f32)
    up_pre = jnp.dot(x, wu, preferred_element_type=f32)
    hidden_grad = contract(g, wd, 1, 1)
    gate_sigmoid = jax.nn.sigmoid(gate_pre)
    act = (gate_pre * gate_sigmoid * up_pre).astype(bf16)
    gate_back = (
        hidden_grad * up_pre * gate_sigmoid * (1.0 + gate_pre * (1.0 - gate_sigmoid))
    ).astype(bf16)
    up_back = (hidden_grad * gate_pre * gate_sigmoid).astype(bf16)
    eo_s[...] += jnp.dot(act, wd, preferred_element_type=f32)
    ib_s[...] += contract(gate_back, wg, 1, 1) + contract(up_back, wu, 1, 1)

    def place(quarter):
        return 2 * lax.rem(lax.rem(quarter, 2) + core, 2) + lax.rem(quarter // 2 + side, 2)

    rows = ga_ref.shape[1]
    for ref, back in ((ga_ref, gate_back), (up_ref, up_back)):
        term = jnp.dot(xt_s[...], back, preferred_element_type=f32).astype(bf16)
        for quarter in range(4):
            ref[place(jnp.int32(quarter))] = term[quarter * rows : (quarter + 1) * rows]
    d_ref[place(i)] = contract(act, g, 0, 0).astype(bf16)

    @pl.when(i == steps - 1)
    def _():
        eo_ref[...] = eo_s[...].astype(bf16)
        ib_ref[...] = ib_s[...].astype(bf16)


def expert(x, g, wg, wu, wd):
    slots, model = g.shape
    inner = wg.shape[1]
    steps = 4
    tile = inner // steps
    quarter = model // 4
    shape = jax.ShapeDtypeStruct
    whole = lambda dims: pl.BlockSpec(dims, lambda i: (0,) * len(dims))
    return pl.pallas_call(
        functools.partial(expert_body, steps),
        grid=(steps,),
        out_shape=[
            shape((slots, model), bf16),
            shape((slots, model), bf16),
            shape((4, quarter, inner), bf16),
            shape((4, quarter, inner), bf16),
            shape((4, tile, model), bf16),
        ],
        in_specs=[
            whole(x.shape),
            whole((slots, model)),
            pl.BlockSpec((model, tile), lambda i: (0, i)),
            pl.BlockSpec((model, tile), lambda i: (0, i)),
            pl.BlockSpec((tile, model), lambda i: (i, 0)),
        ],
        out_specs=[
            whole((slots, model)),
            whole((slots, model)),
            pl.BlockSpec((4, quarter, tile), lambda i: (0, 0, i)),
            pl.BlockSpec((4, quarter, tile), lambda i: (0, 0, i)),
            whole((4, tile, model)),
        ],
        scratch_shapes=[pltpu.VMEM((slots, model), f32)] * 2 + [pltpu.VMEM((slots, model), bf16), pltpu.VMEM((model, slots), bf16)],
        cost_estimate=pl.CostEstimate(flops=6 * 10**9, bytes_accessed=2 * 10**7, transcendentals=4 * 10**5),
        name="ffn",
    )(x, g, wg, wu, wd)


def head_columns(h, shape, axis):
    return lax.broadcasted_iota(jnp.int32, shape, axis) // HEAD_DIM == h


def allowed(block, key_blk, qpos, qstart, prompt):
    kpos = block * key_blk + lax.broadcasted_iota(jnp.int32, (key_blk, qpos.shape[1]), 0)
    return (kpos <= qpos) & ((kpos >= qstart) | (kpos < prompt))


def doc_start(block, info_ref, qinfo_ref):
    docs = qinfo_ref[pl.ds(block, 1), :]
    starts = jnp.zeros(docs.shape, jnp.int32)
    for doc in range(1, DOCS):
        starts = jnp.where(docs == doc, info_ref[0, doc], starts)
    return starts, info_ref[0, info_ref[0, DOCS + block]]


def attend_body(lines, heads, info_ref, q_ref, kv_ref, qinfo_ref, o_ref, low_ref, lse_ref, k_s, vt_s, acc_s, ml_s, qm_s):
    shard = lax.axis_index(SH)
    rows, width = q_ref.shape[1:]
    blocks = vt_s.shape[0]
    key_blk = vt_s.shape[2]
    prompt = info_ref[0, 1]

    @pl.loop(0, blocks)
    def _(j):
        at = pl.ds(pl.multiple_of(j * key_blk, key_blk), key_blk)
        k_s[at, :] = kv_ref[at, :width]
        vt_s[j] = jnp.transpose(kv_ref[at, width:].astype(f32)).astype(bf16)

    @pl.loop(0, lines)
    def _(line):
        start = (line * 4 + shard) * rows
        queries = q_ref[line].astype(f32) * HEAD_DIM**-0.5
        qpos = start + lax.broadcasted_iota(jnp.int32, (1, rows), 1)
        qstart, first = doc_start(line * 4 + shard, info_ref, qinfo_ref)
        for h in range(heads):
            qm_s[h] = jnp.where(head_columns(h, queries.shape, 1), queries, 0.0).astype(bf16)
        acc_s[...] = jnp.zeros_like(acc_s)
        for h in range(heads):
            ml_s[h, 0:1, :] = jnp.full((1, rows), neg_fill, f32)
            ml_s[h, 1:2, :] = jnp.zeros((1, rows), f32)

        @pl.loop(0, (start + rows + key_blk - 1) // key_blk)
        def _(j):
            @pl.when((j * key_blk < prompt) | ((j + 1) * key_blk > first))
            def _():
                keys = k_s[pl.ds(pl.multiple_of(j * key_blk, key_blk), key_blk), :]
                ok = allowed(j, key_blk, qpos, qstart, prompt)
                for h in range(heads):
                    scores = jnp.where(ok, contract(keys, qm_s[h], 1, 1), neg_fill)
                    old = ml_s[h, 0:1, :]
                    new = jnp.maximum(old, jnp.max(scores, axis=0, keepdims=True))
                    probs = jnp.exp(scores - new)
                    scale = jnp.exp(old - new)
                    ml_s[h, 0:1, :] = new
                    ml_s[h, 1:2, :] = ml_s[h, 1:2, :] * scale + jnp.sum(
                        probs, axis=0, keepdims=True
                    )
                    part = slice(h * HEAD_DIM, (h + 1) * HEAD_DIM)
                    acc_s[part, :] = acc_s[part, :] * scale + jnp.dot(
                        vt_s[j, part, :], probs.astype(bf16), preferred_element_type=f32
                    )

        for h in range(heads):
            part = slice(h * HEAD_DIM, (h + 1) * HEAD_DIM)
            total = ml_s[h, 1:2, :]
            acc_s[part, :] = acc_s[part, :] / total
            lse_ref[line, h : h + 1, :] = ml_s[h, 0:1, :] + jnp.log(total)
        result = jnp.transpose(acc_s[...])
        o_ref[line] = result
        low_ref[line] = result.astype(bf16)


def attend(info, q, kv, qinfo):
    lines, rows, width = q.shape
    heads = width // HEAD_DIM
    length = kv.shape[0]
    key_blk = KEY_BLK
    shape = jax.ShapeDtypeStruct
    return pl.pallas_call(
        functools.partial(attend_body, lines, heads),
        out_shape=[
            shape((lines, rows, width), f32),
            shape((lines, rows, width), bf16),
            shape((lines, 8, rows), f32),
        ],
        in_specs=[SM, VM, VM, VM],
        out_specs=[VM] * 3,
        scratch_shapes=[
            pltpu.VMEM((length, width), bf16),
            pltpu.VMEM((length // key_blk, width, key_blk), bf16),
            pltpu.VMEM((width, rows), f32),
            pltpu.VMEM((heads, 8, rows), f32),
            pltpu.VMEM((heads, rows, width), bf16),
        ],
        cost_estimate=pl.CostEstimate(flops=2 * 10**9, bytes_accessed=8 * 10**6, transcendentals=4 * 10**6),
        name="attend",
    )(info, q, kv, qinfo)


def attend_back_body(lines, heads, info_ref, q_ref, kv_ref, qinfo_ref, o_ref, lse_ref, back_ref, dq_ref, dkv_lo, dkv_hi, k_s, v_s, dk_s, dv_s, dq_s, qm_s, bm_s, delta_s):
    shard = lax.axis_index(SH)
    rows, width = q_ref.shape[1:]
    key_blk = KEY_BACK
    blocks = k_s.shape[0] // key_blk
    prompt = info_ref[0, 1]

    @pl.loop(0, blocks)
    def _(j):
        at = pl.ds(pl.multiple_of(j * key_blk, key_blk), key_blk)
        k_s[at, :] = kv_ref[at, :width]
        v_s[at, :] = kv_ref[at, width:]
        dk_s[at, :] = jnp.zeros((key_blk, width), f32)
        dv_s[at, :] = jnp.zeros((key_blk, width), f32)

    @pl.loop(0, lines)
    def _(line):
        start = (line * 4 + shard) * rows
        queries = q_ref[line].astype(f32) * HEAD_DIM**-0.5
        back = back_ref[line].astype(f32)
        qpos = start + lax.broadcasted_iota(jnp.int32, (1, rows), 1)
        qstart, first = doc_start(line * 4 + shard, info_ref, qinfo_ref)
        picks = (
            lax.broadcasted_iota(jnp.int32, (8, width), 1) // HEAD_DIM
            == lax.broadcasted_iota(jnp.int32, (8, width), 0)
        ).astype(f32)
        delta_s[...] = contract(picks, back * o_ref[line], 1, 1, HIGH)
        for h in range(heads):
            mine = head_columns(h, queries.shape, 1)
            qm_s[h] = jnp.where(mine, queries, 0.0).astype(bf16)
            bm_s[h] = jnp.where(mine, back, 0.0).astype(bf16)
        dq_s[...] = jnp.zeros_like(dq_s)

        @pl.loop(0, (start + rows + key_blk - 1) // key_blk)
        def _(j):
            @pl.when((j * key_blk < prompt) | ((j + 1) * key_blk > first))
            def _():
                at = pl.ds(pl.multiple_of(j * key_blk, key_blk), key_blk)
                keys, values = k_s[at, :], v_s[at, :]
                ok = allowed(j, key_blk, qpos, qstart, prompt)
                dk = jnp.zeros((key_blk, width), f32)
                dv = jnp.zeros((key_blk, width), f32)
                for h in range(heads):
                    scores = contract(keys, qm_s[h], 1, 1)
                    probs = jnp.where(ok, jnp.exp(scores - lse_ref[line, h : h + 1, :]), 0.0)
                    grads = contract(values, bm_s[h], 1, 1)
                    slow = (probs * (grads - delta_s[h : h + 1, :])).astype(bf16)
                    dv = dv + jnp.dot(probs.astype(bf16), bm_s[h], preferred_element_type=f32)
                    dk = dk + jnp.dot(slow, qm_s[h], preferred_element_type=f32)
                    dq_s[h] += contract(slow, keys, 0, 0)
                dk_s[at, :] += dk
                dv_s[at, :] += dv

        total = jnp.zeros(queries.shape, f32)
        for h in range(heads):
            total = jnp.where(head_columns(h, queries.shape, 1), dq_s[h], total)
        dq_ref[line] = (total * HEAD_DIM**-0.5).astype(bf16)

    half = lines // 2
    for k, ref in enumerate((dkv_lo, dkv_hi)):

        @pl.loop(0, half)
        def _(line):
            for piece in range(4):
                at = ((k * half + line) * 4 + piece) * rows
                at = pl.ds(pl.multiple_of(at, rows), rows)
                ref[piece, line, :, :width] = dk_s[at, :].astype(bf16)
                ref[piece, line, :, width:] = dv_s[at, :].astype(bf16)


def attend_back(info, q, kv, qinfo, o, lse, back):
    lines, rows, width = q.shape
    heads = width // HEAD_DIM
    length = kv.shape[0]
    shape = jax.ShapeDtypeStruct
    return pl.pallas_call(
        functools.partial(attend_back_body, lines, heads),
        out_shape=[
            shape((lines, rows, width), bf16),
            shape((4, lines // 2, rows, 2 * width), bf16),
            shape((4, lines // 2, rows, 2 * width), bf16),
        ],
        in_specs=[SM] + [VM] * 6,
        out_specs=[VM] * 3,
        scratch_shapes=[
            pltpu.VMEM((length, width), bf16),
            pltpu.VMEM((length, width), bf16),
            pltpu.VMEM((length, width), f32),
            pltpu.VMEM((length, width), f32),
            pltpu.VMEM((heads, rows, width), f32),
            pltpu.VMEM((heads, rows, width), bf16),
            pltpu.VMEM((heads, rows, width), bf16),
            pltpu.VMEM((8, rows), f32),
        ],
        cost_estimate=pl.CostEstimate(flops=5 * 10**9, bytes_accessed=12 * 10**6, transcendentals=4 * 10**6),
        name="attend_back",
    )(info, q, kv, qinfo, o, lse, back)


def finale_body(lines, n_ids, *refs):
    ins, outs = refs[:13], refs[13:]
    for k in range(3):
        outs[k][...] = ins[k][...].astype(f32) + ins[3 + k][...].astype(f32)
    for k in range(2):
        outs[3 + k][...] = ins[6 + k][...]

    @pl.when(pl.program_id(0) == 0)
    def _():
        q_sum, kv_sum, out_sum, small_ref, gain_ref = ins[8:]
        q_out, k_out, v_out, out_out, gain_out, mgain_out, vec_out, rout_out, mix_out = outs[5:]
        width = q_sum.shape[2]
        for line in range(lines):
            at = slice(line * width, (line + 1) * width)
            q_out[:, at] = q_sum[line]
            k_out[:, at] = kv_sum[line, :, :width]
            v_out[:, at] = kv_sum[line, :, width:]
        out_out[...] = out_sum[...]
        gain_out[...] = jnp.sum(gain_ref[...], axis=0)
        small = small_ref[...]
        mgain_out[...] = jnp.sum(small[0:1], axis=0)
        vec_out[...] = small[1:3]
        rout_out[...] = small[3 : 3 + n_ids]
        mix_out[...] = small[3 + n_ids : 7 + n_ids]


def finale(mine, far, input_grad, layer_out, sums, n_ids):
    steps = 4
    shape = jax.ShapeDtypeStruct
    own, model = sums[2].shape
    lines = sums[0].shape[0]

    def tiled(dims, dim):
        block = tuple(d // steps if k == dim else d for k, d in enumerate(dims))
        return pl.BlockSpec(block, lambda i: tuple(i if k == dim else 0 for k in range(2)))

    def whole(dims):
        return pl.BlockSpec(dims, lambda i: (0,) * len(dims))

    wide = [tiled(mine[0].shape, 1), tiled(mine[1].shape, 1), tiled(mine[2].shape, 0)]
    rows = [tiled(input_grad.shape, 0), tiled(layer_out.shape, 0)]
    small = [(own, model)] * 4 + [(model,), (model,), (2, model), (n_ids, model), (4, model)]
    return pl.pallas_call(
        functools.partial(finale_body, lines, n_ids),
        grid=(steps,),
        out_shape=[shape(m.shape, f32) for m in mine]
        + [shape(input_grad.shape, f32), shape(layer_out.shape, bf16)]
        + [shape(d, f32) for d in small],
        in_specs=wide + wide + rows + [whole(x.shape) for x in sums],
        out_specs=wide + rows + [whole(d) for d in small],
        cost_estimate=pl.CostEstimate(flops=10**7, bytes_accessed=10**7, transcendentals=0),
        name="finale",
    )(*mine, *far, input_grad, layer_out, *sums)


def swap(x, axis, partner):
    return lax.ppermute(x, axis, [(i, partner(i)) for i in range(lax.axis_size(axis))])


def fast_shards(
    hidden_in,
    segment_ids,
    routes,
    attn_gain,
    w_query,
    w_key,
    w_value,
    w_out,
    moe_gain,
    w_router,
    const_mix,
    const_vec,
    w_gate,
    w_up,
    w_down,
    out_grad,
):
    rows, model = hidden_in.shape
    lines = lax.axis_size(EX)
    line, shard = lax.axis_index(EX), lax.axis_index(SH)
    width = model // lines
    seg = segment_ids[0]
    length = seg.shape[0]

    w_qkv = jnp.stack([w_query, w_key, w_value])
    w_mine = lax.dynamic_slice_in_dim(w_qkv, line * width, width, axis=2)
    w_mine = jnp.concatenate([w_mine[1], w_mine[2], w_mine[0]], axis=1)
    qinfo = seg.reshape(length // rows, rows)
    attn_in, q, kv_all, place, recv_grads, info = front(
        hidden_in, w_mine, attn_gain, routes.T, out_grad, qinfo
    )
    attn_in = attn_in.reshape(lines * rows, model)
    kv_all, w_out_b, w_qkv = lax.optimization_barrier((kv_all, w_out, w_qkv))
    wo_far = swap(w_out_b, SH, lambda i: i ^ 2)
    w_far = swap(w_qkv, SH, lambda i: i ^ 2)
    kv_all = kv_all.reshape(length, 2 * width)
    attn_vec, attn_heads, lse = attend(info, q, kv_all, qinfo)
    n_ids = w_router.shape[1]
    small_t = jnp.pad(
        jnp.concatenate([w_router.T, const_mix.T], axis=0), ((0, 124 - n_ids), (0, 0))
    )
    gain_two = moe_gain
    recv_rows, wo_full, resid_one, table, attn_low = run_parts(
        [
            route(
                attn_heads, hidden_in, gain_two, small_t, routes.T, place, w_out[None], wo_far[None], n_ids
            )
        ],
        2,
        "route",
    )
    wo_full = wo_full.reshape(model, model)
    slots = lines * CAP

    expert_out, input_back, *terms = expert(
        recv_rows.reshape(slots, model + 128), recv_grads.reshape(slots, model), w_gate[0], w_up[0], w_down[0]
    )
    returned, input_ret, *sums = run_parts(
        [
            exchange(EX, SWAP, expert_out.reshape(lines, CAP, model)),
            exchange(EX, SWAP, input_back.reshape(lines, CAP, model)),
        ]
        + [core_sum(term) for term in terms],
        4,
        "combine",
    )
    far = [swap(there, SH, lambda i: i ^ 2) for there in sums[1::2]]
    down = (sums[4].astype(f32) + far[2].astype(f32)).astype(bf16)

    weights, back_heads, layer_out, resid_grad, out_term, packed = run_parts(
        [
            share_weights(w_qkv, w_far),
            to_heads(
                returned, input_ret, place, table, resid_one, attn_low, out_grad, gain_two, small_t, const_vec, wo_full, n_ids
            )
        ],
        5,
        "to_heads",
    )
    weights = weights.reshape(3, model, model)
    back_heads, down = lax.optimization_barrier((back_heads, down))
    cross = lambda x: swap(x, GR, lambda i: 1 - i)
    down_far = cross(down)
    dq, *dkv = attend_back(info, q, kv_all, qinfo, attn_vec, lse, back_heads)
    pairs = [(sums[0], far[0]), (sums[2], far[1])]
    input_grad, *parts = run_parts(
        [
            tail(
                dkv, dq, attn_in, weights, out_term, packed, hidden_in, resid_grad, attn_gain, pairs
            )
        ],
        6,
        "tail",
        pl.CostEstimate(flops=2 * 10**10, bytes_accessed=10**8, transcendentals=0),
    )
    gate, up, down, input_grad, layer_out, *grads, gain, gain_two, vecs, router, mix = finale(
        [parts[5], parts[7], down],
        [parts[6], parts[8], down_far],
        input_grad,
        layer_out,
        parts[:5],
        n_ids,
    )
    return (
        layer_out,
        input_grad,
        gain,
        *grads,
        gain_two,
        router.T,
        mix.T,
        vecs,
        gate[None],
        up[None],
        down[None],
    )


def solution(mesh):
    placed = (
        P((GR, EX, SH), None),
        P(GR, None),
        P((GR, EX, SH), None),
        P(),
        P(SH, None),
        P(SH, None),
        P(SH, None),
        P(SH, None),
        P(),
        P(),
        P(),
        P(),
        P(EX, None, None),
        P(EX, None, None),
        P(EX, None, None),
        P((GR, EX, SH), None),
    )
    sizes = dict(mesh.shape)
    lines = sizes[EX]
    fast = (sizes[GR], sizes[SH], lines) == (2, 4, 4)
    return jax.shard_map(
        fast_shards if fast else shards,
        mesh=mesh,
        in_specs=placed,
        out_specs=(
            P((GR, EX, SH), None),
            P((GR, EX, SH), None),
            P(),
            P((EX, SH), None),
            P((EX, SH), None),
            P((EX, SH), None),
            P((EX, SH), None),
            P(),
            P(),
            P(),
            P(),
            P(EX, SH, None),
            P(EX, SH, None),
            P(EX, SH, None),
        ),
        check_vma=False,
    )
```

```python
import functools

import jax
import jax.numpy as jnp
from jax import lax
from jax.experimental import pallas as pl
from jax.experimental.pallas import tpu as pltpu
from jax.sharding import PartitionSpec as P

HEADS = 12
HEAD_DIM = 64
CAP = 48
DOCS = 9
KEY_BLK = 256
KEY_BACK = 768
EX, SH, GR = ("expert", "shard", "group")
GATHER, GATHER_SUM, SWAP, SWAP_SUM = range(4)


neg_fill = -1e30
norm_eps = 1e-05
bf16 = jnp.bfloat16
f32 = jnp.float32
VM = pl.BlockSpec(memory_space=pltpu.VMEM)
SM = pl.BlockSpec(memory_space=pltpu.SMEM)
HIGH = lax.Precision.HIGHEST


def contract(a, b, da, db, precision=None):
    return lax.dot_general(
        a, b, (((da,), (db,)), ((), ())), preferred_element_type=f32, precision=precision
    )


def dense32(left_side, right_side):
    return jnp.dot(left_side, right_side, precision=lax.Precision.HIGHEST)


def allowed_mask(query_pos, query_seg, key_pos, key_seg):
    same_doc = (key_seg[None, :] == query_seg[:, None]) | (key_seg[None, :] == 0)
    return same_doc & (key_pos[None, :] <= query_pos[:, None])


def rms_back(inputs, inverse, gain_vec, upstream):
    scaled = upstream * gain_vec
    return inverse * scaled - inputs * inverse**3 * jnp.mean(scaled * inputs, axis=1, keepdims=True)


def block_scores(query_blk, keys_blk, score_scale):
    return (
        jnp.einsum("qhd,khd->hqk", query_blk, keys_blk, preferred_element_type=jnp.float32)
        * score_scale
    )


def grad_pieces(
    query_blk, back_blk, keys_blk, values_blk, norm_blk, delta_blk, key_mask, score_scale
):
    scores = block_scores(query_blk, keys_blk, score_scale)
    prob_rows = jnp.where(key_mask[None], jnp.exp(scores - norm_blk[:, :, None]), 0.0)
    prob_grad = jnp.einsum("qhd,khd->hqk", back_blk, values_blk, preferred_element_type=jnp.float32)
    score_low = (prob_rows * (prob_grad - delta_blk[:, :, None])).astype(jnp.bfloat16)
    return (prob_rows.astype(jnp.bfloat16), score_low)


def shards(
    hidden_in,
    segment_ids,
    routes,
    attn_gain,
    w_query,
    w_key,
    w_value,
    w_out,
    moe_gain,
    w_router,
    const_mix,
    const_vec,
    w_gate,
    w_up,
    w_down,
    out_grad,
):
    tok_rows, model_width = hidden_in.shape
    score_scale = HEAD_DIM ** (-0.5)
    inner_rank = lax.axis_index((EX, SH))
    seg_group = segment_ids[0]
    group_len = seg_group.shape[0]
    key_block = min(512, group_len)
    num_blocks = group_len // key_block
    row_start = inner_rank * tok_rows
    own_pos = row_start + jnp.arange(tok_rows, dtype=jnp.int32)
    own_seg = lax.dynamic_slice_in_dim(seg_group, row_start, tok_rows)
    wq_full, wk_full, wv_full, wo_full = (
        lax.all_gather(w_query, SH, axis=0, tiled=True),
        lax.all_gather(w_key, SH, axis=0, tiled=True),
        lax.all_gather(w_value, SH, axis=0, tiled=True),
        lax.all_gather(w_out, SH, axis=0, tiled=True),
    )
    inputs = hidden_in.astype(jnp.float32)
    inv_one = lax.rsqrt(jnp.mean(inputs * inputs, axis=1, keepdims=True) + norm_eps)
    normed_one = inputs * inv_one
    attn_in = (normed_one * attn_gain).astype(jnp.bfloat16)
    queries = jnp.dot(attn_in, wq_full, preferred_element_type=jnp.float32).astype(jnp.bfloat16)
    keys_own = jnp.dot(attn_in, wk_full, preferred_element_type=jnp.float32).astype(jnp.bfloat16)
    values_own = jnp.dot(attn_in, wv_full, preferred_element_type=jnp.float32).astype(jnp.bfloat16)
    keys_all, values_all = (
        lax.all_gather(keys_own, (EX, SH), axis=0, tiled=True),
        lax.all_gather(values_own, (EX, SH), axis=0, tiled=True),
    )
    query_heads = queries.reshape(tok_rows, HEADS, HEAD_DIM)

    def fetch_block(source, block_index):
        return lax.dynamic_slice_in_dim(source, block_index * key_block, key_block).reshape(
            key_block, HEADS, HEAD_DIM
        )

    def block_mask(block_index):
        key_pos = block_index * key_block + jnp.arange(key_block, dtype=jnp.int32)
        key_seg = lax.dynamic_slice_in_dim(seg_group, block_index * key_block, key_block)
        return allowed_mask(own_pos, own_seg, key_pos, key_seg)

    def stats_step(carry_now, block_index):
        key_mask = block_mask(block_index)

        def stats_live_block(carry_in):
            row_max, row_sum = carry_in
            scores = jnp.where(
                key_mask[None],
                block_scores(query_heads, fetch_block(keys_all, block_index), score_scale),
                neg_fill,
            )
            new_max = jnp.maximum(row_max, jnp.max(scores, axis=2))
            weights = jnp.where(key_mask[None], jnp.exp(scores - new_max[:, :, None]), 0.0)
            return (new_max, row_sum * jnp.exp(row_max - new_max) + jnp.sum(weights, axis=2))

        return (
            lax.cond(jnp.any(key_mask), stats_live_block, lambda carry_in: carry_in, carry_now),
            None,
        )

    start_max = jnp.full((HEADS, tok_rows), neg_fill, jnp.float32)
    row_max, row_sum = lax.scan(
        stats_step, (start_max, jnp.zeros_like(start_max)), jnp.arange(num_blocks)
    )[0]
    log_norm = row_max + jnp.log(row_sum)

    def output_step(running, block_index):
        key_mask = block_mask(block_index)

        def output_live_block(carry_in):
            scores = block_scores(query_heads, fetch_block(keys_all, block_index), score_scale)
            prob_rows = jnp.where(
                key_mask[None], jnp.exp(scores - log_norm[:, :, None]), 0.0
            ).astype(jnp.bfloat16)
            return carry_in + jnp.einsum(
                "hqk,khd->qhd",
                prob_rows,
                fetch_block(values_all, block_index),
                preferred_element_type=jnp.float32,
            )

        return (
            lax.cond(jnp.any(key_mask), output_live_block, lambda carry_in: carry_in, running),
            None,
        )

    zero_heads = jnp.zeros((tok_rows, HEADS, HEAD_DIM), jnp.float32)
    attn_sum = lax.scan(output_step, zero_heads, jnp.arange(num_blocks))[0]
    attn_low = attn_sum.reshape(tok_rows, model_width).astype(jnp.bfloat16)
    resid_one = inputs + jnp.dot(attn_low, wo_full, preferred_element_type=jnp.float32)
    inv_two = lax.rsqrt(jnp.mean(resid_one * resid_one, axis=1, keepdims=True) + norm_eps)
    normed_two = resid_one * inv_two
    moe_in = normed_two * moe_gain
    moe_low = moe_in.astype(jnp.bfloat16)
    n_ids = w_router.shape[1]
    local_experts = w_gate.shape[0]
    owners = lax.axis_size(EX)
    ffn_count = local_experts * owners
    id_table = jnp.arange(n_ids, dtype=jnp.int32)
    route_hot = (routes[:, :, None] == id_table).astype(jnp.float32)
    logits = dense32(moe_in, w_router)
    chosen = jnp.einsum("rkn,rn->rk", route_hot, logits, precision=lax.Precision.HIGHEST)
    gate_probs = jax.nn.softmax(chosen, axis=1)
    mix_alpha = jax.nn.softmax(dense32(moe_in, const_mix).reshape(tok_rows, 2, 2), axis=2)
    const_rows = mix_alpha[:, :, 0:1] * moe_in[:, None, :] + mix_alpha[:, :, 1:2] * const_vec[None]
    ffn_mask = (routes < ffn_count).astype(jnp.float32)
    copy_mask = (routes == ffn_count + 1).astype(jnp.float32)
    const_mask = (routes[:, :, None] == ffn_count + 2 + jnp.arange(2, dtype=jnp.int32)).astype(
        jnp.float32
    )
    copy_gate = jnp.sum(gate_probs * copy_mask, axis=1)
    const_gate = jnp.sum(gate_probs[:, :, None] * const_mask, axis=1)
    ffn_gate = gate_probs * ffn_mask
    flat_ids = routes.reshape(-1)
    id_hot = (flat_ids[:, None] == id_table).astype(jnp.int32)
    earlier = jnp.cumsum(id_hot, axis=0, dtype=jnp.int32) - id_hot
    slot_num = jnp.sum(earlier * id_hot, axis=1, dtype=jnp.int32)
    slot_total = ffn_count * CAP
    slot_of_route = jnp.where(flat_ids < ffn_count, flat_ids * CAP + slot_num, slot_total)
    route_count = flat_ids.shape[0]
    route_of_slot = (
        jnp.zeros(slot_total + 1, jnp.int32)
        .at[slot_of_route]
        .set(jnp.arange(route_count, dtype=jnp.int32))[:slot_total]
    )
    slot_used = jnp.zeros(slot_total + 1, jnp.bool_).at[slot_of_route].set(True)[:slot_total]
    send_rows = jnp.where(
        slot_used[:, None], moe_low[route_of_slot // 2], jnp.zeros((), jnp.bfloat16)
    )
    recv_rows = lax.all_to_all(
        send_rows.reshape(owners, local_experts * CAP, model_width),
        EX,
        split_axis=0,
        concat_axis=0,
        tiled=True,
    )
    expert_in = recv_rows.reshape(owners, local_experts, CAP, model_width)
    gate_pre = jnp.einsum("sjcd,jdf->sjcf", expert_in, w_gate, preferred_element_type=jnp.float32)
    up_pre = jnp.einsum("sjcd,jdf->sjcf", expert_in, w_up, preferred_element_type=jnp.float32)
    gate_sigmoid = jax.nn.sigmoid(gate_pre)
    hidden_act = (gate_pre * gate_sigmoid * up_pre).astype(jnp.bfloat16)
    expert_out = jnp.einsum(
        "sjcf,jfd->sjcd", hidden_act, w_down, preferred_element_type=jnp.float32
    ).astype(jnp.bfloat16)
    returned = lax.all_to_all(
        expert_out.reshape(owners, local_experts * CAP, model_width),
        EX,
        split_axis=0,
        concat_axis=0,
        tiled=True,
    )
    padded_out = jnp.concatenate(
        [returned.reshape(slot_total, model_width), jnp.zeros((1, model_width), jnp.bfloat16)],
        axis=0,
    )
    route_out = padded_out[slot_of_route].astype(jnp.float32).reshape(tok_rows, 2, model_width)
    moe_sum = (
        jnp.sum(ffn_gate[:, :, None] * route_out, axis=1)
        + copy_gate[:, None] * moe_in
        + jnp.sum(const_gate[:, :, None] * const_rows, axis=1)
    )
    layer_out = (resid_one + moe_sum).astype(jnp.bfloat16)
    upstream = out_grad.astype(jnp.float32)
    route_dot = jnp.sum(upstream[:, None, :] * route_out, axis=2)
    copy_dot = jnp.sum(upstream * moe_in, axis=1)
    const_dot = jnp.sum(upstream[:, None, :] * const_rows, axis=2)
    gate_back_r = (
        ffn_mask * route_dot
        + copy_mask * copy_dot[:, None]
        + jnp.sum(const_mask * const_dot[:, None, :], axis=2)
    )
    chosen_grad = gate_probs * (
        gate_back_r - jnp.sum(gate_probs * gate_back_r, axis=1, keepdims=True)
    )
    logit_grad = jnp.einsum("rk,rkn->rn", chosen_grad, route_hot, precision=lax.Precision.HIGHEST)
    const_up = const_gate[:, :, None] * upstream[:, None, :]
    alpha_grad = jnp.stack(
        [
            jnp.sum(const_up * moe_in[:, None, :], axis=2),
            jnp.sum(const_up * const_vec[None], axis=2),
        ],
        axis=2,
    )
    mix_back = (
        mix_alpha * (alpha_grad - jnp.sum(mix_alpha * alpha_grad, axis=2, keepdims=True))
    ).reshape(tok_rows, 4)
    vec_grad = jnp.sum(mix_alpha[:, :, 1:2] * const_up, axis=0)
    route_weight = ffn_gate.reshape(-1)
    grad_send = (route_weight[route_of_slot][:, None] * upstream[route_of_slot // 2]).astype(
        jnp.bfloat16
    )
    grad_send = jnp.where(slot_used[:, None], grad_send, jnp.zeros((), jnp.bfloat16))
    grad_recv = lax.all_to_all(
        grad_send.reshape(owners, local_experts * CAP, model_width),
        EX,
        split_axis=0,
        concat_axis=0,
        tiled=True,
    )
    grad_recv = grad_recv.reshape(owners, local_experts, CAP, model_width)
    hidden_grad = jnp.einsum(
        "sjcd,jfd->sjcf", grad_recv, w_down, preferred_element_type=jnp.float32
    )
    down_term = jnp.einsum(
        "sjcf,sjcd->jfd", hidden_act, grad_recv, preferred_element_type=jnp.float32
    )
    gate_back = (
        hidden_grad * up_pre * gate_sigmoid * (1.0 + gate_pre * (1.0 - gate_sigmoid))
    ).astype(jnp.bfloat16)
    up_back = (hidden_grad * gate_pre * gate_sigmoid).astype(jnp.bfloat16)
    gate_term = jnp.einsum(
        "sjcd,sjcf->jdf", expert_in, gate_back, preferred_element_type=jnp.float32
    )
    up_term = jnp.einsum("sjcd,sjcf->jdf", expert_in, up_back, preferred_element_type=jnp.float32)
    input_back = (
        jnp.einsum("sjcf,jdf->sjcd", gate_back, w_gate, preferred_element_type=jnp.float32)
        + jnp.einsum("sjcf,jdf->sjcd", up_back, w_up, preferred_element_type=jnp.float32)
    ).astype(jnp.bfloat16)
    input_ret = lax.all_to_all(
        input_back.reshape(owners, local_experts * CAP, model_width),
        EX,
        split_axis=0,
        concat_axis=0,
        tiled=True,
    )
    padded_in = jnp.concatenate(
        [input_ret.reshape(slot_total, model_width), jnp.zeros((1, model_width), jnp.bfloat16)],
        axis=0,
    )
    ffn_in_grad = jnp.sum(
        padded_in[slot_of_route].astype(jnp.float32).reshape(tok_rows, 2, model_width), axis=1
    )
    moe_in_grad = (
        ffn_in_grad
        + copy_gate[:, None] * upstream
        + jnp.sum(mix_alpha[:, :, 0:1] * const_up, axis=1)
        + dense32(mix_back, const_mix.T)
        + dense32(logit_grad, w_router.T)
    )
    moe_gain_grad = jnp.sum(moe_in_grad * normed_two, axis=0)
    router_grad = dense32(moe_in.T, logit_grad)
    mix_grad = dense32(moe_in.T, mix_back)
    resid_grad = upstream + rms_back(resid_one, inv_two, moe_gain, moe_in_grad)
    branch_low = resid_grad.astype(jnp.bfloat16)
    out_proj_term = jnp.dot(attn_low.T, branch_low, preferred_element_type=jnp.float32)
    attn_back = jnp.dot(branch_low, wo_full.T, preferred_element_type=jnp.float32).astype(
        jnp.bfloat16
    )
    back_heads = attn_back.reshape(tok_rows, HEADS, HEAD_DIM)
    row_delta = jnp.sum(back_heads.astype(jnp.float32) * attn_sum, axis=2).T

    def back_step(query_acc, block_index):
        key_mask = block_mask(block_index)
        keys_blk = fetch_block(keys_all, block_index)
        values_blk = fetch_block(values_all, block_index)

        def back_live_block(running):
            prob_low, score_low = grad_pieces(
                query_heads,
                back_heads,
                keys_blk,
                values_blk,
                log_norm,
                row_delta,
                key_mask,
                score_scale,
            )
            value_part = jnp.einsum(
                "hqk,qhd->khd", prob_low, back_heads, preferred_element_type=jnp.float32
            )
            key_part = (
                jnp.einsum(
                    "hqk,qhd->khd", score_low, query_heads, preferred_element_type=jnp.float32
                )
                * score_scale
            )
            running = (
                running
                + jnp.einsum(
                    "hqk,khd->qhd", score_low, keys_blk, preferred_element_type=jnp.float32
                )
                * score_scale
            )
            return (
                running,
                (
                    key_part.reshape(key_block, model_width),
                    value_part.reshape(key_block, model_width),
                ),
            )

        def dead_block(running):
            empty_rows = jnp.zeros((key_block, model_width), jnp.float32)
            return (running, (empty_rows, empty_rows))

        return lax.cond(jnp.any(key_mask), back_live_block, dead_block, query_acc)

    query_grad32, key_terms = lax.scan(back_step, zero_heads, jnp.arange(num_blocks))
    key_grad32, value_grad32 = (
        lax.psum_scatter(
            key_terms[0].reshape(group_len, model_width).astype(jnp.bfloat16),
            (EX, SH),
            scatter_dimension=0,
            tiled=True,
        ).astype(jnp.float32),
        lax.psum_scatter(
            key_terms[1].reshape(group_len, model_width).astype(jnp.bfloat16),
            (EX, SH),
            scatter_dimension=0,
            tiled=True,
        ).astype(jnp.float32),
    )
    query_low = query_grad32.reshape(tok_rows, model_width).astype(jnp.bfloat16)
    key_low = key_grad32.astype(jnp.bfloat16)
    value_low = value_grad32.astype(jnp.bfloat16)
    query_term = jnp.dot(attn_in.T, query_low, preferred_element_type=jnp.float32)
    key_term = jnp.dot(attn_in.T, key_low, preferred_element_type=jnp.float32)
    value_term = jnp.dot(attn_in.T, value_low, preferred_element_type=jnp.float32)
    attn_in_grad = (
        jnp.dot(query_low, wq_full.T, preferred_element_type=jnp.float32)
        + jnp.dot(key_low, wk_full.T, preferred_element_type=jnp.float32)
        + jnp.dot(value_low, wv_full.T, preferred_element_type=jnp.float32)
    )
    attn_gain_grad = jnp.sum(attn_in_grad * normed_one, axis=0)
    input_grad = resid_grad + rms_back(inputs, inv_one, attn_gain, attn_in_grad)
    query_part, key_part_w, value_part_w, out_part = (
        lax.psum_scatter(
            query_term.astype(jnp.bfloat16), (EX, SH), scatter_dimension=0, tiled=True
        ).astype(jnp.float32),
        lax.psum_scatter(
            key_term.astype(jnp.bfloat16), (EX, SH), scatter_dimension=0, tiled=True
        ).astype(jnp.float32),
        lax.psum_scatter(
            value_term.astype(jnp.bfloat16), (EX, SH), scatter_dimension=0, tiled=True
        ).astype(jnp.float32),
        lax.psum_scatter(
            out_proj_term.astype(jnp.bfloat16), (EX, SH), scatter_dimension=0, tiled=True
        ).astype(jnp.float32),
    )
    gate_part, up_part, down_part = (
        lax.psum_scatter(
            gate_term.astype(jnp.bfloat16), SH, scatter_dimension=1, tiled=True
        ).astype(jnp.float32),
        lax.psum_scatter(
            up_term.astype(jnp.bfloat16), SH, scatter_dimension=1, tiled=True
        ).astype(jnp.float32),
        lax.psum_scatter(
            down_term.astype(jnp.bfloat16), SH, scatter_dimension=1, tiled=True
        ).astype(jnp.float32),
    )
    summed = (
        lax.psum(query_part.astype(jnp.bfloat16), GR).astype(jnp.float32),
        lax.psum(key_part_w.astype(jnp.bfloat16), GR).astype(jnp.float32),
        lax.psum(value_part_w.astype(jnp.bfloat16), GR).astype(jnp.float32),
        lax.psum(out_part.astype(jnp.bfloat16), GR).astype(jnp.float32),
        lax.psum(gate_part.astype(jnp.bfloat16), GR).astype(jnp.float32),
        lax.psum(up_part.astype(jnp.bfloat16), GR).astype(jnp.float32),
        lax.psum(down_part.astype(jnp.bfloat16), GR).astype(jnp.float32),
    )
    small_sums = lax.psum(
        (attn_gain_grad, moe_gain_grad, router_grad, mix_grad, vec_grad),
        (GR, EX, SH),
    )
    return (
        layer_out,
        input_grad,
        small_sums[0],
        summed[0],
        summed[1],
        summed[2],
        summed[3],
        small_sums[1],
        small_sums[2],
        small_sums[3],
        small_sums[4],
        summed[4],
        summed[5],
        summed[6],
    )


def greet(peers):
    barrier = pltpu.get_barrier_semaphore()
    for axis, peer in peers:
        pl.semaphore_signal(
            barrier, inc=1, device_id={axis: peer}, device_id_type=pl.DeviceIdType.MESH
        )
    pl.semaphore_wait(barrier, len(peers))


def send(src, dst, sems, index, axis, peer):
    copy = pltpu.make_async_remote_copy(
        src_ref=src,
        dst_ref=dst,
        send_sem=sems.at[0, index],
        recv_sem=sems.at[1, index],
        device_id={axis: peer},
        device_id_type=pl.DeviceIdType.MESH,
    )
    copy.start()
    return copy


def shard_peers():
    me = lax.axis_index(SH)
    side, core = me // 2, lax.rem(me, 2)
    return me, side, core, 2 * side + 1 - core, 2 * (1 - side) + core


class Part:
    def __init__(self, axes, ins, outs, scratch, copies, phases, specs=None):
        self.axes, self.ins, self.outs, self.scratch = axes, ins, outs, scratch
        self.copies, self.phases = copies, phases
        self.specs = specs or [VM] * len(ins)


def run_parts(parts, collective_id, name=None, cost=None):
    ins = sum([p.ins for p in parts], [])
    outs = sum([p.outs for p in parts], [])
    scratch = sum([p.scratch for p in parts], [])
    copies = sum(p.copies for p in parts)
    axes = sorted(set(sum([list(p.axes) for p in parts], [])))

    def body(*refs):
        sems = refs[-1]
        in_refs, out_refs = list(refs[: len(ins)]), list(refs[len(ins) : len(ins) + len(outs)])
        scr = list(refs[len(ins) + len(outs) : -1])
        peers = []
        for axis in axes:
            me, n = lax.axis_index(axis), lax.axis_size(axis)
            peers += [(axis, lax.rem(me + d, n)) for d in range(1, n)]
        greet(peers)
        base, running = 0, []
        for p in parts:
            take = lambda pool, k: [pool.pop(0) for _ in range(k)]
            refs_p = (take(in_refs, len(p.ins)), take(out_refs, len(p.outs)), take(scr, len(p.scratch)))
            counter = [base]

            def go(src, dst, axis, peer, counter=counter):
                counter[0] += 1
                return send(src, dst, sems, counter[0] - 1, axis, peer)

            running.append(p.phases(*refs_p, go))
            base += p.copies
        while running:
            running = [r for r in running if next(r, True) is None]

    return pl.pallas_call(
        body,
        out_shape=outs,
        in_specs=sum([p.specs for p in parts], []),
        out_specs=[VM] * len(outs),
        scratch_shapes=scratch + [pltpu.SemaphoreType.DMA((2, copies))],
        compiler_params=pltpu.CompilerParams(collective_id=collective_id, has_side_effects=True),
        cost_estimate=cost,
        name=name,
    )(*ins)


def start_swap(go, src, land, axis, gather):
    me, n = lax.axis_index(axis), lax.axis_size(axis)
    started = []
    for d in range(1, n):
        peer = lax.rem(me + d, n)
        started.append(go(src if gather else src.at[peer], land.at[me], axis, peer))
    land[me] = src[...] if gather else src[me]
    return started


def total_of(land, n):
    total = land[0].astype(f32)
    for j in range(1, n):
        total = total + land[j].astype(f32)
    return total


def exchange(axis, kind, x):
    n = lax.axis_size(axis)
    gather, summed = kind in (GATHER, GATHER_SUM), kind in (GATHER_SUM, SWAP_SUM)
    piece = x.shape if gather else x.shape[1:]
    shape = jax.ShapeDtypeStruct
    outs = [shape(piece, f32) if summed else shape((n,) + piece, x.dtype)]
    scratch = [pltpu.VMEM((n,) + piece, x.dtype)] if summed else []

    def phases(ins, outs, scr, go):
        land = scr[0] if summed else outs[0]
        started = start_swap(go, ins[0], land, axis, gather)
        yield
        for copy in started:
            copy.wait()
        if summed:
            outs[0][...] = total_of(land, n)

    return Part([axis], [x], outs, scratch, n - 1, phases)


def tree_gather(x):
    lines = x.shape[0]
    cuts = [(0, lines // 2), (lines // 2, lines)] if lines > 1 else [(0, 1)]
    cuts = [pl.ds(lo, hi - lo) for lo, hi in cuts]

    def phases(ins, outs, scr, go):
        x_ref, out_ref = ins[0], outs[0]
        me, _, _, near, far = shard_peers()
        across = [go(x_ref.at[c], out_ref.at[c, me], SH, far) for c in cuts]
        own = go(x_ref, out_ref.at[:, me], SH, near)
        out_ref[:, me] = x_ref[...]
        yield
        handed = []
        for c, copy in zip(cuts, across):
            copy.wait_recv()
            handed.append(go(out_ref.at[c, far], out_ref.at[c, far], SH, near))
        yield
        for copy in across:
            copy.wait_send()
        own.wait()
        for copy in handed:
            copy.wait()

    shape = (lines, 4) + x.shape[1:]
    return Part([SH], [x], [jax.ShapeDtypeStruct(shape, x.dtype)], [], 2 * len(cuts) + 1, phases)


def core_sum(x):
    piece = x.shape[1:]
    shape = jax.ShapeDtypeStruct

    def phases(ins, outs, scr, go):
        x_ref, (here, there), (land, kept, sems) = ins[0], outs, scr
        near = shard_peers()[3]
        sent = [go(x_ref.at[3], land.at[1], SH, near), go(x_ref.at[2], land.at[0], SH, near)]
        local = [pltpu.make_async_copy(x_ref.at[k], kept.at[k], sems.at[k]) for k in range(2)]
        for copy in local:
            copy.start()
        yield
        for k, out in ((1, there), (0, here)):
            sent[1 - k].wait()
            local[k].wait()
            out[...] = (kept[k].astype(f32) + land[k].astype(f32)).astype(bf16)

    return Part(
        [SH],
        [x],
        [shape(piece, bf16)] * 2,
        [pltpu.VMEM((2,) + piece, bf16)] * 2 + [pltpu.SemaphoreType.DMA((2,))],
        2,
        phases,
        [pl.BlockSpec(memory_space=pl.ANY)],
    )


class Tree:
    copies = 3

    @staticmethod
    def scratch(piece):
        return [pltpu.VMEM((2,) + piece, bf16)] + [pltpu.VMEM(piece, bf16)] * 2

    def __init__(self, x, scr, go):
        self.x, (self.land, self.mine, self.got), self.go = x, scr, go
        self.me, self.side, self.core, self.near, self.far = shard_peers()
        other = 2 * (1 - self.side) + 1 - self.core
        self.first = [
            go(x.at[other], self.land.at[0], SH, self.near),
            go(x.at[self.near], self.land.at[1], SH, self.near),
        ]

    def across(self):
        self.first[0].wait_recv()
        self.mine[...] = (self.x[self.far].astype(f32) + self.land[0].astype(f32)).astype(bf16)
        self.second = self.go(self.mine, self.got, SH, self.far)

    def result(self):
        self.first[1].wait_recv()
        total = self.x[self.me].astype(f32) + self.land[1].astype(f32)
        self.second.wait_recv()
        return total + self.got[...].astype(f32)

    def close(self):
        for copy in (*self.first, self.second):
            copy.wait_send()


def turned_ids(ids_ref):
    ids = ids_ref[...].astype(f32)
    return jnp.transpose(jnp.concatenate([ids] * 4, axis=0)).astype(jnp.int32)


def slot_places(ids, lines, slots):
    rows = ids.shape[0]
    lane = lax.broadcasted_iota(jnp.int32, (rows, 128), 1)
    hot = [lane == column(ids, k) for k in range(2)]
    before = (
        lax.broadcasted_iota(jnp.int32, (rows, rows), 0)
        > lax.broadcasted_iota(jnp.int32, (rows, rows), 1)
    ).astype(bf16)
    named = jnp.where(hot[0] | hot[1], 1.0, 0.0).astype(bf16)
    earlier = jnp.dot(before, named, preferred_element_type=f32)
    slot_at = lax.broadcasted_iota(jnp.int32, (rows, slots), 1).astype(f32)
    place = []
    for k in range(2):
        number = jnp.sum(jnp.where(hot[k], earlier, 0.0), axis=1, keepdims=True)
        wanted = column(ids, k).astype(f32) * CAP + number
        wanted = jnp.where(column(ids, k) < lines, wanted, -1.0)
        place.append(jnp.where(slot_at == wanted, 1.0, 0.0))
    return place


def front(hidden, w_mine, gain, routes, out_grad, docs):
    rows, model = hidden.shape
    lines = lax.axis_size(EX)
    width = model // lines
    shape = jax.ShapeDtypeStruct
    last = lines - 1

    slots = lines * CAP

    def body(hid_ref, w_ref, gain_ref, ids_ref, up_ref, docs_ref, attn_ref, q_ref, kv_ref, place_ref, rows_out, info_ref, land, w_all, kv_own, rows_s, sems):
        line_me = lax.axis_index(EX)
        me, _, _, near, far = shard_peers()
        left, right = jnp.maximum(line_me - 1, 0), jnp.minimum(line_me + 1, last)
        greet(
            [(EX, lax.rem(line_me + d, lines)) for d in range(1, lines)]
            + [(SH, lax.rem(me + d, 4)) for d in range(1, 4)]
        )

        def copy(src, dst, index, axis, peer):
            return pltpu.make_async_remote_copy(
                src_ref=src,
                dst_ref=dst,
                send_sem=sems.at[0, index],
                recv_sem=sems.at[1, index],
                device_id={axis: peer},
                device_id_type=pl.DeviceIdType.MESH,
            )

        def relay(step, way):
            block = line_me - step if way == 0 else line_me + step
            block = jnp.clip(block, 0, last)
            src = hid_ref if step == 0 else land.at[block]
            return copy(src, land.at[block], last * way + step, EX, right if way == 0 else left)

        def sends(step, way):
            if way == 0:
                return (line_me < last) & (line_me - step >= 0)
            return (line_me > 0) & (line_me + step <= last)

        def comes(step, way):
            return line_me - 1 - step >= 0 if way == 0 else line_me + 1 + step <= last

        def source(step, way):
            line = line_me - 1 - step if way == 0 else line_me + 1 + step
            return jnp.clip(line, 0, last)

        def arrival(step, way):
            line = source(step, way)
            return copy(land.at[line], land.at[line], last * way + step, EX, right if way == 0 else left)

        base = 2 * last
        for way in range(2):

            @pl.when(sends(0, way))
            def _():
                relay(0, way).start()

        w_far = copy(w_ref, w_all.at[me], base, SH, far)
        w_near = copy(w_ref, w_all.at[me], base + 1, SH, near)
        w_pass = copy(w_all.at[far], w_all.at[far], base + 2, SH, near)
        w_far.start()
        w_near.start()
        w_all[me] = w_ref[...]
        docs = docs_ref[...]
        lane = lax.broadcasted_iota(jnp.int32, (docs.shape[0], 128), 1)
        block = lax.broadcasted_iota(jnp.int32, (docs.shape[0], 128), 0)
        table = jnp.where(lane == DOCS + block, jnp.broadcast_to(docs[:, 0:1], lane.shape), 0)
        for doc in range(1, DOCS):
            before = jnp.sum(jnp.where(docs < doc, 1, 0), axis=1, keepdims=True)
            table = table + jnp.where(lane == doc, jnp.broadcast_to(before, lane.shape), 0)
        info_ref[...] = jnp.sum(table, axis=0, keepdims=True)
        ids = turned_ids(ids_ref)
        place = slot_places(ids, lines, slots)
        for k in range(2):
            place_ref[k] = place[k].astype(bf16)
        either = (place[0] + place[1]).astype(bf16)
        rows_s[...] = contract(either, up_ref[...], 0, 0).astype(bf16).reshape(lines, CAP, model)
        base += 3
        kv_far = lambda line: copy(kv_own.at[line], kv_ref.at[line, me], base + line, SH, far)
        kv_near = lambda line: copy(
            kv_own.at[line], kv_ref.at[line, me], base + lines + line, SH, near
        )
        kv_pass = lambda line: copy(
            kv_ref.at[line, far], kv_ref.at[line, far], base + 2 * lines + line, SH, near
        )

        def project(line, x):
            inputs = x.astype(f32)
            inv = lax.rsqrt(jnp.mean(inputs * inputs, axis=1, keepdims=True) + norm_eps)
            attn_in = (inputs * inv * gain_ref[...][None]).astype(bf16)
            attn_ref[line] = attn_in
            value = jnp.dot(
                attn_in, w_all[...].reshape(model, 3 * width), preferred_element_type=f32
            ).astype(bf16)
            kv_own[line] = value[:, : 2 * width]
            kv_far(line).start()
            kv_near(line).start()
            kv_ref[line, me] = value[:, : 2 * width]
            q_ref[line] = value[:, 2 * width :]

        def hand(line):
            kv_far(line).wait_recv()
            kv_pass(line).start()

        w_far.wait_recv()
        w_pass.start()
        w_near.wait_recv()
        w_pass.wait_recv()
        project(line_me, hid_ref[...])
        for step in range(last):
            for way in range(2):

                @pl.when(comes(step, way))
                def _():
                    arrival(step, way).wait_recv()

                if step + 1 < last:

                    @pl.when(sends(step + 1, way))
                    def _():
                        relay(step + 1, way).start()

            for way in range(2):

                @pl.when(comes(step, way))
                def _():
                    line = source(step, way)
                    project(line, land[line])

            if step == last - 2:
                first = base + 3 * lines
                ups = []
                for d in range(1, lines):
                    peer = lax.rem(line_me + d, lines)
                    ups.append(copy(rows_s.at[peer], rows_out.at[line_me], first + d - 1, EX, peer))
                    ups[-1].start()
                rows_out[line_me] = rows_s[line_me]
            if step == 0:
                hand(line_me)
            else:
                for way in range(2):

                    @pl.when(comes(step - 1, way))
                    def _():
                        hand(source(step - 1, way))

        for way in range(2):

            @pl.when(comes(last - 1, way))
            def _():
                hand(source(last - 1, way))

        for way in range(2):
            for step in range(last):

                @pl.when(sends(step, way))
                def _():
                    relay(step, way).wait_send()

        w_far.wait_send()
        w_near.wait_send()
        w_pass.wait_send()
        for line in range(lines):
            kv_far(line).wait_send()
            kv_near(line).wait()
            kv_pass(line).wait()
        for up in ups:
            up.wait()

    return pl.pallas_call(
        body,
        out_shape=[
            shape((lines, rows, model), bf16),
            shape((lines, rows, width), bf16),
            shape((lines, 4, rows, 2 * width), bf16),
            shape((2, rows, slots), bf16),
            shape((lines, CAP, model), bf16),
            shape((1, 128), jnp.int32),
        ],
        in_specs=[VM] * 6,
        out_specs=[VM] * 6,
        scratch_shapes=[
            pltpu.VMEM((lines, rows, model), bf16),
            pltpu.VMEM((4, rows, 3 * width), bf16),
            pltpu.VMEM((lines, rows, 2 * width), bf16),
            pltpu.VMEM((lines, CAP, model), bf16),
            pltpu.SemaphoreType.DMA((2, 3 * last + 3 + 3 * lines)),
        ],
        compiler_params=pltpu.CompilerParams(collective_id=0, has_side_effects=True),
        name="front",
    )(hidden, w_mine, gain, routes, out_grad, docs)


def column(x, k):
    return x[:, k : k + 1]


def core_share(go, own, far, out):
    me, _, _, near, other = shard_peers()
    sent = [go(own, out.at[:, me], SH, near), go(far, out.at[:, other], SH, near)]
    out[:, me] = own[...]
    out[:, other] = far[...]
    return sent


def route(heads, hidden, gain, small_w, routes, place, wo, wo_far, n_ids):
    lines, rows, width = heads.shape
    model = lines * width
    slots = lines * CAP
    shape = jax.ShapeDtypeStruct

    def phases(ins, outs, scr, go):
        heads_ref, hid_ref, gain_ref, small_ref, routes_ref, place_ref, wo_ref, wof_ref = ins
        rows_out, wo_all, resid_ref, table_ref, low_ref = outs
        land, rows_s = scr
        swaps = start_swap(go, heads_ref, land, EX, False)
        swaps += core_share(go, wo_ref, wof_ref, wo_all)
        ids = turned_ids(routes_ref)
        lane = lax.broadcasted_iota(jnp.int32, (rows, 128), 1)
        hot = [lane == column(ids, k) for k in range(2)]
        place = [place_ref[k].astype(f32) for k in range(2)]
        either = place_ref[0] + place_ref[1]
        for copy in swaps:
            copy.wait()
        for line in range(lines):
            low_ref[:, line * width : (line + 1) * width] = land[line]
        w_out = wo_all[...].reshape(model, model)
        resid = hid_ref[...].astype(f32) + jnp.dot(
            low_ref[...], w_out, preferred_element_type=f32
        )
        resid_ref[...] = resid
        inv = lax.rsqrt(jnp.mean(resid * resid, axis=1, keepdims=True) + norm_eps)
        moe_in = resid * inv * gain_ref[...][None]
        small = contract(moe_in, small_ref[...], 1, 1, HIGH)
        chosen = [jnp.sum(jnp.where(h, small, 0.0), axis=1, keepdims=True) for h in hot]
        top = jnp.maximum(chosen[0], chosen[1])
        powers = [jnp.exp(c - top) for c in chosen]
        gates = [p / (powers[0] + powers[1]) for p in powers]
        weight = place[0] * gates[0] + place[1] * gates[1]
        weight = contract(weight, jnp.ones((rows, 128), f32), 0, 0, HIGH)[:, 0:1]
        high = weight.astype(bf16)
        low = (weight - high.astype(f32)).astype(bf16)
        slot_lane = lax.broadcasted_iota(jnp.int32, (slots, 128), 1)
        extra = jnp.where(slot_lane == 0, high, jnp.where(slot_lane == 1, low, jnp.zeros_like(low)))
        rows_s[:, :, :model] = (
            contract(either, moe_in.astype(bf16), 0, 0).astype(bf16).reshape(lines, CAP, model)
        )
        rows_s[:, :, model:] = extra.reshape(lines, CAP, 128)
        row_swap = start_swap(go, rows_s, rows_out, EX, False)
        table = jnp.zeros((rows, 128), f32)
        entries = list(gates)
        for j in range(2):
            pair = [column(small, n_ids + 2 * j + k) for k in range(2)]
            top = jnp.maximum(pair[0], pair[1])
            powers = [jnp.exp(c - top) for c in pair]
            entries += [p / (powers[0] + powers[1]) for p in powers]
        entries += [column(ids, k).astype(f32) for k in range(2)]
        for k, entry in enumerate(entries):
            table = jnp.where(lane == k, entry, table)
        table_ref[...] = table
        for copy in row_swap:
            copy.wait()
        yield

    ins = [heads, hidden, gain, small_w, routes, place, wo, wo_far]
    outs = [
        shape((lines, CAP, model + 128), bf16),
        shape((1, 4, model // 4, model), bf16),
        shape((rows, model), f32),
        shape((rows, 128), f32),
        shape((rows, model), bf16),
    ]
    scratch = [
        pltpu.VMEM((lines, rows, width), bf16),
        pltpu.VMEM((lines, CAP, model + 128), bf16),
    ]
    return Part([EX, SH], ins, outs, scratch, 2 * (lines - 1) + 2, phases)


def share_weights(own, far):
    def phases(ins, outs, scr, go):
        copies = core_share(go, ins[0], ins[1], outs[0])
        yield
        for copy in copies:
            copy.wait()

    dims = (own.shape[0], 4) + own.shape[1:]
    return Part([SH], [own, far], [jax.ShapeDtypeStruct(dims, bf16)], [], 2, phases)


def to_heads(returned, input_ret, place, table, resid, low, out_grad, gain, small_t, const_vec, wo, n_ids):
    rows, model = resid.shape
    lines = returned.shape[0]
    width = model // lines
    own = rows // lines
    slots = lines * CAP
    shape = jax.ShapeDtypeStruct

    def phases(ins, outs, scr, go):
        ret_ref, iret_ref, place_ref, table_ref, resid_ref, low_ref, up_ref, gain_ref, st_ref, vec_ref, wo_ref = ins
        heads_out, layer_ref, rgrad_ref, term_ref, packed_ref = outs
        (back_s,) = scr
        table = table_ref[...]
        gates = [column(table, k) for k in range(2)]
        alpha = [[column(table, 2 + 2 * j + k) for k in range(2)] for j in range(2)]
        ids = [column(table, 6 + k) for k in range(2)]
        vecs = [vec_ref[j : j + 1, :] for j in range(2)]
        resid = resid_ref[...]
        upstream = up_ref[...].astype(f32)
        inv = lax.rsqrt(jnp.mean(resid * resid, axis=1, keepdims=True) + norm_eps)
        normed = resid * inv
        moe_in = normed * gain_ref[...][None]
        returned = ret_ref[...].reshape(slots, model)
        total = lambda x: jnp.sum(x, axis=1, keepdims=True)
        flag = lambda x: jnp.where(x, 1.0, 0.0)
        copy_dot = total(upstream * moe_in)
        vec_dot = [total(upstream * v) for v in vecs]
        const_dot = [alpha[j][0] * copy_dot + alpha[j][1] * vec_dot[j] for j in range(2)]
        output = resid
        backs = []
        copy_gate = jnp.zeros((rows, 1), f32)
        const_gate = [jnp.zeros((rows, 1), f32) for _ in range(2)]
        for k in range(2):
            rows_k = jnp.dot(place_ref[k], returned, preferred_element_type=f32)
            is_ffn, is_copy = flag(ids[k] < lines), flag(ids[k] == lines + 1)
            is_const = [flag(ids[k] == lines + 2 + j) for j in range(2)]
            output = output + (gates[k] * is_ffn) * rows_k
            backs.append(
                is_ffn * total(upstream * rows_k)
                + is_copy * copy_dot
                + is_const[0] * const_dot[0]
                + is_const[1] * const_dot[1]
            )
            copy_gate = copy_gate + gates[k] * is_copy
            const_gate = [const_gate[j] + gates[k] * is_const[j] for j in range(2)]
        through = copy_gate + const_gate[0] * alpha[0][0] + const_gate[1] * alpha[1][0]
        output = output + through * moe_in
        for j in range(2):
            output = output + (const_gate[j] * alpha[j][1]) * vecs[j]
        layer_ref[...] = output.astype(bf16)
        mean_back = gates[0] * backs[0] + gates[1] * backs[1]
        lane = lax.broadcasted_iota(jnp.int32, (rows, 128), 1)
        lane_f = lane.astype(f32)
        small = jnp.zeros((rows, 128), f32)
        for k in range(2):
            small = jnp.where(lane_f == ids[k], gates[k] * (backs[k] - mean_back), small)
        for j in range(2):
            grads = [const_gate[j] * copy_dot, const_gate[j] * vec_dot[j]]
            mean = alpha[j][0] * grads[0] + alpha[j][1] * grads[1]
            for k in range(2):
                small = jnp.where(
                    lane == n_ids + 2 * j + k, alpha[j][k] * (grads[k] - mean), small
                )
            small = jnp.where(lane == n_ids + 4 + j, alpha[j][1] * const_gate[j], small)
        either = place_ref[0] + place_ref[1]
        moe_grad = (
            jnp.dot(either, iret_ref[...].reshape(slots, model), preferred_element_type=f32)
            + through * upstream
            + jnp.dot(small, st_ref[...], preferred_element_type=f32, precision=HIGH)
        )
        resid_grad = upstream + rms_back(resid, inv, gain_ref[...][None], moe_grad)
        branch = resid_grad.astype(bf16)
        back = contract(branch, wo_ref[...], 1, 1).astype(bf16)
        for line in range(lines):
            back_s[line] = back[:, line * width : (line + 1) * width]
        swaps = start_swap(go, back_s, heads_out, EX, False)
        rgrad_ref[...] = resid_grad
        packed_ref[...] = jnp.zeros_like(packed_ref)
        packed_ref[0:1] = jnp.sum(moe_grad * normed, axis=0, keepdims=True)
        small_grad = contract(small, moe_in, 0, 0, HIGH)
        vec_grad = contract(small, upstream, 0, 0, HIGH)
        packed_ref[1:3] = vec_grad[n_ids + 4 : n_ids + 6]
        packed_ref[3 : 7 + n_ids] = small_grad[: n_ids + 4]
        term = contract(low_ref[...], branch, 0, 0).astype(bf16)
        for line in range(lines):
            for piece in range(4):
                at = (line * 4 + piece) * own
                term_ref[piece, line] = term[at : at + own]
        for copy in swaps:
            copy.wait()
        yield

    ins = [returned, input_ret, place, table, resid, low, out_grad, gain, small_t, const_vec, wo]
    outs = [
        shape((lines, rows, width), bf16),
        shape((rows, model), bf16),
        shape((rows, model), f32),
        shape((4, lines, own, model), bf16),
        shape((-(-(7 + n_ids) // 8) * 8, model), f32),
    ]
    return Part([EX], ins, outs, [pltpu.VMEM((lines, rows, width), bf16)], lines - 1, phases)


def tail(dkv, dq, attn_in, weights, out_term, packed, hidden, resid_grad, gain, pairs):
    lines, rows, width = dq.shape
    model = lines * width
    own = rows // lines
    groups = lax.axis_size(GR)
    shape = jax.ShapeDtypeStruct
    vmem = pltpu.VMEM
    tok = lines * rows
    few = lines // 2
    dkv_piece, q_piece = (few, rows, 2 * width), (lines, own, width)
    kv_piece, o_piece = (lines, own, 2 * width), (lines, own, model)
    part_dims = (width, 2 * width, model)

    def phases(ins, outs, scr, go):
        lo_ref, hi_ref, dq_ref, attn_ref, w_ref, wf_ref, o_ref, packed_ref, hid_ref, resid_ref, gain_ref = ins[:11]
        input_ref, q_out, kv_out, out_out, packed_out, gain_out = outs[:6]
        scr = list(scr)
        take = lambda k: [scr.pop(0) for _ in range(k)]
        lo_scr, hi_scr, q_scr, kvw_scr, o_scr = take(3), take(3), take(3), take(3), take(3)
        own_kv, q_t, kv_t, dq_all, dkv_all, dq_full = take(6)
        kv_sems, w_s, w_sem, turned = take(4)
        held = take(2 * len(pairs))
        me, _, _, near, far = shard_peers()
        w_copies = [
            pltpu.make_async_copy(ref, w_s.at[:, at], w_sem.at[2 * len(pairs) + k])
            for k, (ref, at) in enumerate(((w_ref, me), (wf_ref, far)))
        ]
        fetch = [
            pltpu.make_async_copy(ins[11 + k], held[k], w_sem.at[k]) for k in range(2 * len(pairs))
        ]
        for copy in fetch:
            copy.start()
        for copy in w_copies:
            copy.start()
        sums, lands, halves, gots = take(3), take(3), take(3), take(3)
        pk_l, pk_s, pk_g = take(3)
        mid_l, mid_s = take(2)
        gn_l, gn_s, gn_g, gn_0, gn_1, gn_2 = take(6)
        me = lax.axis_index(SH)

        line_me, group_me = lax.axis_index(EX), lax.axis_index(GR)
        kv_trees = [Tree(lo_ref, lo_scr, go), Tree(hi_ref, hi_scr, go)]

        def kv_copy(sender, target):
            return pltpu.make_async_remote_copy(
                src_ref=own_kv.at[target],
                dst_ref=dkv_all.at[sender],
                send_sem=kv_sems.at[0, target],
                recv_sem=kv_sems.at[1, sender],
                device_id={EX: target},
                device_id_type=pl.DeviceIdType.MESH,
            )

        def push_kv(k):
            own_kv[k * few : (k + 1) * few] = kv_trees[k].result().astype(bf16)
            for target in range(k * few, (k + 1) * few):

                @pl.when(line_me != target)
                def _():
                    kv_copy(line_me, jnp.int32(target)).start()

                @pl.when(line_me == target)
                def _():
                    dkv_all[target] = own_kv[target]

        dq_swap = start_swap(go, dq_ref, dq_all, EX, False)
        o_tree = Tree(o_ref, o_scr, go)
        pk1 = start_swap(go, packed_ref, pk_l, EX, True)
        def term(rows_ref, out):
            value = jnp.dot(
                turned[...],
                rows_ref[...].reshape(tok, rows_ref.shape[-1]),
                preferred_element_type=f32,
            ).astype(bf16)
            for line in range(lines):
                for piece in range(4):
                    at = (line * 4 + piece) * own
                    out[piece, line] = value[at : at + own]

        for tree in kv_trees:
            tree.across()
        wide = []
        for k in range(len(pairs)):
            mine, other = outs[6 + 2 * k : 8 + 2 * k]
            here, there = held[2 * k : 2 * k + 2]
            fetch[2 * k].wait()
            fetch[2 * k + 1].wait()
            mine[...] = (here[...].astype(f32) + there[...].astype(f32)).astype(bf16)
            wide.append(go(mine, other, GR, lax.rem(group_me + 1, groups)))
        w_copies.append(go(w_ref, w_s.at[:, me], SH, near))
        w_copies.append(go(wf_ref, w_s.at[:, far], SH, near))
        turned[...] = jnp.transpose(attn_ref[...])
        term(dq_ref, q_t)
        o_tree.across()
        q_tree = Tree(q_t, q_scr, go)
        trees = [q_tree, None, o_tree]

        def lines_out(k):
            sums[k][...] = trees[k].result().astype(bf16)
            return start_swap(go, sums[k], lands[k], EX, False)

        push_kv(0)
        q_tree.across()
        push_kv(1)
        term(own_kv, kv_t)
        kvw_tree = Tree(kv_t, kvw_scr, go)
        trees[1] = kvw_tree
        o_lines = lines_out(2)
        for copy in pk1:
            copy.wait()
        mid_l[...] = total_of(pk_l, lines)
        pk2 = start_swap(go, mid_l, pk_s, SH, True)
        kvw_tree.across()
        q_lines = lines_out(0)
        for copy in dq_swap:
            copy.wait()
        for line in range(lines):
            dq_full[:, line * width : (line + 1) * width] = dq_all[line]
        for copy in w_copies:
            copy.wait()
        grad = contract(dq_full[...], w_s[0].reshape(model, model), 1, 1)
        for copy in pk2:
            copy.wait()
        mid_s[...] = total_of(pk_s, 4)
        pk3 = start_swap(go, mid_s, pk_g, GR, True)
        kv_lines = lines_out(1)
        for other in range(lines):

            @pl.when(line_me != other)
            def _():
                kv_copy(jnp.int32(other), line_me).wait_recv()
                kv_copy(line_me, jnp.int32(other)).wait_send()

        for half in range(2):
            for line in range(lines):
                dq_full[:, line * width : (line + 1) * width] = dkv_all[
                    line, :, half * width : (half + 1) * width
                ]
            grad = grad + contract(dq_full[...], w_s[1 + half].reshape(model, model), 1, 1)
        inputs = hid_ref[...].astype(f32)
        inv = lax.rsqrt(jnp.mean(inputs * inputs, axis=1, keepdims=True) + norm_eps)
        normed = inputs * inv
        gn_0[...] = jnp.sum(grad * normed, axis=0, keepdims=True)
        gn1 = start_swap(go, gn_0, gn_l, EX, True)
        input_ref[...] = resid_ref[...] + rms_back(inputs, inv, gain_ref[...][None], grad)
        swaps = [None] * 3
        for k, copies in ((2, o_lines), (0, q_lines)):
            for copy in copies:
                copy.wait()
            if k == 2:
                halves[k][...] = total_of(lands[k], lines).astype(bf16)
            else:
                halves[k][...] = lands[k][...]
            swaps[k] = start_swap(go, halves[k], gots[k], GR, True)
        for copy in gn1:
            copy.wait()
        gn_1[...] = total_of(gn_l, lines)
        gn2 = start_swap(go, gn_1, gn_s, SH, True)
        for copy in kv_lines:
            copy.wait()
        halves[1][...] = lands[1][...]
        swaps[1] = start_swap(go, halves[1], gots[1], GR, True)
        for copy in gn2:
            copy.wait()
        gn_2[...] = total_of(gn_s, 4)
        gn3 = start_swap(go, gn_2, gn_g, GR, True)
        for copy in pk3:
            copy.wait()
        packed_out[...] = total_of(pk_g, groups)
        for k, out in ((2, out_out), (0, q_out), (1, kv_out)):
            for copy in swaps[k]:
                copy.wait()
            out[...] = total_of(gots[k], groups)
        for copy in gn3:
            copy.wait()
        gain_out[...] = total_of(gn_g, groups)
        for copy in wide:
            copy.wait()
        for tree in (*kv_trees, o_tree, q_tree, kvw_tree):
            tree.close()
        yield

    pieces = [(lines, own, d) for d in part_dims]
    got_pieces = pieces[:2] + [(own, model)]
    scratch = Tree.scratch(dkv_piece) * 2 + Tree.scratch(q_piece) + Tree.scratch(kv_piece)
    scratch += Tree.scratch(o_piece)
    scratch += [
        vmem((lines, rows, 2 * width), bf16),
        vmem((4,) + q_piece, bf16),
        vmem((4,) + kv_piece, bf16),
        vmem((lines, rows, width), bf16),
        vmem((lines, rows, 2 * width), bf16),
        vmem((rows, model), bf16),
        pltpu.SemaphoreType.DMA((2, lines)),
        vmem((3, 4) + weights[0].shape[1:], bf16),
        pltpu.SemaphoreType.DMA((2 * len(pairs) + 2,)),
        vmem((model, tok), bf16),
    ]
    scratch += [vmem(x.shape, bf16) for pair in pairs for x in pair]
    scratch += [vmem(p, bf16) for p in pieces] + [vmem(p, bf16) for p in pieces]
    scratch += [vmem(p, bf16) for p in got_pieces] + [vmem((groups,) + p, bf16) for p in got_pieces]
    scratch += [vmem((n,) + packed.shape, f32) for n in (lines, 4, groups)]
    scratch += [vmem(packed.shape, f32)] * 2
    scratch += [vmem((n, 1, model), f32) for n in (lines, 4, groups)] + [vmem((1, model), f32)] * 3
    copies = 2 + len(pairs) + 5 * Tree.copies + 6 * (lines - 1) + 2 * 3 + 5 * (groups - 1)
    outs = [
        shape((rows, model), f32),
        shape((lines, own, width), f32),
        shape((lines, own, 2 * width), f32),
        shape((own, model), f32),
        shape(packed.shape, f32),
        shape((1, model), f32),
    ] + [shape(x.shape, bf16) for pair in pairs for x in pair]
    ins = [*dkv, dq, attn_in, *weights, out_term, packed, hidden, resid_grad, gain]
    ins += [x for pair in pairs for x in pair]
    hbm = pl.BlockSpec(memory_space=pl.ANY)
    specs = [hbm if k in (4, 5) or k >= 11 else VM for k in range(len(ins))]
    return Part([EX, SH, GR], ins, outs, scratch, copies, phases, specs)


def expert_body(steps, x_ref, g_ref, wg_ref, wu_ref, wd_ref, eo_ref, ib_ref, ga_ref, up_ref, d_ref, eo_s, ib_s, g_s, xt_s):
    i = pl.program_id(0)
    me, side, core, _, _ = shard_peers()

    @pl.when(i == 0)
    def _():
        eo_s[...] = jnp.zeros_like(eo_s)
        ib_s[...] = jnp.zeros_like(ib_s)
        model = g_ref.shape[1]
        high, low = x_ref[:, model : model + 1], x_ref[:, model + 1 : model + 2]
        gate = high.astype(f32) + low.astype(f32)
        g_s[...] = (g_ref[...].astype(f32) * gate).astype(bf16)
        xt_s[...] = jnp.transpose(x_ref[:, :model])

    x, g = x_ref[:, : g_ref.shape[1]], g_s[...]
    wg, wu, wd = wg_ref[...], wu_ref[...], wd_ref[...]
    gate_pre = jnp.dot(x, wg, preferred_element_type=f32)
    up_pre = jnp.dot(x, wu, preferred_element_type=f32)
    hidden_grad = contract(g, wd, 1, 1)
    gate_sigmoid = jax.nn.sigmoid(gate_pre)
    act = (gate_pre * gate_sigmoid * up_pre).astype(bf16)
    gate_back = (
        hidden_grad * up_pre * gate_sigmoid * (1.0 + gate_pre * (1.0 - gate_sigmoid))
    ).astype(bf16)
    up_back = (hidden_grad * gate_pre * gate_sigmoid).astype(bf16)
    eo_s[...] += jnp.dot(act, wd, preferred_element_type=f32)
    ib_s[...] += contract(gate_back, wg, 1, 1) + contract(up_back, wu, 1, 1)

    def place(quarter):
        return 2 * lax.rem(lax.rem(quarter, 2) + core, 2) + lax.rem(quarter // 2 + side, 2)

    rows = ga_ref.shape[1]
    for ref, back in ((ga_ref, gate_back), (up_ref, up_back)):
        term = jnp.dot(xt_s[...], back, preferred_element_type=f32).astype(bf16)
        for quarter in range(4):
            ref[place(jnp.int32(quarter))] = term[quarter * rows : (quarter + 1) * rows]
    d_ref[place(i)] = contract(act, g, 0, 0).astype(bf16)

    @pl.when(i == steps - 1)
    def _():
        eo_ref[...] = eo_s[...].astype(bf16)
        ib_ref[...] = ib_s[...].astype(bf16)


def expert(x, g, wg, wu, wd):
    slots, model = g.shape
    inner = wg.shape[1]
    steps = 4
    tile = inner // steps
    quarter = model // 4
    shape = jax.ShapeDtypeStruct
    whole = lambda dims: pl.BlockSpec(dims, lambda i: (0,) * len(dims))
    return pl.pallas_call(
        functools.partial(expert_body, steps),
        grid=(steps,),
        out_shape=[
            shape((slots, model), bf16),
            shape((slots, model), bf16),
            shape((4, quarter, inner), bf16),
            shape((4, quarter, inner), bf16),
            shape((4, tile, model), bf16),
        ],
        in_specs=[
            whole(x.shape),
            whole((slots, model)),
            pl.BlockSpec((model, tile), lambda i: (0, i)),
            pl.BlockSpec((model, tile), lambda i: (0, i)),
            pl.BlockSpec((tile, model), lambda i: (i, 0)),
        ],
        out_specs=[
            whole((slots, model)),
            whole((slots, model)),
            pl.BlockSpec((4, quarter, tile), lambda i: (0, 0, i)),
            pl.BlockSpec((4, quarter, tile), lambda i: (0, 0, i)),
            whole((4, tile, model)),
        ],
        scratch_shapes=[pltpu.VMEM((slots, model), f32)] * 2 + [pltpu.VMEM((slots, model), bf16), pltpu.VMEM((model, slots), bf16)],
        cost_estimate=pl.CostEstimate(flops=6 * 10**9, bytes_accessed=2 * 10**7, transcendentals=4 * 10**5),
        name="ffn",
    )(x, g, wg, wu, wd)


def head_columns(h, shape, axis):
    return lax.broadcasted_iota(jnp.int32, shape, axis) // HEAD_DIM == h


def allowed(block, key_blk, qpos, qstart, prompt):
    kpos = block * key_blk + lax.broadcasted_iota(jnp.int32, (key_blk, qpos.shape[1]), 0)
    return (kpos <= qpos) & ((kpos >= qstart) | (kpos < prompt))


def doc_start(block, info_ref, qinfo_ref):
    docs = qinfo_ref[pl.ds(block, 1), :]
    starts = jnp.zeros(docs.shape, jnp.int32)
    for doc in range(1, DOCS):
        starts = jnp.where(docs == doc, info_ref[0, doc], starts)
    return starts, info_ref[0, info_ref[0, DOCS + block]]


def attend_body(lines, heads, info_ref, q_ref, kv_ref, qinfo_ref, o_ref, low_ref, lse_ref, k_s, vt_s, acc_s, ml_s, qm_s):
    shard = lax.axis_index(SH)
    rows, width = q_ref.shape[1:]
    blocks = vt_s.shape[0]
    key_blk = vt_s.shape[2]
    prompt = info_ref[0, 1]

    @pl.loop(0, blocks)
    def _(j):
        at = pl.ds(pl.multiple_of(j * key_blk, key_blk), key_blk)
        k_s[at, :] = kv_ref[at, :width]
        vt_s[j] = jnp.transpose(kv_ref[at, width:].astype(f32)).astype(bf16)

    @pl.loop(0, lines)
    def _(line):
        start = (line * 4 + shard) * rows
        queries = q_ref[line].astype(f32) * HEAD_DIM**-0.5
        qpos = start + lax.broadcasted_iota(jnp.int32, (1, rows), 1)
        qstart, first = doc_start(line * 4 + shard, info_ref, qinfo_ref)
        for h in range(heads):
            qm_s[h] = jnp.where(head_columns(h, queries.shape, 1), queries, 0.0).astype(bf16)
        acc_s[...] = jnp.zeros_like(acc_s)
        for h in range(heads):
            ml_s[h, 0:1, :] = jnp.full((1, rows), neg_fill, f32)
            ml_s[h, 1:2, :] = jnp.zeros((1, rows), f32)

        @pl.loop(0, (start + rows + key_blk - 1) // key_blk)
        def _(j):
            @pl.when((j * key_blk < prompt) | ((j + 1) * key_blk > first))
            def _():
                keys = k_s[pl.ds(pl.multiple_of(j * key_blk, key_blk), key_blk), :]
                ok = allowed(j, key_blk, qpos, qstart, prompt)
                for h in range(heads):
                    scores = jnp.where(ok, contract(keys, qm_s[h], 1, 1), neg_fill)
                    old = ml_s[h, 0:1, :]
                    new = jnp.maximum(old, jnp.max(scores, axis=0, keepdims=True))
                    probs = jnp.exp(scores - new)
                    scale = jnp.exp(old - new)
                    ml_s[h, 0:1, :] = new
                    ml_s[h, 1:2, :] = ml_s[h, 1:2, :] * scale + jnp.sum(
                        probs, axis=0, keepdims=True
                    )
                    part = slice(h * HEAD_DIM, (h + 1) * HEAD_DIM)
                    acc_s[part, :] = acc_s[part, :] * scale + jnp.dot(
                        vt_s[j, part, :], probs.astype(bf16), preferred_element_type=f32
                    )

        for h in range(heads):
            part = slice(h * HEAD_DIM, (h + 1) * HEAD_DIM)
            total = ml_s[h, 1:2, :]
            acc_s[part, :] = acc_s[part, :] / total
            lse_ref[line, h : h + 1, :] = ml_s[h, 0:1, :] + jnp.log(total)
        result = jnp.transpose(acc_s[...])
        o_ref[line] = result
        low_ref[line] = result.astype(bf16)


def attend(info, q, kv, qinfo):
    lines, rows, width = q.shape
    heads = width // HEAD_DIM
    length = kv.shape[0]
    key_blk = KEY_BLK
    shape = jax.ShapeDtypeStruct
    return pl.pallas_call(
        functools.partial(attend_body, lines, heads),
        out_shape=[
            shape((lines, rows, width), f32),
            shape((lines, rows, width), bf16),
            shape((lines, 8, rows), f32),
        ],
        in_specs=[SM, VM, VM, VM],
        out_specs=[VM] * 3,
        scratch_shapes=[
            pltpu.VMEM((length, width), bf16),
            pltpu.VMEM((length // key_blk, width, key_blk), bf16),
            pltpu.VMEM((width, rows), f32),
            pltpu.VMEM((heads, 8, rows), f32),
            pltpu.VMEM((heads, rows, width), bf16),
        ],
        cost_estimate=pl.CostEstimate(flops=2 * 10**9, bytes_accessed=8 * 10**6, transcendentals=4 * 10**6),
        name="attend",
    )(info, q, kv, qinfo)


def attend_back_body(lines, heads, info_ref, q_ref, kv_ref, qinfo_ref, o_ref, lse_ref, back_ref, dq_ref, dkv_lo, dkv_hi, k_s, v_s, dk_s, dv_s, dq_s, qm_s, bm_s, delta_s):
    shard = lax.axis_index(SH)
    rows, width = q_ref.shape[1:]
    key_blk = KEY_BACK
    blocks = k_s.shape[0] // key_blk
    prompt = info_ref[0, 1]

    @pl.loop(0, blocks)
    def _(j):
        at = pl.ds(pl.multiple_of(j * key_blk, key_blk), key_blk)
        k_s[at, :] = kv_ref[at, :width]
        v_s[at, :] = kv_ref[at, width:]
        dk_s[at, :] = jnp.zeros((key_blk, width), f32)
        dv_s[at, :] = jnp.zeros((key_blk, width), f32)

    @pl.loop(0, lines)
    def _(line):
        start = (line * 4 + shard) * rows
        queries = q_ref[line].astype(f32) * HEAD_DIM**-0.5
        back = back_ref[line].astype(f32)
        qpos = start + lax.broadcasted_iota(jnp.int32, (1, rows), 1)
        qstart, first = doc_start(line * 4 + shard, info_ref, qinfo_ref)
        picks = (
            lax.broadcasted_iota(jnp.int32, (8, width), 1) // HEAD_DIM
            == lax.broadcasted_iota(jnp.int32, (8, width), 0)
        ).astype(f32)
        delta_s[...] = contract(picks, back * o_ref[line], 1, 1, HIGH)
        for h in range(heads):
            mine = head_columns(h, queries.shape, 1)
            qm_s[h] = jnp.where(mine, queries, 0.0).astype(bf16)
            bm_s[h] = jnp.where(mine, back, 0.0).astype(bf16)
        dq_s[...] = jnp.zeros_like(dq_s)

        @pl.loop(0, (start + rows + key_blk - 1) // key_blk)
        def _(j):
            @pl.when((j * key_blk < prompt) | ((j + 1) * key_blk > first))
            def _():
                at = pl.ds(pl.multiple_of(j * key_blk, key_blk), key_blk)
                keys, values = k_s[at, :], v_s[at, :]
                ok = allowed(j, key_blk, qpos, qstart, prompt)
                dk = jnp.zeros((key_blk, width), f32)
                dv = jnp.zeros((key_blk, width), f32)
                for h in range(heads):
                    scores = contract(keys, qm_s[h], 1, 1)
                    probs = jnp.where(ok, jnp.exp(scores - lse_ref[line, h : h + 1, :]), 0.0)
                    grads = contract(values, bm_s[h], 1, 1)
                    slow = (probs * (grads - delta_s[h : h + 1, :])).astype(bf16)
                    dv = dv + jnp.dot(probs.astype(bf16), bm_s[h], preferred_element_type=f32)
                    dk = dk + jnp.dot(slow, qm_s[h], preferred_element_type=f32)
                    dq_s[h] += contract(slow, keys, 0, 0)
                dk_s[at, :] += dk
                dv_s[at, :] += dv

        total = jnp.zeros(queries.shape, f32)
        for h in range(heads):
            total = jnp.where(head_columns(h, queries.shape, 1), dq_s[h], total)
        dq_ref[line] = (total * HEAD_DIM**-0.5).astype(bf16)

    half = lines // 2
    for k, ref in enumerate((dkv_lo, dkv_hi)):

        @pl.loop(0, half)
        def _(line):
            for piece in range(4):
                at = ((k * half + line) * 4 + piece) * rows
                at = pl.ds(pl.multiple_of(at, rows), rows)
                ref[piece, line, :, :width] = dk_s[at, :].astype(bf16)
                ref[piece, line, :, width:] = dv_s[at, :].astype(bf16)


def attend_back(info, q, kv, qinfo, o, lse, back):
    lines, rows, width = q.shape
    heads = width // HEAD_DIM
    length = kv.shape[0]
    shape = jax.ShapeDtypeStruct
    return pl.pallas_call(
        functools.partial(attend_back_body, lines, heads),
        out_shape=[
            shape((lines, rows, width), bf16),
            shape((4, lines // 2, rows, 2 * width), bf16),
            shape((4, lines // 2, rows, 2 * width), bf16),
        ],
        in_specs=[SM] + [VM] * 6,
        out_specs=[VM] * 3,
        scratch_shapes=[
            pltpu.VMEM((length, width), bf16),
            pltpu.VMEM((length, width), bf16),
            pltpu.VMEM((length, width), f32),
            pltpu.VMEM((length, width), f32),
            pltpu.VMEM((heads, rows, width), f32),
            pltpu.VMEM((heads, rows, width), bf16),
            pltpu.VMEM((heads, rows, width), bf16),
            pltpu.VMEM((8, rows), f32),
        ],
        cost_estimate=pl.CostEstimate(flops=5 * 10**9, bytes_accessed=12 * 10**6, transcendentals=4 * 10**6),
        name="attend_back",
    )(info, q, kv, qinfo, o, lse, back)


def finale_body(lines, n_ids, *refs):
    ins, outs = refs[:13], refs[13:]
    for k in range(3):
        outs[k][...] = ins[k][...].astype(f32) + ins[3 + k][...].astype(f32)
    for k in range(2):
        outs[3 + k][...] = ins[6 + k][...]

    @pl.when(pl.program_id(0) == 0)
    def _():
        q_sum, kv_sum, out_sum, small_ref, gain_ref = ins[8:]
        q_out, k_out, v_out, out_out, gain_out, mgain_out, vec_out, rout_out, mix_out = outs[5:]
        width = q_sum.shape[2]
        for line in range(lines):
            at = slice(line * width, (line + 1) * width)
            q_out[:, at] = q_sum[line]
            k_out[:, at] = kv_sum[line, :, :width]
            v_out[:, at] = kv_sum[line, :, width:]
        out_out[...] = out_sum[...]
        gain_out[...] = jnp.sum(gain_ref[...], axis=0)
        small = small_ref[...]
        mgain_out[...] = jnp.sum(small[0:1], axis=0)
        vec_out[...] = small[1:3]
        rout_out[...] = small[3 : 3 + n_ids]
        mix_out[...] = small[3 + n_ids : 7 + n_ids]


def finale(mine, far, input_grad, layer_out, sums, n_ids):
    steps = 4
    shape = jax.ShapeDtypeStruct
    own, model = sums[2].shape
    lines = sums[0].shape[0]

    def tiled(dims, dim):
        block = tuple(d // steps if k == dim else d for k, d in enumerate(dims))
        return pl.BlockSpec(block, lambda i: tuple(i if k == dim else 0 for k in range(2)))

    def whole(dims):
        return pl.BlockSpec(dims, lambda i: (0,) * len(dims))

    wide = [tiled(mine[0].shape, 1), tiled(mine[1].shape, 1), tiled(mine[2].shape, 0)]
    rows = [tiled(input_grad.shape, 0), tiled(layer_out.shape, 0)]
    small = [(own, model)] * 4 + [(model,), (model,), (2, model), (n_ids, model), (4, model)]
    return pl.pallas_call(
        functools.partial(finale_body, lines, n_ids),
        grid=(steps,),
        out_shape=[shape(m.shape, f32) for m in mine]
        + [shape(input_grad.shape, f32), shape(layer_out.shape, bf16)]
        + [shape(d, f32) for d in small],
        in_specs=wide + wide + rows + [whole(x.shape) for x in sums],
        out_specs=wide + rows + [whole(d) for d in small],
        cost_estimate=pl.CostEstimate(flops=10**7, bytes_accessed=10**7, transcendentals=0),
        name="finale",
    )(*mine, *far, input_grad, layer_out, *sums)


def swap(x, axis, partner):
    return lax.ppermute(x, axis, [(i, partner(i)) for i in range(lax.axis_size(axis))])


def fast_shards(
    hidden_in,
    segment_ids,
    routes,
    attn_gain,
    w_query,
    w_key,
    w_value,
    w_out,
    moe_gain,
    w_router,
    const_mix,
    const_vec,
    w_gate,
    w_up,
    w_down,
    out_grad,
):
    rows, model = hidden_in.shape
    lines = lax.axis_size(EX)
    line, shard = lax.axis_index(EX), lax.axis_index(SH)
    width = model // lines
    length = segment_ids.shape[1]

    w_qkv = jnp.stack([w_query, w_key, w_value])
    w_mine = lax.dynamic_slice_in_dim(w_qkv, line * width, width, axis=2)
    w_mine = jnp.concatenate([w_mine[1], w_mine[2], w_mine[0]], axis=1)
    qinfo = segment_ids.reshape(length // rows, rows)
    attn_in, q, kv_all, place, recv_grads, info = front(
        hidden_in, w_mine, attn_gain, routes.T, out_grad, qinfo
    )
    attn_in = attn_in.reshape(lines * rows, model)
    kv_all, w_out_b = lax.optimization_barrier((kv_all, w_out))
    wo_far = swap(w_out_b, SH, lambda i: i ^ 2)
    kv_all = kv_all.reshape(length, 2 * width)
    attn_vec, attn_heads, lse = attend(info, q, kv_all, qinfo)
    attn_heads, w_qkv = lax.optimization_barrier((attn_heads, w_qkv))
    w_far = swap(w_qkv, SH, lambda i: i ^ 2)
    n_ids = w_router.shape[1]
    small_t = jnp.pad(
        jnp.concatenate([w_router.T, const_mix.T], axis=0), ((0, 124 - n_ids), (0, 0))
    )
    gain_two = moe_gain
    recv_rows, wo_full, resid_one, table, attn_low = run_parts(
        [
            route(
                attn_heads, hidden_in, gain_two, small_t, routes.T, place, w_out[None], wo_far[None], n_ids
            )
        ],
        2,
        "route",
    )
    wo_full = wo_full.reshape(model, model)
    recv_rows, w_far = lax.optimization_barrier((recv_rows, w_far))
    slots = lines * CAP

    expert_out, input_back, *terms = expert(
        recv_rows.reshape(slots, model + 128), recv_grads.reshape(slots, model), w_gate[0], w_up[0], w_down[0]
    )
    returned, input_ret, *sums = run_parts(
        [
            exchange(EX, SWAP, expert_out.reshape(lines, CAP, model)),
            exchange(EX, SWAP, input_back.reshape(lines, CAP, model)),
        ]
        + [core_sum(term) for term in terms],
        4,
        "combine",
    )
    far = [swap(there, SH, lambda i: i ^ 2) for there in sums[1::2]]
    down = (sums[4].astype(f32) + far[2].astype(f32)).astype(bf16)

    back_heads, layer_out, resid_grad, out_term, packed = run_parts(
        [
            to_heads(
                returned, input_ret, place, table, resid_one, attn_low, out_grad, gain_two, small_t, const_vec, wo_full, n_ids
            )
        ],
        5,
        "to_heads",
    )
    back_heads, down = lax.optimization_barrier((back_heads, down))
    cross = lambda x: swap(x, GR, lambda i: 1 - i)
    down_far = cross(down)
    dq, *dkv = attend_back(info, q, kv_all, qinfo, attn_vec, lse, back_heads)
    pairs = [(sums[0], far[0]), (sums[2], far[1])]
    input_grad, *parts = run_parts(
        [
            tail(
                dkv, dq, attn_in, (w_qkv, w_far), out_term, packed, hidden_in, resid_grad, attn_gain, pairs
            )
        ],
        6,
        "tail",
        pl.CostEstimate(flops=2 * 10**10, bytes_accessed=10**8, transcendentals=0),
    )
    gate, up, down, input_grad, layer_out, *grads, gain, gain_two, vecs, router, mix = finale(
        [parts[5], parts[7], down],
        [parts[6], parts[8], down_far],
        input_grad,
        layer_out,
        parts[:5],
        n_ids,
    )
    return (
        layer_out,
        input_grad,
        gain,
        *grads,
        gain_two,
        router.T,
        mix.T,
        vecs,
        gate[None],
        up[None],
        down[None],
    )


def solution(mesh):
    placed = (
        P((GR, EX, SH), None),
        P(GR, None),
        P((GR, EX, SH), None),
        P(),
        P(SH, None),
        P(SH, None),
        P(SH, None),
        P(SH, None),
        P(),
        P(),
        P(),
        P(),
        P(EX, None, None),
        P(EX, None, None),
        P(EX, None, None),
        P((GR, EX, SH), None),
    )
    sizes = dict(mesh.shape)
    lines = sizes[EX]
    fast = (sizes[GR], sizes[SH], lines) == (2, 4, 4)
    return jax.shard_map(
        fast_shards if fast else shards,
        mesh=mesh,
        in_specs=placed,
        out_specs=(
            P((GR, EX, SH), None),
            P((GR, EX, SH), None),
            P(),
            P((EX, SH), None),
            P((EX, SH), None),
            P((EX, SH), None),
            P((EX, SH), None),
            P(),
            P(),
            P(),
            P(),
            P(EX, SH, None),
            P(EX, SH, None),
            P(EX, SH, None),
        ),
        check_vma=False,
    )
```

```python
import functools

import jax
import jax.numpy as jnp
from jax import lax
from jax.experimental import pallas as pl
from jax.experimental.pallas import tpu as pltpu
from jax.sharding import PartitionSpec as P

HEADS = 12
HEAD_DIM = 64
CAP = 48
DOCS = 9
KEY_BLK = 256
KEY_BACK = 768
EX, SH, GR = ("expert", "shard", "group")
GATHER, GATHER_SUM, SWAP, SWAP_SUM = range(4)


neg_fill = -1e30
norm_eps = 1e-05
bf16 = jnp.bfloat16
f32 = jnp.float32
VM = pl.BlockSpec(memory_space=pltpu.VMEM)
SM = pl.BlockSpec(memory_space=pltpu.SMEM)
HIGH = lax.Precision.HIGHEST


def contract(a, b, da, db, precision=None):
    return lax.dot_general(
        a, b, (((da,), (db,)), ((), ())), preferred_element_type=f32, precision=precision
    )


def dense32(left_side, right_side):
    return jnp.dot(left_side, right_side, precision=lax.Precision.HIGHEST)


def allowed_mask(query_pos, query_seg, key_pos, key_seg):
    same_doc = (key_seg[None, :] == query_seg[:, None]) | (key_seg[None, :] == 0)
    return same_doc & (key_pos[None, :] <= query_pos[:, None])


def rms_back(inputs, inverse, gain_vec, upstream):
    scaled = upstream * gain_vec
    return inverse * scaled - inputs * inverse**3 * jnp.mean(scaled * inputs, axis=1, keepdims=True)


def block_scores(query_blk, keys_blk, score_scale):
    return (
        jnp.einsum("qhd,khd->hqk", query_blk, keys_blk, preferred_element_type=jnp.float32)
        * score_scale
    )


def grad_pieces(
    query_blk, back_blk, keys_blk, values_blk, norm_blk, delta_blk, key_mask, score_scale
):
    scores = block_scores(query_blk, keys_blk, score_scale)
    prob_rows = jnp.where(key_mask[None], jnp.exp(scores - norm_blk[:, :, None]), 0.0)
    prob_grad = jnp.einsum("qhd,khd->hqk", back_blk, values_blk, preferred_element_type=jnp.float32)
    score_low = (prob_rows * (prob_grad - delta_blk[:, :, None])).astype(jnp.bfloat16)
    return (prob_rows.astype(jnp.bfloat16), score_low)


def shards(
    hidden_in,
    segment_ids,
    routes,
    attn_gain,
    w_query,
    w_key,
    w_value,
    w_out,
    moe_gain,
    w_router,
    const_mix,
    const_vec,
    w_gate,
    w_up,
    w_down,
    out_grad,
):
    tok_rows, model_width = hidden_in.shape
    score_scale = HEAD_DIM ** (-0.5)
    inner_rank = lax.axis_index((EX, SH))
    seg_group = segment_ids[0]
    group_len = seg_group.shape[0]
    key_block = min(512, group_len)
    num_blocks = group_len // key_block
    row_start = inner_rank * tok_rows
    own_pos = row_start + jnp.arange(tok_rows, dtype=jnp.int32)
    own_seg = lax.dynamic_slice_in_dim(seg_group, row_start, tok_rows)
    wq_full, wk_full, wv_full, wo_full = (
        lax.all_gather(w_query, SH, axis=0, tiled=True),
        lax.all_gather(w_key, SH, axis=0, tiled=True),
        lax.all_gather(w_value, SH, axis=0, tiled=True),
        lax.all_gather(w_out, SH, axis=0, tiled=True),
    )
    inputs = hidden_in.astype(jnp.float32)
    inv_one = lax.rsqrt(jnp.mean(inputs * inputs, axis=1, keepdims=True) + norm_eps)
    normed_one = inputs * inv_one
    attn_in = (normed_one * attn_gain).astype(jnp.bfloat16)
    queries = jnp.dot(attn_in, wq_full, preferred_element_type=jnp.float32).astype(jnp.bfloat16)
    keys_own = jnp.dot(attn_in, wk_full, preferred_element_type=jnp.float32).astype(jnp.bfloat16)
    values_own = jnp.dot(attn_in, wv_full, preferred_element_type=jnp.float32).astype(jnp.bfloat16)
    keys_all, values_all = (
        lax.all_gather(keys_own, (EX, SH), axis=0, tiled=True),
        lax.all_gather(values_own, (EX, SH), axis=0, tiled=True),
    )
    query_heads = queries.reshape(tok_rows, HEADS, HEAD_DIM)

    def fetch_block(source, block_index):
        return lax.dynamic_slice_in_dim(source, block_index * key_block, key_block).reshape(
            key_block, HEADS, HEAD_DIM
        )

    def block_mask(block_index):
        key_pos = block_index * key_block + jnp.arange(key_block, dtype=jnp.int32)
        key_seg = lax.dynamic_slice_in_dim(seg_group, block_index * key_block, key_block)
        return allowed_mask(own_pos, own_seg, key_pos, key_seg)

    def stats_step(carry_now, block_index):
        key_mask = block_mask(block_index)

        def stats_live_block(carry_in):
            row_max, row_sum = carry_in
            scores = jnp.where(
                key_mask[None],
                block_scores(query_heads, fetch_block(keys_all, block_index), score_scale),
                neg_fill,
            )
            new_max = jnp.maximum(row_max, jnp.max(scores, axis=2))
            weights = jnp.where(key_mask[None], jnp.exp(scores - new_max[:, :, None]), 0.0)
            return (new_max, row_sum * jnp.exp(row_max - new_max) + jnp.sum(weights, axis=2))

        return (
            lax.cond(jnp.any(key_mask), stats_live_block, lambda carry_in: carry_in, carry_now),
            None,
        )

    start_max = jnp.full((HEADS, tok_rows), neg_fill, jnp.float32)
    row_max, row_sum = lax.scan(
        stats_step, (start_max, jnp.zeros_like(start_max)), jnp.arange(num_blocks)
    )[0]
    log_norm = row_max + jnp.log(row_sum)

    def output_step(running, block_index):
        key_mask = block_mask(block_index)

        def output_live_block(carry_in):
            scores = block_scores(query_heads, fetch_block(keys_all, block_index), score_scale)
            prob_rows = jnp.where(
                key_mask[None], jnp.exp(scores - log_norm[:, :, None]), 0.0
            ).astype(jnp.bfloat16)
            return carry_in + jnp.einsum(
                "hqk,khd->qhd",
                prob_rows,
                fetch_block(values_all, block_index),
                preferred_element_type=jnp.float32,
            )

        return (
            lax.cond(jnp.any(key_mask), output_live_block, lambda carry_in: carry_in, running),
            None,
        )

    zero_heads = jnp.zeros((tok_rows, HEADS, HEAD_DIM), jnp.float32)
    attn_sum = lax.scan(output_step, zero_heads, jnp.arange(num_blocks))[0]
    attn_low = attn_sum.reshape(tok_rows, model_width).astype(jnp.bfloat16)
    resid_one = inputs + jnp.dot(attn_low, wo_full, preferred_element_type=jnp.float32)
    inv_two = lax.rsqrt(jnp.mean(resid_one * resid_one, axis=1, keepdims=True) + norm_eps)
    normed_two = resid_one * inv_two
    moe_in = normed_two * moe_gain
    moe_low = moe_in.astype(jnp.bfloat16)
    n_ids = w_router.shape[1]
    local_experts = w_gate.shape[0]
    owners = lax.axis_size(EX)
    ffn_count = local_experts * owners
    id_table = jnp.arange(n_ids, dtype=jnp.int32)
    route_hot = (routes[:, :, None] == id_table).astype(jnp.float32)
    logits = dense32(moe_in, w_router)
    chosen = jnp.einsum("rkn,rn->rk", route_hot, logits, precision=lax.Precision.HIGHEST)
    gate_probs = jax.nn.softmax(chosen, axis=1)
    mix_alpha = jax.nn.softmax(dense32(moe_in, const_mix).reshape(tok_rows, 2, 2), axis=2)
    const_rows = mix_alpha[:, :, 0:1] * moe_in[:, None, :] + mix_alpha[:, :, 1:2] * const_vec[None]
    ffn_mask = (routes < ffn_count).astype(jnp.float32)
    copy_mask = (routes == ffn_count + 1).astype(jnp.float32)
    const_mask = (routes[:, :, None] == ffn_count + 2 + jnp.arange(2, dtype=jnp.int32)).astype(
        jnp.float32
    )
    copy_gate = jnp.sum(gate_probs * copy_mask, axis=1)
    const_gate = jnp.sum(gate_probs[:, :, None] * const_mask, axis=1)
    ffn_gate = gate_probs * ffn_mask
    flat_ids = routes.reshape(-1)
    id_hot = (flat_ids[:, None] == id_table).astype(jnp.int32)
    earlier = jnp.cumsum(id_hot, axis=0, dtype=jnp.int32) - id_hot
    slot_num = jnp.sum(earlier * id_hot, axis=1, dtype=jnp.int32)
    slot_total = ffn_count * CAP
    slot_of_route = jnp.where(flat_ids < ffn_count, flat_ids * CAP + slot_num, slot_total)
    route_count = flat_ids.shape[0]
    route_of_slot = (
        jnp.zeros(slot_total + 1, jnp.int32)
        .at[slot_of_route]
        .set(jnp.arange(route_count, dtype=jnp.int32))[:slot_total]
    )
    slot_used = jnp.zeros(slot_total + 1, jnp.bool_).at[slot_of_route].set(True)[:slot_total]
    send_rows = jnp.where(
        slot_used[:, None], moe_low[route_of_slot // 2], jnp.zeros((), jnp.bfloat16)
    )
    recv_rows = lax.all_to_all(
        send_rows.reshape(owners, local_experts * CAP, model_width),
        EX,
        split_axis=0,
        concat_axis=0,
        tiled=True,
    )
    expert_in = recv_rows.reshape(owners, local_experts, CAP, model_width)
    gate_pre = jnp.einsum("sjcd,jdf->sjcf", expert_in, w_gate, preferred_element_type=jnp.float32)
    up_pre = jnp.einsum("sjcd,jdf->sjcf", expert_in, w_up, preferred_element_type=jnp.float32)
    gate_sigmoid = jax.nn.sigmoid(gate_pre)
    hidden_act = (gate_pre * gate_sigmoid * up_pre).astype(jnp.bfloat16)
    expert_out = jnp.einsum(
        "sjcf,jfd->sjcd", hidden_act, w_down, preferred_element_type=jnp.float32
    ).astype(jnp.bfloat16)
    returned = lax.all_to_all(
        expert_out.reshape(owners, local_experts * CAP, model_width),
        EX,
        split_axis=0,
        concat_axis=0,
        tiled=True,
    )
    padded_out = jnp.concatenate(
        [returned.reshape(slot_total, model_width), jnp.zeros((1, model_width), jnp.bfloat16)],
        axis=0,
    )
    route_out = padded_out[slot_of_route].astype(jnp.float32).reshape(tok_rows, 2, model_width)
    moe_sum = (
        jnp.sum(ffn_gate[:, :, None] * route_out, axis=1)
        + copy_gate[:, None] * moe_in
        + jnp.sum(const_gate[:, :, None] * const_rows, axis=1)
    )
    layer_out = (resid_one + moe_sum).astype(jnp.bfloat16)
    upstream = out_grad.astype(jnp.float32)
    route_dot = jnp.sum(upstream[:, None, :] * route_out, axis=2)
    copy_dot = jnp.sum(upstream * moe_in, axis=1)
    const_dot = jnp.sum(upstream[:, None, :] * const_rows, axis=2)
    gate_back_r = (
        ffn_mask * route_dot
        + copy_mask * copy_dot[:, None]
        + jnp.sum(const_mask * const_dot[:, None, :], axis=2)
    )
    chosen_grad = gate_probs * (
        gate_back_r - jnp.sum(gate_probs * gate_back_r, axis=1, keepdims=True)
    )
    logit_grad = jnp.einsum("rk,rkn->rn", chosen_grad, route_hot, precision=lax.Precision.HIGHEST)
    const_up = const_gate[:, :, None] * upstream[:, None, :]
    alpha_grad = jnp.stack(
        [
            jnp.sum(const_up * moe_in[:, None, :], axis=2),
            jnp.sum(const_up * const_vec[None], axis=2),
        ],
        axis=2,
    )
    mix_back = (
        mix_alpha * (alpha_grad - jnp.sum(mix_alpha * alpha_grad, axis=2, keepdims=True))
    ).reshape(tok_rows, 4)
    vec_grad = jnp.sum(mix_alpha[:, :, 1:2] * const_up, axis=0)
    route_weight = ffn_gate.reshape(-1)
    grad_send = (route_weight[route_of_slot][:, None] * upstream[route_of_slot // 2]).astype(
        jnp.bfloat16
    )
    grad_send = jnp.where(slot_used[:, None], grad_send, jnp.zeros((), jnp.bfloat16))
    grad_recv = lax.all_to_all(
        grad_send.reshape(owners, local_experts * CAP, model_width),
        EX,
        split_axis=0,
        concat_axis=0,
        tiled=True,
    )
    grad_recv = grad_recv.reshape(owners, local_experts, CAP, model_width)
    hidden_grad = jnp.einsum(
        "sjcd,jfd->sjcf", grad_recv, w_down, preferred_element_type=jnp.float32
    )
    down_term = jnp.einsum(
        "sjcf,sjcd->jfd", hidden_act, grad_recv, preferred_element_type=jnp.float32
    )
    gate_back = (
        hidden_grad * up_pre * gate_sigmoid * (1.0 + gate_pre * (1.0 - gate_sigmoid))
    ).astype(jnp.bfloat16)
    up_back = (hidden_grad * gate_pre * gate_sigmoid).astype(jnp.bfloat16)
    gate_term = jnp.einsum(
        "sjcd,sjcf->jdf", expert_in, gate_back, preferred_element_type=jnp.float32
    )
    up_term = jnp.einsum("sjcd,sjcf->jdf", expert_in, up_back, preferred_element_type=jnp.float32)
    input_back = (
        jnp.einsum("sjcf,jdf->sjcd", gate_back, w_gate, preferred_element_type=jnp.float32)
        + jnp.einsum("sjcf,jdf->sjcd", up_back, w_up, preferred_element_type=jnp.float32)
    ).astype(jnp.bfloat16)
    input_ret = lax.all_to_all(
        input_back.reshape(owners, local_experts * CAP, model_width),
        EX,
        split_axis=0,
        concat_axis=0,
        tiled=True,
    )
    padded_in = jnp.concatenate(
        [input_ret.reshape(slot_total, model_width), jnp.zeros((1, model_width), jnp.bfloat16)],
        axis=0,
    )
    ffn_in_grad = jnp.sum(
        padded_in[slot_of_route].astype(jnp.float32).reshape(tok_rows, 2, model_width), axis=1
    )
    moe_in_grad = (
        ffn_in_grad
        + copy_gate[:, None] * upstream
        + jnp.sum(mix_alpha[:, :, 0:1] * const_up, axis=1)
        + dense32(mix_back, const_mix.T)
        + dense32(logit_grad, w_router.T)
    )
    moe_gain_grad = jnp.sum(moe_in_grad * normed_two, axis=0)
    router_grad = dense32(moe_in.T, logit_grad)
    mix_grad = dense32(moe_in.T, mix_back)
    resid_grad = upstream + rms_back(resid_one, inv_two, moe_gain, moe_in_grad)
    branch_low = resid_grad.astype(jnp.bfloat16)
    out_proj_term = jnp.dot(attn_low.T, branch_low, preferred_element_type=jnp.float32)
    attn_back = jnp.dot(branch_low, wo_full.T, preferred_element_type=jnp.float32).astype(
        jnp.bfloat16
    )
    back_heads = attn_back.reshape(tok_rows, HEADS, HEAD_DIM)
    row_delta = jnp.sum(back_heads.astype(jnp.float32) * attn_sum, axis=2).T

    def back_step(query_acc, block_index):
        key_mask = block_mask(block_index)
        keys_blk = fetch_block(keys_all, block_index)
        values_blk = fetch_block(values_all, block_index)

        def back_live_block(running):
            prob_low, score_low = grad_pieces(
                query_heads,
                back_heads,
                keys_blk,
                values_blk,
                log_norm,
                row_delta,
                key_mask,
                score_scale,
            )
            value_part = jnp.einsum(
                "hqk,qhd->khd", prob_low, back_heads, preferred_element_type=jnp.float32
            )
            key_part = (
                jnp.einsum(
                    "hqk,qhd->khd", score_low, query_heads, preferred_element_type=jnp.float32
                )
                * score_scale
            )
            running = (
                running
                + jnp.einsum(
                    "hqk,khd->qhd", score_low, keys_blk, preferred_element_type=jnp.float32
                )
                * score_scale
            )
            return (
                running,
                (
                    key_part.reshape(key_block, model_width),
                    value_part.reshape(key_block, model_width),
                ),
            )

        def dead_block(running):
            empty_rows = jnp.zeros((key_block, model_width), jnp.float32)
            return (running, (empty_rows, empty_rows))

        return lax.cond(jnp.any(key_mask), back_live_block, dead_block, query_acc)

    query_grad32, key_terms = lax.scan(back_step, zero_heads, jnp.arange(num_blocks))
    key_grad32, value_grad32 = (
        lax.psum_scatter(
            key_terms[0].reshape(group_len, model_width).astype(jnp.bfloat16),
            (EX, SH),
            scatter_dimension=0,
            tiled=True,
        ).astype(jnp.float32),
        lax.psum_scatter(
            key_terms[1].reshape(group_len, model_width).astype(jnp.bfloat16),
            (EX, SH),
            scatter_dimension=0,
            tiled=True,
        ).astype(jnp.float32),
    )
    query_low = query_grad32.reshape(tok_rows, model_width).astype(jnp.bfloat16)
    key_low = key_grad32.astype(jnp.bfloat16)
    value_low = value_grad32.astype(jnp.bfloat16)
    query_term = jnp.dot(attn_in.T, query_low, preferred_element_type=jnp.float32)
    key_term = jnp.dot(attn_in.T, key_low, preferred_element_type=jnp.float32)
    value_term = jnp.dot(attn_in.T, value_low, preferred_element_type=jnp.float32)
    attn_in_grad = (
        jnp.dot(query_low, wq_full.T, preferred_element_type=jnp.float32)
        + jnp.dot(key_low, wk_full.T, preferred_element_type=jnp.float32)
        + jnp.dot(value_low, wv_full.T, preferred_element_type=jnp.float32)
    )
    attn_gain_grad = jnp.sum(attn_in_grad * normed_one, axis=0)
    input_grad = resid_grad + rms_back(inputs, inv_one, attn_gain, attn_in_grad)
    query_part, key_part_w, value_part_w, out_part = (
        lax.psum_scatter(
            query_term.astype(jnp.bfloat16), (EX, SH), scatter_dimension=0, tiled=True
        ).astype(jnp.float32),
        lax.psum_scatter(
            key_term.astype(jnp.bfloat16), (EX, SH), scatter_dimension=0, tiled=True
        ).astype(jnp.float32),
        lax.psum_scatter(
            value_term.astype(jnp.bfloat16), (EX, SH), scatter_dimension=0, tiled=True
        ).astype(jnp.float32),
        lax.psum_scatter(
            out_proj_term.astype(jnp.bfloat16), (EX, SH), scatter_dimension=0, tiled=True
        ).astype(jnp.float32),
    )
    gate_part, up_part, down_part = (
        lax.psum_scatter(
            gate_term.astype(jnp.bfloat16), SH, scatter_dimension=1, tiled=True
        ).astype(jnp.float32),
        lax.psum_scatter(
            up_term.astype(jnp.bfloat16), SH, scatter_dimension=1, tiled=True
        ).astype(jnp.float32),
        lax.psum_scatter(
            down_term.astype(jnp.bfloat16), SH, scatter_dimension=1, tiled=True
        ).astype(jnp.float32),
    )
    summed = (
        lax.psum(query_part.astype(jnp.bfloat16), GR).astype(jnp.float32),
        lax.psum(key_part_w.astype(jnp.bfloat16), GR).astype(jnp.float32),
        lax.psum(value_part_w.astype(jnp.bfloat16), GR).astype(jnp.float32),
        lax.psum(out_part.astype(jnp.bfloat16), GR).astype(jnp.float32),
        lax.psum(gate_part.astype(jnp.bfloat16), GR).astype(jnp.float32),
        lax.psum(up_part.astype(jnp.bfloat16), GR).astype(jnp.float32),
        lax.psum(down_part.astype(jnp.bfloat16), GR).astype(jnp.float32),
    )
    small_sums = lax.psum(
        (attn_gain_grad, moe_gain_grad, router_grad, mix_grad, vec_grad),
        (GR, EX, SH),
    )
    return (
        layer_out,
        input_grad,
        small_sums[0],
        summed[0],
        summed[1],
        summed[2],
        summed[3],
        small_sums[1],
        small_sums[2],
        small_sums[3],
        small_sums[4],
        summed[4],
        summed[5],
        summed[6],
    )


def greet(peers):
    barrier = pltpu.get_barrier_semaphore()
    for axis, peer in peers:
        pl.semaphore_signal(
            barrier, inc=1, device_id={axis: peer}, device_id_type=pl.DeviceIdType.MESH
        )
    pl.semaphore_wait(barrier, len(peers))


def send(src, dst, sems, index, axis, peer):
    copy = pltpu.make_async_remote_copy(
        src_ref=src,
        dst_ref=dst,
        send_sem=sems.at[0, index],
        recv_sem=sems.at[1, index],
        device_id={axis: peer},
        device_id_type=pl.DeviceIdType.MESH,
    )
    copy.start()
    return copy


def shard_peers():
    me = lax.axis_index(SH)
    side, core = me // 2, lax.rem(me, 2)
    return me, side, core, 2 * side + 1 - core, 2 * (1 - side) + core


class Part:
    def __init__(self, axes, ins, outs, scratch, copies, phases, specs=None):
        self.axes, self.ins, self.outs, self.scratch = axes, ins, outs, scratch
        self.copies, self.phases = copies, phases
        self.specs = specs or [VM] * len(ins)


def run_parts(parts, collective_id, name=None, cost=None):
    ins = sum([p.ins for p in parts], [])
    outs = sum([p.outs for p in parts], [])
    scratch = sum([p.scratch for p in parts], [])
    copies = sum(p.copies for p in parts)
    axes = sorted(set(sum([list(p.axes) for p in parts], [])))

    def body(*refs):
        sems = refs[-1]
        in_refs, out_refs = list(refs[: len(ins)]), list(refs[len(ins) : len(ins) + len(outs)])
        scr = list(refs[len(ins) + len(outs) : -1])
        peers = []
        for axis in axes:
            me, n = lax.axis_index(axis), lax.axis_size(axis)
            peers += [(axis, lax.rem(me + d, n)) for d in range(1, n)]
        greet(peers)
        base, running = 0, []
        for p in parts:
            take = lambda pool, k: [pool.pop(0) for _ in range(k)]
            refs_p = (take(in_refs, len(p.ins)), take(out_refs, len(p.outs)), take(scr, len(p.scratch)))
            counter = [base]

            def go(src, dst, axis, peer, counter=counter):
                counter[0] += 1
                return send(src, dst, sems, counter[0] - 1, axis, peer)

            running.append(p.phases(*refs_p, go))
            base += p.copies
        while running:
            running = [r for r in running if next(r, True) is None]

    return pl.pallas_call(
        body,
        out_shape=outs,
        in_specs=sum([p.specs for p in parts], []),
        out_specs=[VM] * len(outs),
        scratch_shapes=scratch + [pltpu.SemaphoreType.DMA((2, copies))],
        compiler_params=pltpu.CompilerParams(collective_id=collective_id, has_side_effects=True),
        cost_estimate=cost,
        name=name,
    )(*ins)


def start_swap(go, src, land, axis, gather):
    me, n = lax.axis_index(axis), lax.axis_size(axis)
    started = []
    for d in range(1, n):
        peer = lax.rem(me + d, n)
        started.append(go(src if gather else src.at[peer], land.at[me], axis, peer))
    land[me] = src[...] if gather else src[me]
    return started


def total_of(land, n):
    total = land[0].astype(f32)
    for j in range(1, n):
        total = total + land[j].astype(f32)
    return total


def exchange(axis, kind, x):
    n = lax.axis_size(axis)
    gather, summed = kind in (GATHER, GATHER_SUM), kind in (GATHER_SUM, SWAP_SUM)
    piece = x.shape if gather else x.shape[1:]
    shape = jax.ShapeDtypeStruct
    outs = [shape(piece, f32) if summed else shape((n,) + piece, x.dtype)]
    scratch = [pltpu.VMEM((n,) + piece, x.dtype)] if summed else []

    def phases(ins, outs, scr, go):
        land = scr[0] if summed else outs[0]
        started = start_swap(go, ins[0], land, axis, gather)
        yield
        for copy in started:
            copy.wait()
        if summed:
            outs[0][...] = total_of(land, n)

    return Part([axis], [x], outs, scratch, n - 1, phases)


def tree_gather(x):
    lines = x.shape[0]
    cuts = [(0, lines // 2), (lines // 2, lines)] if lines > 1 else [(0, 1)]
    cuts = [pl.ds(lo, hi - lo) for lo, hi in cuts]

    def phases(ins, outs, scr, go):
        x_ref, out_ref = ins[0], outs[0]
        me, _, _, near, far = shard_peers()
        across = [go(x_ref.at[c], out_ref.at[c, me], SH, far) for c in cuts]
        own = go(x_ref, out_ref.at[:, me], SH, near)
        out_ref[:, me] = x_ref[...]
        yield
        handed = []
        for c, copy in zip(cuts, across):
            copy.wait_recv()
            handed.append(go(out_ref.at[c, far], out_ref.at[c, far], SH, near))
        yield
        for copy in across:
            copy.wait_send()
        own.wait()
        for copy in handed:
            copy.wait()

    shape = (lines, 4) + x.shape[1:]
    return Part([SH], [x], [jax.ShapeDtypeStruct(shape, x.dtype)], [], 2 * len(cuts) + 1, phases)


def core_sum(x):
    piece = x.shape[1:]
    shape = jax.ShapeDtypeStruct

    def phases(ins, outs, scr, go):
        x_ref, (here, there), (land, kept, sems) = ins[0], outs, scr
        near = shard_peers()[3]
        sent = [go(x_ref.at[3], land.at[1], SH, near), go(x_ref.at[2], land.at[0], SH, near)]
        local = [pltpu.make_async_copy(x_ref.at[k], kept.at[k], sems.at[k]) for k in range(2)]
        for copy in local:
            copy.start()
        yield
        for k, out in ((1, there), (0, here)):
            sent[1 - k].wait()
            local[k].wait()
            out[...] = (kept[k].astype(f32) + land[k].astype(f32)).astype(bf16)

    return Part(
        [SH],
        [x],
        [shape(piece, bf16)] * 2,
        [pltpu.VMEM((2,) + piece, bf16)] * 2 + [pltpu.SemaphoreType.DMA((2,))],
        2,
        phases,
        [pl.BlockSpec(memory_space=pl.ANY)],
    )


class Tree:
    copies = 3

    @staticmethod
    def scratch(piece):
        return [pltpu.VMEM((2,) + piece, bf16)] + [pltpu.VMEM(piece, bf16)] * 2

    def __init__(self, x, scr, go):
        self.x, (self.land, self.mine, self.got), self.go = x, scr, go
        self.me, self.side, self.core, self.near, self.far = shard_peers()
        other = 2 * (1 - self.side) + 1 - self.core
        self.first = [
            go(x.at[other], self.land.at[0], SH, self.near),
            go(x.at[self.near], self.land.at[1], SH, self.near),
        ]

    def across(self):
        self.first[0].wait_recv()
        self.mine[...] = (self.x[self.far].astype(f32) + self.land[0].astype(f32)).astype(bf16)
        self.second = self.go(self.mine, self.got, SH, self.far)

    def result(self):
        self.first[1].wait_recv()
        total = self.x[self.me].astype(f32) + self.land[1].astype(f32)
        self.second.wait_recv()
        return total + self.got[...].astype(f32)

    def close(self):
        for copy in (*self.first, self.second):
            copy.wait_send()


def turned_ids(ids_ref):
    ids = ids_ref[...].astype(f32)
    return jnp.transpose(jnp.concatenate([ids] * 4, axis=0)).astype(jnp.int32)


def slot_places(ids, lines, slots):
    rows = ids.shape[0]
    lane = lax.broadcasted_iota(jnp.int32, (rows, 128), 1)
    hot = [lane == column(ids, k) for k in range(2)]
    before = (
        lax.broadcasted_iota(jnp.int32, (rows, rows), 0)
        > lax.broadcasted_iota(jnp.int32, (rows, rows), 1)
    ).astype(bf16)
    named = jnp.where(hot[0] | hot[1], 1.0, 0.0).astype(bf16)
    earlier = jnp.dot(before, named, preferred_element_type=f32)
    slot_at = lax.broadcasted_iota(jnp.int32, (rows, slots), 1).astype(f32)
    place = []
    for k in range(2):
        number = jnp.sum(jnp.where(hot[k], earlier, 0.0), axis=1, keepdims=True)
        wanted = column(ids, k).astype(f32) * CAP + number
        wanted = jnp.where(column(ids, k) < lines, wanted, -1.0)
        place.append(jnp.where(slot_at == wanted, 1.0, 0.0))
    return place


def front(hidden, w_mine, gain, routes, out_grad, docs):
    rows, model = hidden.shape
    lines = lax.axis_size(EX)
    width = model // lines
    shape = jax.ShapeDtypeStruct
    last = lines - 1

    slots = lines * CAP

    def body(hid_ref, w_ref, gain_ref, ids_ref, up_ref, docs_ref, attn_ref, q_ref, kv_ref, place_ref, rows_out, info_ref, land, w_all, kv_own, rows_s, sems):
        line_me = lax.axis_index(EX)
        me, _, _, near, far = shard_peers()
        left, right = jnp.maximum(line_me - 1, 0), jnp.minimum(line_me + 1, last)
        greet(
            [(EX, lax.rem(line_me + d, lines)) for d in range(1, lines)]
            + [(SH, lax.rem(me + d, 4)) for d in range(1, 4)]
        )

        def copy(src, dst, index, axis, peer):
            return pltpu.make_async_remote_copy(
                src_ref=src,
                dst_ref=dst,
                send_sem=sems.at[0, index],
                recv_sem=sems.at[1, index],
                device_id={axis: peer},
                device_id_type=pl.DeviceIdType.MESH,
            )

        def relay(step, way):
            block = line_me - step if way == 0 else line_me + step
            block = jnp.clip(block, 0, last)
            src = hid_ref if step == 0 else land.at[block]
            return copy(src, land.at[block], last * way + step, EX, right if way == 0 else left)

        def sends(step, way):
            if way == 0:
                return (line_me < last) & (line_me - step >= 0)
            return (line_me > 0) & (line_me + step <= last)

        def comes(step, way):
            return line_me - 1 - step >= 0 if way == 0 else line_me + 1 + step <= last

        def source(step, way):
            line = line_me - 1 - step if way == 0 else line_me + 1 + step
            return jnp.clip(line, 0, last)

        def arrival(step, way):
            line = source(step, way)
            return copy(land.at[line], land.at[line], last * way + step, EX, right if way == 0 else left)

        base = 2 * last
        for way in range(2):

            @pl.when(sends(0, way))
            def _():
                relay(0, way).start()

        w_far = copy(w_ref, w_all.at[me], base, SH, far)
        w_near = copy(w_ref, w_all.at[me], base + 1, SH, near)
        w_pass = copy(w_all.at[far], w_all.at[far], base + 2, SH, near)
        w_far.start()
        w_near.start()
        w_all[me] = w_ref[...]
        docs = docs_ref[...]
        lane = lax.broadcasted_iota(jnp.int32, (docs.shape[0], 128), 1)
        block = lax.broadcasted_iota(jnp.int32, (docs.shape[0], 128), 0)
        table = jnp.where(lane == DOCS + block, jnp.broadcast_to(docs[:, 0:1], lane.shape), 0)
        for doc in range(1, DOCS):
            before = jnp.sum(jnp.where(docs < doc, 1, 0), axis=1, keepdims=True)
            table = table + jnp.where(lane == doc, jnp.broadcast_to(before, lane.shape), 0)
        info_ref[...] = jnp.sum(table, axis=0, keepdims=True)
        ids = turned_ids(ids_ref)
        place = slot_places(ids, lines, slots)
        for k in range(2):
            place_ref[k] = place[k].astype(bf16)
        either = (place[0] + place[1]).astype(bf16)
        rows_s[...] = contract(either, up_ref[...], 0, 0).astype(bf16).reshape(lines, CAP, model)
        base += 3
        kv_far = lambda line: copy(kv_own.at[line], kv_ref.at[line, me], base + line, SH, far)
        kv_near = lambda line: copy(
            kv_own.at[line], kv_ref.at[line, me], base + lines + line, SH, near
        )
        kv_pass = lambda line: copy(
            kv_ref.at[line, far], kv_ref.at[line, far], base + 2 * lines + line, SH, near
        )

        def project(line, x):
            inputs = x.astype(f32)
            inv = lax.rsqrt(jnp.mean(inputs * inputs, axis=1, keepdims=True) + norm_eps)
            attn_in = (inputs * inv * gain_ref[...][None]).astype(bf16)
            attn_ref[line] = attn_in
            value = jnp.dot(
                attn_in, w_all[...].reshape(model, 3 * width), preferred_element_type=f32
            ).astype(bf16)
            kv_own[line] = value[:, : 2 * width]
            kv_far(line).start()
            kv_near(line).start()
            kv_ref[line, me] = value[:, : 2 * width]
            q_ref[line] = value[:, 2 * width :]

        def hand(line):
            kv_far(line).wait_recv()
            kv_pass(line).start()

        w_far.wait_recv()
        w_pass.start()
        w_near.wait_recv()
        w_pass.wait_recv()
        project(line_me, hid_ref[...])
        for step in range(last):
            for way in range(2):

                @pl.when(comes(step, way))
                def _():
                    arrival(step, way).wait_recv()

                if step + 1 < last:

                    @pl.when(sends(step + 1, way))
                    def _():
                        relay(step + 1, way).start()

            for way in range(2):

                @pl.when(comes(step, way))
                def _():
                    line = source(step, way)
                    project(line, land[line])

            if step == last - 2:
                first = base + 3 * lines
                ups = []
                for d in range(1, lines):
                    peer = lax.rem(line_me + d, lines)
                    ups.append(copy(rows_s.at[peer], rows_out.at[line_me], first + d - 1, EX, peer))
                    ups[-1].start()
                rows_out[line_me] = rows_s[line_me]
            if step == 0:
                hand(line_me)
            else:
                for way in range(2):

                    @pl.when(comes(step - 1, way))
                    def _():
                        hand(source(step - 1, way))

        for way in range(2):

            @pl.when(comes(last - 1, way))
            def _():
                hand(source(last - 1, way))

        for way in range(2):
            for step in range(last):

                @pl.when(sends(step, way))
                def _():
                    relay(step, way).wait_send()

        w_far.wait_send()
        w_near.wait_send()
        w_pass.wait_send()
        for line in range(lines):
            kv_far(line).wait_send()
            kv_near(line).wait()
            kv_pass(line).wait()
        for up in ups:
            up.wait()

    return pl.pallas_call(
        body,
        out_shape=[
            shape((lines, rows, model), bf16),
            shape((lines, rows, width), bf16),
            shape((lines, 4, rows, 2 * width), bf16),
            shape((2, rows, slots), bf16),
            shape((lines, CAP, model), bf16),
            shape((1, 128), jnp.int32),
        ],
        in_specs=[VM] * 6,
        out_specs=[VM] * 6,
        scratch_shapes=[
            pltpu.VMEM((lines, rows, model), bf16),
            pltpu.VMEM((4, rows, 3 * width), bf16),
            pltpu.VMEM((lines, rows, 2 * width), bf16),
            pltpu.VMEM((lines, CAP, model), bf16),
            pltpu.SemaphoreType.DMA((2, 3 * last + 3 + 3 * lines)),
        ],
        compiler_params=pltpu.CompilerParams(collective_id=0, has_side_effects=True),
        name="front",
    )(hidden, w_mine, gain, routes, out_grad, docs)


def column(x, k):
    return x[:, k : k + 1]


def core_share(go, own, far, out):
    me, _, _, near, other = shard_peers()
    sent = [go(own, out.at[:, me], SH, near), go(far, out.at[:, other], SH, near)]
    out[:, me] = own[...]
    out[:, other] = far[...]
    return sent


def route(heads, hidden, gain, small_w, routes, place, wo, wo_far, n_ids):
    lines, rows, width = heads.shape
    model = lines * width
    slots = lines * CAP
    shape = jax.ShapeDtypeStruct

    def phases(ins, outs, scr, go):
        heads_ref, hid_ref, gain_ref, small_ref, routes_ref, place_ref, wo_ref, wof_ref = ins
        rows_out, wo_all, resid_ref, table_ref, low_ref = outs
        land, rows_s = scr
        swaps = start_swap(go, heads_ref, land, EX, False)
        swaps += core_share(go, wo_ref, wof_ref, wo_all)
        ids = turned_ids(routes_ref)
        lane = lax.broadcasted_iota(jnp.int32, (rows, 128), 1)
        hot = [lane == column(ids, k) for k in range(2)]
        place = [place_ref[k].astype(f32) for k in range(2)]
        either = place_ref[0] + place_ref[1]
        for copy in swaps:
            copy.wait()
        for line in range(lines):
            low_ref[:, line * width : (line + 1) * width] = land[line]
        w_out = wo_all[...].reshape(model, model)
        resid = hid_ref[...].astype(f32) + jnp.dot(
            low_ref[...], w_out, preferred_element_type=f32
        )
        resid_ref[...] = resid
        inv = lax.rsqrt(jnp.mean(resid * resid, axis=1, keepdims=True) + norm_eps)
        moe_in = resid * inv * gain_ref[...][None]
        small = contract(moe_in, small_ref[...], 1, 1, HIGH)
        chosen = [jnp.sum(jnp.where(h, small, 0.0), axis=1, keepdims=True) for h in hot]
        top = jnp.maximum(chosen[0], chosen[1])
        powers = [jnp.exp(c - top) for c in chosen]
        gates = [p / (powers[0] + powers[1]) for p in powers]
        weight = place[0] * gates[0] + place[1] * gates[1]
        weight = contract(weight, jnp.ones((rows, 128), f32), 0, 0, HIGH)[:, 0:1]
        high = weight.astype(bf16)
        low = (weight - high.astype(f32)).astype(bf16)
        slot_lane = lax.broadcasted_iota(jnp.int32, (slots, 128), 1)
        extra = jnp.where(slot_lane == 0, high, jnp.where(slot_lane == 1, low, jnp.zeros_like(low)))
        rows_s[:, :, :model] = (
            contract(either, moe_in.astype(bf16), 0, 0).astype(bf16).reshape(lines, CAP, model)
        )
        rows_s[:, :, model:] = extra.reshape(lines, CAP, 128)
        row_swap = start_swap(go, rows_s, rows_out, EX, False)
        table = jnp.zeros((rows, 128), f32)
        entries = list(gates)
        for j in range(2):
            pair = [column(small, n_ids + 2 * j + k) for k in range(2)]
            top = jnp.maximum(pair[0], pair[1])
            powers = [jnp.exp(c - top) for c in pair]
            entries += [p / (powers[0] + powers[1]) for p in powers]
        entries += [column(ids, k).astype(f32) for k in range(2)]
        for k, entry in enumerate(entries):
            table = jnp.where(lane == k, entry, table)
        table_ref[...] = table
        for copy in row_swap:
            copy.wait()
        yield

    ins = [heads, hidden, gain, small_w, routes, place, wo, wo_far]
    outs = [
        shape((lines, CAP, model + 128), bf16),
        shape((1, 4, model // 4, model), bf16),
        shape((rows, model), f32),
        shape((rows, 128), f32),
        shape((rows, model), bf16),
    ]
    scratch = [
        pltpu.VMEM((lines, rows, width), bf16),
        pltpu.VMEM((lines, CAP, model + 128), bf16),
    ]
    return Part([EX, SH], ins, outs, scratch, 2 * (lines - 1) + 2, phases)


def share_weights(own, far):
    def phases(ins, outs, scr, go):
        copies = core_share(go, ins[0], ins[1], outs[0])
        yield
        for copy in copies:
            copy.wait()

    dims = (own.shape[0], 4) + own.shape[1:]
    return Part([SH], [own, far], [jax.ShapeDtypeStruct(dims, bf16)], [], 2, phases)


def to_heads(returned, input_ret, place, table, resid, low, out_grad, gain, small_t, const_vec, wo, n_ids):
    rows, model = resid.shape
    lines = returned.shape[0]
    width = model // lines
    own = rows // lines
    slots = lines * CAP
    shape = jax.ShapeDtypeStruct

    def phases(ins, outs, scr, go):
        ret_ref, iret_ref, place_ref, table_ref, resid_ref, low_ref, up_ref, gain_ref, st_ref, vec_ref, wo_ref = ins
        heads_out, layer_ref, rgrad_ref, term_ref, packed_ref = outs
        (back_s,) = scr
        table = table_ref[...]
        gates = [column(table, k) for k in range(2)]
        alpha = [[column(table, 2 + 2 * j + k) for k in range(2)] for j in range(2)]
        ids = [column(table, 6 + k) for k in range(2)]
        vecs = [vec_ref[j : j + 1, :] for j in range(2)]
        resid = resid_ref[...]
        upstream = up_ref[...].astype(f32)
        inv = lax.rsqrt(jnp.mean(resid * resid, axis=1, keepdims=True) + norm_eps)
        normed = resid * inv
        moe_in = normed * gain_ref[...][None]
        returned = ret_ref[...].reshape(slots, model)
        total = lambda x: jnp.sum(x, axis=1, keepdims=True)
        flag = lambda x: jnp.where(x, 1.0, 0.0)
        copy_dot = total(upstream * moe_in)
        vec_dot = [total(upstream * v) for v in vecs]
        const_dot = [alpha[j][0] * copy_dot + alpha[j][1] * vec_dot[j] for j in range(2)]
        output = resid
        backs = []
        copy_gate = jnp.zeros((rows, 1), f32)
        const_gate = [jnp.zeros((rows, 1), f32) for _ in range(2)]
        for k in range(2):
            rows_k = jnp.dot(place_ref[k], returned, preferred_element_type=f32)
            is_ffn, is_copy = flag(ids[k] < lines), flag(ids[k] == lines + 1)
            is_const = [flag(ids[k] == lines + 2 + j) for j in range(2)]
            output = output + (gates[k] * is_ffn) * rows_k
            backs.append(
                is_ffn * total(upstream * rows_k)
                + is_copy * copy_dot
                + is_const[0] * const_dot[0]
                + is_const[1] * const_dot[1]
            )
            copy_gate = copy_gate + gates[k] * is_copy
            const_gate = [const_gate[j] + gates[k] * is_const[j] for j in range(2)]
        through = copy_gate + const_gate[0] * alpha[0][0] + const_gate[1] * alpha[1][0]
        output = output + through * moe_in
        for j in range(2):
            output = output + (const_gate[j] * alpha[j][1]) * vecs[j]
        layer_ref[...] = output.astype(bf16)
        mean_back = gates[0] * backs[0] + gates[1] * backs[1]
        lane = lax.broadcasted_iota(jnp.int32, (rows, 128), 1)
        lane_f = lane.astype(f32)
        small = jnp.zeros((rows, 128), f32)
        for k in range(2):
            small = jnp.where(lane_f == ids[k], gates[k] * (backs[k] - mean_back), small)
        for j in range(2):
            grads = [const_gate[j] * copy_dot, const_gate[j] * vec_dot[j]]
            mean = alpha[j][0] * grads[0] + alpha[j][1] * grads[1]
            for k in range(2):
                small = jnp.where(
                    lane == n_ids + 2 * j + k, alpha[j][k] * (grads[k] - mean), small
                )
            small = jnp.where(lane == n_ids + 4 + j, alpha[j][1] * const_gate[j], small)
        either = place_ref[0] + place_ref[1]
        moe_grad = (
            jnp.dot(either, iret_ref[...].reshape(slots, model), preferred_element_type=f32)
            + through * upstream
            + jnp.dot(small, st_ref[...], preferred_element_type=f32, precision=HIGH)
        )
        resid_grad = upstream + rms_back(resid, inv, gain_ref[...][None], moe_grad)
        branch = resid_grad.astype(bf16)
        back = contract(branch, wo_ref[...], 1, 1).astype(bf16)
        for line in range(lines):
            back_s[line] = back[:, line * width : (line + 1) * width]
        swaps = start_swap(go, back_s, heads_out, EX, False)
        rgrad_ref[...] = resid_grad
        packed_ref[...] = jnp.zeros_like(packed_ref)
        packed_ref[0:1] = jnp.sum(moe_grad * normed, axis=0, keepdims=True)
        small_grad = contract(small, moe_in, 0, 0, HIGH)
        vec_grad = contract(small, upstream, 0, 0, HIGH)
        packed_ref[1:3] = vec_grad[n_ids + 4 : n_ids + 6]
        packed_ref[3 : 7 + n_ids] = small_grad[: n_ids + 4]
        term = contract(low_ref[...], branch, 0, 0).astype(bf16)
        for line in range(lines):
            for piece in range(4):
                at = (line * 4 + piece) * own
                term_ref[piece, line] = term[at : at + own]
        for copy in swaps:
            copy.wait()
        yield

    ins = [returned, input_ret, place, table, resid, low, out_grad, gain, small_t, const_vec, wo]
    outs = [
        shape((lines, rows, width), bf16),
        shape((rows, model), bf16),
        shape((rows, model), f32),
        shape((4, lines, own, model), bf16),
        shape((-(-(7 + n_ids) // 8) * 8, model), f32),
    ]
    return Part([EX], ins, outs, [pltpu.VMEM((lines, rows, width), bf16)], lines - 1, phases)


def tail(dkv, dq, attn_in, weights, out_term, packed, hidden, resid_grad, gain, pairs):
    lines, rows, width = dq.shape
    model = lines * width
    own = rows // lines
    groups = lax.axis_size(GR)
    shape = jax.ShapeDtypeStruct
    vmem = pltpu.VMEM
    tok = lines * rows
    few = lines // 2
    dkv_piece, q_piece = (few, rows, 2 * width), (lines, own, width)
    kv_piece, o_piece = (lines, own, 2 * width), (lines, own, model)
    part_dims = (width, 2 * width, model)

    def phases(ins, outs, scr, go):
        lo_ref, hi_ref, dq_ref, attn_ref, w_ref, wf_ref, o_ref, packed_ref, hid_ref, resid_ref, gain_ref = ins[:11]
        input_ref, q_out, kv_out, out_out, packed_out, gain_out = outs[:6]
        scr = list(scr)
        take = lambda k: [scr.pop(0) for _ in range(k)]
        lo_scr, hi_scr, q_scr, kvw_scr, o_scr = take(3), take(3), take(3), take(3), take(3)
        own_kv, q_t, kv_t, dq_all, dkv_all, dq_full = take(6)
        kv_sems, w_s, w_sem, turned = take(4)
        held = take(2 * len(pairs))
        me, _, _, near, far = shard_peers()
        w_copies = [
            pltpu.make_async_copy(ref, w_s.at[:, at], w_sem.at[2 * len(pairs) + k])
            for k, (ref, at) in enumerate(((w_ref, me), (wf_ref, far)))
        ]
        fetch = [
            pltpu.make_async_copy(ins[11 + k], held[k], w_sem.at[k]) for k in range(2 * len(pairs))
        ]
        for copy in fetch:
            copy.start()
        for copy in w_copies:
            copy.start()
        sums, lands, halves, gots = take(3), take(3), take(3), take(3)
        pk_l, pk_s, pk_g = take(3)
        mid_l, mid_s = take(2)
        gn_l, gn_s, gn_g, gn_0, gn_1, gn_2 = take(6)
        me = lax.axis_index(SH)

        line_me, group_me = lax.axis_index(EX), lax.axis_index(GR)
        kv_trees = [Tree(lo_ref, lo_scr, go), Tree(hi_ref, hi_scr, go)]

        def kv_copy(sender, target):
            return pltpu.make_async_remote_copy(
                src_ref=own_kv.at[target],
                dst_ref=dkv_all.at[sender],
                send_sem=kv_sems.at[0, target],
                recv_sem=kv_sems.at[1, sender],
                device_id={EX: target},
                device_id_type=pl.DeviceIdType.MESH,
            )

        def push_kv(k):
            own_kv[k * few : (k + 1) * few] = kv_trees[k].result().astype(bf16)
            for target in range(k * few, (k + 1) * few):

                @pl.when(line_me != target)
                def _():
                    kv_copy(line_me, jnp.int32(target)).start()

                @pl.when(line_me == target)
                def _():
                    dkv_all[target] = own_kv[target]

        dq_swap = start_swap(go, dq_ref, dq_all, EX, False)
        o_tree = Tree(o_ref, o_scr, go)
        pk1 = start_swap(go, packed_ref, pk_l, EX, True)
        def term(rows_ref, out):
            value = jnp.dot(
                turned[...],
                rows_ref[...].reshape(tok, rows_ref.shape[-1]),
                preferred_element_type=f32,
            ).astype(bf16)
            for line in range(lines):
                for piece in range(4):
                    at = (line * 4 + piece) * own
                    out[piece, line] = value[at : at + own]

        for tree in kv_trees:
            tree.across()
        wide = []
        for k in range(len(pairs)):
            mine, other = outs[6 + 2 * k : 8 + 2 * k]
            here, there = held[2 * k : 2 * k + 2]
            fetch[2 * k].wait()
            fetch[2 * k + 1].wait()
            mine[...] = (here[...].astype(f32) + there[...].astype(f32)).astype(bf16)
            wide.append(go(mine, other, GR, lax.rem(group_me + 1, groups)))
        w_copies.append(go(w_ref, w_s.at[:, me], SH, near))
        w_copies.append(go(wf_ref, w_s.at[:, far], SH, near))
        turned[...] = jnp.transpose(attn_ref[...])
        term(dq_ref, q_t)
        o_tree.across()
        q_tree = Tree(q_t, q_scr, go)
        trees = [q_tree, None, o_tree]

        def lines_out(k):
            sums[k][...] = trees[k].result().astype(bf16)
            return start_swap(go, sums[k], lands[k], EX, False)

        push_kv(0)
        q_tree.across()
        push_kv(1)
        term(own_kv, kv_t)
        kvw_tree = Tree(kv_t, kvw_scr, go)
        trees[1] = kvw_tree
        o_lines = lines_out(2)
        for copy in pk1:
            copy.wait()
        mid_l[...] = total_of(pk_l, lines)
        pk2 = start_swap(go, mid_l, pk_s, SH, True)
        kvw_tree.across()
        q_lines = lines_out(0)
        for copy in dq_swap:
            copy.wait()
        for line in range(lines):
            dq_full[:, line * width : (line + 1) * width] = dq_all[line]
        for copy in w_copies:
            copy.wait()
        grad = contract(dq_full[...], w_s[0].reshape(model, model), 1, 1)
        for copy in pk2:
            copy.wait()
        mid_s[...] = total_of(pk_s, 4)
        pk3 = start_swap(go, mid_s, pk_g, GR, True)
        kv_lines = lines_out(1)
        for other in range(lines):

            @pl.when(line_me != other)
            def _():
                kv_copy(jnp.int32(other), line_me).wait_recv()
                kv_copy(line_me, jnp.int32(other)).wait_send()

        for half in range(2):
            for line in range(lines):
                dq_full[:, line * width : (line + 1) * width] = dkv_all[
                    line, :, half * width : (half + 1) * width
                ]
            grad = grad + contract(dq_full[...], w_s[1 + half].reshape(model, model), 1, 1)
        inputs = hid_ref[...].astype(f32)
        inv = lax.rsqrt(jnp.mean(inputs * inputs, axis=1, keepdims=True) + norm_eps)
        normed = inputs * inv
        gn_0[...] = jnp.sum(grad * normed, axis=0, keepdims=True)
        gn1 = start_swap(go, gn_0, gn_l, EX, True)
        input_ref[...] = resid_ref[...] + rms_back(inputs, inv, gain_ref[...][None], grad)
        swaps = [None] * 3
        for k, copies in ((2, o_lines), (0, q_lines)):
            for copy in copies:
                copy.wait()
            if k == 2:
                halves[k][...] = total_of(lands[k], lines).astype(bf16)
            else:
                halves[k][...] = lands[k][...]
            swaps[k] = start_swap(go, halves[k], gots[k], GR, True)
        for copy in gn1:
            copy.wait()
        gn_1[...] = total_of(gn_l, lines)
        gn2 = start_swap(go, gn_1, gn_s, SH, True)
        for copy in kv_lines:
            copy.wait()
        halves[1][...] = lands[1][...]
        swaps[1] = start_swap(go, halves[1], gots[1], GR, True)
        for copy in gn2:
            copy.wait()
        gn_2[...] = total_of(gn_s, 4)
        gn3 = start_swap(go, gn_2, gn_g, GR, True)
        for copy in pk3:
            copy.wait()
        packed_out[...] = total_of(pk_g, groups)
        for k, out in ((2, out_out), (0, q_out), (1, kv_out)):
            for copy in swaps[k]:
                copy.wait()
            out[...] = total_of(gots[k], groups)
        for copy in gn3:
            copy.wait()
        gain_out[...] = total_of(gn_g, groups)
        for copy in wide:
            copy.wait()
        for tree in (*kv_trees, o_tree, q_tree, kvw_tree):
            tree.close()
        yield

    pieces = [(lines, own, d) for d in part_dims]
    got_pieces = pieces[:2] + [(own, model)]
    scratch = Tree.scratch(dkv_piece) * 2 + Tree.scratch(q_piece) + Tree.scratch(kv_piece)
    scratch += Tree.scratch(o_piece)
    scratch += [
        vmem((lines, rows, 2 * width), bf16),
        vmem((4,) + q_piece, bf16),
        vmem((4,) + kv_piece, bf16),
        vmem((lines, rows, width), bf16),
        vmem((lines, rows, 2 * width), bf16),
        vmem((rows, model), bf16),
        pltpu.SemaphoreType.DMA((2, lines)),
        vmem((3, 4) + weights[0].shape[1:], bf16),
        pltpu.SemaphoreType.DMA((2 * len(pairs) + 2,)),
        vmem((model, tok), bf16),
    ]
    scratch += [vmem(x.shape, bf16) for pair in pairs for x in pair]
    scratch += [vmem(p, bf16) for p in pieces] + [vmem(p, bf16) for p in pieces]
    scratch += [vmem(p, bf16) for p in got_pieces] + [vmem((groups,) + p, bf16) for p in got_pieces]
    scratch += [vmem((n,) + packed.shape, f32) for n in (lines, 4, groups)]
    scratch += [vmem(packed.shape, f32)] * 2
    scratch += [vmem((n, 1, model), f32) for n in (lines, 4, groups)] + [vmem((1, model), f32)] * 3
    copies = 2 + len(pairs) + 5 * Tree.copies + 6 * (lines - 1) + 2 * 3 + 5 * (groups - 1)
    outs = [
        shape((rows, model), f32),
        shape((lines, own, width), f32),
        shape((lines, own, 2 * width), f32),
        shape((own, model), f32),
        shape(packed.shape, f32),
        shape((1, model), f32),
    ] + [shape(x.shape, bf16) for pair in pairs for x in pair]
    ins = [*dkv, dq, attn_in, *weights, out_term, packed, hidden, resid_grad, gain]
    ins += [x for pair in pairs for x in pair]
    hbm = pl.BlockSpec(memory_space=pl.ANY)
    specs = [hbm if k in (4, 5) or k >= 11 else VM for k in range(len(ins))]
    return Part([EX, SH, GR], ins, outs, scratch, copies, phases, specs)


def expert_body(steps, x_ref, g_ref, wg_ref, wu_ref, wd_ref, eo_ref, ib_ref, ga_ref, up_ref, d_ref, eo_s, ib_s, g_s, xt_s):
    i = pl.program_id(0)
    me, side, core, _, _ = shard_peers()

    @pl.when(i == 0)
    def _():
        eo_s[...] = jnp.zeros_like(eo_s)
        ib_s[...] = jnp.zeros_like(ib_s)
        model = g_ref.shape[1]
        high, low = x_ref[:, model : model + 1], x_ref[:, model + 1 : model + 2]
        gate = high.astype(f32) + low.astype(f32)
        g_s[...] = (g_ref[...].astype(f32) * gate).astype(bf16)
        xt_s[...] = jnp.transpose(x_ref[:, :model])

    x, g = x_ref[:, : g_ref.shape[1]], g_s[...]
    wg, wu, wd = wg_ref[...], wu_ref[...], wd_ref[...]
    gate_pre = jnp.dot(x, wg, preferred_element_type=f32)
    up_pre = jnp.dot(x, wu, preferred_element_type=f32)
    hidden_grad = contract(g, wd, 1, 1)
    gate_sigmoid = jax.nn.sigmoid(gate_pre)
    act = (gate_pre * gate_sigmoid * up_pre).astype(bf16)
    gate_back = (
        hidden_grad * up_pre * gate_sigmoid * (1.0 + gate_pre * (1.0 - gate_sigmoid))
    ).astype(bf16)
    up_back = (hidden_grad * gate_pre * gate_sigmoid).astype(bf16)
    eo_s[...] += jnp.dot(act, wd, preferred_element_type=f32)
    ib_s[...] += contract(gate_back, wg, 1, 1) + contract(up_back, wu, 1, 1)

    def place(quarter):
        return 2 * lax.rem(lax.rem(quarter, 2) + core, 2) + lax.rem(quarter // 2 + side, 2)

    rows = ga_ref.shape[1]
    for ref, back in ((ga_ref, gate_back), (up_ref, up_back)):
        term = jnp.dot(xt_s[...], back, preferred_element_type=f32).astype(bf16)
        for quarter in range(4):
            ref[place(jnp.int32(quarter))] = term[quarter * rows : (quarter + 1) * rows]
    d_ref[place(i)] = contract(act, g, 0, 0).astype(bf16)

    @pl.when(i == steps - 1)
    def _():
        eo_ref[...] = eo_s[...].astype(bf16)
        ib_ref[...] = ib_s[...].astype(bf16)


def expert(x, g, wg, wu, wd):
    slots, model = g.shape
    inner = wg.shape[1]
    steps = 4
    tile = inner // steps
    quarter = model // 4
    shape = jax.ShapeDtypeStruct
    whole = lambda dims: pl.BlockSpec(dims, lambda i: (0,) * len(dims))
    return pl.pallas_call(
        functools.partial(expert_body, steps),
        grid=(steps,),
        out_shape=[
            shape((slots, model), bf16),
            shape((slots, model), bf16),
            shape((4, quarter, inner), bf16),
            shape((4, quarter, inner), bf16),
            shape((4, tile, model), bf16),
        ],
        in_specs=[
            whole(x.shape),
            whole((slots, model)),
            pl.BlockSpec((model, tile), lambda i: (0, i)),
            pl.BlockSpec((model, tile), lambda i: (0, i)),
            pl.BlockSpec((tile, model), lambda i: (i, 0)),
        ],
        out_specs=[
            whole((slots, model)),
            whole((slots, model)),
            pl.BlockSpec((4, quarter, tile), lambda i: (0, 0, i)),
            pl.BlockSpec((4, quarter, tile), lambda i: (0, 0, i)),
            whole((4, tile, model)),
        ],
        scratch_shapes=[pltpu.VMEM((slots, model), f32)] * 2 + [pltpu.VMEM((slots, model), bf16), pltpu.VMEM((model, slots), bf16)],
        cost_estimate=pl.CostEstimate(flops=6 * 10**9, bytes_accessed=2 * 10**7, transcendentals=4 * 10**5),
        name="ffn",
    )(x, g, wg, wu, wd)


def head_columns(h, shape, axis):
    return lax.broadcasted_iota(jnp.int32, shape, axis) // HEAD_DIM == h


def allowed(block, key_blk, qpos, qstart, prompt):
    kpos = block * key_blk + lax.broadcasted_iota(jnp.int32, (key_blk, qpos.shape[1]), 0)
    return (kpos <= qpos) & ((kpos >= qstart) | (kpos < prompt))


def doc_start(block, info_ref, qinfo_ref):
    docs = qinfo_ref[pl.ds(block, 1), :]
    starts = jnp.zeros(docs.shape, jnp.int32)
    for doc in range(1, DOCS):
        starts = jnp.where(docs == doc, info_ref[0, doc], starts)
    return starts, info_ref[0, info_ref[0, DOCS + block]]


def attend_body(lines, heads, info_ref, q_ref, kv_ref, qinfo_ref, o_ref, low_ref, lse_ref, k_s, vt_s, acc_s, ml_s, qm_s):
    shard = lax.axis_index(SH)
    rows, width = q_ref.shape[1:]
    blocks = vt_s.shape[0]
    key_blk = vt_s.shape[2]
    prompt = info_ref[0, 1]

    @pl.loop(0, blocks)
    def _(j):
        at = pl.ds(pl.multiple_of(j * key_blk, key_blk), key_blk)
        k_s[at, :] = kv_ref[at, :width]
        vt_s[j] = jnp.transpose(kv_ref[at, width:].astype(f32)).astype(bf16)

    @pl.loop(0, lines)
    def _(line):
        start = (line * 4 + shard) * rows
        queries = q_ref[line].astype(f32) * HEAD_DIM**-0.5
        qpos = start + lax.broadcasted_iota(jnp.int32, (1, rows), 1)
        qstart, first = doc_start(line * 4 + shard, info_ref, qinfo_ref)
        for h in range(heads):
            qm_s[h] = jnp.where(head_columns(h, queries.shape, 1), queries, 0.0).astype(bf16)
        acc_s[...] = jnp.zeros_like(acc_s)
        for h in range(heads):
            ml_s[h, 0:1, :] = jnp.full((1, rows), neg_fill, f32)
            ml_s[h, 1:2, :] = jnp.zeros((1, rows), f32)

        @pl.loop(0, (start + rows + key_blk - 1) // key_blk)
        def _(j):
            @pl.when((j * key_blk < prompt) | ((j + 1) * key_blk > first))
            def _():
                keys = k_s[pl.ds(pl.multiple_of(j * key_blk, key_blk), key_blk), :]
                ok = allowed(j, key_blk, qpos, qstart, prompt)
                for h in range(heads):
                    scores = jnp.where(ok, contract(keys, qm_s[h], 1, 1), neg_fill)
                    old = ml_s[h, 0:1, :]
                    new = jnp.maximum(old, jnp.max(scores, axis=0, keepdims=True))
                    probs = jnp.exp(scores - new)
                    scale = jnp.exp(old - new)
                    ml_s[h, 0:1, :] = new
                    ml_s[h, 1:2, :] = ml_s[h, 1:2, :] * scale + jnp.sum(
                        probs, axis=0, keepdims=True
                    )
                    part = slice(h * HEAD_DIM, (h + 1) * HEAD_DIM)
                    acc_s[part, :] = acc_s[part, :] * scale + jnp.dot(
                        vt_s[j, part, :], probs.astype(bf16), preferred_element_type=f32
                    )

        for h in range(heads):
            part = slice(h * HEAD_DIM, (h + 1) * HEAD_DIM)
            total = ml_s[h, 1:2, :]
            acc_s[part, :] = acc_s[part, :] / total
            lse_ref[line, h : h + 1, :] = ml_s[h, 0:1, :] + jnp.log(total)
        result = jnp.transpose(acc_s[...])
        o_ref[line] = result
        low_ref[line] = result.astype(bf16)


def attend(info, q, kv, qinfo):
    lines, rows, width = q.shape
    heads = width // HEAD_DIM
    length = kv.shape[0]
    key_blk = KEY_BLK
    shape = jax.ShapeDtypeStruct
    return pl.pallas_call(
        functools.partial(attend_body, lines, heads),
        out_shape=[
            shape((lines, rows, width), f32),
            shape((lines, rows, width), bf16),
            shape((lines, 8, rows), f32),
        ],
        in_specs=[SM, VM, VM, VM],
        out_specs=[VM] * 3,
        scratch_shapes=[
            pltpu.VMEM((length, width), bf16),
            pltpu.VMEM((length // key_blk, width, key_blk), bf16),
            pltpu.VMEM((width, rows), f32),
            pltpu.VMEM((heads, 8, rows), f32),
            pltpu.VMEM((heads, rows, width), bf16),
        ],
        cost_estimate=pl.CostEstimate(flops=2 * 10**9, bytes_accessed=8 * 10**6, transcendentals=4 * 10**6),
        name="attend",
    )(info, q, kv, qinfo)


def attend_back_body(lines, heads, info_ref, q_ref, kv_ref, qinfo_ref, o_ref, lse_ref, back_ref, dq_ref, dkv_lo, dkv_hi, k_s, v_s, dk_s, dv_s, dq_s, qm_s, bm_s, delta_s):
    shard = lax.axis_index(SH)
    rows, width = q_ref.shape[1:]
    key_blk = KEY_BACK
    blocks = k_s.shape[0] // key_blk
    prompt = info_ref[0, 1]

    @pl.loop(0, blocks)
    def _(j):
        at = pl.ds(pl.multiple_of(j * key_blk, key_blk), key_blk)
        k_s[at, :] = kv_ref[at, :width]
        v_s[at, :] = kv_ref[at, width:]
        dk_s[at, :] = jnp.zeros((key_blk, width), f32)
        dv_s[at, :] = jnp.zeros((key_blk, width), f32)

    @pl.loop(0, lines)
    def _(line):
        start = (line * 4 + shard) * rows
        queries = q_ref[line].astype(f32) * HEAD_DIM**-0.5
        back = back_ref[line].astype(f32)
        qpos = start + lax.broadcasted_iota(jnp.int32, (1, rows), 1)
        qstart, first = doc_start(line * 4 + shard, info_ref, qinfo_ref)
        picks = (
            lax.broadcasted_iota(jnp.int32, (8, width), 1) // HEAD_DIM
            == lax.broadcasted_iota(jnp.int32, (8, width), 0)
        ).astype(f32)
        delta_s[...] = contract(picks, back * o_ref[line], 1, 1, HIGH)
        for h in range(heads):
            mine = head_columns(h, queries.shape, 1)
            qm_s[h] = jnp.where(mine, queries, 0.0).astype(bf16)
            bm_s[h] = jnp.where(mine, back, 0.0).astype(bf16)
        dq_s[...] = jnp.zeros_like(dq_s)

        @pl.loop(0, (start + rows + key_blk - 1) // key_blk)
        def _(j):
            @pl.when((j * key_blk < prompt) | ((j + 1) * key_blk > first))
            def _():
                at = pl.ds(pl.multiple_of(j * key_blk, key_blk), key_blk)
                keys, values = k_s[at, :], v_s[at, :]
                ok = allowed(j, key_blk, qpos, qstart, prompt)
                dk = jnp.zeros((key_blk, width), f32)
                dv = jnp.zeros((key_blk, width), f32)
                for h in range(heads):
                    scores = contract(keys, qm_s[h], 1, 1)
                    probs = jnp.where(ok, jnp.exp(scores - lse_ref[line, h : h + 1, :]), 0.0)
                    grads = contract(values, bm_s[h], 1, 1)
                    slow = (probs * (grads - delta_s[h : h + 1, :])).astype(bf16)
                    dv = dv + jnp.dot(probs.astype(bf16), bm_s[h], preferred_element_type=f32)
                    dk = dk + jnp.dot(slow, qm_s[h], preferred_element_type=f32)
                    dq_s[h] += contract(slow, keys, 0, 0)
                dk_s[at, :] += dk
                dv_s[at, :] += dv

        total = jnp.zeros(queries.shape, f32)
        for h in range(heads):
            total = jnp.where(head_columns(h, queries.shape, 1), dq_s[h], total)
        dq_ref[line] = (total * HEAD_DIM**-0.5).astype(bf16)

    half = lines // 2
    for k, ref in enumerate((dkv_lo, dkv_hi)):

        @pl.loop(0, half)
        def _(line):
            for piece in range(4):
                at = ((k * half + line) * 4 + piece) * rows
                at = pl.ds(pl.multiple_of(at, rows), rows)
                ref[piece, line, :, :width] = dk_s[at, :].astype(bf16)
                ref[piece, line, :, width:] = dv_s[at, :].astype(bf16)


def attend_back(info, q, kv, qinfo, o, lse, back):
    lines, rows, width = q.shape
    heads = width // HEAD_DIM
    length = kv.shape[0]
    shape = jax.ShapeDtypeStruct
    return pl.pallas_call(
        functools.partial(attend_back_body, lines, heads),
        out_shape=[
            shape((lines, rows, width), bf16),
            shape((4, lines // 2, rows, 2 * width), bf16),
            shape((4, lines // 2, rows, 2 * width), bf16),
        ],
        in_specs=[SM] + [VM] * 6,
        out_specs=[VM] * 3,
        scratch_shapes=[
            pltpu.VMEM((length, width), bf16),
            pltpu.VMEM((length, width), bf16),
            pltpu.VMEM((length, width), f32),
            pltpu.VMEM((length, width), f32),
            pltpu.VMEM((heads, rows, width), f32),
            pltpu.VMEM((heads, rows, width), bf16),
            pltpu.VMEM((heads, rows, width), bf16),
            pltpu.VMEM((8, rows), f32),
        ],
        cost_estimate=pl.CostEstimate(flops=5 * 10**9, bytes_accessed=12 * 10**6, transcendentals=4 * 10**6),
        name="attend_back",
    )(info, q, kv, qinfo, o, lse, back)


def finale_body(lines, n_ids, *refs):
    ins, outs = refs[:13], refs[13:]
    for k in range(3):
        outs[k][...] = ins[k][...].astype(f32) + ins[3 + k][...].astype(f32)
    for k in range(2):
        outs[3 + k][...] = ins[6 + k][...]

    @pl.when(pl.program_id(0) == 0)
    def _():
        q_sum, kv_sum, out_sum, small_ref, gain_ref = ins[8:]
        q_out, k_out, v_out, out_out, gain_out, mgain_out, vec_out, rout_out, mix_out = outs[5:]
        width = q_sum.shape[2]
        for line in range(lines):
            at = slice(line * width, (line + 1) * width)
            q_out[:, at] = q_sum[line]
            k_out[:, at] = kv_sum[line, :, :width]
            v_out[:, at] = kv_sum[line, :, width:]
        out_out[...] = out_sum[...]
        gain_out[...] = jnp.sum(gain_ref[...], axis=0)
        small = small_ref[...]
        mgain_out[...] = jnp.sum(small[0:1], axis=0)
        vec_out[...] = small[1:3]
        rout_out[...] = small[3 : 3 + n_ids]
        mix_out[...] = small[3 + n_ids : 7 + n_ids]


def finale(mine, far, input_grad, layer_out, sums, n_ids):
    steps = 4
    shape = jax.ShapeDtypeStruct
    own, model = sums[2].shape
    lines = sums[0].shape[0]

    def tiled(dims, dim):
        block = tuple(d // steps if k == dim else d for k, d in enumerate(dims))
        return pl.BlockSpec(block, lambda i: tuple(i if k == dim else 0 for k in range(2)))

    def whole(dims):
        return pl.BlockSpec(dims, lambda i: (0,) * len(dims))

    wide = [tiled(mine[0].shape, 1), tiled(mine[1].shape, 1), tiled(mine[2].shape, 0)]
    rows = [tiled(input_grad.shape, 0), tiled(layer_out.shape, 0)]
    small = [(own, model)] * 4 + [(model,), (model,), (2, model), (n_ids, model), (4, model)]
    return pl.pallas_call(
        functools.partial(finale_body, lines, n_ids),
        grid=(steps,),
        out_shape=[shape(m.shape, f32) for m in mine]
        + [shape(input_grad.shape, f32), shape(layer_out.shape, bf16)]
        + [shape(d, f32) for d in small],
        in_specs=wide + wide + rows + [whole(x.shape) for x in sums],
        out_specs=wide + rows + [whole(d) for d in small],
        cost_estimate=pl.CostEstimate(flops=10**7, bytes_accessed=10**7, transcendentals=0),
        name="finale",
    )(*mine, *far, input_grad, layer_out, *sums)


def swap(x, axis, partner):
    return lax.ppermute(x, axis, [(i, partner(i)) for i in range(lax.axis_size(axis))])


def fast_shards(
    hidden_in,
    segment_ids,
    routes,
    attn_gain,
    w_query,
    w_key,
    w_value,
    w_out,
    moe_gain,
    w_router,
    const_mix,
    const_vec,
    w_gate,
    w_up,
    w_down,
    out_grad,
):
    rows, model = hidden_in.shape
    lines = lax.axis_size(EX)
    line, shard = lax.axis_index(EX), lax.axis_index(SH)
    width = model // lines
    length = segment_ids.shape[1]

    w_qkv = jnp.stack([w_query, w_key, w_value])
    w_mine = lax.dynamic_slice_in_dim(w_qkv, line * width, width, axis=2)
    w_mine = jnp.concatenate([w_mine[1], w_mine[2], w_mine[0]], axis=1)
    qinfo = segment_ids.reshape(length // rows, rows)
    attn_in, q, kv_all, place, recv_grads, info = front(
        hidden_in, w_mine, attn_gain, routes.T, out_grad, qinfo
    )
    attn_in = attn_in.reshape(lines * rows, model)
    kv_all, w_out_b = lax.optimization_barrier((kv_all, w_out))
    wo_far = swap(w_out_b, SH, lambda i: i ^ 2)
    kv_all = kv_all.reshape(length, 2 * width)
    attn_vec, attn_heads, lse = attend(info, q, kv_all, qinfo)
    attn_heads, w_qkv, wo_far = lax.optimization_barrier((attn_heads, w_qkv, wo_far))
    w_far = swap(w_qkv, SH, lambda i: i ^ 2)
    n_ids = w_router.shape[1]
    small_t = jnp.pad(
        jnp.concatenate([w_router.T, const_mix.T], axis=0), ((0, 124 - n_ids), (0, 0))
    )
    gain_two = moe_gain
    recv_rows, wo_full, resid_one, table, attn_low = run_parts(
        [
            route(
                attn_heads, hidden_in, gain_two, small_t, routes.T, place, w_out[None], wo_far[None], n_ids
            )
        ],
        2,
        "route",
    )
    wo_full = wo_full.reshape(model, model)
    recv_rows, w_far = lax.optimization_barrier((recv_rows, w_far))
    slots = lines * CAP

    expert_out, input_back, *terms = expert(
        recv_rows.reshape(slots, model + 128), recv_grads.reshape(slots, model), w_gate[0], w_up[0], w_down[0]
    )
    returned, input_ret, *sums = run_parts(
        [
            exchange(EX, SWAP, expert_out.reshape(lines, CAP, model)),
            exchange(EX, SWAP, input_back.reshape(lines, CAP, model)),
        ]
        + [core_sum(term) for term in terms],
        4,
        "combine",
    )
    far = [swap(there, SH, lambda i: i ^ 2) for there in sums[1::2]]
    down = (sums[4].astype(f32) + far[2].astype(f32)).astype(bf16)

    back_heads, layer_out, resid_grad, out_term, packed = run_parts(
        [
            to_heads(
                returned, input_ret, place, table, resid_one, attn_low, out_grad, gain_two, small_t, const_vec, wo_full, n_ids
            )
        ],
        5,
        "to_heads",
    )
    back_heads, down = lax.optimization_barrier((back_heads, down))
    cross = lambda x: swap(x, GR, lambda i: 1 - i)
    down_far = cross(down)
    dq, *dkv = attend_back(info, q, kv_all, qinfo, attn_vec, lse, back_heads)
    pairs = [(sums[0], far[0]), (sums[2], far[1])]
    input_grad, *parts = run_parts(
        [
            tail(
                dkv, dq, attn_in, (w_qkv, w_far), out_term, packed, hidden_in, resid_grad, attn_gain, pairs
            )
        ],
        6,
        "tail",
        pl.CostEstimate(flops=2 * 10**10, bytes_accessed=10**8, transcendentals=0),
    )
    gate, up, down, input_grad, layer_out, *grads, gain, gain_two, vecs, router, mix = finale(
        [parts[5], parts[7], down],
        [parts[6], parts[8], down_far],
        input_grad,
        layer_out,
        parts[:5],
        n_ids,
    )
    return (
        layer_out,
        input_grad,
        gain,
        *grads,
        gain_two,
        router.T,
        mix.T,
        vecs,
        gate[None],
        up[None],
        down[None],
    )


def solution(mesh):
    placed = (
        P((GR, EX, SH), None),
        P(GR, None),
        P((GR, EX, SH), None),
        P(),
        P(SH, None),
        P(SH, None),
        P(SH, None),
        P(SH, None),
        P(),
        P(),
        P(),
        P(),
        P(EX, None, None),
        P(EX, None, None),
        P(EX, None, None),
        P((GR, EX, SH), None),
    )
    sizes = dict(mesh.shape)
    lines = sizes[EX]
    fast = (sizes[GR], sizes[SH], lines) == (2, 4, 4)
    return jax.shard_map(
        fast_shards if fast else shards,
        mesh=mesh,
        in_specs=placed,
        out_specs=(
            P((GR, EX, SH), None),
            P((GR, EX, SH), None),
            P(),
            P((EX, SH), None),
            P((EX, SH), None),
            P((EX, SH), None),
            P((EX, SH), None),
            P(),
            P(),
            P(),
            P(),
            P(EX, SH, None),
            P(EX, SH, None),
            P(EX, SH, None),
        ),
        check_vma=False,
    )
```
